32 devices in a mesh: lat: 8 (over z, core), rad: 4 (over y, x).
Axes of the slice: x: 2, y: 2, z: 4, core: 2. Of those that a mesh axis runs over, the one named last changes fastest.
Arguments:
- residual: float32 [3, 32, 64, 256], P(None, 'rad', 'lat'), may hold values from -30 to 30
- prev_basis: float32 [4, 3, 32, 64, 256], P(None, None, 'rad', 'lat'), may hold values from -30 to 30
- layer_ids: int32 [16, 32, 128], P('rad', 'lat'), may hold values from 0 to 7
- viscosity: float32 [8], replicated, may hold values from 0.1 to 1
- shifts: float32 [4], replicated, may hold values from 0.3 to 2
Outputs:
- new_basis: float32 [4, 3, 32, 64, 256], P(None, None, 'rad', 'lat')
- gram_matrix: float32 [9, 9], replicated
The draws below stay inside these ranges and needn't reach their ends.
All inputs are finite; a program needn't handle non-finite values.
Results may differ from the reference program's by a relative error of at most 0.00019.
Values sent between devices are 32-bit elements; how exact they have to be, the bound alone decides.
A program may use at most 128 MiB of HBM per device.

```python
import math
import jax
import jax.numpy as jnp
from jax import lax

COMP = 3
S = 4
PREV = 4
LAYERS = 8
ER = 4
EY = 128
BASIS = 9
NRE = 16
NXE = 32
NRN = 32
NXN = 64
NYN = 256
N_RAD = 4


def ramp_field(key, leading):
    full_shape = (leading, COMP, NRN, NXN, NYN)
    radial = (jnp.arange(NRN, dtype=jnp.float32) / NRN)[:, None, None]
    lateral = (jnp.arange(NXN, dtype=jnp.float32) / NXN)[None, :, None]
    across = (jnp.arange(NYN, dtype=jnp.float32) / NYN)[None, None, :]
    smooth = jnp.sin(6.0 * radial + 4.0 * lateral + 3.0 * across + 0.5)
    coef_key = jax.random.fold_in(key, 7)
    coefs = jax.random.truncated_normal(coef_key, -2.0, 2.0, (leading, COMP, 1, 1, 1), jnp.float32)
    noise_vals = jax.random.truncated_normal(key, -4.0, 4.0, full_shape, jnp.float32)
    amplitude = 3.0 ** (radial + lateral - 1.0)
    return (amplitude * (noise_vals + coefs * smooth)).astype(jnp.float32)


def draw_residual(key, part):
    return ramp_field(jax.random.fold_in(key, 11), 1)[0]


def draw_prev_basis(key, part):
    return ramp_field(jax.random.fold_in(key, 23), PREV)


def touch_ends(values, stream_key, low, largest):
    spot = [jax.random.randint(jax.random.fold_in(stream_key, axis), (), 0, length) for axis, length in enumerate(values.shape)]
    widest = values.shape.index(max(values.shape))
    beside = spot[:widest] + [(spot[widest] + 1) % values.shape[widest]] + spot[widest + 1:]
    return values.at[tuple(spot)].set(low).at[tuple(beside)].set(largest)


def setup_inputs(seed: int = 0) -> dict:
    splits = jax.random.split(jax.random.key(seed), 6)
    residual = draw_residual(jax.random.fold_in(splits[5], 71), 0)
    prev_basis = draw_prev_basis(jax.random.fold_in(splits[5], 71), 0)
    layer_ids = touch_ends(jax.random.randint(splits[2], (NRE, NXE, EY), 0, LAYERS), jax.random.fold_in(splits[2], 1), 0, LAYERS - 1).astype(jnp.int32)
    viscosity = jnp.clip(jnp.exp(jax.random.uniform(splits[3], (LAYERS,), jnp.float32, math.log(0.1), math.log(1.0))), 0.1, 1.0)
    shifts = jnp.clip(jax.random.uniform(splits[4], (S,), jnp.float32, 0.3, 2.0), 0.3, 2.0)
    return {"residual": residual, "prev_basis": prev_basis, "layer_ids": layer_ids, "viscosity": viscosity, "shifts": shifts}


stiff_line = ((7.0 / 3, -8.0 / 3, 1.0 / 3), (-8.0 / 3, 16.0 / 3, -8.0 / 3), (1.0 / 3, -8.0 / 3, 7.0 / 3))
mass_line = ((4.0 / 30, 2.0 / 30, -1.0 / 30), (2.0 / 30, 16.0 / 30, 2.0 / 30), (-1.0 / 30, 2.0 / 30, 4.0 / 30))


def contract(line_table, element_vals, axis_pos):
    pieces = [lax.index_in_dim(element_vals, j, axis_pos, keepdims=False) for j in range(3)]
    row_terms = [line_table[i][0] * pieces[0] + line_table[i][1] * pieces[1] + line_table[i][2] * pieces[2] for i in range(3)]
    return jnp.stack(row_terms, axis_pos)


def split_local(field_in, axis_pos):
    el_count = field_in.shape[axis_pos] // 2 - 1
    return jnp.stack([lax.slice_in_dim(field_in, k, k + 2 * el_count - 1, 2, axis_pos) for k in range(3)], 0)


def join_local(element_vals, axis_pos):
    lower_side = element_vals[0]
    middle = element_vals[1]
    upper_side = element_vals[2]
    el_count = lower_side.shape[axis_pos]
    even_nodes = lax.slice_in_dim(lower_side, 1, el_count, 1, axis_pos) + lax.slice_in_dim(upper_side, 0, el_count - 1, 1, axis_pos)
    odd_nodes = lax.slice_in_dim(middle, 1, el_count, 1, axis_pos)
    alternated = jnp.stack([even_nodes, odd_nodes], axis_pos + 1)
    new_shape = list(even_nodes.shape)
    new_shape[axis_pos] = 2 * (el_count - 1)
    return alternated.reshape(new_shape)


def stiffness(field_in, viscous):
    padded = jnp.pad(field_in, ((0, 0), (0, 0), (0, 0), (2, 2)))
    element_vals = split_local(padded, 1)
    element_vals = split_local(element_vals, 3)
    element_vals = split_local(element_vals, 5)
    along_y = contract(mass_line, element_vals, 0)
    mass_rx = contract(mass_line, along_y, 1)
    term_r = contract(stiff_line, mass_rx, 2)
    term_x = contract(mass_line, contract(stiff_line, along_y, 1), 2)
    term_y = contract(stiff_line, contract(mass_line, contract(mass_line, element_vals, 2), 1), 0)
    viscous_wide = jnp.pad(viscous, ((0, 0), (0, 0), (1, 0)))
    weighted = (term_r + term_x + term_y) * viscous_wide
    assembled = join_local(weighted, 5)
    assembled = join_local(assembled, 3)
    return join_local(assembled, 1)


def reference(residual, prev_basis, layer_ids, viscosity, shifts):
    viscous = jnp.take(viscosity, layer_ids)
    eta_pad = jnp.pad(viscous, ((1, 1), (1, 1), (0, 0)))

    def apply_op(field_in):
        padded = jnp.pad(field_in, ((0, 0), (2, 2), (2, 2), (0, 0)))

        def slab_apply(j):
            slab_nodes = lax.dynamic_slice_in_dim(padded, j * (2 * ER), 2 * ER + 4, 1)
            slab_visc = lax.dynamic_slice_in_dim(eta_pad, j * ER, ER + 1, 0)
            return stiffness(slab_nodes, slab_visc[:, :NXE + 1])

        pieces = lax.map(slab_apply, jnp.arange(N_RAD, dtype=jnp.int32))
        return jnp.transpose(pieces, (1, 0, 2, 3, 4)).reshape(field_in.shape)

    vectors = [residual]
    for k in range(S):
        vectors.append(apply_op(vectors[-1]) - shifts[k] * vectors[-1])
    new_basis = jnp.stack(vectors[1:], 0)
    stacked = jnp.concatenate([prev_basis, jnp.stack(vectors, 0)], 0).reshape(BASIS, -1)
    gram_matrix = jnp.dot(stacked, stacked.T, precision=lax.Precision.HIGHEST, preferred_element_type=jnp.float32)
    gram_matrix = gram_matrix / (COMP * NRN * NXN * NYN)
    return new_basis, gram_matrix
```

```python
import functools

import jax
import jax.numpy as jnp
from jax import lax
from jax.experimental import pallas as pl
from jax.experimental.pallas import tpu as pltpu
from jax.sharding import PartitionSpec as P

MESH = pl.DeviceIdType.MESH
F32 = jnp.float32

mass = (1.0 / 36, 1.0 / 12, 1.0 / 45)
stiff = (0.0, 1.0, 4.0 / 3)

DIRS = ((-1, -1), (-1, 0), (-1, 1), (0, -1), (0, 1), (1, -1), (1, 0), (1, 1))
R_DIRS = {(-1, 0): 0, (1, 0): 1}
X_DIRS = {(0, -1): 0, (0, 1): 1}
C_DIRS = {(-1, -1): 0, (-1, 1): 1, (1, -1): 2, (1, 1): 3}
FIRST = ((-1, 0), (0, -1), (-1, -1))
LAST = ((1, 0), (0, 1), (1, 1))


def weight(a, b, c):
    return (
        stiff[a] * mass[b] * mass[c] + mass[a] * stiff[b] * mass[c] + mass[a] * mass[b] * stiff[c]
    )


def forward(u0, u1, u2):
    total = u0 + u2
    twice = u1 + u1
    return total + (twice + twice), u0 - u2, total - twice


def backward(m0, m1, m2):
    both = m0 + m2
    half = m0 + m0 - m2
    return both + m1, half + half, both - m1


def kernel(
    n_lat,
    n_rad,
    n_steps,
    n_prev,
    comps,
    res_ref,
    prev_ref,
    ids_hbm,
    visc_hbm,
    shift_hbm,
    out_ref,
    gram_ref,
    stage,
    ids_ref,
    visc_ref,
    shift_ref,
    work,
    vec,
    ghost_r,
    ghost_x,
    ghost_c,
    scaled,
    send_r,
    send_x,
    send_c,
    recv_r,
    recv_x,
    recv_c,
    gram_send,
    gram_recv,
    bulk,
    in_sem,
    send_sem,
    recv_sem,
    gram_sems,
    token_sem,
):
    n_dev = n_lat * n_rad
    lat = lax.axis_index("lat")
    rad = lax.axis_index("rad")
    me = lat * n_rad + rad
    rows = res_ref.shape[0]
    half_y = res_ref.shape[1] // 2
    n_vec = n_prev + n_steps + 1

    res_copy = pltpu.make_async_copy(res_ref, stage.at[n_prev], in_sem.at[0])
    res_copy.start()
    prev_copy = pltpu.make_async_copy(prev_ref, stage.at[pl.ds(0, n_prev)], in_sem.at[1])
    small_copies = [
        pltpu.make_async_copy(a, b, in_sem.at[2 + i])
        for i, (a, b) in enumerate(
            ((ids_hbm, ids_ref), (visc_hbm, visc_ref), (shift_hbm, shift_ref))
        )
    ]
    for copy in small_copies:
        copy.start()
    prev_copy.start()

    barrier = pltpu.get_barrier_semaphore()

    def spread(pos, count, far):
        return jnp.where(pos >= far, 1, 0) + jnp.where(pos < count - far, 1, 0)

    def around(far):
        return (1 + spread(rad, n_rad, far)) * (1 + spread(lat, n_lat, far)) - 1

    def within(dr, dx):
        ok = None
        for pos, step, count in ((rad, dr, n_rad), (lat, dx, n_lat)):
            if step:
                one = (pos >= -step) if step < 0 else (pos < count - step)
                ok = one if ok is None else jnp.logical_and(ok, one)
        return ok

    def signal_around(sem, far):
        for dr, dx in DIRS:
            if (dr and n_rad <= far) or (dx and n_lat <= far):
                continue

            @pl.when(within(dr * far, dx * far))
            def _(dr=dr, dx=dx):
                pl.semaphore_signal(
                    sem,
                    inc=1,
                    device_id={"lat": lat + dx * far, "rad": rad + dr * far},
                    device_id_type=MESH,
                )

    signal_around(barrier, 1)

    for d in DIRS:
        if d in R_DIRS:
            ref, slot = recv_r, R_DIRS[d]
        elif d in X_DIRS:
            ref, slot = recv_x, X_DIRS[d]
        else:
            ref, slot = recv_c, C_DIRS[d]

        @pl.when(jnp.logical_not(within(-d[0], -d[1])))
        def _(ref=ref, slot=slot):
            ref[:, :, slot] = jnp.zeros(ref.shape[:2] + ref.shape[3:], F32)

    reaches = []
    while (1 << len(reaches)) < max(n_lat, n_rad) - 1:
        reaches.append(1 << len(reaches))

    def send_token(j):
        if j < len(reaches):
            signal_around(token_sem.at[j], reaches[j])

    def take_token(j):
        if j < len(reaches):
            pl.semaphore_wait(token_sem.at[j], around(reaches[j]))

    rad_targets = [lax.rem(rad + d, n_rad) for d in range(n_rad)]

    def each_other(visit):
        def row(i, carry):
            lat_target = lax.rem(lat + n_lat // 2 + i, n_lat)
            for d in range(n_rad):
                ahead = lax.rem(n_lat // 2 + i, n_lat)
                visit(ahead * n_rad + d - 1, {"lat": lat_target, "rad": rad_targets[d]})
            return carry

        lax.fori_loop(0, n_lat // 2, row, 0, unroll=n_lat <= 8)
        lax.fori_loop(n_lat // 2 + 1, n_lat, row, 0, unroll=n_lat <= 8)
        for d in range(1, n_rad):
            visit(d - 1, {"lat": lat, "rad": rad_targets[d]})

    sub = lax.broadcasted_iota(jnp.int32, (8, half_y), 0)
    lane = lax.broadcasted_iota(jnp.int32, (8, half_y), 1)
    upper = sub >= 4
    ex = lax.rem(sub, 4)
    first_x = ex == 0
    last_x = ex == 3
    corner0 = sub == 0
    corner3 = sub == 3
    corner4 = sub == 4
    corner7 = sub == 7
    has_up = rad < n_rad - 1
    has_right = lat < n_lat - 1
    up_f = jnp.where(has_up, 1.0, 0.0).astype(F32)
    right_f = jnp.where(has_right, 1.0, 0.0).astype(F32)
    both_f = up_f * right_f

    def roll_s(v, k):
        return pltpu.roll(v, k % 8, 0)

    def keep(mask, v):
        return jnp.where(mask, v, 0.0)

    src = lax.broadcasted_iota(jnp.int32, (2 * half_y, 2 * half_y), 0)
    dst = lax.broadcasted_iota(jnp.int32, (2 * half_y, 2 * half_y), 1)
    split_perm = jnp.where(
        src == jnp.where(dst < half_y, 2 * dst, 2 * (dst - half_y) + 1), 1.0, 0.0
    ).astype(jnp.bfloat16)
    join_perm = jnp.where(
        dst == jnp.where(src < half_y, 2 * src, 2 * (src - half_y) + 1), 1.0, 0.0
    ).astype(jnp.bfloat16)

    def exact_dot(a, b):
        high = a.astype(jnp.bfloat16)
        rest = a - high.astype(F32)
        mid = rest.astype(jnp.bfloat16)
        low = (rest - mid.astype(F32)).astype(jnp.bfloat16)
        out = [jnp.dot(part, b, preferred_element_type=F32) for part in (high, mid, low)]
        return out[0] + (out[1] + out[2])

    def split_columns(i):
        z = exact_dot(stage[i], split_perm)
        work[i, 0] = z[:, :half_y]
        work[i, 1] = z[:, half_y:]

    def native(c, ro, p, h):
        return pl.ds(c * 64 + (4 * h + ro) * 8 + p, 4, stride=2)

    kinds = {}
    for a in range(3):
        for b in range(3):
            for c in range(3):
                key = tuple(sorted((a, b, c)))
                if key != (0, 0, 0) and key not in kinds:
                    kinds[key] = len(kinds)
    def copy_of(step, c, d):
        if d in R_DIRS:
            a, b = send_r.at[step, c, R_DIRS[d]], recv_r.at[step, c, R_DIRS[d]]
        elif d in X_DIRS:
            a, b = send_x.at[step, c, X_DIRS[d]], recv_x.at[step, c, X_DIRS[d]]
        else:
            a, b = send_c.at[step, c, C_DIRS[d]], recv_c.at[step, c, C_DIRS[d]]
        return pltpu.make_async_remote_copy(
            src_ref=a,
            dst_ref=b,
            send_sem=send_sem.at[0],
            recv_sem=recv_sem.at[step % 2, c],
            device_id={"lat": lat + d[1], "rad": rad + d[0]},
            device_id_type=MESH,
        )

    order = ((-1, -1), (1, 1), (-1, 1), (1, -1), (1, 0), (-1, 0), (0, 1), (0, -1))

    def dirs_of(step):
        wanted = FIRST if step == 0 else (LAST if step == n_steps else DIRS)
        return [d for d in order if d in wanted]

    def start_round(step, c):
        for d in dirs_of(step):

            @pl.when(within(*d))
            def _(d=d):
                copy_of(step, c, d).start()

    def places(pos, count):
        out = [(pos == 0, False, True), (pos == count - 1, True, False)]
        if count > 2:
            middle = jnp.logical_and(pos > 0, pos < count - 1)
            out.append((middle, True, True))
        return out if count > 1 else [(pos == 0, False, False)]

    def rows_of(dirs, down, up, left, right):
        have = {-1: {0: True, -1: down, 1: up}, 1: {0: True, -1: left, 1: right}}
        total = 0
        for dr, dx in dirs:
            if have[-1][dr] and have[1][dx]:
                total += 2 if dr and dx else 18
        return total

    def settle(sem, dir_lists):
        groups = {}
        for at_r, down, up in places(rad, n_rad):
            for at_x, left, right in places(lat, n_lat):
                n = sum(rows_of(dirs, down, up, left, right) for dirs in dir_lists)
                here = jnp.logical_and(at_r, at_x)
                groups[n] = jnp.logical_or(groups[n], here) if n in groups else here
        for n, here in groups.items():
            if n:

                @pl.when(here)
                def _(n=n):
                    pltpu.make_async_copy(bulk.at[pl.ds(0, n)], bulk.at[pl.ds(0, n)], sem).wait()

    def finish_round(step, c):
        settle(recv_sem.at[step % 2, c], [[(-d[0], -d[1]) for d in dirs_of(step)]])

    def pack_x(vals, at):
        out = None
        for ro in range(4):
            moved = roll_s(vals[ro], ro - at)
            out = moved if out is None else jnp.where(ex == ro, moved, out)
        return out

    def apply(k, c):
        s = shift_ref[k]
        cur = k % 2
        new = 1 - cur
        u = {}
        gx = {}
        for q in range(2):
            for ro in range(4):
                gx[ro, q] = ghost_x[cur, c, ro, q]
                for p in range(2):
                    u[ro, p, q] = vec[cur, c, ro, p, q]
            gx[4, q] = jnp.where(upper, ghost_c[cur, c, q], roll_s(gx[0, q], 4))
            for p in range(2):
                u[4, p, q] = jnp.where(upper, ghost_r[cur, c, p, q], roll_s(u[0, p, q], 4))
            for ro in range(5):
                u[ro, 2, q] = jnp.where(last_x, gx[ro, q], roll_s(u[ro, 0, q], -1))
        res = {}
        for e in range(2):
            t = {}
            for p in range(3):
                for q in range(2):
                    t[0, p, q], t[1, p, q], t[2, p, q] = forward(
                        u[2 * e, p, q], u[2 * e + 1, p, q], u[2 * e + 2, p, q]
                    )
            w = {}
            for a in range(3):
                x = {}
                for q in range(2):
                    x[0, q], x[1, q], x[2, q] = forward(t[a, 0, q], t[a, 1, q], t[a, 2, q])
                for b in range(3):
                    nxt = keep(lane != half_y - 1, pltpu.roll(x[b, 0], half_y - 1, 1))
                    m = list(forward(x[b, 0], x[b, 1], nxt))
                    for j in range(3):
                        key = tuple(sorted((a, b, j)))
                        if key in kinds:
                            m[j] = m[j] * scaled[e, kinds[key]]
                        else:
                            m[j] = None
                    if m[0] is None:
                        r0 = m[1] + m[2]
                        r1 = -(m[2] + m[2])
                        r2 = m[2] - m[1]
                    else:
                        r0, r1, r2 = backward(*m)
                    x[b, 0] = r0 + keep(lane != 0, pltpu.roll(r2, 1, 1))
                    x[b, 1] = r1
                for q in range(2):
                    w[a, 0, q], w[a, 1, q], w[a, 2, q] = backward(x[0, q], x[1, q], x[2, q])
            for p in range(3):
                for q in range(2):
                    r = backward(w[0, p, q], w[1, p, q], w[2, p, q])
                    for i in range(3):
                        key = (2 * e + i, p, q)
                        res[key] = res[key] + r[i] if key in res else r[i]
        px = {}
        for q in range(2):
            for ro in range(5):
                edge = res[ro, 2, q]
                px[ro, q] = edge
                res[ro, 0, q] = res[ro, 0, q] + keep(ex != 0, roll_s(edge, 1))
            for p in range(2):
                res[0, p, q] = res[0, p, q] + keep(upper, roll_s(res[4, p, q], 4))
            px[0, q] = px[0, q] + keep(upper, roll_s(px[4, q], 4))
        step = k + 1
        last = step == n_steps
        for q in range(2):
            face = slice(8 * q, 8 * q + 8)
            edge = slice(16 + q, 17 + q)
            row = slice(q, q + 1)
            send_r[step, c, 1, face] = jnp.where(upper, res[4, 1, q], roll_s(res[4, 0, q], 4))
            send_r[step, c, 1, edge] = px[4, q][7:8]
            send_x[step, c, 1, face] = pack_x([px[ro, q] for ro in range(4)], 3)
            send_x[step, c, 1, edge] = px[4, q][7:8]
            send_c[step, c, 3, row] = px[4, q][7:8]
            if not last:
                send_r[step, c, 0, face] = jnp.where(upper, roll_s(res[0, 1, q], 4), res[0, 0, q])
                send_r[step, c, 0, edge] = px[0, q][3:4]
                send_x[step, c, 0, face] = pack_x([res[ro, 0, q] for ro in range(4)], 0)
                send_x[step, c, 0, edge] = res[4, 0, q][4:5]
                send_c[step, c, 0, row] = res[0, 0, q][0:1]
                send_c[step, c, 1, row] = px[0, q][3:4]
                send_c[step, c, 2, row] = res[4, 0, q][4:5]
            for ro in range(4):
                for p in range(2):
                    vec[new, c, ro, p, q] = res[ro, p, q] - s * u[ro, p, q]
                if not last:
                    ghost_x[new, c, ro, q] = px[ro, q] - s * gx[ro, q]
            if not last:
                for p in range(2):
                    ghost_r[new, c, p, q] = res[4, p, q] - s * u[4, p, q]
                ghost_c[new, c, q] = px[4, q] - s * gx[4, q]

    def absorb(step, c):
        new = step % 2
        first, last = step == 0, step == n_steps
        for q in range(2):
            face = slice(8 * q, 8 * q + 8)
            line = slice(16 + q, 17 + q)
            row = slice(q, q + 1)

            def spot(ref_row, mask):
                return keep(mask, jnp.broadcast_to(ref_row, (8, half_y)))

            if not first:
                from_low = recv_r[step, c, 1, face]
                from_left = recv_x[step, c, 1, face]
                corner = spot(recv_c[step, c, 3, row], corner0)
                vec[new, c, 0, 0, q] += (
                    keep(~upper, from_low) + keep(first_x, from_left) + corner
                )
                vec[new, c, 0, 1, q] += keep(~upper, roll_s(from_low, 4))
                for ro in range(1, 4):
                    vec[new, c, ro, 0, q] += keep(first_x, roll_s(from_left, -ro))
            if not last:
                from_up = recv_r[step, c, 0, face]
                from_right = recv_x[step, c, 0, face]
                add0 = keep(upper, roll_s(from_up, 4))
                add1 = keep(upper, from_up)
                edge = keep(last_x, roll_s(from_right, 3))
                far = (
                    spot(recv_r[step, c, 0, line], corner7)
                    + spot(recv_x[step, c, 0, line], corner7)
                    + spot(recv_c[step, c, 0, row], corner7)
                )
                if not first:
                    add0 = (
                        add0
                        + spot(recv_x[step, c, 1, line], corner4)
                        + spot(recv_c[step, c, 1, row], corner4)
                    )
                    edge = (
                        edge
                        + spot(recv_r[step, c, 1, line], corner3)
                        + spot(recv_c[step, c, 2, row], corner3)
                    )
                    add0 = add0 + ghost_r[new, c, 0, q]
                    add1 = add1 + ghost_r[new, c, 1, q]
                    edge = edge + ghost_x[new, c, 0, q]
                    far = far + ghost_c[new, c, q]
                ghost_r[new, c, 0, q] = add0 * up_f
                ghost_r[new, c, 1, q] = add1 * up_f
                ghost_x[new, c, 0, q] = edge * right_f
                ghost_c[new, c, q] = far * both_f
                for ro in range(1, 4):
                    edge = keep(last_x, roll_s(from_right, 3 - ro))
                    if not first:
                        edge = edge + ghost_x[new, c, ro, q]
                    ghost_x[new, c, ro, q] = edge * right_f

    def to_native(k, c):
        cur = k % 2
        for ro in range(4):
            for p in range(2):
                for q in range(2):
                    v = vec[cur, c, ro, p, q]
                    for h in range(2):
                        work[n_prev + k, q, native(c, ro, p, h), :] = v[4 * h : 4 * h + 4]

    def write_out(k):
        z = jnp.concatenate([work[n_prev + k, 0], work[n_prev + k, 1]], 1)
        out_ref[k - 1] = exact_dot(z, join_perm)

    lane16 = lax.broadcasted_iota(jnp.int32, (16, half_y), 1)
    row16 = lax.broadcasted_iota(jnp.int32, (16, half_y), 0)

    def gram_part(i, acc, first, count):
        def chunk(t, acc):
            at = pl.ds(pl.multiple_of(8 * t, 8), 8)
            for q in range(2):
                mine = work[i, q, at, :]
                acc = tuple(
                    acc[j] + mine * (mine if j == i else work[j, q, at, :]) for j in range(i + 1)
                )
            return acc

        return lax.fori_loop(first, first + count, chunk, acc, unroll=4)

    def gram_zero(i):
        return (jnp.zeros((8, half_y), F32),) * (i + 1)

    def gram_close(i, acc):
        sums = [jnp.sum(a, axis=0, keepdims=True) for a in acc]
        sums.append(jnp.zeros((16 - len(sums), half_y), F32))
        total = jnp.sum(jnp.concatenate(sums, 0), axis=1, keepdims=True)
        hit = jnp.logical_or(lane16 == i * n_vec + row16, lane16 == row16 * n_vec + i)
        hit = jnp.logical_and(hit, row16 <= i)
        return jnp.sum(jnp.where(hit, jnp.broadcast_to(total, hit.shape), 0.0), 0, keepdims=True)

    def gram_row(i):
        return gram_close(i, gram_part(i, gram_zero(i), 0, rows // 8))

    res_copy.wait()
    split_columns(n_prev)
    for c in range(comps):
        for ro in range(4):
            for p in range(2):
                for q in range(2):
                    vec[0, c, ro, p, q] = jnp.concatenate(
                        [work[n_prev, q, native(c, ro, p, h), :] for h in range(2)], 0
                    )
    zero_rows = jnp.zeros((2, half_y), F32)
    for c in range(comps):
        send_r[0, c, 0, 16:18] = zero_rows
        send_x[0, c, 0, 16:18] = zero_rows
        for q in range(2):
            face = slice(8 * q, 8 * q + 8)
            send_r[0, c, 0, face] = jnp.where(
                upper, roll_s(vec[0, c, 0, 1, q], 4), vec[0, c, 0, 0, q]
            )
            send_x[0, c, 0, face] = pack_x([vec[0, c, ro, 0, q] for ro in range(4)], 0)
            send_c[0, c, 0, q : q + 1] = vec[0, c, 0, 0, q, 0:1]

    pl.semaphore_wait(barrier, around(1))
    for c in range(comps):
        start_round(0, c)
    send_token(0)
    for copy in small_copies:
        copy.wait()
    for e in range(2):
        ids = jnp.concatenate([ids_ref[e], ids_ref[2 + e]], 0)
        eta = jnp.zeros((8, half_y), F32)
        for layer in range(visc_ref.shape[0]):
            eta = eta + jnp.where(ids == layer, visc_ref[layer], 0.0)
        for key, i in kinds.items():
            scaled[e, i] = eta * weight(*key)
    prev_copy.wait()
    for i in range(n_prev):
        split_columns(i)

    total = jnp.zeros((1, half_y), F32)
    for k in range(n_steps):
        for c in range(comps):
            finish_round(k, c)
            absorb(k, c)
            apply(k, c)
            start_round(k + 1, c)
        take_token(k)
        send_token(k + 1)
        if k == 0:
            for i in range(n_prev + 1):
                total = total + gram_row(i)
        else:
            for c in range(comps):
                to_native(k, c)
            write_out(k)
            total = total + gram_row(n_prev + k)
    for j in range(n_steps, len(reaches)):
        take_token(j)
        send_token(j + 1)
    acc = gram_zero(n_vec - 1)
    per = rows // 8 // comps
    for c in range(comps):
        finish_round(n_steps, c)
        absorb(n_steps, c)
        to_native(n_steps, c)
        acc = gram_part(n_vec - 1, acc, c * per, per)
    total = total + gram_close(n_vec - 1, acc)
    gram_send[...] = total

    def scatter(slot, device):
        pltpu.make_async_remote_copy(
            src_ref=gram_send,
            dst_ref=gram_recv.at[slot],
            send_sem=gram_sems.at[0],
            recv_sem=gram_sems.at[1],
            device_id=device,
            device_id_type=MESH,
        ).start()

    each_other(scatter)
    write_out(n_steps)
    settle(send_sem.at[0], [dirs_of(step) for step in range(n_steps + 1)] * comps)
    for i in range(2):
        pltpu.make_async_copy(gram_recv, gram_recv, gram_sems.at[i]).wait()
    full = (total + jnp.sum(gram_recv[...], axis=0)) * (1.0 / (rows * 2 * half_y * n_dev))
    for i in range(n_vec):
        line = full if i == 0 else pltpu.roll(full, half_y - i * n_vec, 1)
        gram_ref[i : i + 1, :] = line[:, :n_vec]


def on_device(residual, prev_basis, layer_ids, viscosity, shifts):
    n_lat = lax.axis_size("lat")
    n_rad = lax.axis_size("rad")
    comps, node_r, node_x, node_y = residual.shape
    n_prev = prev_basis.shape[0]
    n_steps = shifts.shape[0]
    n_vec = n_prev + n_steps + 1
    rows = comps * node_r * node_x
    half_y = node_y // 2
    assert node_r == 8 and node_x == 8 and half_y == 128
    rounds = n_steps + 1
    tile = (8, half_y)
    vmem = pltpu.VMEM
    hbm_spec = pl.BlockSpec(memory_space=pltpu.HBM)
    vmem_spec = pl.BlockSpec(memory_space=pltpu.VMEM)
    out, gram = pl.pallas_call(
        functools.partial(kernel, n_lat, n_rad, n_steps, n_prev, comps),
        out_shape=(
            pltpu.VMEM((n_steps, rows, node_y), F32),
            pltpu.VMEM((n_vec, n_vec), F32),
        ),
        in_specs=[hbm_spec] * 5,
        out_specs=(vmem_spec, vmem_spec),
        scratch_shapes=[
            vmem((n_prev + 1, rows, node_y), F32),
            vmem(layer_ids.shape, jnp.int32),
            pltpu.SMEM(viscosity.shape, F32),
            pltpu.SMEM(shifts.shape, F32),
            vmem((n_vec, 2, rows, half_y), F32),
            vmem((2, comps, 4, 2, 2) + tile, F32),
            vmem((2, comps, 2, 2) + tile, F32),
            vmem((2, comps, 4, 2) + tile, F32),
            vmem((2, comps, 2) + tile, F32),
            vmem((2, 9) + tile, F32),
            vmem((rounds, comps, 2, 18, half_y), F32),
            vmem((rounds, comps, 2, 18, half_y), F32),
            vmem((rounds, comps, 4, 2, half_y), F32),
            vmem((rounds, comps, 2, 18, half_y), F32),
            vmem((rounds, comps, 2, 18, half_y), F32),
            vmem((rounds, comps, 4, 2, half_y), F32),
            vmem((1, half_y), F32),
            vmem((n_lat * n_rad - 1, 1, half_y), F32),
            vmem((rounds * comps * 80, half_y), F32),
            pltpu.SemaphoreType.DMA((5,)),
            pltpu.SemaphoreType.DMA((1,)),
            pltpu.SemaphoreType.DMA((2, comps)),
            pltpu.SemaphoreType.DMA((2,)),
            pltpu.SemaphoreType.REGULAR((max(n_lat, n_rad).bit_length(),)),
        ],
        compiler_params=pltpu.CompilerParams(
            collective_id=0, has_side_effects=True, vmem_limit_bytes=65000000
        ),
    )(
        residual.reshape(rows, node_y),
        prev_basis.reshape(n_prev, rows, node_y),
        layer_ids,
        viscosity,
        shifts,
    )
    return out.reshape((n_steps,) + residual.shape), gram


def solution(mesh):
    placed = (
        P(None, "rad", "lat", None),
        P(None, None, "rad", "lat", None),
        P("rad", "lat", None),
        P(),
        P(),
    )
    return jax.shard_map(
        on_device,
        mesh=mesh,
        in_specs=placed,
        out_specs=(P(None, None, "rad", "lat", None), P()),
        check_vma=False,
    )
```

```python
import functools

import jax
import jax.numpy as jnp
from jax import lax
from jax.experimental import pallas as pl
from jax.experimental.pallas import tpu as pltpu
from jax.sharding import PartitionSpec as P

MESH = pl.DeviceIdType.MESH
F32 = jnp.float32

mass = (1.0 / 36, 1.0 / 12, 1.0 / 45)
stiff = (0.0, 1.0, 4.0 / 3)

DIRS = ((-1, -1), (-1, 0), (-1, 1), (0, -1), (0, 1), (1, -1), (1, 0), (1, 1))
R_DIRS = {(-1, 0): 0, (1, 0): 1}
X_DIRS = {(0, -1): 0, (0, 1): 1}
C_DIRS = {(-1, -1): 0, (-1, 1): 1, (1, -1): 2, (1, 1): 3}
FIRST = ((-1, 0), (0, -1), (-1, -1))
LAST = ((1, 0), (0, 1), (1, 1))


def weight(a, b, c):
    return (
        stiff[a] * mass[b] * mass[c] + mass[a] * stiff[b] * mass[c] + mass[a] * mass[b] * stiff[c]
    )


def forward(u0, u1, u2):
    total = u0 + u2
    twice = u1 + u1
    return total + (twice + twice), u0 - u2, total - twice


def backward(m0, m1, m2):
    both = m0 + m2
    half = m0 + m0 - m2
    return both + m1, half + half, both - m1


def kernel(
    n_lat,
    n_rad,
    n_steps,
    n_prev,
    comps,
    res_ref,
    prev_ref,
    ids_hbm,
    visc_hbm,
    shift_hbm,
    out_ref,
    gram_ref,
    stage,
    ids_ref,
    visc_ref,
    shift_ref,
    work,
    vec,
    ghost_r,
    ghost_x,
    ghost_c,
    scaled,
    send_r,
    send_x,
    send_c,
    recv_r,
    recv_x,
    recv_c,
    gram_send,
    gram_recv,
    bulk,
    in_sem,
    send_sem,
    recv_sem,
    gram_sems,
    token_sem,
):
    n_dev = n_lat * n_rad
    lat = lax.axis_index("lat")
    rad = lax.axis_index("rad")
    me = lat * n_rad + rad
    rows = res_ref.shape[0]
    half_y = res_ref.shape[1] // 2
    n_vec = n_prev + n_steps + 1

    res_copy = pltpu.make_async_copy(res_ref, stage.at[n_prev], in_sem.at[0])
    res_copy.start()
    prev_copy = pltpu.make_async_copy(prev_ref, stage.at[pl.ds(0, n_prev)], in_sem.at[1])
    small_copies = [
        pltpu.make_async_copy(a, b, in_sem.at[2 + i])
        for i, (a, b) in enumerate(
            ((ids_hbm, ids_ref), (visc_hbm, visc_ref), (shift_hbm, shift_ref))
        )
    ]
    for copy in small_copies:
        copy.start()
    prev_copy.start()

    barrier = pltpu.get_barrier_semaphore()

    def spread(pos, count, far):
        return jnp.where(pos >= far, 1, 0) + jnp.where(pos < count - far, 1, 0)

    def around(far):
        return (1 + spread(rad, n_rad, far)) * (1 + spread(lat, n_lat, far)) - 1

    def within(dr, dx):
        ok = None
        for pos, step, count in ((rad, dr, n_rad), (lat, dx, n_lat)):
            if step:
                one = (pos >= -step) if step < 0 else (pos < count - step)
                ok = one if ok is None else jnp.logical_and(ok, one)
        return ok

    def signal_around(sem, far):
        for dr, dx in DIRS:
            if (dr and n_rad <= far) or (dx and n_lat <= far):
                continue

            @pl.when(within(dr * far, dx * far))
            def _(dr=dr, dx=dx):
                pl.semaphore_signal(
                    sem,
                    inc=1,
                    device_id={"lat": lat + dx * far, "rad": rad + dr * far},
                    device_id_type=MESH,
                )

    signal_around(barrier, 1)

    for d in DIRS:
        if d in R_DIRS:
            ref, slot = recv_r, R_DIRS[d]
        elif d in X_DIRS:
            ref, slot = recv_x, X_DIRS[d]
        else:
            ref, slot = recv_c, C_DIRS[d]

        @pl.when(jnp.logical_not(within(-d[0], -d[1])))
        def _(ref=ref, slot=slot):
            ref[:, :, slot] = jnp.zeros(ref.shape[:2] + ref.shape[3:], F32)

    reaches = []
    while (1 << len(reaches)) < max(n_lat, n_rad) - 1:
        reaches.append(1 << len(reaches))

    def send_token(j):
        if j < len(reaches):
            signal_around(token_sem.at[j], reaches[j])

    def take_token(j):
        if j < len(reaches):
            pl.semaphore_wait(token_sem.at[j], around(reaches[j]))

    rad_targets = [lax.rem(rad + d, n_rad) for d in range(n_rad)]

    def each_other(visit):
        def row(i, carry):
            lat_target = lax.rem(lat + n_lat // 2 + i, n_lat)
            for d in range(n_rad):
                ahead = lax.rem(n_lat // 2 + i, n_lat)
                visit(ahead * n_rad + d - 1, {"lat": lat_target, "rad": rad_targets[d]})
            return carry

        lax.fori_loop(0, n_lat // 2, row, 0, unroll=n_lat <= 8)
        lax.fori_loop(n_lat // 2 + 1, n_lat, row, 0, unroll=n_lat <= 8)
        for d in range(1, n_rad):
            visit(d - 1, {"lat": lat, "rad": rad_targets[d]})

    sub = lax.broadcasted_iota(jnp.int32, (8, half_y), 0)
    lane = lax.broadcasted_iota(jnp.int32, (8, half_y), 1)
    upper = sub >= 4
    ex = lax.rem(sub, 4)
    first_x = ex == 0
    last_x = ex == 3
    corner0 = sub == 0
    corner3 = sub == 3
    corner4 = sub == 4
    corner7 = sub == 7
    has_up = rad < n_rad - 1
    has_right = lat < n_lat - 1
    up_f = jnp.where(has_up, 1.0, 0.0).astype(F32)
    right_f = jnp.where(has_right, 1.0, 0.0).astype(F32)
    both_f = up_f * right_f

    def roll_s(v, k):
        return pltpu.roll(v, k % 8, 0)

    def keep(mask, v):
        return jnp.where(mask, v, 0.0)

    src = lax.broadcasted_iota(jnp.int32, (2 * half_y, 2 * half_y), 0)
    dst = lax.broadcasted_iota(jnp.int32, (2 * half_y, 2 * half_y), 1)
    split_perm = jnp.where(
        src == jnp.where(dst < half_y, 2 * dst, 2 * (dst - half_y) + 1), 1.0, 0.0
    ).astype(jnp.bfloat16)
    join_perm = jnp.where(
        dst == jnp.where(src < half_y, 2 * src, 2 * (src - half_y) + 1), 1.0, 0.0
    ).astype(jnp.bfloat16)

    def exact_dot(a, b):
        high = a.astype(jnp.bfloat16)
        rest = a - high.astype(F32)
        mid = rest.astype(jnp.bfloat16)
        low = (rest - mid.astype(F32)).astype(jnp.bfloat16)
        out = [jnp.dot(part, b, preferred_element_type=F32) for part in (high, mid, low)]
        return out[0] + (out[1] + out[2])

    def split_columns(i):
        z = exact_dot(stage[i], split_perm)
        work[i, 0] = z[:, :half_y]
        work[i, 1] = z[:, half_y:]

    def native(c, ro, p, h):
        return pl.ds(c * 64 + (4 * h + ro) * 8 + p, 4, stride=2)

    kinds = {}
    for a in range(3):
        for b in range(3):
            for c in range(3):
                key = tuple(sorted((a, b, c)))
                if key != (0, 0, 0) and key not in kinds:
                    kinds[key] = len(kinds)
    def copy_of(step, c, d):
        if d in R_DIRS:
            a, b = send_r.at[step, c, R_DIRS[d]], recv_r.at[step, c, R_DIRS[d]]
        elif d in X_DIRS:
            a, b = send_x.at[step, c, X_DIRS[d]], recv_x.at[step, c, X_DIRS[d]]
        else:
            a, b = send_c.at[step, c, C_DIRS[d]], recv_c.at[step, c, C_DIRS[d]]
        return pltpu.make_async_remote_copy(
            src_ref=a,
            dst_ref=b,
            send_sem=send_sem.at[0],
            recv_sem=recv_sem.at[step % 2, c],
            device_id={"lat": lat + d[1], "rad": rad + d[0]},
            device_id_type=MESH,
        )

    order = ((-1, -1), (1, 1), (-1, 1), (1, -1), (1, 0), (-1, 0), (0, 1), (0, -1))

    def dirs_of(step):
        wanted = FIRST if step == 0 else (LAST if step == n_steps else DIRS)
        return [d for d in order if d in wanted]

    def start_round(step, c):
        for d in dirs_of(step):

            @pl.when(within(*d))
            def _(d=d):
                copy_of(step, c, d).start()

    def places(pos, count):
        out = [(pos == 0, False, True), (pos == count - 1, True, False)]
        if count > 2:
            middle = jnp.logical_and(pos > 0, pos < count - 1)
            out.append((middle, True, True))
        return out if count > 1 else [(pos == 0, False, False)]

    def rows_of(dirs, down, up, left, right):
        have = {-1: {0: True, -1: down, 1: up}, 1: {0: True, -1: left, 1: right}}
        total = 0
        for dr, dx in dirs:
            if have[-1][dr] and have[1][dx]:
                total += 2 if dr and dx else 18
        return total

    def settle(sem, dir_lists):
        groups = {}
        for at_r, down, up in places(rad, n_rad):
            for at_x, left, right in places(lat, n_lat):
                n = sum(rows_of(dirs, down, up, left, right) for dirs in dir_lists)
                here = jnp.logical_and(at_r, at_x)
                groups[n] = jnp.logical_or(groups[n], here) if n in groups else here
        for n, here in groups.items():
            if n:

                @pl.when(here)
                def _(n=n):
                    pltpu.make_async_copy(bulk.at[pl.ds(0, n)], bulk.at[pl.ds(0, n)], sem).wait()

    def finish_round(step, c):
        settle(recv_sem.at[step % 2, c], [[(-d[0], -d[1]) for d in dirs_of(step)]])

    def pack_x(vals, at):
        out = None
        for ro in range(4):
            moved = roll_s(vals[ro], ro - at)
            out = moved if out is None else jnp.where(ex == ro, moved, out)
        return out

    def apply(k, c):
        s = shift_ref[k]
        cur = k % 2
        new = 1 - cur
        u = {}
        gx = {}
        for q in range(2):
            for ro in range(4):
                gx[ro, q] = ghost_x[cur, c, ro, q]
                for p in range(2):
                    u[ro, p, q] = vec[cur, c, ro, p, q]
            gx[4, q] = jnp.where(upper, ghost_c[cur, c, q], roll_s(gx[0, q], 4))
            for p in range(2):
                u[4, p, q] = jnp.where(upper, ghost_r[cur, c, p, q], roll_s(u[0, p, q], 4))
            for ro in range(5):
                u[ro, 2, q] = jnp.where(last_x, gx[ro, q], roll_s(u[ro, 0, q], -1))
        res = {}
        for e in range(2):
            t = {}
            for p in range(3):
                for q in range(2):
                    t[0, p, q], t[1, p, q], t[2, p, q] = forward(
                        u[2 * e, p, q], u[2 * e + 1, p, q], u[2 * e + 2, p, q]
                    )
            w = {}
            for a in range(3):
                x = {}
                for q in range(2):
                    x[0, q], x[1, q], x[2, q] = forward(t[a, 0, q], t[a, 1, q], t[a, 2, q])
                for b in range(3):
                    nxt = keep(lane != half_y - 1, pltpu.roll(x[b, 0], half_y - 1, 1))
                    m = list(forward(x[b, 0], x[b, 1], nxt))
                    for j in range(3):
                        key = tuple(sorted((a, b, j)))
                        if key in kinds:
                            m[j] = m[j] * scaled[e, kinds[key]]
                        else:
                            m[j] = None
                    if m[0] is None:
                        r0 = m[1] + m[2]
                        r1 = -(m[2] + m[2])
                        r2 = m[2] - m[1]
                    else:
                        r0, r1, r2 = backward(*m)
                    x[b, 0] = r0 + keep(lane != 0, pltpu.roll(r2, 1, 1))
                    x[b, 1] = r1
                for q in range(2):
                    w[a, 0, q], w[a, 1, q], w[a, 2, q] = backward(x[0, q], x[1, q], x[2, q])
            for p in range(3):
                for q in range(2):
                    r = backward(w[0, p, q], w[1, p, q], w[2, p, q])
                    for i in range(3):
                        key = (2 * e + i, p, q)
                        res[key] = res[key] + r[i] if key in res else r[i]
        px = {}
        for q in range(2):
            for ro in range(5):
                edge = res[ro, 2, q]
                px[ro, q] = edge
                res[ro, 0, q] = res[ro, 0, q] + keep(ex != 0, roll_s(edge, 1))
            for p in range(2):
                res[0, p, q] = res[0, p, q] + keep(upper, roll_s(res[4, p, q], 4))
            px[0, q] = px[0, q] + keep(upper, roll_s(px[4, q], 4))
        step = k + 1
        last = step == n_steps
        for q in range(2):
            face = slice(8 * q, 8 * q + 8)
            edge = slice(16 + q, 17 + q)
            row = slice(q, q + 1)
            send_r[step, c, 1, face] = jnp.where(upper, res[4, 1, q], roll_s(res[4, 0, q], 4))
            send_r[step, c, 1, edge] = px[4, q][7:8]
            send_x[step, c, 1, face] = pack_x([px[ro, q] for ro in range(4)], 3)
            send_x[step, c, 1, edge] = px[4, q][7:8]
            send_c[step, c, 3, row] = px[4, q][7:8]
            if not last:
                send_r[step, c, 0, face] = jnp.where(upper, roll_s(res[0, 1, q], 4), res[0, 0, q])
                send_r[step, c, 0, edge] = px[0, q][3:4]
                send_x[step, c, 0, face] = pack_x([res[ro, 0, q] for ro in range(4)], 0)
                send_x[step, c, 0, edge] = res[4, 0, q][4:5]
                send_c[step, c, 0, row] = res[0, 0, q][0:1]
                send_c[step, c, 1, row] = px[0, q][3:4]
                send_c[step, c, 2, row] = res[4, 0, q][4:5]
            for ro in range(4):
                for p in range(2):
                    vec[new, c, ro, p, q] = res[ro, p, q] - s * u[ro, p, q]
                if not last:
                    ghost_x[new, c, ro, q] = px[ro, q] - s * gx[ro, q]
            if not last:
                for p in range(2):
                    ghost_r[new, c, p, q] = res[4, p, q] - s * u[4, p, q]
                ghost_c[new, c, q] = px[4, q] - s * gx[4, q]

    def absorb(step, c):
        new = step % 2
        first, last = step == 0, step == n_steps
        for q in range(2):
            face = slice(8 * q, 8 * q + 8)
            line = slice(16 + q, 17 + q)
            row = slice(q, q + 1)

            def spot(ref_row, mask):
                return keep(mask, jnp.broadcast_to(ref_row, (8, half_y)))

            if not first:
                from_low = recv_r[step, c, 1, face]
                from_left = recv_x[step, c, 1, face]
                corner = spot(recv_c[step, c, 3, row], corner0)
                vec[new, c, 0, 0, q] += (
                    keep(~upper, from_low) + keep(first_x, from_left) + corner
                )
                vec[new, c, 0, 1, q] += keep(~upper, roll_s(from_low, 4))
                for ro in range(1, 4):
                    vec[new, c, ro, 0, q] += keep(first_x, roll_s(from_left, -ro))
            if not last:
                from_up = recv_r[step, c, 0, face]
                from_right = recv_x[step, c, 0, face]
                add0 = keep(upper, roll_s(from_up, 4))
                add1 = keep(upper, from_up)
                edge = keep(last_x, roll_s(from_right, 3))
                far = (
                    spot(recv_r[step, c, 0, line], corner7)
                    + spot(recv_x[step, c, 0, line], corner7)
                    + spot(recv_c[step, c, 0, row], corner7)
                )
                if not first:
                    add0 = (
                        add0
                        + spot(recv_x[step, c, 1, line], corner4)
                        + spot(recv_c[step, c, 1, row], corner4)
                    )
                    edge = (
                        edge
                        + spot(recv_r[step, c, 1, line], corner3)
                        + spot(recv_c[step, c, 2, row], corner3)
                    )
                    add0 = add0 + ghost_r[new, c, 0, q]
                    add1 = add1 + ghost_r[new, c, 1, q]
                    edge = edge + ghost_x[new, c, 0, q]
                    far = far + ghost_c[new, c, q]
                ghost_r[new, c, 0, q] = add0 * up_f
                ghost_r[new, c, 1, q] = add1 * up_f
                ghost_x[new, c, 0, q] = edge * right_f
                ghost_c[new, c, q] = far * both_f
                for ro in range(1, 4):
                    edge = keep(last_x, roll_s(from_right, 3 - ro))
                    if not first:
                        edge = edge + ghost_x[new, c, ro, q]
                    ghost_x[new, c, ro, q] = edge * right_f

    def to_native(k, c):
        cur = k % 2
        for ro in range(4):
            for p in range(2):
                for q in range(2):
                    v = vec[cur, c, ro, p, q]
                    for h in range(2):
                        work[n_prev + k, q, native(c, ro, p, h), :] = v[4 * h : 4 * h + 4]

    def write_out(k):
        z = jnp.concatenate([work[n_prev + k, 0], work[n_prev + k, 1]], 1)
        out_ref[k - 1] = exact_dot(z, join_perm)

    lane16 = lax.broadcasted_iota(jnp.int32, (16, half_y), 1)
    row16 = lax.broadcasted_iota(jnp.int32, (16, half_y), 0)

    def gram_part(i, acc, first, count):
        def chunk(t, acc):
            at = pl.ds(pl.multiple_of(8 * t, 8), 8)
            for q in range(2):
                mine = work[i, q, at, :]
                acc = tuple(
                    acc[j] + mine * (mine if j == i else work[j, q, at, :]) for j in range(i + 1)
                )
            return acc

        return lax.fori_loop(first, first + count, chunk, acc, unroll=4)

    def gram_zero(i):
        return (jnp.zeros((8, half_y), F32),) * (i + 1)

    def gram_close(i, acc):
        sums = [jnp.sum(a, axis=0, keepdims=True) for a in acc]
        sums.append(jnp.zeros((16 - len(sums), half_y), F32))
        total = jnp.sum(jnp.concatenate(sums, 0), axis=1, keepdims=True)
        hit = jnp.logical_or(lane16 == i * n_vec + row16, lane16 == row16 * n_vec + i)
        hit = jnp.logical_and(hit, row16 <= i)
        return jnp.sum(jnp.where(hit, jnp.broadcast_to(total, hit.shape), 0.0), 0, keepdims=True)

    def gram_row(i):
        return gram_close(i, gram_part(i, gram_zero(i), 0, rows // 8))

    res_copy.wait()
    split_columns(n_prev)
    for c in range(comps):
        for ro in range(4):
            for p in range(2):
                for q in range(2):
                    vec[0, c, ro, p, q] = jnp.concatenate(
                        [work[n_prev, q, native(c, ro, p, h), :] for h in range(2)], 0
                    )
    zero_rows = jnp.zeros((2, half_y), F32)
    for c in range(comps):
        send_r[0, c, 0, 16:18] = zero_rows
        send_x[0, c, 0, 16:18] = zero_rows
        for q in range(2):
            face = slice(8 * q, 8 * q + 8)
            send_r[0, c, 0, face] = jnp.where(
                upper, roll_s(vec[0, c, 0, 1, q], 4), vec[0, c, 0, 0, q]
            )
            send_x[0, c, 0, face] = pack_x([vec[0, c, ro, 0, q] for ro in range(4)], 0)
            send_c[0, c, 0, q : q + 1] = vec[0, c, 0, 0, q, 0:1]

    pl.semaphore_wait(barrier, around(1))
    for c in range(comps):
        start_round(0, c)
    send_token(0)
    for copy in small_copies:
        copy.wait()
    for e in range(2):
        ids = jnp.concatenate([ids_ref[e], ids_ref[2 + e]], 0)
        eta = jnp.zeros((8, half_y), F32)
        for layer in range(visc_ref.shape[0]):
            eta = eta + jnp.where(ids == layer, visc_ref[layer], 0.0)
        for key, i in kinds.items():
            scaled[e, i] = eta * weight(*key)
    prev_copy.wait()
    for i in range(n_prev):
        split_columns(i)

    total = jnp.zeros((1, half_y), F32)
    for k in range(n_steps):
        for c in range(comps):
            finish_round(k, c)
            absorb(k, c)
            apply(k, c)
            start_round(k + 1, c)
        take_token(k)
        send_token(k + 1)
        if k == 0:
            for i in range(n_prev + 1):
                total = total + gram_row(i)
        else:
            for c in range(comps):
                to_native(k, c)
            write_out(k)
            total = total + gram_row(n_prev + k)
    for j in range(n_steps, len(reaches)):
        take_token(j)
        send_token(j + 1)
    acc = gram_zero(n_vec - 1)
    per = rows // 8 // comps
    for c in range(comps):
        finish_round(n_steps, c)
        absorb(n_steps, c)
        to_native(n_steps, c)
        acc = gram_part(n_vec - 1, acc, c * per, per)
    total = total + gram_close(n_vec - 1, acc)
    gram_send[...] = total

    def scatter(slot, device):
        pltpu.make_async_remote_copy(
            src_ref=gram_send,
            dst_ref=gram_recv.at[slot],
            send_sem=gram_sems.at[0],
            recv_sem=gram_sems.at[1],
            device_id=device,
            device_id_type=MESH,
        ).start()

    each_other(scatter)
    write_out(n_steps)
    settle(send_sem.at[0], [dirs_of(step) for step in range(n_steps + 1)] * comps)
    for i in range(2):
        pltpu.make_async_copy(gram_recv, gram_recv, gram_sems.at[i]).wait()
    full = (total + jnp.sum(gram_recv[...], axis=0)) * (1.0 / (rows * 2 * half_y * n_dev))
    for i in range(n_vec):
        line = full if i == 0 else pltpu.roll(full, half_y - i * n_vec, 1)
        gram_ref[i : i + 1, :] = line[:, :n_vec]


def store(vec_ref, gram_ref, vec_out, gram_out, sems):
    copies = [
        pltpu.make_async_copy(vec_ref, vec_out, sems.at[0]),
        pltpu.make_async_copy(gram_ref, gram_out, sems.at[1]),
    ]
    for copy in copies:
        copy.start()
    for copy in copies:
        copy.wait()


def on_device(residual, prev_basis, layer_ids, viscosity, shifts):
    n_lat = lax.axis_size("lat")
    n_rad = lax.axis_size("rad")
    comps, node_r, node_x, node_y = residual.shape
    n_prev = prev_basis.shape[0]
    n_steps = shifts.shape[0]
    n_vec = n_prev + n_steps + 1
    rows = comps * node_r * node_x
    half_y = node_y // 2
    assert node_r == 8 and node_x == 8 and half_y == 128
    rounds = n_steps + 1
    tile = (8, half_y)
    vmem = pltpu.VMEM
    hbm_spec = pl.BlockSpec(memory_space=pltpu.HBM)
    vmem_spec = pl.BlockSpec(memory_space=pltpu.VMEM)
    out, gram = pl.pallas_call(
        functools.partial(kernel, n_lat, n_rad, n_steps, n_prev, comps),
        out_shape=(
            pltpu.VMEM((n_steps, rows, node_y), F32),
            pltpu.VMEM((n_vec, n_vec), F32),
        ),
        in_specs=[hbm_spec] * 5,
        out_specs=(vmem_spec, vmem_spec),
        scratch_shapes=[
            vmem((n_prev + 1, rows, node_y), F32),
            vmem(layer_ids.shape, jnp.int32),
            pltpu.SMEM(viscosity.shape, F32),
            pltpu.SMEM(shifts.shape, F32),
            vmem((n_vec, 2, rows, half_y), F32),
            vmem((2, comps, 4, 2, 2) + tile, F32),
            vmem((2, comps, 2, 2) + tile, F32),
            vmem((2, comps, 4, 2) + tile, F32),
            vmem((2, comps, 2) + tile, F32),
            vmem((2, 9) + tile, F32),
            vmem((rounds, comps, 2, 18, half_y), F32),
            vmem((rounds, comps, 2, 18, half_y), F32),
            vmem((rounds, comps, 4, 2, half_y), F32),
            vmem((rounds, comps, 2, 18, half_y), F32),
            vmem((rounds, comps, 2, 18, half_y), F32),
            vmem((rounds, comps, 4, 2, half_y), F32),
            vmem((1, half_y), F32),
            vmem((n_lat * n_rad - 1, 1, half_y), F32),
            vmem((rounds * comps * 80, half_y), F32),
            pltpu.SemaphoreType.DMA((5,)),
            pltpu.SemaphoreType.DMA((1,)),
            pltpu.SemaphoreType.DMA((2, comps)),
            pltpu.SemaphoreType.DMA((2,)),
            pltpu.SemaphoreType.REGULAR((max(n_lat, n_rad).bit_length(),)),
        ],
        compiler_params=pltpu.CompilerParams(
            collective_id=0, has_side_effects=True, vmem_limit_bytes=65000000
        ),
    )(
        residual.reshape(rows, node_y),
        prev_basis.reshape(n_prev, rows, node_y),
        layer_ids,
        viscosity,
        shifts,
    )
    out, gram = pl.pallas_call(
        store,
        out_shape=(
            jax.ShapeDtypeStruct(out.shape, F32),
            jax.ShapeDtypeStruct(gram.shape, F32),
        ),
        in_specs=[vmem_spec] * 2,
        out_specs=(hbm_spec, hbm_spec),
        scratch_shapes=[pltpu.SemaphoreType.DMA((2,))],
    )(*(pltpu.with_memory_space_constraint(a, pltpu.VMEM) for a in (out, gram)))
    return out.reshape((n_steps,) + residual.shape), gram


def solution(mesh):
    placed = (
        P(None, "rad", "lat", None),
        P(None, None, "rad", "lat", None),
        P("rad", "lat", None),
        P(),
        P(),
    )
    return jax.shard_map(
        on_device,
        mesh=mesh,
        in_specs=placed,
        out_specs=(P(None, None, "rad", "lat", None), P()),
        check_vma=False,
    )
```

```python
import functools

import jax
import jax.numpy as jnp
from jax import lax
from jax.experimental import pallas as pl
from jax.experimental.pallas import tpu as pltpu
from jax.sharding import PartitionSpec as P

MESH = pl.DeviceIdType.MESH
F32 = jnp.float32

mass = (1.0 / 36, 1.0 / 12, 1.0 / 45)
stiff = (0.0, 1.0, 4.0 / 3)

DIRS = ((-1, -1), (-1, 0), (-1, 1), (0, -1), (0, 1), (1, -1), (1, 0), (1, 1))
R_DIRS = {(-1, 0): 0, (1, 0): 1}
X_DIRS = {(0, -1): 0, (0, 1): 1}
C_DIRS = {(-1, -1): 0, (-1, 1): 1, (1, -1): 2, (1, 1): 3}
FIRST = ((-1, 0), (0, -1), (-1, -1))
LAST = ((1, 0), (0, 1), (1, 1))


def weight(a, b, c):
    return (
        stiff[a] * mass[b] * mass[c] + mass[a] * stiff[b] * mass[c] + mass[a] * mass[b] * stiff[c]
    )


def forward(u0, u1, u2):
    total = u0 + u2
    twice = u1 + u1
    return total + (twice + twice), u0 - u2, total - twice


def backward(m0, m1, m2):
    both = m0 + m2
    half = m0 + m0 - m2
    return both + m1, half + half, both - m1


def kernel(
    n_lat,
    n_rad,
    n_steps,
    n_prev,
    comps,
    res_ref,
    prev_ref,
    ids_hbm,
    visc_hbm,
    shift_hbm,
    out_ref,
    gram_ref,
    stage,
    ids_ref,
    visc_ref,
    shift_ref,
    work,
    vec,
    ghost_r,
    ghost_x,
    ghost_c,
    scaled,
    send_r,
    send_x,
    send_c,
    recv_r,
    recv_x,
    recv_c,
    gram_send,
    gram_recv,
    bulk,
    in_sem,
    send_sem,
    recv_sem,
    gram_sems,
    token_sem,
):
    n_dev = n_lat * n_rad
    lat = lax.axis_index("lat")
    rad = lax.axis_index("rad")
    me = lat * n_rad + rad
    rows = res_ref.shape[0]
    half_y = res_ref.shape[1] // 2
    n_vec = n_prev + n_steps + 1

    res_copy = pltpu.make_async_copy(res_ref, stage.at[n_prev], in_sem.at[0])
    res_copy.start()
    prev_copy = pltpu.make_async_copy(prev_ref, stage.at[pl.ds(0, n_prev)], in_sem.at[1])
    small_copies = [
        pltpu.make_async_copy(a, b, in_sem.at[2 + i])
        for i, (a, b) in enumerate(
            ((ids_hbm, ids_ref), (visc_hbm, visc_ref), (shift_hbm, shift_ref))
        )
    ]
    for copy in small_copies:
        copy.start()
    prev_copy.start()

    barrier = pltpu.get_barrier_semaphore()

    def around(far, dirs):
        total = 0
        for dr, dx in dirs:
            if not ((dr and n_rad <= far) or (dx and n_lat <= far)):
                total += jnp.where(within(dr * far, dx * far), 1, 0)
        return total

    def within(dr, dx):
        ok = None
        for pos, step, count in ((rad, dr, n_rad), (lat, dx, n_lat)):
            if step:
                one = (pos >= -step) if step < 0 else (pos < count - step)
                ok = one if ok is None else jnp.logical_and(ok, one)
        return ok

    def signal_around(sem, far, dirs):
        for dr, dx in dirs:
            if (dr and n_rad <= far) or (dx and n_lat <= far):
                continue

            @pl.when(within(dr * far, dx * far))
            def _(dr=dr, dx=dx):
                pl.semaphore_signal(
                    sem,
                    inc=1,
                    device_id={"lat": lat + dx * far, "rad": rad + dr * far},
                    device_id_type=MESH,
                )

    signal_around(barrier, 1, LAST)

    for d in DIRS:
        if d in R_DIRS:
            ref, slot = recv_r, R_DIRS[d]
        elif d in X_DIRS:
            ref, slot = recv_x, X_DIRS[d]
        else:
            ref, slot = recv_c, C_DIRS[d]

        @pl.when(jnp.logical_not(within(-d[0], -d[1])))
        def _(ref=ref, slot=slot):
            ref[:, :, slot] = jnp.zeros(ref.shape[:2] + ref.shape[3:], F32)

    reaches = []
    while (2 << len(reaches)) < max(n_lat, n_rad) - 1:
        reaches.append(2 << len(reaches))

    def send_token(j):
        if j < len(reaches):
            signal_around(token_sem.at[j], reaches[j], DIRS)

    def take_token(j):
        if j < len(reaches):
            pl.semaphore_wait(token_sem.at[j], around(reaches[j], DIRS))

    rad_targets = [lax.rem(rad + d, n_rad) for d in range(n_rad)]

    def each_other(visit):
        def row(i, carry):
            lat_target = lax.rem(lat + n_lat // 2 + i, n_lat)
            for d in range(n_rad):
                ahead = lax.rem(n_lat // 2 + i, n_lat)
                visit(ahead * n_rad + d - 1, {"lat": lat_target, "rad": rad_targets[d]})
            return carry

        lax.fori_loop(0, n_lat // 2, row, 0, unroll=n_lat <= 8)
        lax.fori_loop(n_lat // 2 + 1, n_lat, row, 0, unroll=n_lat <= 8)
        for d in range(1, n_rad):
            visit(d - 1, {"lat": lat, "rad": rad_targets[d]})

    sub = lax.broadcasted_iota(jnp.int32, (8, half_y), 0)
    lane = lax.broadcasted_iota(jnp.int32, (8, half_y), 1)
    upper = sub >= 4
    ex = lax.rem(sub, 4)
    first_x = ex == 0
    last_x = ex == 3
    corner0 = sub == 0
    corner3 = sub == 3
    corner4 = sub == 4
    corner7 = sub == 7
    has_up = rad < n_rad - 1
    has_right = lat < n_lat - 1
    up_f = jnp.where(has_up, 1.0, 0.0).astype(F32)
    right_f = jnp.where(has_right, 1.0, 0.0).astype(F32)
    both_f = up_f * right_f

    def roll_s(v, k):
        return pltpu.roll(v, k % 8, 0)

    def keep(mask, v):
        return jnp.where(mask, v, 0.0)

    src = lax.broadcasted_iota(jnp.int32, (2 * half_y, 2 * half_y), 0)
    dst = lax.broadcasted_iota(jnp.int32, (2 * half_y, 2 * half_y), 1)
    split_perm = jnp.where(
        src == jnp.where(dst < half_y, 2 * dst, 2 * (dst - half_y) + 1), 1.0, 0.0
    ).astype(jnp.bfloat16)
    join_perm = jnp.where(
        dst == jnp.where(src < half_y, 2 * src, 2 * (src - half_y) + 1), 1.0, 0.0
    ).astype(jnp.bfloat16)

    def exact_dot(a, b):
        high = a.astype(jnp.bfloat16)
        rest = a - high.astype(F32)
        mid = rest.astype(jnp.bfloat16)
        low = (rest - mid.astype(F32)).astype(jnp.bfloat16)
        out = [jnp.dot(part, b, preferred_element_type=F32) for part in (high, mid, low)]
        return out[0] + (out[1] + out[2])

    def split_columns(i):
        z = exact_dot(stage[i], split_perm)
        work[i, 0] = z[:, :half_y]
        work[i, 1] = z[:, half_y:]

    def native(c, ro, p, h):
        return pl.ds(c * 64 + (4 * h + ro) * 8 + p, 4, stride=2)

    kinds = {}
    for a in range(3):
        for b in range(3):
            for c in range(3):
                key = tuple(sorted((a, b, c)))
                if key != (0, 0, 0) and key not in kinds:
                    kinds[key] = len(kinds)
    def copy_of(step, c, d):
        if d in R_DIRS:
            a, b = send_r.at[step, c, R_DIRS[d]], recv_r.at[step, c, R_DIRS[d]]
        elif d in X_DIRS:
            a, b = send_x.at[step, c, X_DIRS[d]], recv_x.at[step, c, X_DIRS[d]]
        else:
            a, b = send_c.at[step, c, C_DIRS[d]], recv_c.at[step, c, C_DIRS[d]]
        return pltpu.make_async_remote_copy(
            src_ref=a,
            dst_ref=b,
            send_sem=send_sem.at[0],
            recv_sem=recv_sem.at[step % 2, c],
            device_id={"lat": lat + d[1], "rad": rad + d[0]},
            device_id_type=MESH,
        )

    order = ((-1, -1), (1, 1), (-1, 1), (1, -1), (1, 0), (-1, 0), (0, 1), (0, -1))

    def dirs_of(step):
        wanted = FIRST if step == 0 else (LAST if step == n_steps else DIRS)
        return [d for d in order if d in wanted]

    def start_round(step, c):
        for d in dirs_of(step):

            @pl.when(within(*d))
            def _(d=d):
                copy_of(step, c, d).start()

    def places(pos, count):
        out = [(pos == 0, False, True), (pos == count - 1, True, False)]
        if count > 2:
            middle = jnp.logical_and(pos > 0, pos < count - 1)
            out.append((middle, True, True))
        return out if count > 1 else [(pos == 0, False, False)]

    def rows_of(dirs, down, up, left, right):
        have = {-1: {0: True, -1: down, 1: up}, 1: {0: True, -1: left, 1: right}}
        total = 0
        for dr, dx in dirs:
            if have[-1][dr] and have[1][dx]:
                total += 2 if dr and dx else 18
        return total

    def settle(sem, dir_lists):
        groups = {}
        for at_r, down, up in places(rad, n_rad):
            for at_x, left, right in places(lat, n_lat):
                n = sum(rows_of(dirs, down, up, left, right) for dirs in dir_lists)
                here = jnp.logical_and(at_r, at_x)
                groups[n] = jnp.logical_or(groups[n], here) if n in groups else here
        for n, here in groups.items():
            if n:

                @pl.when(here)
                def _(n=n):
                    pltpu.make_async_copy(bulk.at[pl.ds(0, n)], bulk.at[pl.ds(0, n)], sem).wait()

    def finish_round(step, c):
        settle(recv_sem.at[step % 2, c], [[(-d[0], -d[1]) for d in dirs_of(step)]])

    def pack_x(vals, at):
        out = None
        for ro in range(4):
            moved = roll_s(vals[ro], ro - at)
            out = moved if out is None else jnp.where(ex == ro, moved, out)
        return out

    def apply(k, c):
        s = shift_ref[k]
        cur = k % 2
        new = 1 - cur
        u = {}
        gx = {}
        for q in range(2):
            for ro in range(4):
                gx[ro, q] = ghost_x[cur, c, ro, q]
                for p in range(2):
                    u[ro, p, q] = vec[cur, c, ro, p, q]
            gx[4, q] = jnp.where(upper, ghost_c[cur, c, q], roll_s(gx[0, q], 4))
            for p in range(2):
                u[4, p, q] = jnp.where(upper, ghost_r[cur, c, p, q], roll_s(u[0, p, q], 4))
            for ro in range(5):
                u[ro, 2, q] = jnp.where(last_x, gx[ro, q], roll_s(u[ro, 0, q], -1))
        res = {}
        for e in range(2):
            t = {}
            for p in range(3):
                for q in range(2):
                    t[0, p, q], t[1, p, q], t[2, p, q] = forward(
                        u[2 * e, p, q], u[2 * e + 1, p, q], u[2 * e + 2, p, q]
                    )
            w = {}
            for a in range(3):
                x = {}
                for q in range(2):
                    x[0, q], x[1, q], x[2, q] = forward(t[a, 0, q], t[a, 1, q], t[a, 2, q])
                for b in range(3):
                    nxt = keep(lane != half_y - 1, pltpu.roll(x[b, 0], half_y - 1, 1))
                    m = list(forward(x[b, 0], x[b, 1], nxt))
                    for j in range(3):
                        key = tuple(sorted((a, b, j)))
                        if key in kinds:
                            m[j] = m[j] * scaled[e, kinds[key]]
                        else:
                            m[j] = None
                    if m[0] is None:
                        r0 = m[1] + m[2]
                        r1 = -(m[2] + m[2])
                        r2 = m[2] - m[1]
                    else:
                        r0, r1, r2 = backward(*m)
                    x[b, 0] = r0 + keep(lane != 0, pltpu.roll(r2, 1, 1))
                    x[b, 1] = r1
                for q in range(2):
                    w[a, 0, q], w[a, 1, q], w[a, 2, q] = backward(x[0, q], x[1, q], x[2, q])
            for p in range(3):
                for q in range(2):
                    r = backward(w[0, p, q], w[1, p, q], w[2, p, q])
                    for i in range(3):
                        key = (2 * e + i, p, q)
                        res[key] = res[key] + r[i] if key in res else r[i]
        px = {}
        for q in range(2):
            for ro in range(5):
                edge = res[ro, 2, q]
                px[ro, q] = edge
                res[ro, 0, q] = res[ro, 0, q] + keep(ex != 0, roll_s(edge, 1))
            for p in range(2):
                res[0, p, q] = res[0, p, q] + keep(upper, roll_s(res[4, p, q], 4))
            px[0, q] = px[0, q] + keep(upper, roll_s(px[4, q], 4))
        step = k + 1
        last = step == n_steps
        for q in range(2):
            face = slice(8 * q, 8 * q + 8)
            edge = slice(16 + q, 17 + q)
            row = slice(q, q + 1)
            send_r[step, c, 1, face] = jnp.where(upper, res[4, 1, q], roll_s(res[4, 0, q], 4))
            send_r[step, c, 1, edge] = px[4, q][7:8]
            send_x[step, c, 1, face] = pack_x([px[ro, q] for ro in range(4)], 3)
            send_x[step, c, 1, edge] = px[4, q][7:8]
            send_c[step, c, 3, row] = px[4, q][7:8]
            if not last:
                send_r[step, c, 0, face] = jnp.where(upper, roll_s(res[0, 1, q], 4), res[0, 0, q])
                send_r[step, c, 0, edge] = px[0, q][3:4]
                send_x[step, c, 0, face] = pack_x([res[ro, 0, q] for ro in range(4)], 0)
                send_x[step, c, 0, edge] = res[4, 0, q][4:5]
                send_c[step, c, 0, row] = res[0, 0, q][0:1]
                send_c[step, c, 1, row] = px[0, q][3:4]
                send_c[step, c, 2, row] = res[4, 0, q][4:5]
            for ro in range(4):
                for p in range(2):
                    vec[new, c, ro, p, q] = res[ro, p, q] - s * u[ro, p, q]
                if not last:
                    ghost_x[new, c, ro, q] = px[ro, q] - s * gx[ro, q]
            if not last:
                for p in range(2):
                    ghost_r[new, c, p, q] = res[4, p, q] - s * u[4, p, q]
                ghost_c[new, c, q] = px[4, q] - s * gx[4, q]

    def absorb(step, c):
        new = step % 2
        first, last = step == 0, step == n_steps
        for q in range(2):
            face = slice(8 * q, 8 * q + 8)
            line = slice(16 + q, 17 + q)
            row = slice(q, q + 1)

            def spot(ref_row, mask):
                return keep(mask, jnp.broadcast_to(ref_row, (8, half_y)))

            if not first:
                from_low = recv_r[step, c, 1, face]
                from_left = recv_x[step, c, 1, face]
                corner = spot(recv_c[step, c, 3, row], corner0)
                vec[new, c, 0, 0, q] += (
                    keep(~upper, from_low) + keep(first_x, from_left) + corner
                )
                vec[new, c, 0, 1, q] += keep(~upper, roll_s(from_low, 4))
                for ro in range(1, 4):
                    vec[new, c, ro, 0, q] += keep(first_x, roll_s(from_left, -ro))
            if not last:
                from_up = recv_r[step, c, 0, face]
                from_right = recv_x[step, c, 0, face]
                add0 = keep(upper, roll_s(from_up, 4))
                add1 = keep(upper, from_up)
                edge = keep(last_x, roll_s(from_right, 3))
                far = (
                    spot(recv_r[step, c, 0, line], corner7)
                    + spot(recv_x[step, c, 0, line], corner7)
                    + spot(recv_c[step, c, 0, row], corner7)
                )
                if not first:
                    add0 = (
                        add0
                        + spot(recv_x[step, c, 1, line], corner4)
                        + spot(recv_c[step, c, 1, row], corner4)
                    )
                    edge = (
                        edge
                        + spot(recv_r[step, c, 1, line], corner3)
                        + spot(recv_c[step, c, 2, row], corner3)
                    )
                    add0 = add0 + ghost_r[new, c, 0, q]
                    add1 = add1 + ghost_r[new, c, 1, q]
                    edge = edge + ghost_x[new, c, 0, q]
                    far = far + ghost_c[new, c, q]
                ghost_r[new, c, 0, q] = add0 * up_f
                ghost_r[new, c, 1, q] = add1 * up_f
                ghost_x[new, c, 0, q] = edge * right_f
                ghost_c[new, c, q] = far * both_f
                for ro in range(1, 4):
                    edge = keep(last_x, roll_s(from_right, 3 - ro))
                    if not first:
                        edge = edge + ghost_x[new, c, ro, q]
                    ghost_x[new, c, ro, q] = edge * right_f

    def to_native(k, c):
        cur = k % 2
        for ro in range(4):
            for p in range(2):
                for q in range(2):
                    v = vec[cur, c, ro, p, q]
                    for h in range(2):
                        work[n_prev + k, q, native(c, ro, p, h), :] = v[4 * h : 4 * h + 4]

    def write_out(k):
        z = jnp.concatenate([work[n_prev + k, 0], work[n_prev + k, 1]], 1)
        out_ref[k - 1] = exact_dot(z, join_perm)

    lane16 = lax.broadcasted_iota(jnp.int32, (16, half_y), 1)
    row16 = lax.broadcasted_iota(jnp.int32, (16, half_y), 0)

    def gram_part(i, acc, first, count):
        def chunk(t, acc):
            at = pl.ds(pl.multiple_of(8 * t, 8), 8)
            for q in range(2):
                mine = work[i, q, at, :]
                acc = tuple(
                    acc[j] + mine * (mine if j == i else work[j, q, at, :]) for j in range(i + 1)
                )
            return acc

        return lax.fori_loop(first, first + count, chunk, acc, unroll=4)

    def gram_zero(i):
        return (jnp.zeros((8, half_y), F32),) * (i + 1)

    def gram_close(i, acc):
        sums = [jnp.sum(a, axis=0, keepdims=True) for a in acc]
        sums.append(jnp.zeros((16 - len(sums), half_y), F32))
        total = jnp.sum(jnp.concatenate(sums, 0), axis=1, keepdims=True)
        hit = jnp.logical_or(lane16 == i * n_vec + row16, lane16 == row16 * n_vec + i)
        hit = jnp.logical_and(hit, row16 <= i)
        return jnp.sum(jnp.where(hit, jnp.broadcast_to(total, hit.shape), 0.0), 0, keepdims=True)

    def gram_row(i):
        return gram_close(i, gram_part(i, gram_zero(i), 0, rows // 8))

    res_copy.wait()
    edge_rows = []
    for c in range(comps):
        picked = [2 * x + p for p in range(2) for x in range(4)] + [8 * r for r in range(8)]
        edge_rows += [stage[n_prev, pl.ds(c * 64 + at, 1), :] for at in picked]
    edge = exact_dot(jnp.concatenate(edge_rows, 0), split_perm)
    zero_rows = jnp.zeros((2, half_y), F32)
    for c in range(comps):
        send_r[0, c, 0, 16:18] = zero_rows
        send_x[0, c, 0, 16:18] = zero_rows
        for q in range(2):
            face = slice(8 * q, 8 * q + 8)
            lanes = slice(half_y * q, half_y * (q + 1))
            send_r[0, c, 0, face] = edge[16 * c : 16 * c + 8, lanes]
            send_x[0, c, 0, face] = edge[16 * c + 8 : 16 * c + 16, lanes]
            send_c[0, c, 0, q : q + 1] = edge[16 * c : 16 * c + 1, lanes]

    @pl.when(jnp.logical_or(rad > 0, lat > 0))
    def _():
        pl.semaphore_wait(barrier, around(1, FIRST))

    for c in range(comps):
        start_round(0, c)
    split_columns(n_prev)
    for c in range(comps):
        for ro in range(4):
            for p in range(2):
                for q in range(2):
                    vec[0, c, ro, p, q] = jnp.concatenate(
                        [work[n_prev, q, native(c, ro, p, h), :] for h in range(2)], 0
                    )
    for copy in small_copies:
        copy.wait()
    for e in range(2):
        ids = jnp.concatenate([ids_ref[e], ids_ref[2 + e]], 0)
        eta = jnp.zeros((8, half_y), F32)
        for layer in range(visc_ref.shape[0]):
            eta = eta + jnp.where(ids == layer, visc_ref[layer], 0.0)
        for key, i in kinds.items():
            scaled[e, i] = eta * weight(*key)
    prev_copy.wait()
    for i in range(n_prev):
        split_columns(i)

    total = jnp.zeros((1, half_y), F32)
    for k in range(n_steps):
        for c in range(comps):
            finish_round(k, c)
            absorb(k, c)
            apply(k, c)
            start_round(k + 1, c)
        if k >= 2:
            take_token(k - 2)
        if k >= 1:
            send_token(k - 1)
        if k == 0:
            for i in range(n_prev + 1):
                total = total + gram_row(i)
        else:
            for c in range(comps):
                to_native(k, c)
            write_out(k)
            total = total + gram_row(n_prev + k)
    assert n_steps >= 2
    for j in range(n_steps - 2, len(reaches)):
        take_token(j)
        send_token(j + 1)
    acc = gram_zero(n_vec - 1)
    per = rows // 8 // comps
    for c in range(comps):
        finish_round(n_steps, c)
        absorb(n_steps, c)
        to_native(n_steps, c)
        acc = gram_part(n_vec - 1, acc, c * per, per)
    total = total + gram_close(n_vec - 1, acc)
    gram_send[...] = total

    def scatter(slot, device):
        pltpu.make_async_remote_copy(
            src_ref=gram_send,
            dst_ref=gram_recv.at[slot],
            send_sem=gram_sems.at[0],
            recv_sem=gram_sems.at[1],
            device_id=device,
            device_id_type=MESH,
        ).start()

    each_other(scatter)
    write_out(n_steps)
    settle(send_sem.at[0], [dirs_of(step) for step in range(n_steps + 1)] * comps)
    for i in range(2):
        pltpu.make_async_copy(gram_recv, gram_recv, gram_sems.at[i]).wait()
    full = (total + jnp.sum(gram_recv[...], axis=0)) * (1.0 / (rows * 2 * half_y * n_dev))
    for i in range(n_vec):
        line = full if i == 0 else pltpu.roll(full, half_y - i * n_vec, 1)
        gram_ref[i : i + 1, :] = line[:, :n_vec]


def store(vec_ref, gram_ref, vec_out, gram_out, sems):
    copies = [
        pltpu.make_async_copy(vec_ref, vec_out, sems.at[0]),
        pltpu.make_async_copy(gram_ref, gram_out, sems.at[1]),
    ]
    for copy in copies:
        copy.start()
    for copy in copies:
        copy.wait()


def on_device(residual, prev_basis, layer_ids, viscosity, shifts):
    n_lat = lax.axis_size("lat")
    n_rad = lax.axis_size("rad")
    comps, node_r, node_x, node_y = residual.shape
    n_prev = prev_basis.shape[0]
    n_steps = shifts.shape[0]
    n_vec = n_prev + n_steps + 1
    rows = comps * node_r * node_x
    half_y = node_y // 2
    assert node_r == 8 and node_x == 8 and half_y == 128
    rounds = n_steps + 1
    tile = (8, half_y)
    vmem = pltpu.VMEM
    hbm_spec = pl.BlockSpec(memory_space=pltpu.HBM)
    vmem_spec = pl.BlockSpec(memory_space=pltpu.VMEM)
    out, gram = pl.pallas_call(
        functools.partial(kernel, n_lat, n_rad, n_steps, n_prev, comps),
        out_shape=(
            pltpu.VMEM((n_steps, rows, node_y), F32),
            pltpu.VMEM((n_vec, n_vec), F32),
        ),
        in_specs=[hbm_spec] * 5,
        out_specs=(vmem_spec, vmem_spec),
        scratch_shapes=[
            vmem((n_prev + 1, rows, node_y), F32),
            vmem(layer_ids.shape, jnp.int32),
            pltpu.SMEM(viscosity.shape, F32),
            pltpu.SMEM(shifts.shape, F32),
            vmem((n_vec, 2, rows, half_y), F32),
            vmem((2, comps, 4, 2, 2) + tile, F32),
            vmem((2, comps, 2, 2) + tile, F32),
            vmem((2, comps, 4, 2) + tile, F32),
            vmem((2, comps, 2) + tile, F32),
            vmem((2, 9) + tile, F32),
            vmem((rounds, comps, 2, 18, half_y), F32),
            vmem((rounds, comps, 2, 18, half_y), F32),
            vmem((rounds, comps, 4, 2, half_y), F32),
            vmem((rounds, comps, 2, 18, half_y), F32),
            vmem((rounds, comps, 2, 18, half_y), F32),
            vmem((rounds, comps, 4, 2, half_y), F32),
            vmem((1, half_y), F32),
            vmem((n_lat * n_rad - 1, 1, half_y), F32),
            vmem((rounds * comps * 80, half_y), F32),
            pltpu.SemaphoreType.DMA((5,)),
            pltpu.SemaphoreType.DMA((1,)),
            pltpu.SemaphoreType.DMA((2, comps)),
            pltpu.SemaphoreType.DMA((2,)),
            pltpu.SemaphoreType.REGULAR((max(n_lat, n_rad).bit_length(),)),
        ],
        compiler_params=pltpu.CompilerParams(
            collective_id=0, has_side_effects=True, vmem_limit_bytes=65000000
        ),
    )(
        residual.reshape(rows, node_y),
        prev_basis.reshape(n_prev, rows, node_y),
        layer_ids,
        viscosity,
        shifts,
    )
    out, gram = pl.pallas_call(
        store,
        out_shape=(
            jax.ShapeDtypeStruct(out.shape, F32),
            jax.ShapeDtypeStruct(gram.shape, F32),
        ),
        in_specs=[vmem_spec] * 2,
        out_specs=(hbm_spec, hbm_spec),
        scratch_shapes=[pltpu.SemaphoreType.DMA((2,))],
    )(*(pltpu.with_memory_space_constraint(a, pltpu.VMEM) for a in (out, gram)))
    return out.reshape((n_steps,) + residual.shape), gram


def solution(mesh):
    placed = (
        P(None, "rad", "lat", None),
        P(None, None, "rad", "lat", None),
        P("rad", "lat", None),
        P(),
        P(),
    )
    return jax.shard_map(
        on_device,
        mesh=mesh,
        in_specs=placed,
        out_specs=(P(None, None, "rad", "lat", None), P()),
        check_vma=False,
    )
```

```python
import functools

import jax
import jax.numpy as jnp
from jax import lax
from jax.experimental import pallas as pl
from jax.experimental.pallas import tpu as pltpu
from jax.sharding import PartitionSpec as P

MESH = pl.DeviceIdType.MESH
F32 = jnp.float32

mass = (1.0 / 36, 1.0 / 12, 1.0 / 45)
stiff = (0.0, 1.0, 4.0 / 3)

DIRS = ((-1, -1), (-1, 0), (-1, 1), (0, -1), (0, 1), (1, -1), (1, 0), (1, 1))
R_DIRS = {(-1, 0): 0, (1, 0): 1}
X_DIRS = {(0, -1): 0, (0, 1): 1}
C_DIRS = {(-1, -1): 0, (-1, 1): 1, (1, -1): 2, (1, 1): 3}
FIRST = ((-1, 0), (0, -1), (-1, -1))
LAST = ((1, 0), (0, 1), (1, 1))
ROWS_X, ROWS_G, ROWS_A, ROWS_C = 0, 8, 12, 16
RIM = (
    ((1, 0), (0, 8), (4, 4), ROWS_X, 0),
    ((1, 0), (16, 4), (7, 1), ROWS_G, 3),
    ((0, 1), (8, 8), (4, 4), ROWS_X, 4),
    ((0, 1), (20, 4), (7, 1), ROWS_G, 7),
    ((1, 1), (24, 4), (7, 1), ROWS_C, 0),
    ((1, 1), (28, 4), (7, 1), ROWS_C, 4),
    ((1, -1), (32, 4), (4, 1), ROWS_A, 3),
    ((-1, 1), (36, 4), (3, 1), ROWS_A, 7),
)


def weight(a, b, c):
    return (
        stiff[a] * mass[b] * mass[c] + mass[a] * stiff[b] * mass[c] + mass[a] * mass[b] * stiff[c]
    )


def forward(u0, u1, u2):
    total = u0 + u2
    twice = u1 + u1
    return total + (twice + twice), u0 - u2, total - twice


def backward(m0, m1, m2):
    both = m0 + m2
    half = m0 + m0 - m2
    return both + m1, half + half, both - m1


def kernel(
    n_lat,
    n_rad,
    n_steps,
    n_prev,
    comps,
    res_ref,
    prev_ref,
    ids_hbm,
    visc_hbm,
    shift_hbm,
    out_ref,
    gram_ref,
    stage,
    ids_ref,
    visc_ref,
    shift_ref,
    work,
    vec,
    ghost_r,
    ghost_x,
    ghost_c,
    scaled,
    send_r,
    send_x,
    send_c,
    recv_r,
    recv_x,
    recv_c,
    gram_send,
    gram_recv,
    bulk,
    rim_send,
    rim_recv,
    block_send,
    block_recv,
    eta_send,
    eta_recv,
    rim_scaled,
    rim_own,
    in_sem,
    send_sem,
    recv_sem,
    rim_sems,
    gram_sems,
    token_sem,
):
    n_dev = n_lat * n_rad
    lat = lax.axis_index("lat")
    rad = lax.axis_index("rad")
    me = lat * n_rad + rad
    rows = res_ref.shape[0]
    half_y = res_ref.shape[1] // 2
    n_vec = n_prev + n_steps + 1

    res_copy = pltpu.make_async_copy(res_ref, stage.at[n_prev], in_sem.at[0])
    res_copy.start()
    prev_copy = pltpu.make_async_copy(prev_ref, stage.at[pl.ds(0, n_prev)], in_sem.at[1])
    small_copies = [
        pltpu.make_async_copy(a, b, in_sem.at[2 + i])
        for i, (a, b) in enumerate(
            ((ids_hbm, ids_ref), (visc_hbm, visc_ref), (shift_hbm, shift_ref))
        )
    ]
    for copy in small_copies:
        copy.start()
    prev_copy.start()

    barrier = pltpu.get_barrier_semaphore()

    def around(far, dirs):
        total = 0
        for dr, dx in dirs:
            if not ((dr and n_rad <= far) or (dx and n_lat <= far)):
                total += jnp.where(within(dr * far, dx * far), 1, 0)
        return total

    def within(dr, dx):
        ok = None
        for pos, step, count in ((rad, dr, n_rad), (lat, dx, n_lat)):
            if step:
                one = (pos >= -step) if step < 0 else (pos < count - step)
                ok = one if ok is None else jnp.logical_and(ok, one)
        return ok

    def signal_around(sem, far, dirs):
        for dr, dx in dirs:
            if (dr and n_rad <= far) or (dx and n_lat <= far):
                continue

            @pl.when(within(dr * far, dx * far))
            def _(dr=dr, dx=dx):
                pl.semaphore_signal(
                    sem,
                    inc=1,
                    device_id={"lat": lat + dx * far, "rad": rad + dr * far},
                    device_id_type=MESH,
                )

    signal_around(barrier, 1, LAST)

    for d in DIRS:
        if d in R_DIRS:
            ref, slot = recv_r, R_DIRS[d]
        elif d in X_DIRS:
            ref, slot = recv_x, X_DIRS[d]
        else:
            ref, slot = recv_c, C_DIRS[d]

        @pl.when(jnp.logical_not(within(-d[0], -d[1])))
        def _(ref=ref, slot=slot):
            ref[:, :, slot] = jnp.zeros(ref.shape[:2] + ref.shape[3:], F32)

    for ref in (rim_recv, block_recv, eta_recv):
        ref[...] = jnp.zeros_like(ref)

    reaches = []
    while (2 << len(reaches)) < max(n_lat, n_rad) - 1:
        reaches.append(2 << len(reaches))

    def send_token(j):
        if j < len(reaches):
            signal_around(token_sem.at[j], reaches[j], DIRS)

    def take_token(j):
        if j < len(reaches):
            pl.semaphore_wait(token_sem.at[j], around(reaches[j], DIRS))

    rad_targets = [lax.rem(rad + d, n_rad) for d in range(n_rad)]

    def each_other(visit):
        def row(i, carry):
            lat_target = lax.rem(lat + n_lat // 2 + i, n_lat)
            for d in range(n_rad):
                ahead = lax.rem(n_lat // 2 + i, n_lat)
                visit(ahead * n_rad + d - 1, {"lat": lat_target, "rad": rad_targets[d]})
            return carry

        lax.fori_loop(0, n_lat // 2, row, 0, unroll=n_lat <= 8)
        lax.fori_loop(n_lat // 2 + 1, n_lat, row, 0, unroll=n_lat <= 8)
        for d in range(1, n_rad):
            visit(d - 1, {"lat": lat, "rad": rad_targets[d]})

    sub = lax.broadcasted_iota(jnp.int32, (8, half_y), 0)
    lane = lax.broadcasted_iota(jnp.int32, (8, half_y), 1)
    upper = sub >= 4
    ex = lax.rem(sub, 4)
    first_x = ex == 0
    last_x = ex == 3
    corner0 = sub == 0
    corner3 = sub == 3
    corner4 = sub == 4
    corner7 = sub == 7
    has_up = rad < n_rad - 1
    has_right = lat < n_lat - 1
    up_f = jnp.where(has_up, 1.0, 0.0).astype(F32)
    right_f = jnp.where(has_right, 1.0, 0.0).astype(F32)
    both_f = up_f * right_f

    def roll_s(v, k):
        return pltpu.roll(v, k % 8, 0)

    def keep(mask, v):
        return jnp.where(mask, v, 0.0)

    src = lax.broadcasted_iota(jnp.int32, (2 * half_y, 2 * half_y), 0)
    dst = lax.broadcasted_iota(jnp.int32, (2 * half_y, 2 * half_y), 1)
    split_perm = jnp.where(
        src == jnp.where(dst < half_y, 2 * dst, 2 * (dst - half_y) + 1), 1.0, 0.0
    ).astype(jnp.bfloat16)
    join_perm = jnp.where(
        dst == jnp.where(src < half_y, 2 * src, 2 * (src - half_y) + 1), 1.0, 0.0
    ).astype(jnp.bfloat16)

    def exact_dot(a, b):
        high = a.astype(jnp.bfloat16)
        rest = a - high.astype(F32)
        mid = rest.astype(jnp.bfloat16)
        low = (rest - mid.astype(F32)).astype(jnp.bfloat16)
        out = [jnp.dot(part, b, preferred_element_type=F32) for part in (high, mid, low)]
        return out[0] + (out[1] + out[2])

    def split_columns(i):
        z = exact_dot(stage[i], split_perm)
        work[i, 0] = z[:, :half_y]
        work[i, 1] = z[:, half_y:]

    def native(c, ro, p, h):
        return pl.ds(c * 64 + (4 * h + ro) * 8 + p, 4, stride=2)

    kinds = {}
    for a in range(3):
        for b in range(3):
            for c in range(3):
                key = tuple(sorted((a, b, c)))
                if key != (0, 0, 0) and key not in kinds:
                    kinds[key] = len(kinds)
    def copy_of(step, c, d):
        if d in R_DIRS:
            a, b = send_r.at[step, c, R_DIRS[d]], recv_r.at[step, c, R_DIRS[d]]
        elif d in X_DIRS:
            a, b = send_x.at[step, c, X_DIRS[d]], recv_x.at[step, c, X_DIRS[d]]
        else:
            a, b = send_c.at[step, c, C_DIRS[d]], recv_c.at[step, c, C_DIRS[d]]
        return pltpu.make_async_remote_copy(
            src_ref=a,
            dst_ref=b,
            send_sem=send_sem.at[0],
            recv_sem=recv_sem.at[step % 2, c],
            device_id={"lat": lat + d[1], "rad": rad + d[0]},
            device_id_type=MESH,
        )

    order = ((-1, -1), (1, 1), (-1, 1), (1, -1), (1, 0), (-1, 0), (0, 1), (0, -1))

    def dirs_of(step):
        wanted = FIRST if step == 0 else DIRS
        return [d for d in order if d in wanted]

    def start_round(step, c):
        for d in dirs_of(step):

            @pl.when(within(*d))
            def _(d=d):
                copy_of(step, c, d).start()

    def places(pos, count):
        out = [(pos == 0, False, True), (pos == count - 1, True, False)]
        if count > 2:
            middle = jnp.logical_and(pos > 0, pos < count - 1)
            out.append((middle, True, True))
        return out if count > 1 else [(pos == 0, False, False)]

    def rows_of(sizes, down, up, left, right):
        have = {-1: {0: True, -1: down, 1: up}, 1: {0: True, -1: left, 1: right}}
        return sum(n for (dr, dx), n in sizes if have[-1][dr] and have[1][dx])

    def settle(sem, sizes):
        groups = {}
        for at_r, down, up in places(rad, n_rad):
            for at_x, left, right in places(lat, n_lat):
                n = rows_of(sizes, down, up, left, right)
                here = jnp.logical_and(at_r, at_x)
                groups[n] = jnp.logical_or(groups[n], here) if n in groups else here
        for n, here in groups.items():
            if n:

                @pl.when(here)
                def _(n=n):
                    pltpu.make_async_copy(bulk.at[pl.ds(0, n)], bulk.at[pl.ds(0, n)], sem).wait()

    def opposite(sizes):
        return [((-dr, -dx), n) for (dr, dx), n in sizes]

    def round_sizes(step):
        return [(d, 2 if d[0] and d[1] else 18) for d in dirs_of(step)]

    rim_sizes = [(d, comps * count * high) for d, (_, count), (_, high), _, _ in RIM]
    rim_sizes.append(((1, 1), comps * 8))
    eta_sizes = [((1, 0), 4), ((0, 1), 4), ((1, 1), 1)]

    def finish_round(step, c):
        settle(recv_sem.at[step % 2, c], opposite(round_sizes(step)))

    def remote(a, b, recv, d):
        @pl.when(within(*d))
        def _():
            pltpu.make_async_remote_copy(
                src_ref=a,
                dst_ref=b,
                send_sem=send_sem.at[0],
                recv_sem=recv,
                device_id={"lat": lat + d[1], "rad": rad + d[0]},
                device_id_type=MESH,
            ).start()

    def start_rim():
        for d, (first, count), (row, high), to, to_row in RIM:
            remote(
                rim_send.at[:, pl.ds(first, count), pl.ds(row, high)],
                rim_recv.at[:, pl.ds(to, count), pl.ds(to_row, high)],
                rim_sems.at[0],
                d,
            )
        remote(
            block_send.at[:, pl.ds(0, comps)], block_recv.at[:, pl.ds(0, comps)], rim_sems.at[0], (1, 1)
        )

    def start_eta():
        for d, slot, row, high, to, to_row in (
            ((1, 0), 0, 4, 4, 0, 0),
            ((0, 1), 1, 4, 4, 0, 4),
            ((1, 1), 0, 7, 1, 1, 0),
        ):
            remote(
                eta_send.at[slot, pl.ds(row, high)],
                eta_recv.at[to, pl.ds(to_row, high)],
                rim_sems.at[1],
                d,
            )

    def pack_x(vals, at):
        out = None
        for ro in range(4):
            moved = roll_s(vals[ro], ro - at)
            out = moved if out is None else jnp.where(ex == ro, moved, out)
        return out

    def y_pass(x0, x1, a, b, scale):
        nxt = keep(lane != half_y - 1, pltpu.roll(x0, half_y - 1, 1))
        m = list(forward(x0, x1, nxt))
        for j in range(3):
            key = tuple(sorted((a, b, j)))
            m[j] = m[j] * scale(kinds[key]) if key in kinds else None
        if m[0] is None:
            r0 = m[1] + m[2]
            r1 = -(m[2] + m[2])
            r2 = m[2] - m[1]
        else:
            r0, r1, r2 = backward(*m)
        return r0 + keep(lane != 0, pltpu.roll(r2, 1, 1)), r1

    def to_column(low, high):
        moved = jnp.where(sub == 6, roll_s(low, -1), high)
        return jnp.where(sub == 4, roll_s(low, 1), jnp.where(sub == 5, roll_s(high, 2), moved))

    def apply(k, c):
        s = shift_ref[k]
        cur = k % 2
        new = 1 - cur
        u = {}
        gx = {}
        for q in range(2):
            for ro in range(4):
                gx[ro, q] = ghost_x[cur, c, ro, q]
                for p in range(2):
                    u[ro, p, q] = vec[cur, c, ro, p, q]
            gx[4, q] = jnp.where(upper, ghost_c[cur, c, q], roll_s(gx[0, q], 4))
            for p in range(2):
                u[4, p, q] = jnp.where(upper, ghost_r[cur, c, p, q], roll_s(u[0, p, q], 4))
            for ro in range(5):
                u[ro, 2, q] = jnp.where(last_x, gx[ro, q], roll_s(u[ro, 0, q], -1))
        res = {}
        for e in range(2):
            t = {}
            for p in range(3):
                for q in range(2):
                    t[0, p, q], t[1, p, q], t[2, p, q] = forward(
                        u[2 * e, p, q], u[2 * e + 1, p, q], u[2 * e + 2, p, q]
                    )
            w = {}
            for a in range(3):
                x = {}
                for q in range(2):
                    x[0, q], x[1, q], x[2, q] = forward(t[a, 0, q], t[a, 1, q], t[a, 2, q])
                for b in range(3):
                    x[b, 0], x[b, 1] = y_pass(x[b, 0], x[b, 1], a, b, lambda i: scaled[e, i])
                for q in range(2):
                    w[a, 0, q], w[a, 1, q], w[a, 2, q] = backward(x[0, q], x[1, q], x[2, q])
            for p in range(3):
                for q in range(2):
                    r = backward(w[0, p, q], w[1, p, q], w[2, p, q])
                    for i in range(3):
                        key = (2 * e + i, p, q)
                        res[key] = res[key] + r[i] if key in res else r[i]
        px = {}
        for q in range(2):
            for ro in range(5):
                edge = res[ro, 2, q]
                px[ro, q] = edge
                res[ro, 0, q] = res[ro, 0, q] + keep(ex != 0, roll_s(edge, 1))
            for p in range(2):
                res[0, p, q] = res[0, p, q] + keep(upper, roll_s(res[4, p, q], 4))
            px[0, q] = px[0, q] + keep(upper, roll_s(px[4, q], 4))
        step = k + 1
        last = step == n_steps
        for q in range(2):
            face = slice(8 * q, 8 * q + 8)
            edge = slice(16 + q, 17 + q)
            row = slice(q, q + 1)
            if not last:
                send_r[step, c, 1, face] = jnp.where(upper, res[4, 1, q], roll_s(res[4, 0, q], 4))
                send_r[step, c, 1, edge] = px[4, q][7:8]
                send_x[step, c, 1, face] = pack_x([px[ro, q] for ro in range(4)], 3)
                send_x[step, c, 1, edge] = px[4, q][7:8]
                send_c[step, c, 3, row] = px[4, q][7:8]
                send_r[step, c, 0, face] = jnp.where(upper, roll_s(res[0, 1, q], 4), res[0, 0, q])
                send_r[step, c, 0, edge] = px[0, q][3:4]
                send_x[step, c, 0, face] = pack_x([res[ro, 0, q] for ro in range(4)], 0)
                send_x[step, c, 0, edge] = res[4, 0, q][4:5]
                send_c[step, c, 0, row] = res[0, 0, q][0:1]
                send_c[step, c, 1, row] = px[0, q][3:4]
                send_c[step, c, 2, row] = res[4, 0, q][4:5]
            for ro in range(4):
                for p in range(2):
                    vec[new, c, ro, p, q] = res[ro, p, q] - s * u[ro, p, q]
                if not last:
                    ghost_x[new, c, ro, q] = px[ro, q] - s * gx[ro, q]
            if not last:
                for p in range(2):
                    ghost_r[new, c, p, q] = res[4, p, q] - s * u[4, p, q]
                ghost_c[new, c, q] = px[4, q] - s * gx[4, q]
            if step == n_steps - 1:
                for n in range(2):
                    rim_send[c, 24 + 2 * n + q] = px[2 + n, q]
                    rim_send[c, 28 + 2 * n + q] = res[4, n, q]
                    rim_send[c, 32 + 2 * n + q] = res[2 + n, 0, q]
                    rim_send[c, 36 + 2 * n + q] = res[0, n, q]

    def pack_rim(c):
        new = (n_steps - 1) % 2
        for q in range(2):
            for n in range(2):
                for p in range(2):
                    v = vec[new, c, 2 + n, p, q]
                    rim_send[c, 4 * n + 2 * p + q] = v
                    block_send[4 * n + 2 * p + q, c : c + 1] = v[7:8]
                    rim_send[c, 8 + 4 * n + 2 * p + q] = to_column(
                        vec[new, c, p, n, q], vec[new, c, 2 + p, n, q]
                    )
                rim_send[c, 16 + 2 * n + q] = ghost_x[new, c, 2 + n, q]
                rim_send[c, 20 + 2 * n + q] = ghost_r[new, c, n, q]

    group_last = lax.rem(sub, 4) == 3
    group_first = lax.rem(sub, 4) == 0

    def own_planes(c):
        cur = (n_steps - 1) % 2
        for q in range(2):
            side = jnp.where(corner3, ghost_x[cur, c, 0, q], roll_s(ghost_r[cur, c, 0, q], 3))
            for p in range(2):
                column = to_column(
                    roll_s(vec[cur, c, p, 0, q], 3), roll_s(vec[cur, c, 2 + p, 0, q], 3)
                )
                plane = jnp.where(upper, column, vec[cur, c, 0, p, q])
                rim_own[c, 2 * p + q] = plane
                if p == 0:
                    rim_own[c, 4 + q] = jnp.where(group_last, side, roll_s(plane, -1))

    def rim_elements(u, scale):
        t = {}
        for p in range(3):
            for q in range(2):
                t[0, p, q], t[1, p, q], t[2, p, q] = forward(u[0, p, q], u[1, p, q], u[2, p, q])
        w = {}
        for a in range(3):
            x = {}
            for q in range(2):
                x[0, q], x[1, q], x[2, q] = forward(t[a, 0, q], t[a, 1, q], t[a, 2, q])
            for b in range(3):
                x[b, 0], x[b, 1] = y_pass(x[b, 0], x[b, 1], a, b, scale)
            for q in range(2):
                w[a, 0, q], w[a, 1, q], w[a, 2, q] = backward(x[0, q], x[1, q], x[2, q])
        return {
            (p, q): w[0, p, q] + w[2, p, q] - w[1, p, q] for p in range(3) for q in range(2)
        }

    def add_rim():
        cur = (n_steps - 1) % 2
        new = 1 - cur
        inner = jnp.where(upper, up_f, right_f)
        corner = {}
        sides = {}
        for c in range(comps):
            u = {}
            for q in range(2):
                for n in range(2):
                    for p in range(2):
                        u[n, p, q] = rim_recv[c, ROWS_X + 4 * n + 2 * p + q]
                    u[n, 0, q] = u[n, 0, q] + rim_recv[c, ROWS_C + 2 * n + q]
                    ghost = rim_recv[c, ROWS_G + 2 * n + q] + rim_recv[c, ROWS_A + 2 * n + q]
                    u[n, 2, q] = jnp.where(group_last, ghost * inner, roll_s(u[n, 0, q], -1))
                for p in range(3):
                    u[2, p, q] = rim_own[c, 2 * p + q]
            for q in range(2):
                parts = {(2, 2): roll_s(u[2, 0, q], c)}
                for n in range(2):
                    parts[n, 2] = roll_s(u[n, 0, q], c)
                    parts[2, n] = roll_s(u[n, 0, q], c - 4)
                for key, part in parts.items():
                    part = keep(sub == c, part)
                    key = key + (q,)
                    corner[key] = corner[key] + part if c else part
            sides[c] = rim_elements(u, lambda i: rim_scaled[0, i])
        for q in range(2):
            for n in range(2):
                for p in range(2):
                    corner[n, p, q] = block_recv[4 * n + 2 * p + q]
        tip = rim_elements(corner, lambda i: rim_scaled[1, i])
        for c in range(comps):
            for q in range(2):
                out = [
                    sides[c][0, q] + keep(~group_first, roll_s(sides[c][2, q], 1)),
                    sides[c][1, q],
                ]
                for p in range(2):
                    for e in range(2):
                        ro = 2 * e + p
                        add = keep(corner4, roll_s(out[p], -(2 + e)))
                        add = jnp.where(corner0, roll_s(out[p], -(4 + e)), add)
                        if ro == 0:
                            add = add + keep(~upper, out[0]) + keep(corner0, roll_s(tip[2, q], -c))
                        vec[new, c, ro, 0, q] += add
                vec[new, c, 0, 1, q] += keep(~upper, out[1])

    def absorb(step, c):
        new = step % 2
        first, last = step == 0, False
        for q in range(2):
            face = slice(8 * q, 8 * q + 8)
            line = slice(16 + q, 17 + q)
            row = slice(q, q + 1)

            def spot(ref_row, mask):
                return keep(mask, jnp.broadcast_to(ref_row, (8, half_y)))

            if not first:
                from_low = recv_r[step, c, 1, face]
                from_left = recv_x[step, c, 1, face]
                corner = spot(recv_c[step, c, 3, row], corner0)
                vec[new, c, 0, 0, q] += (
                    keep(~upper, from_low) + keep(first_x, from_left) + corner
                )
                vec[new, c, 0, 1, q] += keep(~upper, roll_s(from_low, 4))
                for ro in range(1, 4):
                    vec[new, c, ro, 0, q] += keep(first_x, roll_s(from_left, -ro))
            if not last:
                from_up = recv_r[step, c, 0, face]
                from_right = recv_x[step, c, 0, face]
                add0 = keep(upper, roll_s(from_up, 4))
                add1 = keep(upper, from_up)
                edge = keep(last_x, roll_s(from_right, 3))
                far = (
                    spot(recv_r[step, c, 0, line], corner7)
                    + spot(recv_x[step, c, 0, line], corner7)
                    + spot(recv_c[step, c, 0, row], corner7)
                )
                if not first:
                    add0 = (
                        add0
                        + spot(recv_x[step, c, 1, line], corner4)
                        + spot(recv_c[step, c, 1, row], corner4)
                    )
                    edge = (
                        edge
                        + spot(recv_r[step, c, 1, line], corner3)
                        + spot(recv_c[step, c, 2, row], corner3)
                    )
                    add0 = add0 + ghost_r[new, c, 0, q]
                    add1 = add1 + ghost_r[new, c, 1, q]
                    edge = edge + ghost_x[new, c, 0, q]
                    far = far + ghost_c[new, c, q]
                ghost_r[new, c, 0, q] = add0 * up_f
                ghost_r[new, c, 1, q] = add1 * up_f
                ghost_x[new, c, 0, q] = edge * right_f
                ghost_c[new, c, q] = far * both_f
                for ro in range(1, 4):
                    edge = keep(last_x, roll_s(from_right, 3 - ro))
                    if not first:
                        edge = edge + ghost_x[new, c, ro, q]
                    ghost_x[new, c, ro, q] = edge * right_f

    def to_native(k, c, rim=False):
        cur = k % 2
        for ro in range(4):
            for p in range(2):
                if rim and ro and p:
                    continue
                for q in range(2):
                    v = vec[cur, c, ro, p, q]
                    for h in range(2):
                        work[n_prev + k, q, native(c, ro, p, h), :] = v[4 * h : 4 * h + 4]

    def write_out(k):
        z = jnp.concatenate([work[n_prev + k, 0], work[n_prev + k, 1]], 1)
        out_ref[k - 1] = exact_dot(z, join_perm)

    lane16 = lax.broadcasted_iota(jnp.int32, (16, half_y), 1)
    row16 = lax.broadcasted_iota(jnp.int32, (16, half_y), 0)

    def gram_part(i, acc, first, count):
        def chunk(t, acc):
            at = pl.ds(pl.multiple_of(8 * t, 8), 8)
            for q in range(2):
                mine = work[i, q, at, :]
                acc = tuple(
                    acc[j] + mine * (mine if j == i else work[j, q, at, :]) for j in range(i + 1)
                )
            return acc

        return lax.fori_loop(first, first + count, chunk, acc, unroll=4)

    def gram_add(i, acc, at, mask):
        for q in range(2):
            mine = work[i, q, at, :]
            mine = mine if mask is None else keep(mask, mine)
            acc = tuple(
                acc[j] + mine * (mine if j == i else work[j, q, at, :]) for j in range(i + 1)
            )
        return acc

    def gram_zero(i):
        return (jnp.zeros((8, half_y), F32),) * (i + 1)

    def gram_close(i, acc):
        sums = [jnp.sum(a, axis=0, keepdims=True) for a in acc]
        sums.append(jnp.zeros((16 - len(sums), half_y), F32))
        total = jnp.sum(jnp.concatenate(sums, 0), axis=1, keepdims=True)
        hit = jnp.logical_or(lane16 == i * n_vec + row16, lane16 == row16 * n_vec + i)
        hit = jnp.logical_and(hit, row16 <= i)
        return jnp.sum(jnp.where(hit, jnp.broadcast_to(total, hit.shape), 0.0), 0, keepdims=True)

    def gram_row(i):
        return gram_close(i, gram_part(i, gram_zero(i), 0, rows // 8))

    res_copy.wait()
    edge_rows = []
    for c in range(comps):
        picked = [2 * x + p for p in range(2) for x in range(4)] + [8 * r for r in range(8)]
        edge_rows += [stage[n_prev, pl.ds(c * 64 + at, 1), :] for at in picked]
    edge = exact_dot(jnp.concatenate(edge_rows, 0), split_perm)
    zero_rows = jnp.zeros((2, half_y), F32)
    for c in range(comps):
        send_r[0, c, 0, 16:18] = zero_rows
        send_x[0, c, 0, 16:18] = zero_rows
        for q in range(2):
            face = slice(8 * q, 8 * q + 8)
            lanes = slice(half_y * q, half_y * (q + 1))
            send_r[0, c, 0, face] = edge[16 * c : 16 * c + 8, lanes]
            send_x[0, c, 0, face] = edge[16 * c + 8 : 16 * c + 16, lanes]
            send_c[0, c, 0, q : q + 1] = edge[16 * c : 16 * c + 1, lanes]

    @pl.when(jnp.logical_or(rad > 0, lat > 0))
    def _():
        pl.semaphore_wait(barrier, around(1, FIRST))

    for c in range(comps):
        start_round(0, c)
    split_columns(n_prev)
    for c in range(comps):
        for ro in range(4):
            for p in range(2):
                for q in range(2):
                    vec[0, c, ro, p, q] = jnp.concatenate(
                        [work[n_prev, q, native(c, ro, p, h), :] for h in range(2)], 0
                    )
    for copy in small_copies:
        copy.wait()
    etas = []
    for e in range(2):
        ids = jnp.concatenate([ids_ref[e], ids_ref[2 + e]], 0)
        eta = jnp.zeros((8, half_y), F32)
        for layer in range(visc_ref.shape[0]):
            eta = eta + jnp.where(ids == layer, visc_ref[layer], 0.0)
        etas.append(eta)
        for key, i in kinds.items():
            scaled[e, i] = eta * weight(*key)
    eta_send[0] = etas[1]
    eta_send[1] = to_column(*etas)
    prev_copy.wait()
    for i in range(n_prev):
        split_columns(i)

    total = jnp.zeros((1, half_y), F32)
    for k in range(n_steps):
        for c in range(comps):
            finish_round(k, c)
            absorb(k, c)
            apply(k, c)
            if k + 1 < n_steps:
                start_round(k + 1, c)
        if k == 0:
            start_eta()
        if k == n_steps - 2:
            for c in range(comps):
                pack_rim(c)
            start_rim()
        if k >= 2:
            take_token(k - 2)
        if k >= 1:
            send_token(k - 1)
        if k == 0:
            for i in range(n_prev + 1):
                total = total + gram_row(i)
        else:
            for c in range(comps):
                to_native(k, c)
            write_out(k)
            total = total + gram_row(n_prev + k)
        if k == n_steps - 2:
            settle(rim_sems.at[1], opposite(eta_sizes))
            tip_eta = jnp.broadcast_to(eta_recv[1, 0:1], (8, half_y))
            for key, i in kinds.items():
                rim_scaled[0, i] = eta_recv[0] * weight(*key)
                rim_scaled[1, i] = tip_eta * weight(*key)
    assert n_steps >= 2
    for j in range(n_steps - 2, len(reaches)):
        take_token(j)
        send_token(j + 1)
    for c in range(comps):
        own_planes(c)
        to_native(n_steps, c)
    acc = gram_zero(n_vec - 1)
    for c in range(comps):
        acc = lax.fori_loop(
            8 * c + 1,
            8 * c + 8,
            lambda t, acc: gram_add(
                n_vec - 1, acc, pl.ds(pl.multiple_of(8 * t, 8), 8), jnp.logical_not(corner0)
            ),
            acc,
            unroll=7,
        )
    settle(rim_sems.at[0], opposite(rim_sizes))
    add_rim()
    for c in range(comps):
        to_native(n_steps, c, rim=True)
    for c in range(comps):
        acc = gram_add(n_vec - 1, acc, pl.ds(c * 64, 8), None)
        acc = gram_add(n_vec - 1, acc, pl.ds(c * 64, 8, stride=8), jnp.logical_not(corner0))
    total = total + gram_close(n_vec - 1, acc)
    gram_send[...] = total

    def scatter(slot, device):
        pltpu.make_async_remote_copy(
            src_ref=gram_send,
            dst_ref=gram_recv.at[slot],
            send_sem=gram_sems.at[0],
            recv_sem=gram_sems.at[1],
            device_id=device,
            device_id_type=MESH,
        ).start()

    each_other(scatter)
    write_out(n_steps)
    sent = [size for step in range(n_steps) for size in round_sizes(step)] * comps
    settle(send_sem.at[0], sent + rim_sizes + eta_sizes)
    for i in range(2):
        pltpu.make_async_copy(gram_recv, gram_recv, gram_sems.at[i]).wait()
    full = (total + jnp.sum(gram_recv[...], axis=0)) * (1.0 / (rows * 2 * half_y * n_dev))
    for i in range(n_vec):
        line = full if i == 0 else pltpu.roll(full, half_y - i * n_vec, 1)
        gram_ref[i : i + 1, :] = line[:, :n_vec]


def store(vec_ref, gram_ref, vec_out, gram_out, sems):
    copies = [
        pltpu.make_async_copy(vec_ref, vec_out, sems.at[0]),
        pltpu.make_async_copy(gram_ref, gram_out, sems.at[1]),
    ]
    for copy in copies:
        copy.start()
    for copy in copies:
        copy.wait()


def on_device(residual, prev_basis, layer_ids, viscosity, shifts):
    n_lat = lax.axis_size("lat")
    n_rad = lax.axis_size("rad")
    comps, node_r, node_x, node_y = residual.shape
    n_prev = prev_basis.shape[0]
    n_steps = shifts.shape[0]
    n_vec = n_prev + n_steps + 1
    rows = comps * node_r * node_x
    half_y = node_y // 2
    assert node_r == 8 and node_x == 8 and half_y == 128
    rounds = n_steps
    tile = (8, half_y)
    vmem = pltpu.VMEM
    hbm_spec = pl.BlockSpec(memory_space=pltpu.HBM)
    vmem_spec = pl.BlockSpec(memory_space=pltpu.VMEM)
    out, gram = pl.pallas_call(
        functools.partial(kernel, n_lat, n_rad, n_steps, n_prev, comps),
        out_shape=(
            pltpu.VMEM((n_steps, rows, node_y), F32),
            pltpu.VMEM((n_vec, n_vec), F32),
        ),
        in_specs=[hbm_spec] * 5,
        out_specs=(vmem_spec, vmem_spec),
        scratch_shapes=[
            vmem((n_prev + 1, rows, node_y), F32),
            vmem(layer_ids.shape, jnp.int32),
            pltpu.SMEM(viscosity.shape, F32),
            pltpu.SMEM(shifts.shape, F32),
            vmem((n_vec, 2, rows, half_y), F32),
            vmem((2, comps, 4, 2, 2) + tile, F32),
            vmem((2, comps, 2, 2) + tile, F32),
            vmem((2, comps, 4, 2) + tile, F32),
            vmem((2, comps, 2) + tile, F32),
            vmem((2, 9) + tile, F32),
            vmem((rounds, comps, 2, 18, half_y), F32),
            vmem((rounds, comps, 2, 18, half_y), F32),
            vmem((rounds, comps, 4, 2, half_y), F32),
            vmem((rounds, comps, 2, 18, half_y), F32),
            vmem((rounds, comps, 2, 18, half_y), F32),
            vmem((rounds, comps, 4, 2, half_y), F32),
            vmem((1, half_y), F32),
            vmem((n_lat * n_rad - 1, 1, half_y), F32),
            vmem((rounds * comps * 80 + 128 * comps, half_y), F32),
            vmem((comps, 40) + tile, F32),
            vmem((comps, 20) + tile, F32),
            vmem((8,) + tile, F32),
            vmem((8,) + tile, F32),
            vmem((2,) + tile, F32),
            vmem((2,) + tile, F32),
            vmem((2, 9) + tile, F32),
            vmem((comps, 6) + tile, F32),
            pltpu.SemaphoreType.DMA((5,)),
            pltpu.SemaphoreType.DMA((1,)),
            pltpu.SemaphoreType.DMA((2, comps)),
            pltpu.SemaphoreType.DMA((2,)),
            pltpu.SemaphoreType.DMA((2,)),
            pltpu.SemaphoreType.REGULAR((max(n_lat, n_rad).bit_length(),)),
        ],
        compiler_params=pltpu.CompilerParams(
            collective_id=0, has_side_effects=True, vmem_limit_bytes=65000000
        ),
    )(
        residual.reshape(rows, node_y),
        prev_basis.reshape(n_prev, rows, node_y),
        layer_ids,
        viscosity,
        shifts,
    )
    out, gram = pl.pallas_call(
        store,
        out_shape=(
            jax.ShapeDtypeStruct(out.shape, F32),
            jax.ShapeDtypeStruct(gram.shape, F32),
        ),
        in_specs=[vmem_spec] * 2,
        out_specs=(hbm_spec, hbm_spec),
        scratch_shapes=[pltpu.SemaphoreType.DMA((2,))],
    )(*(pltpu.with_memory_space_constraint(a, pltpu.VMEM) for a in (out, gram)))
    return out.reshape((n_steps,) + residual.shape), gram


def solution(mesh):
    placed = (
        P(None, "rad", "lat", None),
        P(None, None, "rad", "lat", None),
        P("rad", "lat", None),
        P(),
        P(),
    )
    return jax.shard_map(
        on_device,
        mesh=mesh,
        in_specs=placed,
        out_specs=(P(None, None, "rad", "lat", None), P()),
        check_vma=False,
    )
```

```python
import functools

import jax
import jax.numpy as jnp
from jax import lax
from jax.experimental import pallas as pl
from jax.experimental.pallas import tpu as pltpu
from jax.sharding import PartitionSpec as P

MESH = pl.DeviceIdType.MESH
F32 = jnp.float32

mass = (1.0 / 36, 1.0 / 12, 1.0 / 45)
stiff = (0.0, 1.0, 4.0 / 3)

DIRS = ((-1, -1), (-1, 0), (-1, 1), (0, -1), (0, 1), (1, -1), (1, 0), (1, 1))
R_DIRS = {(-1, 0): 0, (1, 0): 1}
X_DIRS = {(0, -1): 0, (0, 1): 1}
C_DIRS = {(-1, -1): 0, (-1, 1): 1, (1, -1): 2, (1, 1): 3}
FIRST = ((-1, 0), (0, -1), (-1, -1))
LAST = ((1, 0), (0, 1), (1, 1))
ROWS_X, ROWS_G, ROWS_A, ROWS_C = 0, 8, 12, 16
RIM = (
    ((1, 0), (0, 8), (4, 4), ROWS_X, 0),
    ((0, 1), (8, 8), (4, 4), ROWS_X, 4),
    ((1, 0), (16, 4), (7, 1), ROWS_G, 3),
    ((0, 1), (20, 4), (7, 1), ROWS_G, 7),
    ((1, 1), (24, 4), (7, 1), ROWS_C, 0),
    ((1, 1), (28, 4), (7, 1), ROWS_C, 4),
    ((1, -1), (32, 4), (4, 1), ROWS_A, 3),
    ((-1, 1), (36, 4), (3, 1), ROWS_A, 7),
)


def weight(a, b, c):
    return (
        stiff[a] * mass[b] * mass[c] + mass[a] * stiff[b] * mass[c] + mass[a] * mass[b] * stiff[c]
    )


def forward(u0, u1, u2):
    total = u0 + u2
    twice = u1 + u1
    return total + (twice + twice), u0 - u2, total - twice


def backward(m0, m1, m2):
    both = m0 + m2
    half = m0 + m0 - m2
    return both + m1, half + half, both - m1


def kernel(
    n_lat,
    n_rad,
    n_steps,
    n_prev,
    comps,
    res_ref,
    prev_ref,
    ids_hbm,
    visc_hbm,
    shift_hbm,
    out_ref,
    gram_ref,
    stage,
    ids_ref,
    visc_ref,
    shift_ref,
    work,
    vec,
    ghost_r,
    ghost_x,
    ghost_c,
    scaled,
    send_r,
    send_x,
    send_c,
    recv_r,
    recv_x,
    recv_c,
    gram_send,
    gram_recv,
    bulk,
    rim_send,
    rim_recv,
    block_send,
    block_recv,
    eta_send,
    eta_recv,
    rim_scaled,
    rim_own,
    in_sem,
    send_sem,
    recv_sem,
    rim_sems,
    gram_sems,
    token_sem,
):
    n_dev = n_lat * n_rad
    lat = lax.axis_index("lat")
    rad = lax.axis_index("rad")
    me = lat * n_rad + rad
    rows = res_ref.shape[0]
    half_y = res_ref.shape[1] // 2
    n_vec = n_prev + n_steps + 1

    res_copy = pltpu.make_async_copy(res_ref, stage.at[n_prev], in_sem.at[0])
    res_copy.start()
    prev_copy = pltpu.make_async_copy(prev_ref, stage.at[pl.ds(0, n_prev)], in_sem.at[1])
    small_copies = [
        pltpu.make_async_copy(a, b, in_sem.at[2 + i])
        for i, (a, b) in enumerate(
            ((ids_hbm, ids_ref), (visc_hbm, visc_ref), (shift_hbm, shift_ref))
        )
    ]
    for copy in small_copies:
        copy.start()
    prev_copy.start()

    barrier = pltpu.get_barrier_semaphore()

    def around(far, dirs):
        total = 0
        for dr, dx in dirs:
            if not ((dr and n_rad <= far) or (dx and n_lat <= far)):
                total += jnp.where(within(dr * far, dx * far), 1, 0)
        return total

    def within(dr, dx):
        ok = None
        for pos, step, count in ((rad, dr, n_rad), (lat, dx, n_lat)):
            if step:
                one = (pos >= -step) if step < 0 else (pos < count - step)
                ok = one if ok is None else jnp.logical_and(ok, one)
        return ok

    def signal_around(sem, far, dirs):
        for dr, dx in dirs:
            if (dr and n_rad <= far) or (dx and n_lat <= far):
                continue

            @pl.when(within(dr * far, dx * far))
            def _(dr=dr, dx=dx):
                pl.semaphore_signal(
                    sem,
                    inc=1,
                    device_id={"lat": lat + dx * far, "rad": rad + dr * far},
                    device_id_type=MESH,
                )

    signal_around(barrier, 1, LAST)

    for d in DIRS:
        if d in R_DIRS:
            ref, slot = recv_r, R_DIRS[d]
        elif d in X_DIRS:
            ref, slot = recv_x, X_DIRS[d]
        else:
            ref, slot = recv_c, C_DIRS[d]

        @pl.when(jnp.logical_not(within(-d[0], -d[1])))
        def _(ref=ref, slot=slot):
            ref[:, :, slot] = jnp.zeros(ref.shape[:2] + ref.shape[3:], F32)

    for ref in (rim_recv, block_recv, eta_recv):
        ref[...] = jnp.zeros_like(ref)

    reaches = []
    while (2 << len(reaches)) < max(n_lat, n_rad) - 1:
        reaches.append(2 << len(reaches))

    def send_token(j):
        if j < len(reaches):
            signal_around(token_sem.at[j], reaches[j], DIRS)

    def take_token(j):
        if j < len(reaches):
            pl.semaphore_wait(token_sem.at[j], around(reaches[j], DIRS))

    rad_targets = [lax.rem(rad + d, n_rad) for d in range(n_rad)]

    def each_other(visit):
        def row(i, carry):
            lat_target = lax.rem(lat + n_lat // 2 + i, n_lat)
            for d in range(n_rad):
                ahead = lax.rem(n_lat // 2 + i, n_lat)
                visit(ahead * n_rad + d - 1, {"lat": lat_target, "rad": rad_targets[d]})
            return carry

        lax.fori_loop(0, n_lat // 2, row, 0, unroll=n_lat <= 8)
        lax.fori_loop(n_lat // 2 + 1, n_lat, row, 0, unroll=n_lat <= 8)
        for d in range(1, n_rad):
            visit(d - 1, {"lat": lat, "rad": rad_targets[d]})

    sub = lax.broadcasted_iota(jnp.int32, (8, half_y), 0)
    lane = lax.broadcasted_iota(jnp.int32, (8, half_y), 1)
    upper = sub >= 4
    ex = lax.rem(sub, 4)
    first_x = ex == 0
    last_x = ex == 3
    corner0 = sub == 0
    corner3 = sub == 3
    corner4 = sub == 4
    corner7 = sub == 7
    has_up = rad < n_rad - 1
    has_right = lat < n_lat - 1
    up_f = jnp.where(has_up, 1.0, 0.0).astype(F32)
    right_f = jnp.where(has_right, 1.0, 0.0).astype(F32)
    both_f = up_f * right_f

    def roll_s(v, k):
        return pltpu.roll(v, k % 8, 0)

    def keep(mask, v):
        return jnp.where(mask, v, 0.0)

    src = lax.broadcasted_iota(jnp.int32, (2 * half_y, 2 * half_y), 0)
    dst = lax.broadcasted_iota(jnp.int32, (2 * half_y, 2 * half_y), 1)
    split_perm = jnp.where(
        src == jnp.where(dst < half_y, 2 * dst, 2 * (dst - half_y) + 1), 1.0, 0.0
    ).astype(jnp.bfloat16)
    join_perm = jnp.where(
        dst == jnp.where(src < half_y, 2 * src, 2 * (src - half_y) + 1), 1.0, 0.0
    ).astype(jnp.bfloat16)

    def exact_dot(a, b):
        high = a.astype(jnp.bfloat16)
        rest = a - high.astype(F32)
        mid = rest.astype(jnp.bfloat16)
        low = (rest - mid.astype(F32)).astype(jnp.bfloat16)
        out = [jnp.dot(part, b, preferred_element_type=F32) for part in (high, mid, low)]
        return out[0] + (out[1] + out[2])

    def split_columns(i):
        z = exact_dot(stage[i], split_perm)
        work[i, 0] = z[:, :half_y]
        work[i, 1] = z[:, half_y:]

    def native(c, ro, p, h):
        return pl.ds(c * 64 + (4 * h + ro) * 8 + p, 4, stride=2)

    kinds = {}
    for a in range(3):
        for b in range(3):
            for c in range(3):
                key = tuple(sorted((a, b, c)))
                if key != (0, 0, 0) and key not in kinds:
                    kinds[key] = len(kinds)
    def copy_of(step, c, d):
        if d in R_DIRS:
            a, b = send_r.at[step, c, R_DIRS[d]], recv_r.at[step, c, R_DIRS[d]]
        elif d in X_DIRS:
            a, b = send_x.at[step, c, X_DIRS[d]], recv_x.at[step, c, X_DIRS[d]]
        else:
            a, b = send_c.at[step, c, C_DIRS[d]], recv_c.at[step, c, C_DIRS[d]]
        return pltpu.make_async_remote_copy(
            src_ref=a,
            dst_ref=b,
            send_sem=send_sem.at[0],
            recv_sem=recv_sem.at[step % 2, c],
            device_id={"lat": lat + d[1], "rad": rad + d[0]},
            device_id_type=MESH,
        )

    order = ((-1, -1), (1, 1), (-1, 1), (1, -1), (1, 0), (-1, 0), (0, 1), (0, -1))

    def dirs_of(step):
        wanted = FIRST if step == 0 else DIRS
        return [d for d in order if d in wanted]

    def start_round(step, c):
        for d in dirs_of(step):

            @pl.when(within(*d))
            def _(d=d):
                copy_of(step, c, d).start()

    def places(pos, count):
        out = [(pos == 0, False, True), (pos == count - 1, True, False)]
        if count > 2:
            middle = jnp.logical_and(pos > 0, pos < count - 1)
            out.append((middle, True, True))
        return out if count > 1 else [(pos == 0, False, False)]

    def rows_of(sizes, down, up, left, right):
        have = {-1: {0: True, -1: down, 1: up}, 1: {0: True, -1: left, 1: right}}
        return sum(n for (dr, dx), n in sizes if have[-1][dr] and have[1][dx])

    def settle(sem, sizes):
        groups = {}
        for at_r, down, up in places(rad, n_rad):
            for at_x, left, right in places(lat, n_lat):
                n = rows_of(sizes, down, up, left, right)
                here = jnp.logical_and(at_r, at_x)
                groups[n] = jnp.logical_or(groups[n], here) if n in groups else here
        for n, here in groups.items():
            if n:

                @pl.when(here)
                def _(n=n):
                    pltpu.make_async_copy(bulk.at[pl.ds(0, n)], bulk.at[pl.ds(0, n)], sem).wait()

    def opposite(sizes):
        return [((-dr, -dx), n) for (dr, dx), n in sizes]

    def round_sizes(step):
        return [(d, 2 if d[0] and d[1] else 18) for d in dirs_of(step)]

    rim_sizes = [(d, comps * count * high) for d, (_, count), (_, high), _, _ in RIM]
    rim_sizes.append(((1, 1), comps * 8))
    eta_sizes = [((1, 0), 4), ((0, 1), 4), ((1, 1), 1)]

    def finish_round(step, c):
        settle(recv_sem.at[step % 2, c], opposite(round_sizes(step)))

    def remote(a, b, recv, d):
        @pl.when(within(*d))
        def _():
            pltpu.make_async_remote_copy(
                src_ref=a,
                dst_ref=b,
                send_sem=send_sem.at[0],
                recv_sem=recv,
                device_id={"lat": lat + d[1], "rad": rad + d[0]},
                device_id_type=MESH,
            ).start()

    def start_layers(c):
        for d, (first, count), (row, high), to, to_row in RIM[:2]:
            remote(
                rim_send.at[c, pl.ds(first, count), pl.ds(row, high)],
                rim_recv.at[c, pl.ds(to, count), pl.ds(to_row, high)],
                rim_sems.at[0],
                d,
            )

    def start_rim():
        for d, (first, count), (row, high), to, to_row in RIM[2:]:
            remote(
                rim_send.at[:, pl.ds(first, count), pl.ds(row, high)],
                rim_recv.at[:, pl.ds(to, count), pl.ds(to_row, high)],
                rim_sems.at[0],
                d,
            )
        remote(
            block_send.at[:, pl.ds(0, comps)], block_recv.at[:, pl.ds(0, comps)], rim_sems.at[0], (1, 1)
        )

    def start_eta():
        for d, slot, row, high, to, to_row in (
            ((1, 0), 0, 4, 4, 0, 0),
            ((0, 1), 1, 4, 4, 0, 4),
            ((1, 1), 0, 7, 1, 1, 0),
        ):
            remote(
                eta_send.at[slot, pl.ds(row, high)],
                eta_recv.at[to, pl.ds(to_row, high)],
                rim_sems.at[1],
                d,
            )

    def pack_x(vals, at):
        out = None
        for ro in range(4):
            moved = roll_s(vals[ro], ro - at)
            out = moved if out is None else jnp.where(ex == ro, moved, out)
        return out

    def y_pass(x0, x1, a, b, scale):
        nxt = keep(lane != half_y - 1, pltpu.roll(x0, half_y - 1, 1))
        m = list(forward(x0, x1, nxt))
        for j in range(3):
            key = tuple(sorted((a, b, j)))
            m[j] = m[j] * scale(kinds[key]) if key in kinds else None
        if m[0] is None:
            r0 = m[1] + m[2]
            r1 = -(m[2] + m[2])
            r2 = m[2] - m[1]
        else:
            r0, r1, r2 = backward(*m)
        return r0 + keep(lane != 0, pltpu.roll(r2, 1, 1)), r1

    def to_column(low, high):
        moved = jnp.where(sub == 6, roll_s(low, -1), high)
        return jnp.where(sub == 4, roll_s(low, 1), jnp.where(sub == 5, roll_s(high, 2), moved))

    def apply(k, c):
        s = shift_ref[k]
        cur = k % 2
        new = 1 - cur
        u = {}
        gx = {}
        for q in range(2):
            for ro in range(4):
                gx[ro, q] = ghost_x[cur, c, ro, q]
                for p in range(2):
                    u[ro, p, q] = vec[cur, c, ro, p, q]
            gx[4, q] = jnp.where(upper, ghost_c[cur, c, q], roll_s(gx[0, q], 4))
            for p in range(2):
                u[4, p, q] = jnp.where(upper, ghost_r[cur, c, p, q], roll_s(u[0, p, q], 4))
            for ro in range(5):
                u[ro, 2, q] = jnp.where(last_x, gx[ro, q], roll_s(u[ro, 0, q], -1))
        res = {}
        for e in range(2):
            t = {}
            for p in range(3):
                for q in range(2):
                    t[0, p, q], t[1, p, q], t[2, p, q] = forward(
                        u[2 * e, p, q], u[2 * e + 1, p, q], u[2 * e + 2, p, q]
                    )
            w = {}
            for a in range(3):
                x = {}
                for q in range(2):
                    x[0, q], x[1, q], x[2, q] = forward(t[a, 0, q], t[a, 1, q], t[a, 2, q])
                for b in range(3):
                    x[b, 0], x[b, 1] = y_pass(x[b, 0], x[b, 1], a, b, lambda i: scaled[e, i])
                for q in range(2):
                    w[a, 0, q], w[a, 1, q], w[a, 2, q] = backward(x[0, q], x[1, q], x[2, q])
            for p in range(3):
                for q in range(2):
                    r = backward(w[0, p, q], w[1, p, q], w[2, p, q])
                    for i in range(3):
                        key = (2 * e + i, p, q)
                        res[key] = res[key] + r[i] if key in res else r[i]
        px = {}
        for q in range(2):
            for ro in range(5):
                edge = res[ro, 2, q]
                px[ro, q] = edge
                res[ro, 0, q] = res[ro, 0, q] + keep(ex != 0, roll_s(edge, 1))
            for p in range(2):
                res[0, p, q] = res[0, p, q] + keep(upper, roll_s(res[4, p, q], 4))
            px[0, q] = px[0, q] + keep(upper, roll_s(px[4, q], 4))
        step = k + 1
        last = step == n_steps
        for q in range(2):
            face = slice(8 * q, 8 * q + 8)
            edge = slice(16 + q, 17 + q)
            row = slice(q, q + 1)
            if not last:
                send_r[step, c, 1, face] = jnp.where(upper, res[4, 1, q], roll_s(res[4, 0, q], 4))
                send_r[step, c, 1, edge] = px[4, q][7:8]
                send_x[step, c, 1, face] = pack_x([px[ro, q] for ro in range(4)], 3)
                send_x[step, c, 1, edge] = px[4, q][7:8]
                send_c[step, c, 3, row] = px[4, q][7:8]
                send_r[step, c, 0, face] = jnp.where(upper, roll_s(res[0, 1, q], 4), res[0, 0, q])
                send_r[step, c, 0, edge] = px[0, q][3:4]
                send_x[step, c, 0, face] = pack_x([res[ro, 0, q] for ro in range(4)], 0)
                send_x[step, c, 0, edge] = res[4, 0, q][4:5]
                send_c[step, c, 0, row] = res[0, 0, q][0:1]
                send_c[step, c, 1, row] = px[0, q][3:4]
                send_c[step, c, 2, row] = res[4, 0, q][4:5]
            for ro in range(4):
                for p in range(2):
                    vec[new, c, ro, p, q] = res[ro, p, q] - s * u[ro, p, q]
                if not last:
                    ghost_x[new, c, ro, q] = px[ro, q] - s * gx[ro, q]
            if not last:
                for p in range(2):
                    ghost_r[new, c, p, q] = res[4, p, q] - s * u[4, p, q]
                ghost_c[new, c, q] = px[4, q] - s * gx[4, q]
            if step == n_steps - 1:
                for n in range(2):
                    rim_send[c, 24 + 2 * n + q] = px[2 + n, q]
                    rim_send[c, 28 + 2 * n + q] = res[4, n, q]
                    rim_send[c, 32 + 2 * n + q] = res[2 + n, 0, q]
                    rim_send[c, 36 + 2 * n + q] = res[0, n, q]

    def pack_rim(c):
        new = (n_steps - 1) % 2
        for q in range(2):
            for n in range(2):
                for p in range(2):
                    v = vec[new, c, 2 + n, p, q]
                    rim_send[c, 4 * n + 2 * p + q] = v
                    block_send[4 * n + 2 * p + q, c : c + 1] = v[7:8]
                    rim_send[c, 8 + 4 * n + 2 * p + q] = to_column(
                        vec[new, c, p, n, q], vec[new, c, 2 + p, n, q]
                    )
                rim_send[c, 16 + 2 * n + q] = ghost_x[new, c, 2 + n, q]
                rim_send[c, 20 + 2 * n + q] = ghost_r[new, c, n, q]

    group_last = lax.rem(sub, 4) == 3
    group_first = lax.rem(sub, 4) == 0

    def own_planes(c):
        cur = (n_steps - 1) % 2
        for q in range(2):
            side = jnp.where(corner3, ghost_x[cur, c, 0, q], roll_s(ghost_r[cur, c, 0, q], 3))
            for p in range(2):
                column = to_column(
                    roll_s(vec[cur, c, p, 0, q], 3), roll_s(vec[cur, c, 2 + p, 0, q], 3)
                )
                plane = jnp.where(upper, column, vec[cur, c, 0, p, q])
                rim_own[c, 2 * p + q] = plane
                if p == 0:
                    rim_own[c, 4 + q] = jnp.where(group_last, side, roll_s(plane, -1))

    def rim_elements(u, scale):
        t = {}
        for p in range(3):
            for q in range(2):
                t[0, p, q], t[1, p, q], t[2, p, q] = forward(u[0, p, q], u[1, p, q], u[2, p, q])
        w = {}
        for a in range(3):
            x = {}
            for q in range(2):
                x[0, q], x[1, q], x[2, q] = forward(t[a, 0, q], t[a, 1, q], t[a, 2, q])
            for b in range(3):
                x[b, 0], x[b, 1] = y_pass(x[b, 0], x[b, 1], a, b, scale)
            for q in range(2):
                w[a, 0, q], w[a, 1, q], w[a, 2, q] = backward(x[0, q], x[1, q], x[2, q])
        return {
            (p, q): w[0, p, q] + w[2, p, q] - w[1, p, q] for p in range(3) for q in range(2)
        }

    def add_rim():
        cur = (n_steps - 1) % 2
        new = 1 - cur
        inner = jnp.where(upper, up_f, right_f)
        corner = {}
        sides = {}
        for c in range(comps):
            u = {}
            for q in range(2):
                for n in range(2):
                    for p in range(2):
                        u[n, p, q] = rim_recv[c, ROWS_X + 4 * n + 2 * p + q]
                    u[n, 0, q] = u[n, 0, q] + rim_recv[c, ROWS_C + 2 * n + q]
                    ghost = rim_recv[c, ROWS_G + 2 * n + q] + rim_recv[c, ROWS_A + 2 * n + q]
                    u[n, 2, q] = jnp.where(group_last, ghost * inner, roll_s(u[n, 0, q], -1))
                for p in range(3):
                    u[2, p, q] = rim_own[c, 2 * p + q]
            for q in range(2):
                parts = {(2, 2): roll_s(u[2, 0, q], c)}
                for n in range(2):
                    parts[n, 2] = roll_s(u[n, 0, q], c)
                    parts[2, n] = roll_s(u[n, 0, q], c - 4)
                for key, part in parts.items():
                    part = keep(sub == c, part)
                    key = key + (q,)
                    corner[key] = corner[key] + part if c else part
            sides[c] = rim_elements(u, lambda i: rim_scaled[0, i])
        for q in range(2):
            for n in range(2):
                for p in range(2):
                    corner[n, p, q] = block_recv[4 * n + 2 * p + q]
        tip = rim_elements(corner, lambda i: rim_scaled[1, i])
        for c in range(comps):
            for q in range(2):
                out = [
                    sides[c][0, q] + keep(~group_first, roll_s(sides[c][2, q], 1)),
                    sides[c][1, q],
                ]
                for p in range(2):
                    for e in range(2):
                        ro = 2 * e + p
                        add = keep(corner4, roll_s(out[p], -(2 + e)))
                        add = jnp.where(corner0, roll_s(out[p], -(4 + e)), add)
                        if ro == 0:
                            add = add + keep(~upper, out[0]) + keep(corner0, roll_s(tip[2, q], -c))
                        vec[new, c, ro, 0, q] += add
                vec[new, c, 0, 1, q] += keep(~upper, out[1])

    def absorb(step, c):
        new = step % 2
        first, last = step == 0, False
        for q in range(2):
            face = slice(8 * q, 8 * q + 8)
            line = slice(16 + q, 17 + q)
            row = slice(q, q + 1)

            def spot(ref_row, mask):
                return keep(mask, jnp.broadcast_to(ref_row, (8, half_y)))

            if not first:
                from_low = recv_r[step, c, 1, face]
                from_left = recv_x[step, c, 1, face]
                corner = spot(recv_c[step, c, 3, row], corner0)
                vec[new, c, 0, 0, q] += (
                    keep(~upper, from_low) + keep(first_x, from_left) + corner
                )
                vec[new, c, 0, 1, q] += keep(~upper, roll_s(from_low, 4))
                for ro in range(1, 4):
                    vec[new, c, ro, 0, q] += keep(first_x, roll_s(from_left, -ro))
            if not last:
                from_up = recv_r[step, c, 0, face]
                from_right = recv_x[step, c, 0, face]
                add0 = keep(upper, roll_s(from_up, 4))
                add1 = keep(upper, from_up)
                edge = keep(last_x, roll_s(from_right, 3))
                far = (
                    spot(recv_r[step, c, 0, line], corner7)
                    + spot(recv_x[step, c, 0, line], corner7)
                    + spot(recv_c[step, c, 0, row], corner7)
                )
                if not first:
                    add0 = (
                        add0
                        + spot(recv_x[step, c, 1, line], corner4)
                        + spot(recv_c[step, c, 1, row], corner4)
                    )
                    edge = (
                        edge
                        + spot(recv_r[step, c, 1, line], corner3)
                        + spot(recv_c[step, c, 2, row], corner3)
                    )
                    add0 = add0 + ghost_r[new, c, 0, q]
                    add1 = add1 + ghost_r[new, c, 1, q]
                    edge = edge + ghost_x[new, c, 0, q]
                    far = far + ghost_c[new, c, q]
                ghost_r[new, c, 0, q] = add0 * up_f
                ghost_r[new, c, 1, q] = add1 * up_f
                ghost_x[new, c, 0, q] = edge * right_f
                ghost_c[new, c, q] = far * both_f
                for ro in range(1, 4):
                    edge = keep(last_x, roll_s(from_right, 3 - ro))
                    if not first:
                        edge = edge + ghost_x[new, c, ro, q]
                    ghost_x[new, c, ro, q] = edge * right_f

    def to_native(k, c, rim=False):
        cur = k % 2
        for ro in range(4):
            for p in range(2):
                if rim and ro and p:
                    continue
                for q in range(2):
                    v = vec[cur, c, ro, p, q]
                    for h in range(2):
                        work[n_prev + k, q, native(c, ro, p, h), :] = v[4 * h : 4 * h + 4]

    def write_out(k):
        z = jnp.concatenate([work[n_prev + k, 0], work[n_prev + k, 1]], 1)
        out_ref[k - 1] = exact_dot(z, join_perm)

    lane16 = lax.broadcasted_iota(jnp.int32, (16, half_y), 1)
    row16 = lax.broadcasted_iota(jnp.int32, (16, half_y), 0)

    def gram_part(i, acc, first, count):
        def chunk(t, acc):
            at = pl.ds(pl.multiple_of(8 * t, 8), 8)
            for q in range(2):
                mine = work[i, q, at, :]
                acc = tuple(
                    acc[j] + mine * (mine if j == i else work[j, q, at, :]) for j in range(i + 1)
                )
            return acc

        return lax.fori_loop(first, first + count, chunk, acc, unroll=4)

    def gram_add(i, acc, at, mask):
        for q in range(2):
            mine = work[i, q, at, :]
            mine = mine if mask is None else keep(mask, mine)
            acc = tuple(
                acc[j] + mine * (mine if j == i else work[j, q, at, :]) for j in range(i + 1)
            )
        return acc

    def gram_zero(i):
        return (jnp.zeros((8, half_y), F32),) * (i + 1)

    def gram_close(i, acc):
        sums = [jnp.sum(a, axis=0, keepdims=True) for a in acc]
        sums.append(jnp.zeros((16 - len(sums), half_y), F32))
        total = jnp.sum(jnp.concatenate(sums, 0), axis=1, keepdims=True)
        hit = jnp.logical_or(lane16 == i * n_vec + row16, lane16 == row16 * n_vec + i)
        hit = jnp.logical_and(hit, row16 <= i)
        return jnp.sum(jnp.where(hit, jnp.broadcast_to(total, hit.shape), 0.0), 0, keepdims=True)

    def gram_row(i):
        return gram_close(i, gram_part(i, gram_zero(i), 0, rows // 8))

    res_copy.wait()
    edge_rows = []
    for c in range(comps):
        picked = [2 * x + p for p in range(2) for x in range(4)] + [8 * r for r in range(8)]
        edge_rows += [stage[n_prev, pl.ds(c * 64 + at, 1), :] for at in picked]
    edge = exact_dot(jnp.concatenate(edge_rows, 0), split_perm)
    zero_rows = jnp.zeros((2, half_y), F32)
    for c in range(comps):
        send_r[0, c, 0, 16:18] = zero_rows
        send_x[0, c, 0, 16:18] = zero_rows
        for q in range(2):
            face = slice(8 * q, 8 * q + 8)
            lanes = slice(half_y * q, half_y * (q + 1))
            send_r[0, c, 0, face] = edge[16 * c : 16 * c + 8, lanes]
            send_x[0, c, 0, face] = edge[16 * c + 8 : 16 * c + 16, lanes]
            send_c[0, c, 0, q : q + 1] = edge[16 * c : 16 * c + 1, lanes]

    @pl.when(jnp.logical_or(rad > 0, lat > 0))
    def _():
        pl.semaphore_wait(barrier, around(1, FIRST))

    for c in range(comps):
        start_round(0, c)
    split_columns(n_prev)
    for c in range(comps):
        for ro in range(4):
            for p in range(2):
                for q in range(2):
                    vec[0, c, ro, p, q] = jnp.concatenate(
                        [work[n_prev, q, native(c, ro, p, h), :] for h in range(2)], 0
                    )
    for copy in small_copies:
        copy.wait()
    etas = []
    for e in range(2):
        ids = jnp.concatenate([ids_ref[e], ids_ref[2 + e]], 0)
        eta = jnp.zeros((8, half_y), F32)
        for layer in range(visc_ref.shape[0]):
            eta = eta + jnp.where(ids == layer, visc_ref[layer], 0.0)
        etas.append(eta)
        for key, i in kinds.items():
            scaled[e, i] = eta * weight(*key)
    eta_send[0] = etas[1]
    eta_send[1] = to_column(*etas)
    prev_copy.wait()
    for i in range(n_prev):
        split_columns(i)

    total = jnp.zeros((1, half_y), F32)
    for k in range(n_steps - 1):
        for c in range(comps):
            finish_round(k, c)
            absorb(k, c)
            apply(k, c)
            start_round(k + 1, c)
            if k == n_steps - 2:
                if c:
                    start_layers(c - 1)
                pack_rim(c)
        if k == n_steps - 2:
            start_layers(comps - 1)
            start_rim()
        if k == 0:
            start_eta()
        if k >= 2:
            take_token(k - 2)
        if k >= 1:
            send_token(k - 1)
        if k == 0:
            for i in range(n_prev + 1):
                total = total + gram_row(i)
        else:
            for c in range(comps):
                to_native(k, c)
            write_out(k)
            total = total + gram_row(n_prev + k)
        if k == n_steps - 2:
            settle(rim_sems.at[1], opposite(eta_sizes))
            tip_eta = jnp.broadcast_to(eta_recv[1, 0:1], (8, half_y))
            for key, i in kinds.items():
                rim_scaled[0, i] = eta_recv[0] * weight(*key)
                rim_scaled[1, i] = tip_eta * weight(*key)
    assert n_steps >= 2
    k = n_steps - 1
    per = rows // 8 // comps
    whole = gram_zero(n_vec - 2)
    acc = gram_zero(n_vec - 1)
    for c in range(comps):
        finish_round(k, c)
        absorb(k, c)
        apply(k, c)
        own_planes(c)
        to_native(k, c)
        to_native(n_steps, c)
        whole = gram_part(n_vec - 2, whole, c * per, per)
        acc = lax.fori_loop(
            8 * c + 1,
            8 * c + 8,
            lambda t, acc: gram_add(
                n_vec - 1, acc, pl.ds(pl.multiple_of(8 * t, 8), 8), jnp.logical_not(corner0)
            ),
            acc,
            unroll=7,
        )
    total = total + gram_close(n_vec - 2, whole)
    for j in range(max(k - 2, 0), len(reaches)):
        take_token(j)
        send_token(j + 1)
    settle(rim_sems.at[0], opposite(rim_sizes))
    add_rim()
    for c in range(comps):
        to_native(n_steps, c, rim=True)
    for c in range(comps):
        acc = gram_add(n_vec - 1, acc, pl.ds(c * 64, 8), None)
        acc = gram_add(n_vec - 1, acc, pl.ds(c * 64, 8, stride=8), jnp.logical_not(corner0))
    total = total + gram_close(n_vec - 1, acc)
    gram_send[...] = total

    def scatter(slot, device):
        pltpu.make_async_remote_copy(
            src_ref=gram_send,
            dst_ref=gram_recv.at[slot],
            send_sem=gram_sems.at[0],
            recv_sem=gram_sems.at[1],
            device_id=device,
            device_id_type=MESH,
        ).start()

    each_other(scatter)
    write_out(n_steps - 1)
    write_out(n_steps)
    sent = [size for step in range(n_steps) for size in round_sizes(step)] * comps
    settle(send_sem.at[0], sent + rim_sizes + eta_sizes)
    for i in range(2):
        pltpu.make_async_copy(gram_recv, gram_recv, gram_sems.at[i]).wait()
    full = (total + jnp.sum(gram_recv[...], axis=0)) * (1.0 / (rows * 2 * half_y * n_dev))
    for i in range(n_vec):
        line = full if i == 0 else pltpu.roll(full, half_y - i * n_vec, 1)
        gram_ref[i : i + 1, :] = line[:, :n_vec]


def store(vec_ref, gram_ref, vec_out, gram_out, sems):
    copies = [pltpu.make_async_copy(gram_ref, gram_out, sems.at[0])]
    for i in range(vec_ref.shape[0]):
        copies.append(pltpu.make_async_copy(vec_ref.at[i], vec_out.at[i], sems.at[1 + i]))
    for copy in copies:
        copy.start()
    for copy in copies:
        copy.wait()


def on_device(residual, prev_basis, layer_ids, viscosity, shifts):
    n_lat = lax.axis_size("lat")
    n_rad = lax.axis_size("rad")
    comps, node_r, node_x, node_y = residual.shape
    n_prev = prev_basis.shape[0]
    n_steps = shifts.shape[0]
    n_vec = n_prev + n_steps + 1
    rows = comps * node_r * node_x
    half_y = node_y // 2
    assert node_r == 8 and node_x == 8 and half_y == 128
    rounds = n_steps
    tile = (8, half_y)
    vmem = pltpu.VMEM
    hbm_spec = pl.BlockSpec(memory_space=pltpu.HBM)
    vmem_spec = pl.BlockSpec(memory_space=pltpu.VMEM)
    out, gram = pl.pallas_call(
        functools.partial(kernel, n_lat, n_rad, n_steps, n_prev, comps),
        out_shape=(
            pltpu.VMEM((n_steps, rows, node_y), F32),
            pltpu.VMEM((n_vec, n_vec), F32),
        ),
        in_specs=[hbm_spec] * 5,
        out_specs=(vmem_spec, vmem_spec),
        scratch_shapes=[
            vmem((n_prev + 1, rows, node_y), F32),
            vmem(layer_ids.shape, jnp.int32),
            pltpu.SMEM(viscosity.shape, F32),
            pltpu.SMEM(shifts.shape, F32),
            vmem((n_vec, 2, rows, half_y), F32),
            vmem((2, comps, 4, 2, 2) + tile, F32),
            vmem((2, comps, 2, 2) + tile, F32),
            vmem((2, comps, 4, 2) + tile, F32),
            vmem((2, comps, 2) + tile, F32),
            vmem((2, 9) + tile, F32),
            vmem((rounds, comps, 2, 18, half_y), F32),
            vmem((rounds, comps, 2, 18, half_y), F32),
            vmem((rounds, comps, 4, 2, half_y), F32),
            vmem((rounds, comps, 2, 18, half_y), F32),
            vmem((rounds, comps, 2, 18, half_y), F32),
            vmem((rounds, comps, 4, 2, half_y), F32),
            vmem((1, half_y), F32),
            vmem((n_lat * n_rad - 1, 1, half_y), F32),
            vmem((rounds * comps * 80 + 128 * comps, half_y), F32),
            vmem((comps, 40) + tile, F32),
            vmem((comps, 20) + tile, F32),
            vmem((8,) + tile, F32),
            vmem((8,) + tile, F32),
            vmem((2,) + tile, F32),
            vmem((2,) + tile, F32),
            vmem((2, 9) + tile, F32),
            vmem((comps, 6) + tile, F32),
            pltpu.SemaphoreType.DMA((5,)),
            pltpu.SemaphoreType.DMA((1,)),
            pltpu.SemaphoreType.DMA((2, comps)),
            pltpu.SemaphoreType.DMA((2,)),
            pltpu.SemaphoreType.DMA((2,)),
            pltpu.SemaphoreType.REGULAR((max(n_lat, n_rad).bit_length(),)),
        ],
        compiler_params=pltpu.CompilerParams(
            collective_id=0, has_side_effects=True, vmem_limit_bytes=65000000
        ),
    )(
        residual.reshape(rows, node_y),
        prev_basis.reshape(n_prev, rows, node_y),
        layer_ids,
        viscosity,
        shifts,
    )
    out, gram = pl.pallas_call(
        store,
        out_shape=(
            jax.ShapeDtypeStruct(out.shape, F32),
            jax.ShapeDtypeStruct(gram.shape, F32),
        ),
        in_specs=[vmem_spec] * 2,
        out_specs=(hbm_spec, hbm_spec),
        scratch_shapes=[pltpu.SemaphoreType.DMA((1 + n_steps,))],
    )(*(pltpu.with_memory_space_constraint(a, pltpu.VMEM) for a in (out, gram)))
    return out.reshape((n_steps,) + residual.shape), gram


def solution(mesh):
    placed = (
        P(None, "rad", "lat", None),
        P(None, None, "rad", "lat", None),
        P("rad", "lat", None),
        P(),
        P(),
    )
    return jax.shard_map(
        on_device,
        mesh=mesh,
        in_specs=placed,
        out_specs=(P(None, None, "rad", "lat", None), P()),
        check_vma=False,
    )
```

```python
import functools

import jax
import jax.numpy as jnp
from jax import lax
from jax.experimental import pallas as pl
from jax.experimental.pallas import tpu as pltpu
from jax.sharding import PartitionSpec as P

MESH = pl.DeviceIdType.MESH
F32 = jnp.float32

mass = (1.0 / 36, 1.0 / 12, 1.0 / 45)
stiff = (0.0, 1.0, 4.0 / 3)

DIRS = ((-1, -1), (-1, 0), (-1, 1), (0, -1), (0, 1), (1, -1), (1, 0), (1, 1))
R_DIRS = {(-1, 0): 0, (1, 0): 1}
X_DIRS = {(0, -1): 0, (0, 1): 1}
C_DIRS = {(-1, -1): 0, (-1, 1): 1, (1, -1): 2, (1, 1): 3}
FIRST = ((-1, 0), (0, -1), (-1, -1))
LAST = ((1, 0), (0, 1), (1, 1))
ROWS_X, ROWS_G, ROWS_A, ROWS_C = 0, 8, 12, 16
RIM = (
    ((1, 0), (0, 8), (4, 4), ROWS_X, 0),
    ((0, 1), (8, 8), (4, 4), ROWS_X, 4),
    ((1, 0), (16, 4), (7, 1), ROWS_G, 3),
    ((0, 1), (20, 4), (7, 1), ROWS_G, 7),
    ((1, 1), (24, 4), (7, 1), ROWS_C, 0),
    ((1, 1), (28, 4), (7, 1), ROWS_C, 4),
    ((1, -1), (32, 4), (4, 1), ROWS_A, 3),
    ((-1, 1), (36, 4), (3, 1), ROWS_A, 7),
)
EDGE_T, EDGE_U, EDGE_H, EDGE_G = 0, 4, 8, 20
EDGES = (
    ((-1, -1), (8, 6), EDGE_H, 0),
    ((-1, -1), (14, 6), EDGE_H, 4),
    ((-1, 0), (8, 6), EDGE_H + 6, 0),
    ((0, -1), (14, 6), EDGE_H + 6, 4),
    ((1, 0), (0, 4), EDGE_T, 0),
    ((0, 1), (4, 4), EDGE_U, 0),
    ((1, -1), (0, 4), EDGE_G, 0),
    ((-1, 1), (4, 4), EDGE_G, 4),
)
ETAS = (
    ((-1, 0), 2, 0, 3, 2, 0),
    ((0, -1), 2, 4, 3, 2, 4),
    ((1, 0), 0, 4, 4, 0, 0),
    ((0, 1), 1, 4, 4, 0, 4),
    ((1, 1), 0, 7, 1, 1, 0),
    ((-1, 1), 2, 0, 3, 3, 0),
    ((1, -1), 2, 4, 3, 3, 4),
)


def weight(a, b, c):
    return (
        stiff[a] * mass[b] * mass[c] + mass[a] * stiff[b] * mass[c] + mass[a] * mass[b] * stiff[c]
    )


def forward(u0, u1, u2):
    total = u0 + u2
    twice = u1 + u1
    return total + (twice + twice), u0 - u2, total - twice


def backward(m0, m1, m2):
    both = m0 + m2
    half = m0 + m0 - m2
    return both + m1, half + half, both - m1


def kernel(
    n_lat,
    n_rad,
    n_steps,
    n_prev,
    comps,
    res_ref,
    prev_ref,
    ids_hbm,
    visc_hbm,
    shift_hbm,
    out_ref,
    gram_ref,
    stage,
    ids_ref,
    visc_ref,
    shift_ref,
    work,
    vec,
    ghost_r,
    ghost_x,
    ghost_c,
    scaled,
    send_r,
    send_x,
    send_c,
    recv_r,
    recv_x,
    recv_c,
    gram_send,
    gram_recv,
    bulk,
    rim_send,
    rim_recv,
    block_send,
    block_recv,
    edge_send,
    edge_recv,
    eta_send,
    eta_recv,
    rim_scaled,
    rim_own,
    in_sem,
    send_sem,
    recv_sem,
    rim_sems,
    gram_sems,
    token_sem,
):
    n_dev = n_lat * n_rad
    lat = lax.axis_index("lat")
    rad = lax.axis_index("rad")
    me = lat * n_rad + rad
    rows = res_ref.shape[0]
    half_y = res_ref.shape[1] // 2
    n_vec = n_prev + n_steps + 1

    res_copy = pltpu.make_async_copy(res_ref, stage.at[n_prev], in_sem.at[0])
    res_copy.start()
    prev_copy = pltpu.make_async_copy(prev_ref, stage.at[pl.ds(0, n_prev)], in_sem.at[1])
    small_copies = [
        pltpu.make_async_copy(a, b, in_sem.at[2 + i])
        for i, (a, b) in enumerate(
            ((ids_hbm, ids_ref), (visc_hbm, visc_ref), (shift_hbm, shift_ref))
        )
    ]
    for copy in small_copies:
        copy.start()
    prev_copy.start()

    barrier = pltpu.get_barrier_semaphore()

    def around(far, dirs):
        total = 0
        for dr, dx in dirs:
            if not ((dr and n_rad <= far) or (dx and n_lat <= far)):
                total += jnp.where(within(dr * far, dx * far), 1, 0)
        return total

    def within(dr, dx):
        ok = None
        for pos, step, count in ((rad, dr, n_rad), (lat, dx, n_lat)):
            if step:
                one = (pos >= -step) if step < 0 else (pos < count - step)
                ok = one if ok is None else jnp.logical_and(ok, one)
        return ok

    def signal_around(sem, far, dirs):
        for dr, dx in dirs:
            if (dr and n_rad <= far) or (dx and n_lat <= far):
                continue

            @pl.when(within(dr * far, dx * far))
            def _(dr=dr, dx=dx):
                pl.semaphore_signal(
                    sem,
                    inc=1,
                    device_id={"lat": lat + dx * far, "rad": rad + dr * far},
                    device_id_type=MESH,
                )

    for ref in (edge_recv, eta_recv):
        ref[...] = jnp.zeros_like(ref)
    signal_around(barrier, 1, LAST)

    for d in DIRS:
        if d in R_DIRS:
            ref, slot = recv_r, R_DIRS[d]
        elif d in X_DIRS:
            ref, slot = recv_x, X_DIRS[d]
        else:
            ref, slot = recv_c, C_DIRS[d]

        @pl.when(jnp.logical_not(within(-d[0], -d[1])))
        def _(ref=ref, slot=slot):
            ref[:, :, slot] = jnp.zeros(ref.shape[:2] + ref.shape[3:], F32)

    for ref in (rim_recv, block_recv):
        ref[...] = jnp.zeros_like(ref)

    for ref in (ghost_r, ghost_x, ghost_c):
        ref[0] = jnp.zeros(ref.shape[1:], F32)

    reaches = []
    while (2 << len(reaches)) < max(n_lat, n_rad) - 1:
        reaches.append(2 << len(reaches))

    def send_token(j):
        if j < len(reaches):
            signal_around(token_sem.at[j], reaches[j], DIRS)

    def take_token(j):
        if j < len(reaches):
            pl.semaphore_wait(token_sem.at[j], around(reaches[j], DIRS))

    rad_targets = [lax.rem(rad + d, n_rad) for d in range(n_rad)]

    def each_other(visit):
        def row(i, carry):
            lat_target = lax.rem(lat + n_lat // 2 + i, n_lat)
            for d in range(n_rad):
                ahead = lax.rem(n_lat // 2 + i, n_lat)
                visit(ahead * n_rad + d - 1, {"lat": lat_target, "rad": rad_targets[d]})
            return carry

        lax.fori_loop(0, n_lat // 2, row, 0, unroll=n_lat <= 8)
        lax.fori_loop(n_lat // 2 + 1, n_lat, row, 0, unroll=n_lat <= 8)
        for d in range(1, n_rad):
            visit(d - 1, {"lat": lat, "rad": rad_targets[d]})

    sub = lax.broadcasted_iota(jnp.int32, (8, half_y), 0)
    lane = lax.broadcasted_iota(jnp.int32, (8, half_y), 1)
    upper = sub >= 4
    ex = lax.rem(sub, 4)
    first_x = ex == 0
    last_x = ex == 3
    corner0 = sub == 0
    corner3 = sub == 3
    corner4 = sub == 4
    corner7 = sub == 7
    has_up = rad < n_rad - 1
    has_right = lat < n_lat - 1
    up_f = jnp.where(has_up, 1.0, 0.0).astype(F32)
    right_f = jnp.where(has_right, 1.0, 0.0).astype(F32)
    both_f = up_f * right_f

    def roll_s(v, k):
        return pltpu.roll(v, k % 8, 0)

    def keep(mask, v):
        return jnp.where(mask, v, 0.0)

    src = lax.broadcasted_iota(jnp.int32, (2 * half_y, 2 * half_y), 0)
    dst = lax.broadcasted_iota(jnp.int32, (2 * half_y, 2 * half_y), 1)
    split_perm = jnp.where(
        src == jnp.where(dst < half_y, 2 * dst, 2 * (dst - half_y) + 1), 1.0, 0.0
    ).astype(jnp.bfloat16)
    join_perm = jnp.where(
        dst == jnp.where(src < half_y, 2 * src, 2 * (src - half_y) + 1), 1.0, 0.0
    ).astype(jnp.bfloat16)

    def exact_dot(a, b):
        high = a.astype(jnp.bfloat16)
        rest = a - high.astype(F32)
        mid = rest.astype(jnp.bfloat16)
        low = (rest - mid.astype(F32)).astype(jnp.bfloat16)
        out = [jnp.dot(part, b, preferred_element_type=F32) for part in (high, mid, low)]
        return out[0] + (out[1] + out[2])

    def split_columns(i):
        z = exact_dot(stage[i], split_perm)
        work[i, 0] = z[:, :half_y]
        work[i, 1] = z[:, half_y:]

    def native(c, ro, p, h):
        return pl.ds(c * 64 + (4 * h + ro) * 8 + p, 4, stride=2)

    kinds = {}
    for a in range(3):
        for b in range(3):
            for c in range(3):
                key = tuple(sorted((a, b, c)))
                if key != (0, 0, 0) and key not in kinds:
                    kinds[key] = len(kinds)
    def copy_of(step, c, d):
        if d in R_DIRS:
            a, b = send_r.at[step, c, R_DIRS[d]], recv_r.at[step, c, R_DIRS[d]]
        elif d in X_DIRS:
            a, b = send_x.at[step, c, X_DIRS[d]], recv_x.at[step, c, X_DIRS[d]]
        else:
            a, b = send_c.at[step, c, C_DIRS[d]], recv_c.at[step, c, C_DIRS[d]]
        return pltpu.make_async_remote_copy(
            src_ref=a,
            dst_ref=b,
            send_sem=send_sem.at[0],
            recv_sem=recv_sem.at[step % 3, c],
            device_id={"lat": lat + d[1], "rad": rad + d[0]},
            device_id_type=MESH,
        )

    order = ((-1, -1), (1, 1), (-1, 1), (1, -1), (1, 0), (-1, 0), (0, 1), (0, -1))

    def dirs_of(step):
        wanted = FIRST if step == 0 else DIRS
        return [d for d in order if d in wanted]

    def start_round(step, c, among=DIRS):
        for d in dirs_of(step):
            if d not in among:
                continue

            @pl.when(within(*d))
            def _(d=d):
                copy_of(step, c, d).start()

    def places(pos, count):
        out = [(pos == 0, False, True), (pos == count - 1, True, False)]
        if count > 2:
            middle = jnp.logical_and(pos > 0, pos < count - 1)
            out.append((middle, True, True))
        return out if count > 1 else [(pos == 0, False, False)]

    def rows_of(sizes, down, up, left, right):
        have = {-1: {0: True, -1: down, 1: up}, 1: {0: True, -1: left, 1: right}}
        return sum(n for (dr, dx), n in sizes if have[-1][dr] and have[1][dx])

    def settle(sem, sizes):
        groups = {}
        for at_r, down, up in places(rad, n_rad):
            for at_x, left, right in places(lat, n_lat):
                n = rows_of(sizes, down, up, left, right)
                here = jnp.logical_and(at_r, at_x)
                groups[n] = jnp.logical_or(groups[n], here) if n in groups else here
        for n, here in groups.items():
            if n:

                @pl.when(here)
                def _(n=n):
                    pltpu.make_async_copy(bulk.at[pl.ds(0, n)], bulk.at[pl.ds(0, n)], sem).wait()

    def opposite(sizes):
        return [((-dr, -dx), n) for (dr, dx), n in sizes]

    def round_sizes(step):
        return [(d, 2 if d[0] and d[1] else 18) for d in dirs_of(step)]

    rim_sizes = [(d, comps * count * high) for d, (_, count), (_, high), _, _ in RIM]
    rim_sizes.append(((1, 1), comps * 8))
    edge_sizes = [(d, comps * count) for d, (_, count), _, _ in EDGES]
    edge_sizes += [(d, high) for d, _, _, high, _, _ in ETAS]

    def finish_round(step, c):
        settle(recv_sem.at[step % 3, c], opposite(round_sizes(step)))

    def remote(a, b, recv, d):
        @pl.when(within(*d))
        def _():
            pltpu.make_async_remote_copy(
                src_ref=a,
                dst_ref=b,
                send_sem=send_sem.at[0],
                recv_sem=recv,
                device_id={"lat": lat + d[1], "rad": rad + d[0]},
                device_id_type=MESH,
            ).start()

    def start_layers(c):
        for d, (first, count), (row, high), to, to_row in RIM[:2]:
            remote(
                rim_send.at[c, pl.ds(first, count), pl.ds(row, high)],
                rim_recv.at[c, pl.ds(to, count), pl.ds(to_row, high)],
                rim_sems.at[0],
                d,
            )

    def start_rim():
        for d, (first, count), (row, high), to, to_row in RIM[2:]:
            remote(
                rim_send.at[:, pl.ds(first, count), pl.ds(row, high)],
                rim_recv.at[:, pl.ds(to, count), pl.ds(to_row, high)],
                rim_sems.at[0],
                d,
            )
        remote(
            block_send.at[:, pl.ds(0, comps)], block_recv.at[:, pl.ds(0, comps)], rim_sems.at[0], (1, 1)
        )

    def start_edges(among):
        for d, (first, count), to, to_row in EDGES:
            if d in among:
                remote(
                    edge_send.at[pl.ds(first, count), pl.ds(0, comps)],
                    edge_recv.at[pl.ds(to, count), pl.ds(to_row, comps)],
                    rim_sems.at[1],
                    d,
                )

    def start_etas(among):
        for d, slot, row, high, to, to_row in ETAS:
            if d in among:
                remote(
                    eta_send.at[slot, pl.ds(row, high)],
                    eta_recv.at[to, pl.ds(to_row, high)],
                    rim_sems.at[1],
                    d,
                )

    def pack_x(vals, at):
        out = None
        for ro in range(4):
            moved = roll_s(vals[ro], ro - at)
            out = moved if out is None else jnp.where(ex == ro, moved, out)
        return out

    def y_pass(x0, x1, a, b, scale):
        nxt = keep(lane != half_y - 1, pltpu.roll(x0, half_y - 1, 1))
        m = list(forward(x0, x1, nxt))
        for j in range(3):
            key = tuple(sorted((a, b, j)))
            m[j] = m[j] * scale(kinds[key]) if key in kinds else None
        if m[0] is None:
            r0 = m[1] + m[2]
            r1 = -(m[2] + m[2])
            r2 = m[2] - m[1]
        else:
            r0, r1, r2 = backward(*m)
        return r0 + keep(lane != 0, pltpu.roll(r2, 1, 1)), r1

    def to_column(low, high):
        moved = jnp.where(sub == 6, roll_s(low, -1), high)
        return jnp.where(sub == 4, roll_s(low, 1), jnp.where(sub == 5, roll_s(high, 2), moved))

    def apply(k, c, send=True, hold=True):
        s = shift_ref[k]
        cur = k % 2
        new = 1 - cur
        u = {}
        gx = {}
        for q in range(2):
            for ro in range(4):
                gx[ro, q] = ghost_x[cur, c, ro, q]
                for p in range(2):
                    u[ro, p, q] = vec[cur, c, ro, p, q]
            gx[4, q] = jnp.where(upper, ghost_c[cur, c, q], roll_s(gx[0, q], 4))
            for p in range(2):
                u[4, p, q] = jnp.where(upper, ghost_r[cur, c, p, q], roll_s(u[0, p, q], 4))
            for ro in range(5):
                u[ro, 2, q] = jnp.where(last_x, gx[ro, q], roll_s(u[ro, 0, q], -1))
        res = {}
        for e in range(2):
            t = {}
            for p in range(3):
                for q in range(2):
                    t[0, p, q], t[1, p, q], t[2, p, q] = forward(
                        u[2 * e, p, q], u[2 * e + 1, p, q], u[2 * e + 2, p, q]
                    )
            w = {}
            for a in range(3):
                x = {}
                for q in range(2):
                    x[0, q], x[1, q], x[2, q] = forward(t[a, 0, q], t[a, 1, q], t[a, 2, q])
                for b in range(3):
                    x[b, 0], x[b, 1] = y_pass(x[b, 0], x[b, 1], a, b, lambda i: scaled[e, i])
                for q in range(2):
                    w[a, 0, q], w[a, 1, q], w[a, 2, q] = backward(x[0, q], x[1, q], x[2, q])
            for p in range(3):
                for q in range(2):
                    r = backward(w[0, p, q], w[1, p, q], w[2, p, q])
                    for i in range(3):
                        key = (2 * e + i, p, q)
                        res[key] = res[key] + r[i] if key in res else r[i]
        px = {}
        for q in range(2):
            for ro in range(5):
                edge = res[ro, 2, q]
                px[ro, q] = edge
                res[ro, 0, q] = res[ro, 0, q] + keep(ex != 0, roll_s(edge, 1))
            for p in range(2):
                res[0, p, q] = res[0, p, q] + keep(upper, roll_s(res[4, p, q], 4))
            px[0, q] = px[0, q] + keep(upper, roll_s(px[4, q], 4))
        step = k + 1
        send = send and step < n_steps
        ghosts = hold and step < n_steps
        for q in range(2):
            face = slice(8 * q, 8 * q + 8)
            edge = slice(16 + q, 17 + q)
            row = slice(q, q + 1)
            if send:
                send_r[step, c, 1, face] = jnp.where(upper, res[4, 1, q], roll_s(res[4, 0, q], 4))
                send_r[step, c, 1, edge] = px[4, q][7:8]
                send_x[step, c, 1, face] = pack_x([px[ro, q] for ro in range(4)], 3)
                send_x[step, c, 1, edge] = px[4, q][7:8]
                send_c[step, c, 3, row] = px[4, q][7:8]
                send_r[step, c, 0, face] = jnp.where(upper, roll_s(res[0, 1, q], 4), res[0, 0, q])
                send_r[step, c, 0, edge] = px[0, q][3:4]
                send_x[step, c, 0, face] = pack_x([res[ro, 0, q] for ro in range(4)], 0)
                send_x[step, c, 0, edge] = res[4, 0, q][4:5]
                send_c[step, c, 0, row] = res[0, 0, q][0:1]
                send_c[step, c, 1, row] = px[0, q][3:4]
                send_c[step, c, 2, row] = res[4, 0, q][4:5]
            for ro in range(4 if hold else 0):
                for p in range(2):
                    vec[new, c, ro, p, q] = res[ro, p, q] - s * u[ro, p, q]
                if ghosts:
                    ghost_x[new, c, ro, q] = px[ro, q] - s * gx[ro, q]
            if ghosts:
                for p in range(2):
                    ghost_r[new, c, p, q] = res[4, p, q] - s * u[4, p, q]
                ghost_c[new, c, q] = px[4, q] - s * gx[4, q]
            if step == n_steps - 1:
                for n in range(2):
                    rim_send[c, 24 + 2 * n + q] = px[2 + n, q]
                    rim_send[c, 28 + 2 * n + q] = res[4, n, q]
                    rim_send[c, 32 + 2 * n + q] = res[2 + n, 0, q]
                    rim_send[c, 36 + 2 * n + q] = res[0, n, q]

    def pack_rim(c):
        new = (n_steps - 1) % 2
        for q in range(2):
            for n in range(2):
                for p in range(2):
                    v = vec[new, c, 2 + n, p, q]
                    rim_send[c, 4 * n + 2 * p + q] = v
                    block_send[4 * n + 2 * p + q, c : c + 1] = v[7:8]
                    rim_send[c, 8 + 4 * n + 2 * p + q] = to_column(
                        vec[new, c, p, n, q], vec[new, c, 2 + p, n, q]
                    )
                rim_send[c, 16 + 2 * n + q] = ghost_x[new, c, 2 + n, q]
                rim_send[c, 20 + 2 * n + q] = ghost_r[new, c, n, q]

    group_last = lax.rem(sub, 4) == 3
    group_first = lax.rem(sub, 4) == 0

    def own_planes(c, cur):
        for q in range(2):
            side = jnp.where(corner3, ghost_x[cur, c, 0, q], roll_s(ghost_r[cur, c, 0, q], 3))
            for p in range(2):
                column = to_column(
                    roll_s(vec[cur, c, p, 0, q], 3), roll_s(vec[cur, c, 2 + p, 0, q], 3)
                )
                plane = jnp.where(upper, column, vec[cur, c, 0, p, q])
                rim_own[c, 2 * p + q] = plane
                if p == 0:
                    rim_own[c, 4 + q] = jnp.where(group_last, side, roll_s(plane, -1))

    def across(u):
        t = {}
        for p in range(3):
            for q in range(2):
                t[0, p, q], t[1, p, q], t[2, p, q] = forward(u[0, p, q], u[1, p, q], u[2, p, q])
        return t

    def rim_elements(t, scale, upper_plane=True, only_end=False):
        w = {}
        for a in range(3):
            x = {}
            for q in range(2):
                if only_end:
                    end = t[a, 2, q]
                    x[0, q], x[1, q], x[2, q] = end, -end, end
                else:
                    x[0, q], x[1, q], x[2, q] = forward(t[a, 0, q], t[a, 1, q], t[a, 2, q])
            for b in range(3):
                x[b, 0], x[b, 1] = y_pass(x[b, 0], x[b, 1], a, b, scale)
            for q in range(2):
                w[a, 0, q], w[a, 1, q], w[a, 2, q] = backward(x[0, q], x[1, q], x[2, q])
        sign = -1.0 if upper_plane else 1.0
        return {
            (p, q): w[0, p, q] + w[2, p, q] + (w[1, p, q] if sign > 0 else -w[1, p, q])
            for p in range(3)
            for q in range(2)
        }

    def add_planes(new, c, side, tip):
        for q in range(2):
            out = [side[0, q] + keep(~group_first, roll_s(side[2, q], 1)), side[1, q]]
            for p in range(2):
                for e in range(2):
                    ro = 2 * e + p
                    add = keep(corner4, roll_s(out[p], -(2 + e)))
                    add = jnp.where(corner0, roll_s(out[p], -(4 + e)), add)
                    if ro == 0:
                        add = add + keep(~upper, out[0]) + keep(corner0, roll_s(tip[2, q], -c))
                    vec[new, c, ro, 0, q] += add
            vec[new, c, 0, 1, q] += keep(~upper, out[1])

    def add_first():
        sides = {}
        corner = {}
        zero = jnp.zeros((8, half_y), F32)
        for c in range(comps):
            own_planes(c, 0)
            t = {}
            for q in range(2):
                u = [keep(group_last, roll_s(edge_recv[EDGE_G + 2 * n + q], 3 - c)) for n in range(2)]
                for p in range(2):
                    plane = rim_own[c, 2 * p + q]
                    t[0, p, q], t[1, p, q], t[2, p, q] = plane, -plane, plane
                    if p == 0:
                        part = keep(sub == c, roll_s(plane, c))
                        corner[2, 2, q] = corner[2, 2, q] + part if c else part
                t[0, 2, q], t[1, 2, q], t[2, 2, q] = forward(u[0], u[1], rim_own[c, 4 + q])
            sides[c] = rim_elements(t, lambda i: rim_scaled[0, i])
        for q in range(2):
            for n in range(2):
                corner[n, 2, q] = edge_recv[EDGE_T + 2 * n + q]
                corner[2, n, q] = edge_recv[EDGE_U + 2 * n + q]
                for p in range(2):
                    corner[n, p, q] = zero
        tip = rim_elements(across(corner), lambda i: rim_scaled[1, i])
        high = []
        for g in range(2):
            t = {}
            for q in range(2):
                t[0, 2, q], t[1, 2, q], t[2, 2, q] = forward(
                    *(edge_recv[EDGE_H + 6 * g + 2 * n + q] for n in range(3))
                )
            high.append(rim_elements(t, lambda i, g=g: rim_scaled[2 + g, i], False, True))
        for c in range(comps):
            add_planes(1, c, sides[c], tip)
            for q in range(2):
                far = sides[c][2, q]
                ghost_x[1, c, 0, q] += keep(corner3, far + roll_s(high[1][2, q], -1 - c))
                ghost_r[1, c, 0, q] += (
                    keep(corner4, roll_s(far, -3) + roll_s(high[1][2, q], 4 - c))
                    + keep(corner7, roll_s(high[0][0, q], 7 - c))
                )
                ghost_r[1, c, 1, q] += keep(corner7, roll_s(high[0][1, q], 7 - c))
                for t in range(2):
                    ghost_x[1, c, 2 + t, q] += keep(corner7, roll_s(high[0][t, q], 3 - c))
                ghost_c[1, c, q] += keep(
                    corner7, roll_s(high[0][2, q], 7 - c) + roll_s(high[0][2, q], 3 - c)
                )

    def add_rim():
        cur = (n_steps - 1) % 2
        new = 1 - cur
        inner = jnp.where(upper, up_f, right_f)
        corner = {}
        sides = {}
        for c in range(comps):
            u = {}
            for q in range(2):
                for n in range(2):
                    for p in range(2):
                        u[n, p, q] = rim_recv[c, ROWS_X + 4 * n + 2 * p + q]
                    u[n, 0, q] = u[n, 0, q] + rim_recv[c, ROWS_C + 2 * n + q]
                    ghost = rim_recv[c, ROWS_G + 2 * n + q] + rim_recv[c, ROWS_A + 2 * n + q]
                    u[n, 2, q] = jnp.where(group_last, ghost * inner, roll_s(u[n, 0, q], -1))
                for p in range(3):
                    u[2, p, q] = rim_own[c, 2 * p + q]
            for q in range(2):
                parts = {(2, 2): roll_s(u[2, 0, q], c)}
                for n in range(2):
                    parts[n, 2] = roll_s(u[n, 0, q], c)
                    parts[2, n] = roll_s(u[n, 0, q], c - 4)
                for key, part in parts.items():
                    part = keep(sub == c, part)
                    key = key + (q,)
                    corner[key] = corner[key] + part if c else part
            sides[c] = rim_elements(across(u), lambda i: rim_scaled[0, i])
        for q in range(2):
            for n in range(2):
                for p in range(2):
                    corner[n, p, q] = block_recv[4 * n + 2 * p + q]
        tip = rim_elements(across(corner), lambda i: rim_scaled[1, i])
        for c in range(comps):
            add_planes(new, c, sides[c], tip)

    def absorb(step, c):
        new = step % 2
        first, last = step == 0, False
        for q in range(2):
            face = slice(8 * q, 8 * q + 8)
            line = slice(16 + q, 17 + q)
            row = slice(q, q + 1)

            def spot(ref_row, mask):
                return keep(mask, jnp.broadcast_to(ref_row, (8, half_y)))

            if not first:
                from_low = recv_r[step, c, 1, face]
                from_left = recv_x[step, c, 1, face]
                corner = spot(recv_c[step, c, 3, row], corner0)
                vec[new, c, 0, 0, q] += (
                    keep(~upper, from_low) + keep(first_x, from_left) + corner
                )
                vec[new, c, 0, 1, q] += keep(~upper, roll_s(from_low, 4))
                for ro in range(1, 4):
                    vec[new, c, ro, 0, q] += keep(first_x, roll_s(from_left, -ro))
            if not last:
                from_up = recv_r[step, c, 0, face]
                from_right = recv_x[step, c, 0, face]
                add0 = keep(upper, roll_s(from_up, 4))
                add1 = keep(upper, from_up)
                edge = keep(last_x, roll_s(from_right, 3))
                far = (
                    spot(recv_r[step, c, 0, line], corner7)
                    + spot(recv_x[step, c, 0, line], corner7)
                    + spot(recv_c[step, c, 0, row], corner7)
                )
                if not first:
                    add0 = (
                        add0
                        + spot(recv_x[step, c, 1, line], corner4)
                        + spot(recv_c[step, c, 1, row], corner4)
                    )
                    edge = (
                        edge
                        + spot(recv_r[step, c, 1, line], corner3)
                        + spot(recv_c[step, c, 2, row], corner3)
                    )
                    add0 = add0 + ghost_r[new, c, 0, q]
                    add1 = add1 + ghost_r[new, c, 1, q]
                    edge = edge + ghost_x[new, c, 0, q]
                    far = far + ghost_c[new, c, q]
                ghost_r[new, c, 0, q] = add0 * up_f
                ghost_r[new, c, 1, q] = add1 * up_f
                ghost_x[new, c, 0, q] = edge * right_f
                ghost_c[new, c, q] = far * both_f
                for ro in range(1, 4):
                    edge = keep(last_x, roll_s(from_right, 3 - ro))
                    if not first:
                        edge = edge + ghost_x[new, c, ro, q]
                    ghost_x[new, c, ro, q] = edge * right_f

    def to_native(k, c, rim=False):
        cur = k % 2
        for ro in range(4):
            for p in range(2):
                if rim and ro and p:
                    continue
                for q in range(2):
                    v = vec[cur, c, ro, p, q]
                    for h in range(2):
                        work[n_prev + k, q, native(c, ro, p, h), :] = v[4 * h : 4 * h + 4]

    def write_out(k):
        z = jnp.concatenate([work[n_prev + k, 0], work[n_prev + k, 1]], 1)
        out_ref[k - 1] = exact_dot(z, join_perm)

    lane16 = lax.broadcasted_iota(jnp.int32, (16, half_y), 1)
    row16 = lax.broadcasted_iota(jnp.int32, (16, half_y), 0)

    def gram_part(i, acc, first, count):
        def chunk(t, acc):
            at = pl.ds(pl.multiple_of(8 * t, 8), 8)
            for q in range(2):
                mine = work[i, q, at, :]
                acc = tuple(
                    acc[j] + mine * (mine if j == i else work[j, q, at, :]) for j in range(i + 1)
                )
            return acc

        return lax.fori_loop(first, first + count, chunk, acc, unroll=4)

    def gram_add(i, acc, at, mask):
        for q in range(2):
            mine = work[i, q, at, :]
            mine = mine if mask is None else keep(mask, mine)
            acc = tuple(
                acc[j] + mine * (mine if j == i else work[j, q, at, :]) for j in range(i + 1)
            )
        return acc

    def gram_zero(i):
        return (jnp.zeros((8, half_y), F32),) * (i + 1)

    def gram_close(i, acc):
        sums = [jnp.sum(a, axis=0, keepdims=True) for a in acc]
        sums.append(jnp.zeros((16 - len(sums), half_y), F32))
        total = jnp.sum(jnp.concatenate(sums, 0), axis=1, keepdims=True)
        hit = jnp.logical_or(lane16 == i * n_vec + row16, lane16 == row16 * n_vec + i)
        hit = jnp.logical_and(hit, row16 <= i)
        return jnp.sum(jnp.where(hit, jnp.broadcast_to(total, hit.shape), 0.0), 0, keepdims=True)

    def gram_row(i):
        return gram_close(i, gram_part(i, gram_zero(i), 0, rows // 8))

    res_copy.wait()
    edge_rows = []
    for c in range(comps):
        picked = [2 * x + p for p in range(2) for x in range(4)] + [8 * r for r in range(8)]
        edge_rows += [stage[n_prev, pl.ds(c * 64 + at, 1), :] for at in picked]
    edge = exact_dot(jnp.concatenate(edge_rows, 0), split_perm)
    zero_rows = jnp.zeros((2, half_y), F32)
    for c in range(comps):
        send_r[0, c, 0, 16:18] = zero_rows
        send_x[0, c, 0, 16:18] = zero_rows
        for q in range(2):
            face = slice(8 * q, 8 * q + 8)
            lanes = slice(half_y * q, half_y * (q + 1))
            send_r[0, c, 0, face] = edge[16 * c : 16 * c + 8, lanes]
            send_x[0, c, 0, face] = edge[16 * c + 8 : 16 * c + 16, lanes]
            send_c[0, c, 0, q : q + 1] = edge[16 * c : 16 * c + 1, lanes]
            along = [8 + 6, 8 + 7, 3, 7, 8, 9, 10, 0, 4, 1]
            for slot, row in enumerate(along):
                at = 16 * c + row
                edge_send[2 * slot + q, c : c + 1] = edge[at : at + 1, lanes]

    hello = token_sem.at[token_sem.shape[0] - 1]
    others = tuple(d for d in DIRS if d not in FIRST)

    @pl.when(jnp.logical_or(rad > 0, lat > 0))
    def _():
        pl.semaphore_wait(barrier, around(1, FIRST))

    signal_around(hello, 1, FIRST)
    for c in range(comps):
        start_round(0, c)
    start_edges(FIRST)
    split_columns(n_prev)
    for c in range(comps):
        for ro in range(4):
            for p in range(2):
                for q in range(2):
                    vec[0, c, ro, p, q] = jnp.concatenate(
                        [work[n_prev, q, native(c, ro, p, h), :] for h in range(2)], 0
                    )
    for copy in small_copies:
        copy.wait()
    etas = []
    for e in range(2):
        ids = jnp.concatenate([ids_ref[e], ids_ref[2 + e]], 0)
        eta = jnp.zeros((8, half_y), F32)
        for layer in range(visc_ref.shape[0]):
            eta = eta + jnp.where(ids == layer, visc_ref[layer], 0.0)
        etas.append(eta)
        for key, i in kinds.items():
            scaled[e, i] = eta * weight(*key)
    eta_send[0] = etas[1]
    eta_send[1] = to_column(*etas)
    eta_send[2] = jnp.where(
        upper,
        jnp.broadcast_to(etas[1][4:5], (8, half_y)),
        jnp.broadcast_to(etas[0][3:4], (8, half_y)),
    )
    start_etas(FIRST)
    for c in range(comps):
        apply(0, c, hold=False)
        if c < comps - 1:
            start_round(1, c, FIRST)

    @pl.when(jnp.logical_or(rad < n_rad - 1, lat < n_lat - 1))
    def _():
        pl.semaphore_wait(hello, around(1, LAST))

    for c in range(comps):
        start_round(1, c, others if c < comps - 1 else DIRS)
    start_edges(others)
    start_etas(others)

    total = jnp.zeros((1, half_y), F32)
    prev_copy.wait()
    for i in range(n_prev):
        split_columns(i)
    for i in range(n_prev + 1):
        total = total + gram_row(i)

    for c in range(comps):
        finish_round(0, c)
        absorb(0, c)
        apply(0, c, send=False)
    settle(rim_sems.at[1], opposite(edge_sizes))
    tip_eta = jnp.broadcast_to(eta_recv[1, 0:1], (8, half_y))
    for key, i in kinds.items():
        for slot in range(4):
            rim_scaled[slot, i] = (tip_eta if slot == 1 else eta_recv[slot]) * weight(*key)
    add_first()
    for k in range(1, n_steps - 1):
        for c in range(comps):
            finish_round(k, c)
            absorb(k, c)
            apply(k, c)
            start_round(k + 1, c)
            if k == n_steps - 2:
                if c:
                    start_layers(c - 1)
                pack_rim(c)
        if k == n_steps - 2:
            start_layers(comps - 1)
            start_rim()
        if k >= 2:
            take_token(k - 2)
        send_token(k - 1)
        for c in range(comps):
            to_native(k, c)
        write_out(k)
        total = total + gram_row(n_prev + k)
    assert n_steps >= 3
    k = n_steps - 1
    per = rows // 8 // comps
    whole = gram_zero(n_vec - 2)
    acc = gram_zero(n_vec - 1)
    for c in range(comps):
        finish_round(k, c)
        absorb(k, c)
        apply(k, c)
        own_planes(c, k % 2)
        to_native(k, c)
        to_native(n_steps, c)
        whole = gram_part(n_vec - 2, whole, c * per, per)
        acc = lax.fori_loop(
            8 * c + 1,
            8 * c + 8,
            lambda t, acc: gram_add(
                n_vec - 1, acc, pl.ds(pl.multiple_of(8 * t, 8), 8), jnp.logical_not(corner0)
            ),
            acc,
            unroll=7,
        )
    total = total + gram_close(n_vec - 2, whole)
    for j in range(max(k - 2, 0), len(reaches)):
        take_token(j)
        send_token(j + 1)
    settle(rim_sems.at[0], opposite(rim_sizes))
    add_rim()
    for c in range(comps):
        to_native(n_steps, c, rim=True)
    for c in range(comps):
        acc = gram_add(n_vec - 1, acc, pl.ds(c * 64, 8), None)
        acc = gram_add(n_vec - 1, acc, pl.ds(c * 64, 8, stride=8), jnp.logical_not(corner0))
    total = total + gram_close(n_vec - 1, acc)
    gram_send[...] = total

    def scatter(slot, device):
        pltpu.make_async_remote_copy(
            src_ref=gram_send,
            dst_ref=gram_recv.at[slot],
            send_sem=gram_sems.at[0],
            recv_sem=gram_sems.at[1],
            device_id=device,
            device_id_type=MESH,
        ).start()

    each_other(scatter)
    write_out(n_steps - 1)
    write_out(n_steps)
    sent = [size for step in range(n_steps) for size in round_sizes(step)] * comps
    settle(send_sem.at[0], sent + rim_sizes + edge_sizes)
    for i in range(2):
        pltpu.make_async_copy(gram_recv, gram_recv, gram_sems.at[i]).wait()
    full = (total + jnp.sum(gram_recv[...], axis=0)) * (1.0 / (rows * 2 * half_y * n_dev))
    for i in range(n_vec):
        line = full if i == 0 else pltpu.roll(full, half_y - i * n_vec, 1)
        gram_ref[i : i + 1, :] = line[:, :n_vec]


def store(vec_ref, gram_ref, vec_out, gram_out, sems):
    copies = [pltpu.make_async_copy(gram_ref, gram_out, sems.at[0])]
    for i in range(vec_ref.shape[0]):
        copies.append(pltpu.make_async_copy(vec_ref.at[i], vec_out.at[i], sems.at[1 + i]))
    for copy in copies:
        copy.start()
    for copy in copies:
        copy.wait()


def on_device(residual, prev_basis, layer_ids, viscosity, shifts):
    n_lat = lax.axis_size("lat")
    n_rad = lax.axis_size("rad")
    comps, node_r, node_x, node_y = residual.shape
    n_prev = prev_basis.shape[0]
    n_steps = shifts.shape[0]
    n_vec = n_prev + n_steps + 1
    rows = comps * node_r * node_x
    half_y = node_y // 2
    assert node_r == 8 and node_x == 8 and half_y == 128
    rounds = n_steps
    tile = (8, half_y)
    vmem = pltpu.VMEM
    hbm_spec = pl.BlockSpec(memory_space=pltpu.HBM)
    vmem_spec = pl.BlockSpec(memory_space=pltpu.VMEM)
    out, gram = pl.pallas_call(
        functools.partial(kernel, n_lat, n_rad, n_steps, n_prev, comps),
        out_shape=(
            pltpu.VMEM((n_steps, rows, node_y), F32),
            pltpu.VMEM((n_vec, n_vec), F32),
        ),
        in_specs=[hbm_spec] * 5,
        out_specs=(vmem_spec, vmem_spec),
        scratch_shapes=[
            vmem((n_prev + 1, rows, node_y), F32),
            vmem(layer_ids.shape, jnp.int32),
            pltpu.SMEM(viscosity.shape, F32),
            pltpu.SMEM(shifts.shape, F32),
            vmem((n_vec, 2, rows, half_y), F32),
            vmem((2, comps, 4, 2, 2) + tile, F32),
            vmem((2, comps, 2, 2) + tile, F32),
            vmem((2, comps, 4, 2) + tile, F32),
            vmem((2, comps, 2) + tile, F32),
            vmem((2, 9) + tile, F32),
            vmem((rounds, comps, 2, 18, half_y), F32),
            vmem((rounds, comps, 2, 18, half_y), F32),
            vmem((rounds, comps, 4, 2, half_y), F32),
            vmem((rounds, comps, 2, 18, half_y), F32),
            vmem((rounds, comps, 2, 18, half_y), F32),
            vmem((rounds, comps, 4, 2, half_y), F32),
            vmem((1, half_y), F32),
            vmem((n_lat * n_rad - 1, 1, half_y), F32),
            vmem((rounds * comps * 80 + 128 * comps, half_y), F32),
            vmem((comps, 40) + tile, F32),
            vmem((comps, 20) + tile, F32),
            vmem((8,) + tile, F32),
            vmem((8,) + tile, F32),
            vmem((20,) + tile, F32),
            vmem((24,) + tile, F32),
            vmem((3,) + tile, F32),
            vmem((4,) + tile, F32),
            vmem((4, 9) + tile, F32),
            vmem((comps, 6) + tile, F32),
            pltpu.SemaphoreType.DMA((5,)),
            pltpu.SemaphoreType.DMA((1,)),
            pltpu.SemaphoreType.DMA((3, comps)),
            pltpu.SemaphoreType.DMA((2,)),
            pltpu.SemaphoreType.DMA((2,)),
            pltpu.SemaphoreType.REGULAR((max(n_lat, n_rad).bit_length(),)),
        ],
        compiler_params=pltpu.CompilerParams(
            collective_id=0, has_side_effects=True, vmem_limit_bytes=65000000
        ),
    )(
        residual.reshape(rows, node_y),
        prev_basis.reshape(n_prev, rows, node_y),
        layer_ids,
        viscosity,
        shifts,
    )
    out, gram = pl.pallas_call(
        store,
        out_shape=(
            jax.ShapeDtypeStruct(out.shape, F32),
            jax.ShapeDtypeStruct(gram.shape, F32),
        ),
        in_specs=[vmem_spec] * 2,
        out_specs=(hbm_spec, hbm_spec),
        scratch_shapes=[pltpu.SemaphoreType.DMA((1 + n_steps,))],
    )(*(pltpu.with_memory_space_constraint(a, pltpu.VMEM) for a in (out, gram)))
    return out.reshape((n_steps,) + residual.shape), gram


def solution(mesh):
    placed = (
        P(None, "rad", "lat", None),
        P(None, None, "rad", "lat", None),
        P("rad", "lat", None),
        P(),
        P(),
    )
    return jax.shard_map(
        on_device,
        mesh=mesh,
        in_specs=placed,
        out_specs=(P(None, None, "rad", "lat", None), P()),
        check_vma=False,
    )
```

```python
import functools

import jax
import jax.numpy as jnp
from jax import lax
from jax.experimental import pallas as pl
from jax.experimental.pallas import tpu as pltpu
from jax.sharding import PartitionSpec as P

MESH = pl.DeviceIdType.MESH
F32 = jnp.float32

mass = (1.0 / 36, 1.0 / 12, 1.0 / 45)
stiff = (0.0, 1.0, 4.0 / 3)

DIRS = ((-1, -1), (-1, 0), (-1, 1), (0, -1), (0, 1), (1, -1), (1, 0), (1, 1))
R_DIRS = {(-1, 0): 0, (1, 0): 1}
X_DIRS = {(0, -1): 0, (0, 1): 1}
C_DIRS = {(-1, -1): 0, (-1, 1): 1, (1, -1): 2, (1, 1): 3}
FIRST = ((-1, 0), (0, -1), (-1, -1))
LAST = ((1, 0), (0, 1), (1, 1))
ROWS_X, ROWS_G, ROWS_A, ROWS_C = 0, 8, 12, 16
RIM = (
    ((1, 0), (0, 8), (4, 4), ROWS_X, 0),
    ((0, 1), (8, 8), (4, 4), ROWS_X, 4),
    ((1, 0), (16, 4), (7, 1), ROWS_G, 3),
    ((0, 1), (20, 4), (7, 1), ROWS_G, 7),
    ((1, 1), (24, 4), (7, 1), ROWS_C, 0),
    ((1, 1), (28, 4), (7, 1), ROWS_C, 4),
    ((1, -1), (32, 4), (4, 1), ROWS_A, 3),
    ((-1, 1), (36, 4), (3, 1), ROWS_A, 7),
)
EDGE_T, EDGE_U, EDGE_H, EDGE_G = 0, 4, 8, 20
EDGES = (
    ((-1, -1), (8, 6), EDGE_H, 0),
    ((-1, -1), (14, 6), EDGE_H, 4),
    ((-1, 0), (8, 6), EDGE_H + 6, 0),
    ((0, -1), (14, 6), EDGE_H + 6, 4),
    ((1, 0), (0, 4), EDGE_T, 0),
    ((0, 1), (4, 4), EDGE_U, 0),
    ((1, -1), (0, 4), EDGE_G, 0),
    ((-1, 1), (4, 4), EDGE_G, 4),
)
ETAS = (
    ((-1, 0), 2, 0, 3, 2, 0),
    ((0, -1), 2, 4, 3, 2, 4),
    ((1, 0), 0, 4, 4, 0, 0),
    ((0, 1), 1, 4, 4, 0, 4),
    ((1, 1), 0, 7, 1, 1, 0),
    ((-1, 1), 2, 0, 3, 3, 0),
    ((1, -1), 2, 4, 3, 3, 4),
)


def weight(a, b, c):
    return (
        stiff[a] * mass[b] * mass[c] + mass[a] * stiff[b] * mass[c] + mass[a] * mass[b] * stiff[c]
    )


def forward(u0, u1, u2):
    total = u0 + u2
    twice = u1 + u1
    return total + (twice + twice), u0 - u2, total - twice


def backward(m0, m1, m2):
    both = m0 + m2
    half = m0 + m0 - m2
    return both + m1, half + half, both - m1


def kernel(
    n_lat,
    n_rad,
    n_steps,
    n_prev,
    comps,
    res_ref,
    prev_ref,
    ids_hbm,
    visc_hbm,
    shift_hbm,
    out_ref,
    gram_ref,
    stage,
    ids_ref,
    visc_ref,
    shift_ref,
    work,
    vec,
    ghost_r,
    ghost_x,
    ghost_c,
    scaled,
    send_r,
    send_x,
    send_c,
    recv_r,
    recv_x,
    recv_c,
    gram_send,
    gram_recv,
    bulk,
    rim_send,
    rim_recv,
    block_send,
    block_recv,
    edge_send,
    edge_recv,
    eta_send,
    eta_recv,
    rim_scaled,
    rim_own,
    in_sem,
    send_sem,
    recv_sem,
    rim_sems,
    gram_sems,
    token_sem,
):
    n_dev = n_lat * n_rad
    lat = lax.axis_index("lat")
    rad = lax.axis_index("rad")
    me = lat * n_rad + rad
    rows = res_ref.shape[0]
    half_y = res_ref.shape[1] // 2
    n_vec = n_prev + n_steps + 1

    res_copy = pltpu.make_async_copy(res_ref, stage.at[n_prev], in_sem.at[0])
    res_copy.start()
    prev_copy = pltpu.make_async_copy(prev_ref, stage.at[pl.ds(0, n_prev)], in_sem.at[1])
    small_copies = [
        pltpu.make_async_copy(a, b, in_sem.at[2 + i])
        for i, (a, b) in enumerate(
            ((ids_hbm, ids_ref), (visc_hbm, visc_ref), (shift_hbm, shift_ref))
        )
    ]
    for copy in small_copies:
        copy.start()
    prev_copy.start()

    barrier = pltpu.get_barrier_semaphore()

    def around(far, dirs):
        total = 0
        for dr, dx in dirs:
            if not ((dr and n_rad <= far) or (dx and n_lat <= far)):
                total += jnp.where(within(dr * far, dx * far), 1, 0)
        return total

    def within(dr, dx):
        ok = None
        for pos, step, count in ((rad, dr, n_rad), (lat, dx, n_lat)):
            if step:
                one = (pos >= -step) if step < 0 else (pos < count - step)
                ok = one if ok is None else jnp.logical_and(ok, one)
        return ok

    def signal_around(sem, far, dirs):
        for dr, dx in dirs:
            if (dr and n_rad <= far) or (dx and n_lat <= far):
                continue

            @pl.when(within(dr * far, dx * far))
            def _(dr=dr, dx=dx):
                pl.semaphore_signal(
                    sem,
                    inc=1,
                    device_id={"lat": lat + dx * far, "rad": rad + dr * far},
                    device_id_type=MESH,
                )

    for ref in (edge_recv, eta_recv):
        ref[...] = jnp.zeros_like(ref)
    signal_around(barrier, 1, LAST)

    for d in DIRS:
        if d in R_DIRS:
            ref, slot = recv_r, R_DIRS[d]
        elif d in X_DIRS:
            ref, slot = recv_x, X_DIRS[d]
        else:
            ref, slot = recv_c, C_DIRS[d]

        @pl.when(jnp.logical_not(within(-d[0], -d[1])))
        def _(ref=ref, slot=slot):
            ref[:, :, slot] = jnp.zeros(ref.shape[:2] + ref.shape[3:], F32)

    for ref in (rim_recv, block_recv):
        ref[...] = jnp.zeros_like(ref)

    for ref in (ghost_r, ghost_x, ghost_c):
        ref[0] = jnp.zeros(ref.shape[1:], F32)

    hello = token_sem.at[token_sem.shape[0] - 1]
    hello_far = token_sem.at[token_sem.shape[0] - 2]

    def answer():
        @pl.when(jnp.logical_or(rad > 0, lat > 0))
        def _():
            pl.semaphore_wait(barrier, around(1, FIRST))

        signal_around(hello, 1, FIRST[:2])
        signal_around(hello_far, 1, FIRST[2:])

    soon = jnp.logical_or(rad == 0, lax.rem(rad, 2) == 1)
    pl.when(soon)(answer)

    reaches = []
    while (2 << len(reaches)) < max(n_lat, n_rad) - 1:
        reaches.append(2 << len(reaches))

    def send_token(j):
        if j < len(reaches):
            signal_around(token_sem.at[j], reaches[j], DIRS)

    def take_token(j):
        if j < len(reaches):
            pl.semaphore_wait(token_sem.at[j], around(reaches[j], DIRS))

    rad_targets = [lax.rem(rad + d, n_rad) for d in range(n_rad)]

    def each_other(visit):
        def row(i, carry):
            lat_target = lax.rem(lat + n_lat // 2 + i, n_lat)
            for d in range(n_rad):
                ahead = lax.rem(n_lat // 2 + i, n_lat)
                visit(ahead * n_rad + d - 1, {"lat": lat_target, "rad": rad_targets[d]})
            return carry

        lax.fori_loop(0, n_lat // 2, row, 0, unroll=n_lat <= 8)
        lax.fori_loop(n_lat // 2 + 1, n_lat, row, 0, unroll=n_lat <= 8)
        for d in range(1, n_rad):
            visit(d - 1, {"lat": lat, "rad": rad_targets[d]})

    sub = lax.broadcasted_iota(jnp.int32, (8, half_y), 0)
    lane = lax.broadcasted_iota(jnp.int32, (8, half_y), 1)
    upper = sub >= 4
    ex = lax.rem(sub, 4)
    first_x = ex == 0
    last_x = ex == 3
    corner0 = sub == 0
    corner3 = sub == 3
    corner4 = sub == 4
    corner7 = sub == 7
    has_up = rad < n_rad - 1
    has_right = lat < n_lat - 1
    up_f = jnp.where(has_up, 1.0, 0.0).astype(F32)
    right_f = jnp.where(has_right, 1.0, 0.0).astype(F32)
    both_f = up_f * right_f

    def roll_s(v, k):
        return pltpu.roll(v, k % 8, 0)

    def keep(mask, v):
        return jnp.where(mask, v, 0.0)

    src = lax.broadcasted_iota(jnp.int32, (2 * half_y, 2 * half_y), 0)
    dst = lax.broadcasted_iota(jnp.int32, (2 * half_y, 2 * half_y), 1)
    split_perm = jnp.where(
        src == jnp.where(dst < half_y, 2 * dst, 2 * (dst - half_y) + 1), 1.0, 0.0
    ).astype(jnp.bfloat16)
    join_perm = jnp.where(
        dst == jnp.where(src < half_y, 2 * src, 2 * (src - half_y) + 1), 1.0, 0.0
    ).astype(jnp.bfloat16)

    def exact_dot(a, b):
        high = a.astype(jnp.bfloat16)
        rest = a - high.astype(F32)
        mid = rest.astype(jnp.bfloat16)
        low = (rest - mid.astype(F32)).astype(jnp.bfloat16)
        out = [jnp.dot(part, b, preferred_element_type=F32) for part in (high, mid, low)]
        return out[0] + (out[1] + out[2])

    def split_columns(i):
        z = exact_dot(stage[i], split_perm)
        work[i, 0] = z[:, :half_y]
        work[i, 1] = z[:, half_y:]

    def native(c, ro, p, h):
        return pl.ds(c * 64 + (4 * h + ro) * 8 + p, 4, stride=2)

    kinds = {}
    for a in range(3):
        for b in range(3):
            for c in range(3):
                key = tuple(sorted((a, b, c)))
                if key != (0, 0, 0) and key not in kinds:
                    kinds[key] = len(kinds)
    def copy_of(step, c, d):
        if d in R_DIRS:
            a, b = send_r.at[step, c, R_DIRS[d]], recv_r.at[step, c, R_DIRS[d]]
        elif d in X_DIRS:
            a, b = send_x.at[step, c, X_DIRS[d]], recv_x.at[step, c, X_DIRS[d]]
        else:
            a, b = send_c.at[step, c, C_DIRS[d]], recv_c.at[step, c, C_DIRS[d]]
        return pltpu.make_async_remote_copy(
            src_ref=a,
            dst_ref=b,
            send_sem=send_sem.at[0],
            recv_sem=recv_sem.at[step % 3, c],
            device_id={"lat": lat + d[1], "rad": rad + d[0]},
            device_id_type=MESH,
        )

    order = ((-1, -1), (1, 1), (-1, 1), (1, -1), (1, 0), (-1, 0), (0, 1), (0, -1))

    def dirs_of(step):
        wanted = FIRST if step == 0 else DIRS
        return [d for d in order if d in wanted]

    def start_round(step, c, among=DIRS):
        for d in dirs_of(step):
            if d not in among:
                continue

            @pl.when(within(*d))
            def _(d=d):
                copy_of(step, c, d).start()

    def places(pos, count):
        out = [(pos == 0, False, True), (pos == count - 1, True, False)]
        if count > 2:
            middle = jnp.logical_and(pos > 0, pos < count - 1)
            out.append((middle, True, True))
        return out if count > 1 else [(pos == 0, False, False)]

    def rows_of(sizes, down, up, left, right):
        have = {-1: {0: True, -1: down, 1: up}, 1: {0: True, -1: left, 1: right}}
        return sum(n for (dr, dx), n in sizes if have[-1][dr] and have[1][dx])

    def settle(sem, sizes):
        groups = {}
        for at_r, down, up in places(rad, n_rad):
            for at_x, left, right in places(lat, n_lat):
                n = rows_of(sizes, down, up, left, right)
                here = jnp.logical_and(at_r, at_x)
                groups[n] = jnp.logical_or(groups[n], here) if n in groups else here
        for n, here in groups.items():
            if n:

                @pl.when(here)
                def _(n=n):
                    pltpu.make_async_copy(bulk.at[pl.ds(0, n)], bulk.at[pl.ds(0, n)], sem).wait()

    def opposite(sizes):
        return [((-dr, -dx), n) for (dr, dx), n in sizes]

    def round_sizes(step):
        return [(d, 2 if d[0] and d[1] else 18) for d in dirs_of(step)]

    rim_sizes = [(d, comps * count * high) for d, (_, count), (_, high), _, _ in RIM]
    rim_sizes.append(((1, 1), comps * 8))
    edge_sizes = [(d, comps * count) for d, (_, count), _, _ in EDGES]
    edge_sizes += [(d, high) for d, _, _, high, _, _ in ETAS]

    def finish_round(step, c):
        settle(recv_sem.at[step % 3, c], opposite(round_sizes(step)))

    def remote(a, b, recv, d):
        @pl.when(within(*d))
        def _():
            pltpu.make_async_remote_copy(
                src_ref=a,
                dst_ref=b,
                send_sem=send_sem.at[0],
                recv_sem=recv,
                device_id={"lat": lat + d[1], "rad": rad + d[0]},
                device_id_type=MESH,
            ).start()

    def start_layers(c):
        for d, (first, count), (row, high), to, to_row in RIM[:2]:
            remote(
                rim_send.at[c, pl.ds(first, count), pl.ds(row, high)],
                rim_recv.at[c, pl.ds(to, count), pl.ds(to_row, high)],
                rim_sems.at[0],
                d,
            )

    def start_rim():
        for d, (first, count), (row, high), to, to_row in RIM[2:]:
            remote(
                rim_send.at[:, pl.ds(first, count), pl.ds(row, high)],
                rim_recv.at[:, pl.ds(to, count), pl.ds(to_row, high)],
                rim_sems.at[0],
                d,
            )
        remote(
            block_send.at[:, pl.ds(0, comps)], block_recv.at[:, pl.ds(0, comps)], rim_sems.at[0], (1, 1)
        )

    def start_edges(among):
        for d, (first, count), to, to_row in EDGES:
            if d in among:
                remote(
                    edge_send.at[pl.ds(first, count), pl.ds(0, comps)],
                    edge_recv.at[pl.ds(to, count), pl.ds(to_row, comps)],
                    rim_sems.at[1],
                    d,
                )

    def start_etas(among):
        for d, slot, row, high, to, to_row in ETAS:
            if d in among:
                remote(
                    eta_send.at[slot, pl.ds(row, high)],
                    eta_recv.at[to, pl.ds(to_row, high)],
                    rim_sems.at[1],
                    d,
                )

    def pack_x(vals, at):
        out = None
        for ro in range(4):
            moved = roll_s(vals[ro], ro - at)
            out = moved if out is None else jnp.where(ex == ro, moved, out)
        return out

    def y_pass(x0, x1, a, b, scale):
        nxt = keep(lane != half_y - 1, pltpu.roll(x0, half_y - 1, 1))
        m = list(forward(x0, x1, nxt))
        for j in range(3):
            key = tuple(sorted((a, b, j)))
            m[j] = m[j] * scale(kinds[key]) if key in kinds else None
        if m[0] is None:
            r0 = m[1] + m[2]
            r1 = -(m[2] + m[2])
            r2 = m[2] - m[1]
        else:
            r0, r1, r2 = backward(*m)
        return r0 + keep(lane != 0, pltpu.roll(r2, 1, 1)), r1

    def to_column(low, high):
        moved = jnp.where(sub == 6, roll_s(low, -1), high)
        return jnp.where(sub == 4, roll_s(low, 1), jnp.where(sub == 5, roll_s(high, 2), moved))

    def apply(k, c, send=True, hold=True):
        s = shift_ref[k]
        cur = k % 2
        new = 1 - cur
        u = {}
        gx = {}
        for q in range(2):
            for ro in range(4):
                gx[ro, q] = ghost_x[cur, c, ro, q]
                for p in range(2):
                    u[ro, p, q] = vec[cur, c, ro, p, q]
            gx[4, q] = jnp.where(upper, ghost_c[cur, c, q], roll_s(gx[0, q], 4))
            for p in range(2):
                u[4, p, q] = jnp.where(upper, ghost_r[cur, c, p, q], roll_s(u[0, p, q], 4))
            for ro in range(5):
                u[ro, 2, q] = jnp.where(last_x, gx[ro, q], roll_s(u[ro, 0, q], -1))
        res = {}
        for e in range(2):
            t = {}
            for p in range(3):
                for q in range(2):
                    t[0, p, q], t[1, p, q], t[2, p, q] = forward(
                        u[2 * e, p, q], u[2 * e + 1, p, q], u[2 * e + 2, p, q]
                    )
            w = {}
            for a in range(3):
                x = {}
                for q in range(2):
                    x[0, q], x[1, q], x[2, q] = forward(t[a, 0, q], t[a, 1, q], t[a, 2, q])
                for b in range(3):
                    x[b, 0], x[b, 1] = y_pass(x[b, 0], x[b, 1], a, b, lambda i: scaled[e, i])
                for q in range(2):
                    w[a, 0, q], w[a, 1, q], w[a, 2, q] = backward(x[0, q], x[1, q], x[2, q])
            for p in range(3):
                for q in range(2):
                    r = backward(w[0, p, q], w[1, p, q], w[2, p, q])
                    for i in range(3):
                        key = (2 * e + i, p, q)
                        res[key] = res[key] + r[i] if key in res else r[i]
        px = {}
        for q in range(2):
            for ro in range(5):
                edge = res[ro, 2, q]
                px[ro, q] = edge
                res[ro, 0, q] = res[ro, 0, q] + keep(ex != 0, roll_s(edge, 1))
            for p in range(2):
                res[0, p, q] = res[0, p, q] + keep(upper, roll_s(res[4, p, q], 4))
            px[0, q] = px[0, q] + keep(upper, roll_s(px[4, q], 4))
        step = k + 1
        send = send and step < n_steps
        ghosts = hold and step < n_steps
        for q in range(2):
            face = slice(8 * q, 8 * q + 8)
            edge = slice(16 + q, 17 + q)
            row = slice(q, q + 1)
            if send:
                send_r[step, c, 1, face] = jnp.where(upper, res[4, 1, q], roll_s(res[4, 0, q], 4))
                send_r[step, c, 1, edge] = px[4, q][7:8]
                send_x[step, c, 1, face] = pack_x([px[ro, q] for ro in range(4)], 3)
                send_x[step, c, 1, edge] = px[4, q][7:8]
                send_c[step, c, 3, row] = px[4, q][7:8]
                send_r[step, c, 0, face] = jnp.where(upper, roll_s(res[0, 1, q], 4), res[0, 0, q])
                send_r[step, c, 0, edge] = px[0, q][3:4]
                send_x[step, c, 0, face] = pack_x([res[ro, 0, q] for ro in range(4)], 0)
                send_x[step, c, 0, edge] = res[4, 0, q][4:5]
                send_c[step, c, 0, row] = res[0, 0, q][0:1]
                send_c[step, c, 1, row] = px[0, q][3:4]
                send_c[step, c, 2, row] = res[4, 0, q][4:5]
            for ro in range(4 if hold else 0):
                for p in range(2):
                    vec[new, c, ro, p, q] = res[ro, p, q] - s * u[ro, p, q]
                if ghosts:
                    ghost_x[new, c, ro, q] = px[ro, q] - s * gx[ro, q]
            if ghosts:
                for p in range(2):
                    ghost_r[new, c, p, q] = res[4, p, q] - s * u[4, p, q]
                ghost_c[new, c, q] = px[4, q] - s * gx[4, q]
            if step == n_steps - 1:
                for n in range(2):
                    rim_send[c, 24 + 2 * n + q] = px[2 + n, q]
                    rim_send[c, 28 + 2 * n + q] = res[4, n, q]
                    rim_send[c, 32 + 2 * n + q] = res[2 + n, 0, q]
                    rim_send[c, 36 + 2 * n + q] = res[0, n, q]

    def pack_rim(c):
        new = (n_steps - 1) % 2
        for q in range(2):
            for n in range(2):
                for p in range(2):
                    v = vec[new, c, 2 + n, p, q]
                    rim_send[c, 4 * n + 2 * p + q] = v
                    block_send[4 * n + 2 * p + q, c : c + 1] = v[7:8]
                    rim_send[c, 8 + 4 * n + 2 * p + q] = to_column(
                        vec[new, c, p, n, q], vec[new, c, 2 + p, n, q]
                    )
                rim_send[c, 16 + 2 * n + q] = ghost_x[new, c, 2 + n, q]
                rim_send[c, 20 + 2 * n + q] = ghost_r[new, c, n, q]

    group_last = lax.rem(sub, 4) == 3
    group_first = lax.rem(sub, 4) == 0

    def own_planes(c, cur):
        for q in range(2):
            side = jnp.where(corner3, ghost_x[cur, c, 0, q], roll_s(ghost_r[cur, c, 0, q], 3))
            for p in range(2):
                column = to_column(
                    roll_s(vec[cur, c, p, 0, q], 3), roll_s(vec[cur, c, 2 + p, 0, q], 3)
                )
                plane = jnp.where(upper, column, vec[cur, c, 0, p, q])
                rim_own[c, 2 * p + q] = plane
                if p == 0:
                    rim_own[c, 4 + q] = jnp.where(group_last, side, roll_s(plane, -1))

    def across(u):
        t = {}
        for p in range(3):
            for q in range(2):
                t[0, p, q], t[1, p, q], t[2, p, q] = forward(u[0, p, q], u[1, p, q], u[2, p, q])
        return t

    def rim_elements(t, scale, upper_plane=True, only_end=False):
        w = {}
        for a in range(3):
            x = {}
            for q in range(2):
                if only_end:
                    end = t[a, 2, q]
                    x[0, q], x[1, q], x[2, q] = end, -end, end
                else:
                    x[0, q], x[1, q], x[2, q] = forward(t[a, 0, q], t[a, 1, q], t[a, 2, q])
            for b in range(3):
                x[b, 0], x[b, 1] = y_pass(x[b, 0], x[b, 1], a, b, scale)
            for q in range(2):
                w[a, 0, q], w[a, 1, q], w[a, 2, q] = backward(x[0, q], x[1, q], x[2, q])
        sign = -1.0 if upper_plane else 1.0
        return {
            (p, q): w[0, p, q] + w[2, p, q] + (w[1, p, q] if sign > 0 else -w[1, p, q])
            for p in range(3)
            for q in range(2)
        }

    def add_planes(new, c, side, tip):
        for q in range(2):
            out = [side[0, q] + keep(~group_first, roll_s(side[2, q], 1)), side[1, q]]
            for p in range(2):
                for e in range(2):
                    ro = 2 * e + p
                    add = keep(corner4, roll_s(out[p], -(2 + e)))
                    add = jnp.where(corner0, roll_s(out[p], -(4 + e)), add)
                    if ro == 0:
                        add = add + keep(~upper, out[0]) + keep(corner0, roll_s(tip[2, q], -c))
                    vec[new, c, ro, 0, q] += add
            vec[new, c, 0, 1, q] += keep(~upper, out[1])

    def add_first():
        sides = {}
        corner = {}
        zero = jnp.zeros((8, half_y), F32)
        for c in range(comps):
            own_planes(c, 0)
            t = {}
            for q in range(2):
                u = [keep(group_last, roll_s(edge_recv[EDGE_G + 2 * n + q], 3 - c)) for n in range(2)]
                for p in range(2):
                    plane = rim_own[c, 2 * p + q]
                    t[0, p, q], t[1, p, q], t[2, p, q] = plane, -plane, plane
                    if p == 0:
                        part = keep(sub == c, roll_s(plane, c))
                        corner[2, 2, q] = corner[2, 2, q] + part if c else part
                t[0, 2, q], t[1, 2, q], t[2, 2, q] = forward(u[0], u[1], rim_own[c, 4 + q])
            sides[c] = rim_elements(t, lambda i: rim_scaled[0, i])
        for q in range(2):
            for n in range(2):
                corner[n, 2, q] = edge_recv[EDGE_T + 2 * n + q]
                corner[2, n, q] = edge_recv[EDGE_U + 2 * n + q]
                for p in range(2):
                    corner[n, p, q] = zero
        tip = rim_elements(across(corner), lambda i: rim_scaled[1, i])
        high = []
        for g in range(2):
            t = {}
            for q in range(2):
                t[0, 2, q], t[1, 2, q], t[2, 2, q] = forward(
                    *(edge_recv[EDGE_H + 6 * g + 2 * n + q] for n in range(3))
                )
            high.append(rim_elements(t, lambda i, g=g: rim_scaled[2 + g, i], False, True))
        for c in range(comps):
            add_planes(1, c, sides[c], tip)
            for q in range(2):
                far = sides[c][2, q]
                ghost_x[1, c, 0, q] += keep(corner3, far + roll_s(high[1][2, q], -1 - c))
                ghost_r[1, c, 0, q] += (
                    keep(corner4, roll_s(far, -3) + roll_s(high[1][2, q], 4 - c))
                    + keep(corner7, roll_s(high[0][0, q], 7 - c))
                )
                ghost_r[1, c, 1, q] += keep(corner7, roll_s(high[0][1, q], 7 - c))
                for t in range(2):
                    ghost_x[1, c, 2 + t, q] += keep(corner7, roll_s(high[0][t, q], 3 - c))
                ghost_c[1, c, q] += keep(
                    corner7, roll_s(high[0][2, q], 7 - c) + roll_s(high[0][2, q], 3 - c)
                )

    def add_rim():
        cur = (n_steps - 1) % 2
        new = 1 - cur
        inner = jnp.where(upper, up_f, right_f)
        corner = {}
        sides = {}
        for c in range(comps):
            u = {}
            for q in range(2):
                for n in range(2):
                    for p in range(2):
                        u[n, p, q] = rim_recv[c, ROWS_X + 4 * n + 2 * p + q]
                    u[n, 0, q] = u[n, 0, q] + rim_recv[c, ROWS_C + 2 * n + q]
                    ghost = rim_recv[c, ROWS_G + 2 * n + q] + rim_recv[c, ROWS_A + 2 * n + q]
                    u[n, 2, q] = jnp.where(group_last, ghost * inner, roll_s(u[n, 0, q], -1))
                for p in range(3):
                    u[2, p, q] = rim_own[c, 2 * p + q]
            for q in range(2):
                parts = {(2, 2): roll_s(u[2, 0, q], c)}
                for n in range(2):
                    parts[n, 2] = roll_s(u[n, 0, q], c)
                    parts[2, n] = roll_s(u[n, 0, q], c - 4)
                for key, part in parts.items():
                    part = keep(sub == c, part)
                    key = key + (q,)
                    corner[key] = corner[key] + part if c else part
            sides[c] = rim_elements(across(u), lambda i: rim_scaled[0, i])
        for q in range(2):
            for n in range(2):
                for p in range(2):
                    corner[n, p, q] = block_recv[4 * n + 2 * p + q]
        tip = rim_elements(across(corner), lambda i: rim_scaled[1, i])
        for c in range(comps):
            add_planes(new, c, sides[c], tip)

    def absorb(step, c):
        new = step % 2
        first, last = step == 0, False
        for q in range(2):
            face = slice(8 * q, 8 * q + 8)
            line = slice(16 + q, 17 + q)
            row = slice(q, q + 1)

            def spot(ref_row, mask):
                return keep(mask, jnp.broadcast_to(ref_row, (8, half_y)))

            if not first:
                from_low = recv_r[step, c, 1, face]
                from_left = recv_x[step, c, 1, face]
                corner = spot(recv_c[step, c, 3, row], corner0)
                vec[new, c, 0, 0, q] += (
                    keep(~upper, from_low) + keep(first_x, from_left) + corner
                )
                vec[new, c, 0, 1, q] += keep(~upper, roll_s(from_low, 4))
                for ro in range(1, 4):
                    vec[new, c, ro, 0, q] += keep(first_x, roll_s(from_left, -ro))
            if not last:
                from_up = recv_r[step, c, 0, face]
                from_right = recv_x[step, c, 0, face]
                add0 = keep(upper, roll_s(from_up, 4))
                add1 = keep(upper, from_up)
                edge = keep(last_x, roll_s(from_right, 3))
                far = (
                    spot(recv_r[step, c, 0, line], corner7)
                    + spot(recv_x[step, c, 0, line], corner7)
                    + spot(recv_c[step, c, 0, row], corner7)
                )
                if not first:
                    add0 = (
                        add0
                        + spot(recv_x[step, c, 1, line], corner4)
                        + spot(recv_c[step, c, 1, row], corner4)
                    )
                    edge = (
                        edge
                        + spot(recv_r[step, c, 1, line], corner3)
                        + spot(recv_c[step, c, 2, row], corner3)
                    )
                    add0 = add0 + ghost_r[new, c, 0, q]
                    add1 = add1 + ghost_r[new, c, 1, q]
                    edge = edge + ghost_x[new, c, 0, q]
                    far = far + ghost_c[new, c, q]
                ghost_r[new, c, 0, q] = add0 * up_f
                ghost_r[new, c, 1, q] = add1 * up_f
                ghost_x[new, c, 0, q] = edge * right_f
                ghost_c[new, c, q] = far * both_f
                for ro in range(1, 4):
                    edge = keep(last_x, roll_s(from_right, 3 - ro))
                    if not first:
                        edge = edge + ghost_x[new, c, ro, q]
                    ghost_x[new, c, ro, q] = edge * right_f

    def to_native(k, c, rim=False):
        cur = k % 2
        for ro in range(4):
            for p in range(2):
                if rim and ro and p:
                    continue
                for q in range(2):
                    v = vec[cur, c, ro, p, q]
                    for h in range(2):
                        work[n_prev + k, q, native(c, ro, p, h), :] = v[4 * h : 4 * h + 4]

    def write_out(k):
        z = jnp.concatenate([work[n_prev + k, 0], work[n_prev + k, 1]], 1)
        out_ref[k - 1] = exact_dot(z, join_perm)

    lane16 = lax.broadcasted_iota(jnp.int32, (16, half_y), 1)
    row16 = lax.broadcasted_iota(jnp.int32, (16, half_y), 0)

    def gram_part(i, acc, first, count):
        def chunk(t, acc):
            at = pl.ds(pl.multiple_of(8 * t, 8), 8)
            for q in range(2):
                mine = work[i, q, at, :]
                acc = tuple(
                    acc[j] + mine * (mine if j == i else work[j, q, at, :]) for j in range(i + 1)
                )
            return acc

        return lax.fori_loop(first, first + count, chunk, acc, unroll=4)

    def gram_add(i, acc, at, mask):
        for q in range(2):
            mine = work[i, q, at, :]
            mine = mine if mask is None else keep(mask, mine)
            acc = tuple(
                acc[j] + mine * (mine if j == i else work[j, q, at, :]) for j in range(i + 1)
            )
        return acc

    def gram_zero(i):
        return (jnp.zeros((8, half_y), F32),) * (i + 1)

    def gram_close(i, acc):
        sums = [jnp.sum(a, axis=0, keepdims=True) for a in acc]
        sums.append(jnp.zeros((16 - len(sums), half_y), F32))
        total = jnp.sum(jnp.concatenate(sums, 0), axis=1, keepdims=True)
        hit = jnp.logical_or(lane16 == i * n_vec + row16, lane16 == row16 * n_vec + i)
        hit = jnp.logical_and(hit, row16 <= i)
        return jnp.sum(jnp.where(hit, jnp.broadcast_to(total, hit.shape), 0.0), 0, keepdims=True)

    def gram_row(i):
        return gram_close(i, gram_part(i, gram_zero(i), 0, rows // 8))

    res_copy.wait()
    edge_rows = []
    for c in range(comps):
        picked = [2 * x + p for p in range(2) for x in range(4)] + [8 * r for r in range(8)]
        edge_rows += [stage[n_prev, pl.ds(c * 64 + at, 1), :] for at in picked]
    edge = exact_dot(jnp.concatenate(edge_rows, 0), split_perm)
    zero_rows = jnp.zeros((2, half_y), F32)
    for c in range(comps):
        send_r[0, c, 0, 16:18] = zero_rows
        send_x[0, c, 0, 16:18] = zero_rows
        for q in range(2):
            face = slice(8 * q, 8 * q + 8)
            lanes = slice(half_y * q, half_y * (q + 1))
            send_r[0, c, 0, face] = edge[16 * c : 16 * c + 8, lanes]
            send_x[0, c, 0, face] = edge[16 * c + 8 : 16 * c + 16, lanes]
            send_c[0, c, 0, q : q + 1] = edge[16 * c : 16 * c + 1, lanes]
            along = [8 + 6, 8 + 7, 3, 7, 8, 9, 10, 0, 4, 1]
            for slot, row in enumerate(along):
                at = 16 * c + row
                edge_send[2 * slot + q, c : c + 1] = edge[at : at + 1, lanes]

    pl.when(jnp.logical_not(soon))(answer)
    for c in range(comps):
        start_round(0, c)
    start_edges(FIRST)
    split_columns(n_prev)
    for c in range(comps):
        for ro in range(4):
            for p in range(2):
                for q in range(2):
                    vec[0, c, ro, p, q] = jnp.concatenate(
                        [work[n_prev, q, native(c, ro, p, h), :] for h in range(2)], 0
                    )
    for copy in small_copies:
        copy.wait()
    etas = []
    for e in range(2):
        ids = jnp.concatenate([ids_ref[e], ids_ref[2 + e]], 0)
        eta = jnp.zeros((8, half_y), F32)
        for layer in range(visc_ref.shape[0]):
            eta = eta + jnp.where(ids == layer, visc_ref[layer], 0.0)
        etas.append(eta)
        for key, i in kinds.items():
            scaled[e, i] = eta * weight(*key)
    eta_send[0] = etas[1]
    eta_send[1] = to_column(*etas)
    eta_send[2] = jnp.where(
        upper,
        jnp.broadcast_to(etas[1][4:5], (8, half_y)),
        jnp.broadcast_to(etas[0][3:4], (8, half_y)),
    )
    start_etas(FIRST)
    for c in range(comps):
        apply(0, c, hold=False)
        start_round(1, c, FIRST)

    @pl.when(jnp.logical_or(rad < n_rad - 1, lat < n_lat - 1))
    def _():
        pl.semaphore_wait(hello, around(1, LAST[:2]))

    others = tuple(d for d in DIRS if d not in FIRST and d not in LAST[2:])
    start_edges(others)
    start_etas(others)
    for c in range(comps):
        start_round(1, c, others)

    total = jnp.zeros((1, half_y), F32)
    prev_copy.wait()
    for i in range(n_prev):
        split_columns(i)

    @pl.when(jnp.logical_and(rad < n_rad - 1, lat < n_lat - 1))
    def _():
        pl.semaphore_wait(hello_far, 1)

    start_etas(LAST[2:])
    for c in range(comps):
        start_round(1, c, LAST[2:])
    for i in range(n_prev + 1):
        total = total + gram_row(i)

    for c in range(comps):
        finish_round(0, c)
        absorb(0, c)
        apply(0, c, send=False)
    settle(rim_sems.at[1], opposite(edge_sizes))
    tip_eta = jnp.broadcast_to(eta_recv[1, 0:1], (8, half_y))
    for key, i in kinds.items():
        for slot in range(4):
            rim_scaled[slot, i] = (tip_eta if slot == 1 else eta_recv[slot]) * weight(*key)
    add_first()
    for k in range(1, n_steps - 1):
        for c in range(comps):
            finish_round(k, c)
            absorb(k, c)
            apply(k, c)
            start_round(k + 1, c)
            if k == n_steps - 2:
                if c:
                    start_layers(c - 1)
                pack_rim(c)
        if k == n_steps - 2:
            start_layers(comps - 1)
            start_rim()
        if k == n_steps - 2:
            send_token(0)
        for c in range(comps):
            to_native(k, c)
        write_out(k)
        total = total + gram_row(n_prev + k)
    assert n_steps >= 3
    k = n_steps - 1
    per = rows // 8 // comps
    whole = gram_zero(n_vec - 2)
    acc = gram_zero(n_vec - 1)
    for c in range(comps):
        finish_round(k, c)
        absorb(k, c)
        apply(k, c)
        if c == 0:
            take_token(0)
            send_token(1)
        own_planes(c, k % 2)
        to_native(k, c)
        to_native(n_steps, c)
        whole = gram_part(n_vec - 2, whole, c * per, per)
        acc = lax.fori_loop(
            8 * c + 1,
            8 * c + 8,
            lambda t, acc: gram_add(
                n_vec - 1, acc, pl.ds(pl.multiple_of(8 * t, 8), 8), jnp.logical_not(corner0)
            ),
            acc,
            unroll=7,
        )
    total = total + gram_close(n_vec - 2, whole)
    settle(rim_sems.at[0], opposite(rim_sizes))
    add_rim()
    for c in range(comps):
        to_native(n_steps, c, rim=True)
    for c in range(comps):
        acc = gram_add(n_vec - 1, acc, pl.ds(c * 64, 8), None)
        acc = gram_add(n_vec - 1, acc, pl.ds(c * 64, 8, stride=8), jnp.logical_not(corner0))
    total = total + gram_close(n_vec - 1, acc)
    gram_send[...] = total

    def scatter(slot, device):
        pltpu.make_async_remote_copy(
            src_ref=gram_send,
            dst_ref=gram_recv.at[slot],
            send_sem=gram_sems.at[0],
            recv_sem=gram_sems.at[1],
            device_id=device,
            device_id_type=MESH,
        ).start()

    for j in range(1, len(reaches)):
        take_token(j)
        send_token(j + 1)
    each_other(scatter)
    write_out(n_steps - 1)
    write_out(n_steps)
    sent = [size for step in range(n_steps) for size in round_sizes(step)] * comps
    settle(send_sem.at[0], sent + rim_sizes + edge_sizes)
    for i in range(2):
        pltpu.make_async_copy(gram_recv, gram_recv, gram_sems.at[i]).wait()
    full = (total + jnp.sum(gram_recv[...], axis=0)) * (1.0 / (rows * 2 * half_y * n_dev))
    for i in range(n_vec):
        line = full if i == 0 else pltpu.roll(full, half_y - i * n_vec, 1)
        gram_ref[i : i + 1, :] = line[:, :n_vec]


def store(vec_ref, gram_ref, vec_out, gram_out, sems):
    copies = [pltpu.make_async_copy(gram_ref, gram_out, sems.at[0])]
    for i in range(vec_ref.shape[0]):
        copies.append(pltpu.make_async_copy(vec_ref.at[i], vec_out.at[i], sems.at[1 + i]))
    for copy in copies:
        copy.start()
    for copy in copies:
        copy.wait()


def on_device(residual, prev_basis, layer_ids, viscosity, shifts):
    n_lat = lax.axis_size("lat")
    n_rad = lax.axis_size("rad")
    comps, node_r, node_x, node_y = residual.shape
    n_prev = prev_basis.shape[0]
    n_steps = shifts.shape[0]
    n_vec = n_prev + n_steps + 1
    rows = comps * node_r * node_x
    half_y = node_y // 2
    assert node_r == 8 and node_x == 8 and half_y == 128
    rounds = n_steps
    tile = (8, half_y)
    vmem = pltpu.VMEM
    hbm_spec = pl.BlockSpec(memory_space=pltpu.HBM)
    vmem_spec = pl.BlockSpec(memory_space=pltpu.VMEM)
    out, gram = pl.pallas_call(
        functools.partial(kernel, n_lat, n_rad, n_steps, n_prev, comps),
        out_shape=(
            pltpu.VMEM((n_steps, rows, node_y), F32),
            pltpu.VMEM((n_vec, n_vec), F32),
        ),
        in_specs=[hbm_spec] * 5,
        out_specs=(vmem_spec, vmem_spec),
        scratch_shapes=[
            vmem((n_prev + 1, rows, node_y), F32),
            vmem(layer_ids.shape, jnp.int32),
            pltpu.SMEM(viscosity.shape, F32),
            pltpu.SMEM(shifts.shape, F32),
            vmem((n_vec, 2, rows, half_y), F32),
            vmem((2, comps, 4, 2, 2) + tile, F32),
            vmem((2, comps, 2, 2) + tile, F32),
            vmem((2, comps, 4, 2) + tile, F32),
            vmem((2, comps, 2) + tile, F32),
            vmem((2, 9) + tile, F32),
            vmem((rounds, comps, 2, 18, half_y), F32),
            vmem((rounds, comps, 2, 18, half_y), F32),
            vmem((rounds, comps, 4, 2, half_y), F32),
            vmem((rounds, comps, 2, 18, half_y), F32),
            vmem((rounds, comps, 2, 18, half_y), F32),
            vmem((rounds, comps, 4, 2, half_y), F32),
            vmem((1, half_y), F32),
            vmem((n_lat * n_rad - 1, 1, half_y), F32),
            vmem((rounds * comps * 80 + 128 * comps, half_y), F32),
            vmem((comps, 40) + tile, F32),
            vmem((comps, 20) + tile, F32),
            vmem((8,) + tile, F32),
            vmem((8,) + tile, F32),
            vmem((20,) + tile, F32),
            vmem((24,) + tile, F32),
            vmem((3,) + tile, F32),
            vmem((4,) + tile, F32),
            vmem((4, 9) + tile, F32),
            vmem((comps, 6) + tile, F32),
            pltpu.SemaphoreType.DMA((5,)),
            pltpu.SemaphoreType.DMA((1,)),
            pltpu.SemaphoreType.DMA((3, comps)),
            pltpu.SemaphoreType.DMA((2,)),
            pltpu.SemaphoreType.DMA((2,)),
            pltpu.SemaphoreType.REGULAR((max(n_lat, n_rad).bit_length(),)),
        ],
        compiler_params=pltpu.CompilerParams(
            collective_id=0, has_side_effects=True, vmem_limit_bytes=65000000
        ),
    )(
        residual.reshape(rows, node_y),
        prev_basis.reshape(n_prev, rows, node_y),
        layer_ids,
        viscosity,
        shifts,
    )
    out, gram = pl.pallas_call(
        store,
        out_shape=(
            jax.ShapeDtypeStruct(out.shape, F32),
            jax.ShapeDtypeStruct(gram.shape, F32),
        ),
        in_specs=[vmem_spec] * 2,
        out_specs=(hbm_spec, hbm_spec),
        scratch_shapes=[pltpu.SemaphoreType.DMA((1 + n_steps,))],
    )(*(pltpu.with_memory_space_constraint(a, pltpu.VMEM) for a in (out, gram)))
    return out.reshape((n_steps,) + residual.shape), gram


def solution(mesh):
    placed = (
        P(None, "rad", "lat", None),
        P(None, None, "rad", "lat", None),
        P("rad", "lat", None),
        P(),
        P(),
    )
    return jax.shard_map(
        on_device,
        mesh=mesh,
        in_specs=placed,
        out_specs=(P(None, None, "rad", "lat", None), P()),
        check_vma=False,
    )
```

```python
import functools

import jax
import jax.numpy as jnp
from jax import lax
from jax.experimental import pallas as pl
from jax.experimental.pallas import tpu as pltpu
from jax.sharding import PartitionSpec as P

MESH = pl.DeviceIdType.MESH
F32 = jnp.float32

mass = (1.0 / 36, 1.0 / 12, 1.0 / 45)
stiff = (0.0, 1.0, 4.0 / 3)

DIRS = ((-1, -1), (-1, 0), (-1, 1), (0, -1), (0, 1), (1, -1), (1, 0), (1, 1))
R_DIRS = {(-1, 0): 0, (1, 0): 1}
X_DIRS = {(0, -1): 0, (0, 1): 1}
C_DIRS = {(-1, -1): 0, (-1, 1): 1, (1, -1): 2, (1, 1): 3}
FIRST = ((-1, 0), (0, -1), (-1, -1))
LAST = ((1, 0), (0, 1), (1, 1))
ROWS_X, ROWS_G, ROWS_A, ROWS_C = 0, 8, 12, 16
RIM = (
    ((1, 0), (0, 8), (4, 4), ROWS_X, 0),
    ((0, 1), (8, 8), (4, 4), ROWS_X, 4),
    ((1, 0), (16, 4), (7, 1), ROWS_G, 3),
    ((0, 1), (20, 4), (7, 1), ROWS_G, 7),
    ((1, 1), (24, 4), (7, 1), ROWS_C, 0),
    ((1, 1), (28, 4), (7, 1), ROWS_C, 4),
    ((1, -1), (32, 4), (4, 1), ROWS_A, 3),
    ((-1, 1), (36, 4), (3, 1), ROWS_A, 7),
)
EDGE_T, EDGE_U, EDGE_H, EDGE_G = 0, 4, 8, 20
EDGES = (
    ((-1, -1), (8, 6), EDGE_H, 0),
    ((-1, -1), (14, 6), EDGE_H, 4),
    ((-1, 0), (8, 6), EDGE_H + 6, 0),
    ((0, -1), (14, 6), EDGE_H + 6, 4),
    ((1, 0), (0, 4), EDGE_T, 0),
    ((0, 1), (4, 4), EDGE_U, 0),
    ((1, -1), (0, 4), EDGE_G, 0),
    ((-1, 1), (4, 4), EDGE_G, 4),
)
ETAS = (
    ((-1, 0), 2, 0, 3, 2, 0),
    ((0, -1), 2, 4, 3, 2, 4),
    ((1, 0), 0, 4, 4, 0, 0),
    ((0, 1), 1, 4, 4, 0, 4),
    ((1, 1), 0, 7, 1, 1, 0),
    ((-1, 1), 2, 0, 3, 3, 0),
    ((1, -1), 2, 4, 3, 3, 4),
)


def weight(a, b, c):
    return (
        stiff[a] * mass[b] * mass[c] + mass[a] * stiff[b] * mass[c] + mass[a] * mass[b] * stiff[c]
    )


def forward(u0, u1, u2):
    total = u0 + u2
    twice = u1 + u1
    return total + (twice + twice), u0 - u2, total - twice


def backward(m0, m1, m2):
    both = m0 + m2
    half = m0 + m0 - m2
    return both + m1, half + half, both - m1


def kernel(
    n_lat,
    n_rad,
    n_steps,
    n_prev,
    comps,
    res_ref,
    prev_ref,
    ids_hbm,
    visc_hbm,
    shift_hbm,
    out_ref,
    gram_ref,
    stage,
    ids_ref,
    visc_ref,
    shift_ref,
    work,
    vec,
    ghost_r,
    ghost_x,
    ghost_c,
    scaled,
    send_r,
    send_x,
    send_c,
    recv_r,
    recv_x,
    recv_c,
    gram_send,
    gram_recv,
    bulk,
    rim_send,
    rim_recv,
    block_send,
    block_recv,
    edge_send,
    edge_recv,
    eta_send,
    eta_recv,
    rim_scaled,
    rim_own,
    in_sem,
    send_sem,
    recv_sem,
    rim_sems,
    gram_sems,
    token_sem,
):
    n_dev = n_lat * n_rad
    lat = lax.axis_index("lat")
    rad = lax.axis_index("rad")
    me = lat * n_rad + rad
    rows = res_ref.shape[0]
    half_y = res_ref.shape[1] // 2
    n_vec = n_prev + n_steps + 1

    res_copy = pltpu.make_async_copy(res_ref, stage.at[n_prev], in_sem.at[0])
    res_copy.start()
    prev_copy = pltpu.make_async_copy(prev_ref, stage.at[pl.ds(0, n_prev)], in_sem.at[1])
    small_copies = [
        pltpu.make_async_copy(a, b, in_sem.at[2 + i])
        for i, (a, b) in enumerate(
            ((ids_hbm, ids_ref), (visc_hbm, visc_ref), (shift_hbm, shift_ref))
        )
    ]
    for copy in small_copies:
        copy.start()
    prev_copy.start()

    barrier = pltpu.get_barrier_semaphore()

    def around(far, dirs):
        total = 0
        for dr, dx in dirs:
            if not ((dr and n_rad <= far) or (dx and n_lat <= far)):
                total += jnp.where(within(dr * far, dx * far), 1, 0)
        return total

    def within(dr, dx):
        ok = None
        for pos, step, count in ((rad, dr, n_rad), (lat, dx, n_lat)):
            if step:
                one = (pos >= -step) if step < 0 else (pos < count - step)
                ok = one if ok is None else jnp.logical_and(ok, one)
        return ok

    even = lax.rem(lat, 2) == 0
    odd = jnp.logical_not(even)

    def allowed(d, when):
        ok = within(*d)
        return ok if when is None else jnp.logical_and(ok, when)

    def signal_around(sem, far, dirs, when=None):
        for dr, dx in dirs:
            if (dr and n_rad <= far) or (dx and n_lat <= far):
                continue

            @pl.when(allowed((dr * far, dx * far), when))
            def _(dr=dr, dx=dx):
                pl.semaphore_signal(
                    sem,
                    inc=1,
                    device_id={"lat": lat + dx * far, "rad": rad + dr * far},
                    device_id_type=MESH,
                )

    for ref in (edge_recv, eta_recv):
        ref[...] = jnp.zeros_like(ref)
    signal_around(barrier, 1, LAST)
    signal_around(barrier, 1, ((-1, 0),), even)
    signal_around(barrier, 1, ((0, -1), (-1, -1), (-1, 1), (1, -1)), odd)

    for d in DIRS:
        if d in R_DIRS:
            ref, slot = recv_r, R_DIRS[d]
        elif d in X_DIRS:
            ref, slot = recv_x, X_DIRS[d]
        else:
            ref, slot = recv_c, C_DIRS[d]

        @pl.when(jnp.logical_not(within(-d[0], -d[1])))
        def _(ref=ref, slot=slot):
            ref[:, :, slot] = jnp.zeros(ref.shape[:2] + ref.shape[3:], F32)

    for ref in (rim_recv, block_recv):
        ref[...] = jnp.zeros_like(ref)

    for ref in (ghost_r, ghost_x, ghost_c):
        ref[0] = jnp.zeros(ref.shape[1:], F32)

    hello = token_sem.at[token_sem.shape[0] - 1]
    hello_far = token_sem.at[token_sem.shape[0] - 2]

    def answer():
        @pl.when(even)
        def _():
            pl.semaphore_wait(barrier, around(1, DIRS))

        @pl.when(odd)
        def _():
            pl.semaphore_wait(barrier, around(1, FIRST))

        signal_around(hello, 1, ((-1, 0),), odd)
        signal_around(hello, 1, ((0, -1),), even)
        signal_around(hello_far, 1, ((-1, -1),), even)

    soon = jnp.logical_and(odd, jnp.logical_or(rad == 0, lax.rem(rad, 2) == 1))
    pl.when(soon)(answer)

    reaches = []
    while (2 << len(reaches)) < max(n_lat, n_rad) - 1:
        reaches.append(2 << len(reaches))

    def send_token(j):
        if j < len(reaches):
            signal_around(token_sem.at[j], reaches[j], DIRS)

    def take_token(j):
        if j < len(reaches):
            pl.semaphore_wait(token_sem.at[j], around(reaches[j], DIRS))

    rad_targets = [lax.rem(rad + d, n_rad) for d in range(n_rad)]

    def each_other(visit):
        def row(i, carry):
            lat_target = lax.rem(lat + n_lat // 2 + i, n_lat)
            for d in range(n_rad):
                ahead = lax.rem(n_lat // 2 + i, n_lat)
                visit(ahead * n_rad + d - 1, {"lat": lat_target, "rad": rad_targets[d]})
            return carry

        lax.fori_loop(0, n_lat // 2, row, 0, unroll=n_lat <= 8)
        lax.fori_loop(n_lat // 2 + 1, n_lat, row, 0, unroll=n_lat <= 8)
        for d in range(1, n_rad):
            visit(d - 1, {"lat": lat, "rad": rad_targets[d]})

    sub = lax.broadcasted_iota(jnp.int32, (8, half_y), 0)
    lane = lax.broadcasted_iota(jnp.int32, (8, half_y), 1)
    upper = sub >= 4
    ex = lax.rem(sub, 4)
    first_x = ex == 0
    last_x = ex == 3
    corner0 = sub == 0
    corner3 = sub == 3
    corner4 = sub == 4
    corner7 = sub == 7
    has_up = rad < n_rad - 1
    has_right = lat < n_lat - 1
    up_f = jnp.where(has_up, 1.0, 0.0).astype(F32)
    right_f = jnp.where(has_right, 1.0, 0.0).astype(F32)
    both_f = up_f * right_f

    def roll_s(v, k):
        return pltpu.roll(v, k % 8, 0)

    def keep(mask, v):
        return jnp.where(mask, v, 0.0)

    src = lax.broadcasted_iota(jnp.int32, (2 * half_y, 2 * half_y), 0)
    dst = lax.broadcasted_iota(jnp.int32, (2 * half_y, 2 * half_y), 1)
    split_perm = jnp.where(
        src == jnp.where(dst < half_y, 2 * dst, 2 * (dst - half_y) + 1), 1.0, 0.0
    ).astype(jnp.bfloat16)
    join_perm = jnp.where(
        dst == jnp.where(src < half_y, 2 * src, 2 * (src - half_y) + 1), 1.0, 0.0
    ).astype(jnp.bfloat16)

    def exact_dot(a, b):
        high = a.astype(jnp.bfloat16)
        rest = a - high.astype(F32)
        mid = rest.astype(jnp.bfloat16)
        low = (rest - mid.astype(F32)).astype(jnp.bfloat16)
        out = [jnp.dot(part, b, preferred_element_type=F32) for part in (high, mid, low)]
        return out[0] + (out[1] + out[2])

    def split_columns(i):
        z = exact_dot(stage[i], split_perm)
        work[i, 0] = z[:, :half_y]
        work[i, 1] = z[:, half_y:]

    def native(c, ro, p, h):
        return pl.ds(c * 64 + (4 * h + ro) * 8 + p, 4, stride=2)

    kinds = {}
    for a in range(3):
        for b in range(3):
            for c in range(3):
                key = tuple(sorted((a, b, c)))
                if key != (0, 0, 0) and key not in kinds:
                    kinds[key] = len(kinds)
    def copy_of(step, c, d):
        if d in R_DIRS:
            a, b = send_r.at[step, c, R_DIRS[d]], recv_r.at[step, c, R_DIRS[d]]
        elif d in X_DIRS:
            a, b = send_x.at[step, c, X_DIRS[d]], recv_x.at[step, c, X_DIRS[d]]
        else:
            a, b = send_c.at[step, c, C_DIRS[d]], recv_c.at[step, c, C_DIRS[d]]
        return pltpu.make_async_remote_copy(
            src_ref=a,
            dst_ref=b,
            send_sem=send_sem.at[0],
            recv_sem=recv_sem.at[step % 3, c],
            device_id={"lat": lat + d[1], "rad": rad + d[0]},
            device_id_type=MESH,
        )

    order = ((-1, -1), (1, 1), (-1, 1), (1, -1), (1, 0), (-1, 0), (0, 1), (0, -1))

    def dirs_of(step):
        wanted = FIRST if step == 0 else DIRS
        return [d for d in order if d in wanted]

    def start_round(step, c, among=DIRS, when=None):
        for d in dirs_of(step):
            if d not in among:
                continue

            @pl.when(allowed(d, when))
            def _(d=d):
                copy_of(step, c, d).start()

    def places(pos, count):
        out = [(pos == 0, False, True), (pos == count - 1, True, False)]
        if count > 2:
            middle = jnp.logical_and(pos > 0, pos < count - 1)
            out.append((middle, True, True))
        return out if count > 1 else [(pos == 0, False, False)]

    def rows_of(sizes, down, up, left, right):
        have = {-1: {0: True, -1: down, 1: up}, 1: {0: True, -1: left, 1: right}}
        return sum(n for (dr, dx), n in sizes if have[-1][dr] and have[1][dx])

    def settle(sem, sizes):
        groups = {}
        for at_r, down, up in places(rad, n_rad):
            for at_x, left, right in places(lat, n_lat):
                n = rows_of(sizes, down, up, left, right)
                here = jnp.logical_and(at_r, at_x)
                groups[n] = jnp.logical_or(groups[n], here) if n in groups else here
        for n, here in groups.items():
            if n:

                @pl.when(here)
                def _(n=n):
                    pltpu.make_async_copy(bulk.at[pl.ds(0, n)], bulk.at[pl.ds(0, n)], sem).wait()

    def opposite(sizes):
        return [((-dr, -dx), n) for (dr, dx), n in sizes]

    def round_sizes(step):
        return [(d, 2 if d[0] and d[1] else 18) for d in dirs_of(step)]

    rim_sizes = [(d, comps * count * high) for d, (_, count), (_, high), _, _ in RIM]
    rim_sizes.append(((1, 1), comps * 8))
    edge_sizes = [(d, comps * count) for d, (_, count), _, _ in EDGES]
    edge_sizes += [(d, high) for d, _, _, high, _, _ in ETAS]

    def finish_round(step, c):
        settle(recv_sem.at[step % 3, c], opposite(round_sizes(step)))

    def remote(a, b, recv, d, when=None):
        @pl.when(allowed(d, when))
        def _():
            pltpu.make_async_remote_copy(
                src_ref=a,
                dst_ref=b,
                send_sem=send_sem.at[0],
                recv_sem=recv,
                device_id={"lat": lat + d[1], "rad": rad + d[0]},
                device_id_type=MESH,
            ).start()

    def start_layers(c):
        for d, (first, count), (row, high), to, to_row in RIM[:2]:
            remote(
                rim_send.at[c, pl.ds(first, count), pl.ds(row, high)],
                rim_recv.at[c, pl.ds(to, count), pl.ds(to_row, high)],
                rim_sems.at[0],
                d,
            )

    def start_rim():
        for d, (first, count), (row, high), to, to_row in RIM[2:]:
            remote(
                rim_send.at[:, pl.ds(first, count), pl.ds(row, high)],
                rim_recv.at[:, pl.ds(to, count), pl.ds(to_row, high)],
                rim_sems.at[0],
                d,
            )
        remote(
            block_send.at[:, pl.ds(0, comps)], block_recv.at[:, pl.ds(0, comps)], rim_sems.at[0], (1, 1)
        )

    def start_edges(among, when=None):
        for d, (first, count), to, to_row in EDGES:
            if d in among:
                remote(
                    edge_send.at[pl.ds(first, count), pl.ds(0, comps)],
                    edge_recv.at[pl.ds(to, count), pl.ds(to_row, comps)],
                    rim_sems.at[1],
                    d,
                    when,
                )

    def start_etas(among, when=None):
        for d, slot, row, high, to, to_row in ETAS:
            if d in among:
                remote(
                    eta_send.at[slot, pl.ds(row, high)],
                    eta_recv.at[to, pl.ds(to_row, high)],
                    rim_sems.at[1],
                    d,
                    when,
                )

    def pack_x(vals, at):
        out = None
        for ro in range(4):
            moved = roll_s(vals[ro], ro - at)
            out = moved if out is None else jnp.where(ex == ro, moved, out)
        return out

    def y_pass(x0, x1, a, b, scale):
        nxt = keep(lane != half_y - 1, pltpu.roll(x0, half_y - 1, 1))
        m = list(forward(x0, x1, nxt))
        for j in range(3):
            key = tuple(sorted((a, b, j)))
            m[j] = m[j] * scale(kinds[key]) if key in kinds else None
        if m[0] is None:
            r0 = m[1] + m[2]
            r1 = -(m[2] + m[2])
            r2 = m[2] - m[1]
        else:
            r0, r1, r2 = backward(*m)
        return r0 + keep(lane != 0, pltpu.roll(r2, 1, 1)), r1

    def to_column(low, high):
        moved = jnp.where(sub == 6, roll_s(low, -1), high)
        return jnp.where(sub == 4, roll_s(low, 1), jnp.where(sub == 5, roll_s(high, 2), moved))

    def apply(k, c, send=True, hold=True):
        s = shift_ref[k]
        cur = k % 2
        new = 1 - cur
        u = {}
        gx = {}
        for q in range(2):
            for ro in range(4):
                gx[ro, q] = ghost_x[cur, c, ro, q]
                for p in range(2):
                    u[ro, p, q] = vec[cur, c, ro, p, q]
            gx[4, q] = jnp.where(upper, ghost_c[cur, c, q], roll_s(gx[0, q], 4))
            for p in range(2):
                u[4, p, q] = jnp.where(upper, ghost_r[cur, c, p, q], roll_s(u[0, p, q], 4))
            for ro in range(5):
                u[ro, 2, q] = jnp.where(last_x, gx[ro, q], roll_s(u[ro, 0, q], -1))
        res = {}
        for e in range(2):
            t = {}
            for p in range(3):
                for q in range(2):
                    t[0, p, q], t[1, p, q], t[2, p, q] = forward(
                        u[2 * e, p, q], u[2 * e + 1, p, q], u[2 * e + 2, p, q]
                    )
            w = {}
            for a in range(3):
                x = {}
                for q in range(2):
                    x[0, q], x[1, q], x[2, q] = forward(t[a, 0, q], t[a, 1, q], t[a, 2, q])
                for b in range(3):
                    x[b, 0], x[b, 1] = y_pass(x[b, 0], x[b, 1], a, b, lambda i: scaled[e, i])
                for q in range(2):
                    w[a, 0, q], w[a, 1, q], w[a, 2, q] = backward(x[0, q], x[1, q], x[2, q])
            for p in range(3):
                for q in range(2):
                    r = backward(w[0, p, q], w[1, p, q], w[2, p, q])
                    for i in range(3):
                        key = (2 * e + i, p, q)
                        res[key] = res[key] + r[i] if key in res else r[i]
        px = {}
        for q in range(2):
            for ro in range(5):
                edge = res[ro, 2, q]
                px[ro, q] = edge
                res[ro, 0, q] = res[ro, 0, q] + keep(ex != 0, roll_s(edge, 1))
            for p in range(2):
                res[0, p, q] = res[0, p, q] + keep(upper, roll_s(res[4, p, q], 4))
            px[0, q] = px[0, q] + keep(upper, roll_s(px[4, q], 4))
        step = k + 1
        send = send and step < n_steps
        ghosts = hold and step < n_steps
        for q in range(2):
            face = slice(8 * q, 8 * q + 8)
            edge = slice(16 + q, 17 + q)
            row = slice(q, q + 1)
            if send:
                send_r[step, c, 1, face] = jnp.where(upper, res[4, 1, q], roll_s(res[4, 0, q], 4))
                send_r[step, c, 1, edge] = px[4, q][7:8]
                send_x[step, c, 1, face] = pack_x([px[ro, q] for ro in range(4)], 3)
                send_x[step, c, 1, edge] = px[4, q][7:8]
                send_c[step, c, 3, row] = px[4, q][7:8]
                send_r[step, c, 0, face] = jnp.where(upper, roll_s(res[0, 1, q], 4), res[0, 0, q])
                send_r[step, c, 0, edge] = px[0, q][3:4]
                send_x[step, c, 0, face] = pack_x([res[ro, 0, q] for ro in range(4)], 0)
                send_x[step, c, 0, edge] = res[4, 0, q][4:5]
                send_c[step, c, 0, row] = res[0, 0, q][0:1]
                send_c[step, c, 1, row] = px[0, q][3:4]
                send_c[step, c, 2, row] = res[4, 0, q][4:5]
            for ro in range(4 if hold else 0):
                for p in range(2):
                    vec[new, c, ro, p, q] = res[ro, p, q] - s * u[ro, p, q]
                if ghosts:
                    ghost_x[new, c, ro, q] = px[ro, q] - s * gx[ro, q]
            if ghosts:
                for p in range(2):
                    ghost_r[new, c, p, q] = res[4, p, q] - s * u[4, p, q]
                ghost_c[new, c, q] = px[4, q] - s * gx[4, q]
            if step == n_steps - 1:
                for n in range(2):
                    rim_send[c, 24 + 2 * n + q] = px[2 + n, q]
                    rim_send[c, 28 + 2 * n + q] = res[4, n, q]
                    rim_send[c, 32 + 2 * n + q] = res[2 + n, 0, q]
                    rim_send[c, 36 + 2 * n + q] = res[0, n, q]

    def pack_rim(c):
        new = (n_steps - 1) % 2
        for q in range(2):
            for n in range(2):
                for p in range(2):
                    v = vec[new, c, 2 + n, p, q]
                    rim_send[c, 4 * n + 2 * p + q] = v
                    block_send[4 * n + 2 * p + q, c : c + 1] = v[7:8]
                    rim_send[c, 8 + 4 * n + 2 * p + q] = to_column(
                        vec[new, c, p, n, q], vec[new, c, 2 + p, n, q]
                    )
                rim_send[c, 16 + 2 * n + q] = ghost_x[new, c, 2 + n, q]
                rim_send[c, 20 + 2 * n + q] = ghost_r[new, c, n, q]

    group_last = lax.rem(sub, 4) == 3
    group_first = lax.rem(sub, 4) == 0

    def own_planes(c, cur):
        for q in range(2):
            side = jnp.where(corner3, ghost_x[cur, c, 0, q], roll_s(ghost_r[cur, c, 0, q], 3))
            for p in range(2):
                column = to_column(
                    roll_s(vec[cur, c, p, 0, q], 3), roll_s(vec[cur, c, 2 + p, 0, q], 3)
                )
                plane = jnp.where(upper, column, vec[cur, c, 0, p, q])
                rim_own[c, 2 * p + q] = plane
                if p == 0:
                    rim_own[c, 4 + q] = jnp.where(group_last, side, roll_s(plane, -1))

    def across(u):
        t = {}
        for p in range(3):
            for q in range(2):
                t[0, p, q], t[1, p, q], t[2, p, q] = forward(u[0, p, q], u[1, p, q], u[2, p, q])
        return t

    def rim_elements(t, scale, upper_plane=True, only_end=False):
        w = {}
        for a in range(3):
            x = {}
            for q in range(2):
                if only_end:
                    end = t[a, 2, q]
                    x[0, q], x[1, q], x[2, q] = end, -end, end
                else:
                    x[0, q], x[1, q], x[2, q] = forward(t[a, 0, q], t[a, 1, q], t[a, 2, q])
            for b in range(3):
                x[b, 0], x[b, 1] = y_pass(x[b, 0], x[b, 1], a, b, scale)
            for q in range(2):
                w[a, 0, q], w[a, 1, q], w[a, 2, q] = backward(x[0, q], x[1, q], x[2, q])
        sign = -1.0 if upper_plane else 1.0
        return {
            (p, q): w[0, p, q] + w[2, p, q] + (w[1, p, q] if sign > 0 else -w[1, p, q])
            for p in range(3)
            for q in range(2)
        }

    def add_planes(new, c, side, tip):
        for q in range(2):
            out = [side[0, q] + keep(~group_first, roll_s(side[2, q], 1)), side[1, q]]
            for p in range(2):
                for e in range(2):
                    ro = 2 * e + p
                    add = keep(corner4, roll_s(out[p], -(2 + e)))
                    add = jnp.where(corner0, roll_s(out[p], -(4 + e)), add)
                    if ro == 0:
                        add = add + keep(~upper, out[0]) + keep(corner0, roll_s(tip[2, q], -c))
                    vec[new, c, ro, 0, q] += add
            vec[new, c, 0, 1, q] += keep(~upper, out[1])

    def add_first():
        sides = {}
        corner = {}
        zero = jnp.zeros((8, half_y), F32)
        for c in range(comps):
            own_planes(c, 0)
            t = {}
            for q in range(2):
                u = [keep(group_last, roll_s(edge_recv[EDGE_G + 2 * n + q], 3 - c)) for n in range(2)]
                for p in range(2):
                    plane = rim_own[c, 2 * p + q]
                    t[0, p, q], t[1, p, q], t[2, p, q] = plane, -plane, plane
                    if p == 0:
                        part = keep(sub == c, roll_s(plane, c))
                        corner[2, 2, q] = corner[2, 2, q] + part if c else part
                t[0, 2, q], t[1, 2, q], t[2, 2, q] = forward(u[0], u[1], rim_own[c, 4 + q])
            sides[c] = rim_elements(t, lambda i: rim_scaled[0, i])
        for q in range(2):
            for n in range(2):
                corner[n, 2, q] = edge_recv[EDGE_T + 2 * n + q]
                corner[2, n, q] = edge_recv[EDGE_U + 2 * n + q]
                for p in range(2):
                    corner[n, p, q] = zero
        tip = rim_elements(across(corner), lambda i: rim_scaled[1, i])
        high = []
        for g in range(2):
            t = {}
            for q in range(2):
                t[0, 2, q], t[1, 2, q], t[2, 2, q] = forward(
                    *(edge_recv[EDGE_H + 6 * g + 2 * n + q] for n in range(3))
                )
            high.append(rim_elements(t, lambda i, g=g: rim_scaled[2 + g, i], False, True))
        for c in range(comps):
            add_planes(1, c, sides[c], tip)
            for q in range(2):
                far = sides[c][2, q]
                ghost_x[1, c, 0, q] += keep(corner3, far + roll_s(high[1][2, q], -1 - c))
                ghost_r[1, c, 0, q] += (
                    keep(corner4, roll_s(far, -3) + roll_s(high[1][2, q], 4 - c))
                    + keep(corner7, roll_s(high[0][0, q], 7 - c))
                )
                ghost_r[1, c, 1, q] += keep(corner7, roll_s(high[0][1, q], 7 - c))
                for t in range(2):
                    ghost_x[1, c, 2 + t, q] += keep(corner7, roll_s(high[0][t, q], 3 - c))
                ghost_c[1, c, q] += keep(
                    corner7, roll_s(high[0][2, q], 7 - c) + roll_s(high[0][2, q], 3 - c)
                )

    def add_rim():
        cur = (n_steps - 1) % 2
        new = 1 - cur
        inner = jnp.where(upper, up_f, right_f)
        corner = {}
        sides = {}
        for c in range(comps):
            u = {}
            for q in range(2):
                for n in range(2):
                    for p in range(2):
                        u[n, p, q] = rim_recv[c, ROWS_X + 4 * n + 2 * p + q]
                    u[n, 0, q] = u[n, 0, q] + rim_recv[c, ROWS_C + 2 * n + q]
                    ghost = rim_recv[c, ROWS_G + 2 * n + q] + rim_recv[c, ROWS_A + 2 * n + q]
                    u[n, 2, q] = jnp.where(group_last, ghost * inner, roll_s(u[n, 0, q], -1))
                for p in range(3):
                    u[2, p, q] = rim_own[c, 2 * p + q]
            for q in range(2):
                parts = {(2, 2): roll_s(u[2, 0, q], c)}
                for n in range(2):
                    parts[n, 2] = roll_s(u[n, 0, q], c)
                    parts[2, n] = roll_s(u[n, 0, q], c - 4)
                for key, part in parts.items():
                    part = keep(sub == c, part)
                    key = key + (q,)
                    corner[key] = corner[key] + part if c else part
            sides[c] = rim_elements(across(u), lambda i: rim_scaled[0, i])
        for q in range(2):
            for n in range(2):
                for p in range(2):
                    corner[n, p, q] = block_recv[4 * n + 2 * p + q]
        tip = rim_elements(across(corner), lambda i: rim_scaled[1, i])
        for c in range(comps):
            add_planes(new, c, sides[c], tip)

    def absorb(step, c):
        new = step % 2
        first, last = step == 0, False
        for q in range(2):
            face = slice(8 * q, 8 * q + 8)
            line = slice(16 + q, 17 + q)
            row = slice(q, q + 1)

            def spot(ref_row, mask):
                return keep(mask, jnp.broadcast_to(ref_row, (8, half_y)))

            if not first:
                from_low = recv_r[step, c, 1, face]
                from_left = recv_x[step, c, 1, face]
                corner = spot(recv_c[step, c, 3, row], corner0)
                vec[new, c, 0, 0, q] += (
                    keep(~upper, from_low) + keep(first_x, from_left) + corner
                )
                vec[new, c, 0, 1, q] += keep(~upper, roll_s(from_low, 4))
                for ro in range(1, 4):
                    vec[new, c, ro, 0, q] += keep(first_x, roll_s(from_left, -ro))
            if not last:
                from_up = recv_r[step, c, 0, face]
                from_right = recv_x[step, c, 0, face]
                add0 = keep(upper, roll_s(from_up, 4))
                add1 = keep(upper, from_up)
                edge = keep(last_x, roll_s(from_right, 3))
                far = (
                    spot(recv_r[step, c, 0, line], corner7)
                    + spot(recv_x[step, c, 0, line], corner7)
                    + spot(recv_c[step, c, 0, row], corner7)
                )
                if not first:
                    add0 = (
                        add0
                        + spot(recv_x[step, c, 1, line], corner4)
                        + spot(recv_c[step, c, 1, row], corner4)
                    )
                    edge = (
                        edge
                        + spot(recv_r[step, c, 1, line], corner3)
                        + spot(recv_c[step, c, 2, row], corner3)
                    )
                    add0 = add0 + ghost_r[new, c, 0, q]
                    add1 = add1 + ghost_r[new, c, 1, q]
                    edge = edge + ghost_x[new, c, 0, q]
                    far = far + ghost_c[new, c, q]
                ghost_r[new, c, 0, q] = add0 * up_f
                ghost_r[new, c, 1, q] = add1 * up_f
                ghost_x[new, c, 0, q] = edge * right_f
                ghost_c[new, c, q] = far * both_f
                for ro in range(1, 4):
                    edge = keep(last_x, roll_s(from_right, 3 - ro))
                    if not first:
                        edge = edge + ghost_x[new, c, ro, q]
                    ghost_x[new, c, ro, q] = edge * right_f

    def to_native(k, c, rim=False):
        cur = k % 2
        for ro in range(4):
            for p in range(2):
                if rim and ro and p:
                    continue
                for q in range(2):
                    v = vec[cur, c, ro, p, q]
                    for h in range(2):
                        work[n_prev + k, q, native(c, ro, p, h), :] = v[4 * h : 4 * h + 4]

    def write_out(k):
        z = jnp.concatenate([work[n_prev + k, 0], work[n_prev + k, 1]], 1)
        out_ref[k - 1] = exact_dot(z, join_perm)

    lane16 = lax.broadcasted_iota(jnp.int32, (16, half_y), 1)
    row16 = lax.broadcasted_iota(jnp.int32, (16, half_y), 0)

    def gram_part(i, acc, first, count):
        def chunk(t, acc):
            at = pl.ds(pl.multiple_of(8 * t, 8), 8)
            for q in range(2):
                mine = work[i, q, at, :]
                acc = tuple(
                    acc[j] + mine * (mine if j == i else work[j, q, at, :]) for j in range(i + 1)
                )
            return acc

        return lax.fori_loop(first, first + count, chunk, acc, unroll=4)

    def gram_add(i, acc, at, mask):
        for q in range(2):
            mine = work[i, q, at, :]
            mine = mine if mask is None else keep(mask, mine)
            acc = tuple(
                acc[j] + mine * (mine if j == i else work[j, q, at, :]) for j in range(i + 1)
            )
        return acc

    def gram_zero(i):
        return (jnp.zeros((8, half_y), F32),) * (i + 1)

    def gram_close(i, acc):
        sums = [jnp.sum(a, axis=0, keepdims=True) for a in acc]
        sums.append(jnp.zeros((16 - len(sums), half_y), F32))
        total = jnp.sum(jnp.concatenate(sums, 0), axis=1, keepdims=True)
        hit = jnp.logical_or(lane16 == i * n_vec + row16, lane16 == row16 * n_vec + i)
        hit = jnp.logical_and(hit, row16 <= i)
        return jnp.sum(jnp.where(hit, jnp.broadcast_to(total, hit.shape), 0.0), 0, keepdims=True)

    def gram_row(i):
        return gram_close(i, gram_part(i, gram_zero(i), 0, rows // 8))

    res_copy.wait()
    edge_rows = []
    for c in range(comps):
        picked = [2 * x + p for p in range(2) for x in range(4)] + [8 * r for r in range(8)]
        edge_rows += [stage[n_prev, pl.ds(c * 64 + at, 1), :] for at in picked]
    edge = exact_dot(jnp.concatenate(edge_rows, 0), split_perm)
    zero_rows = jnp.zeros((2, half_y), F32)
    for c in range(comps):
        send_r[0, c, 0, 16:18] = zero_rows
        send_x[0, c, 0, 16:18] = zero_rows
        for q in range(2):
            face = slice(8 * q, 8 * q + 8)
            lanes = slice(half_y * q, half_y * (q + 1))
            send_r[0, c, 0, face] = edge[16 * c : 16 * c + 8, lanes]
            send_x[0, c, 0, face] = edge[16 * c + 8 : 16 * c + 16, lanes]
            send_c[0, c, 0, q : q + 1] = edge[16 * c : 16 * c + 1, lanes]
            along = [8 + 6, 8 + 7, 3, 7, 8, 9, 10, 0, 4, 1]
            for slot, row in enumerate(along):
                at = 16 * c + row
                edge_send[2 * slot + q, c : c + 1] = edge[at : at + 1, lanes]

    pl.when(jnp.logical_not(soon))(answer)
    for c in range(comps):
        start_round(0, c)
    others = tuple(d for d in DIRS if d not in FIRST and d not in LAST[2:])
    beyond = others + LAST[2:]
    start_edges(FIRST)
    start_edges(beyond, even)
    split_columns(n_prev)
    for c in range(comps):
        for ro in range(4):
            for p in range(2):
                for q in range(2):
                    vec[0, c, ro, p, q] = jnp.concatenate(
                        [work[n_prev, q, native(c, ro, p, h), :] for h in range(2)], 0
                    )
    for copy in small_copies:
        copy.wait()
    etas = []
    for e in range(2):
        ids = jnp.concatenate([ids_ref[e], ids_ref[2 + e]], 0)
        eta = jnp.zeros((8, half_y), F32)
        for layer in range(visc_ref.shape[0]):
            eta = eta + jnp.where(ids == layer, visc_ref[layer], 0.0)
        etas.append(eta)
        for key, i in kinds.items():
            scaled[e, i] = eta * weight(*key)
    eta_send[0] = etas[1]
    eta_send[1] = to_column(*etas)
    eta_send[2] = jnp.where(
        upper,
        jnp.broadcast_to(etas[1][4:5], (8, half_y)),
        jnp.broadcast_to(etas[0][3:4], (8, half_y)),
    )
    start_etas(FIRST)
    start_etas(beyond, even)
    for c in range(comps):
        apply(0, c, hold=False)
        start_round(1, c, FIRST)
        start_round(1, c, beyond, even)

    edge_up = jnp.logical_or(rad < n_rad - 1, lat < n_lat - 1)

    @pl.when(jnp.logical_and(odd, edge_up))
    def _():
        pl.semaphore_wait(hello, around(1, LAST[:2]))

    start_edges(others, odd)
    start_etas(others, odd)
    for c in range(comps):
        start_round(1, c, others, odd)

    total = jnp.zeros((1, half_y), F32)
    prev_copy.wait()
    for i in range(n_prev):
        split_columns(i)

    @pl.when(jnp.logical_and(odd, jnp.logical_and(rad < n_rad - 1, lat < n_lat - 1)))
    def _():
        pl.semaphore_wait(hello_far, 1)

    start_etas(LAST[2:], odd)
    for c in range(comps):
        start_round(1, c, LAST[2:], odd)
    for i in range(n_prev + 1):
        total = total + gram_row(i)

    for c in range(comps):
        finish_round(0, c)
        absorb(0, c)
        apply(0, c, send=False)
    settle(rim_sems.at[1], opposite(edge_sizes))
    tip_eta = jnp.broadcast_to(eta_recv[1, 0:1], (8, half_y))
    for key, i in kinds.items():
        for slot in range(4):
            rim_scaled[slot, i] = (tip_eta if slot == 1 else eta_recv[slot]) * weight(*key)
    add_first()
    for k in range(1, n_steps - 1):
        for c in range(comps):
            finish_round(k, c)
            absorb(k, c)
            apply(k, c)
            start_round(k + 1, c)
            if k == n_steps - 2:
                if c:
                    start_layers(c - 1)
                pack_rim(c)
        if k == n_steps - 2:
            start_layers(comps - 1)
            start_rim()
        if k == n_steps - 2:
            send_token(0)
        for c in range(comps):
            to_native(k, c)
        write_out(k)
        total = total + gram_row(n_prev + k)
    assert n_steps >= 3
    k = n_steps - 1
    per = rows // 8 // comps
    whole = gram_zero(n_vec - 2)
    acc = gram_zero(n_vec - 1)
    for c in range(comps):
        finish_round(k, c)
        absorb(k, c)
        apply(k, c)
        if c == 0:
            take_token(0)
            send_token(1)
        own_planes(c, k % 2)
        to_native(k, c)
        to_native(n_steps, c)
        whole = gram_part(n_vec - 2, whole, c * per, per)
        acc = lax.fori_loop(
            8 * c + 1,
            8 * c + 8,
            lambda t, acc: gram_add(
                n_vec - 1, acc, pl.ds(pl.multiple_of(8 * t, 8), 8), jnp.logical_not(corner0)
            ),
            acc,
            unroll=7,
        )
    total = total + gram_close(n_vec - 2, whole)
    settle(rim_sems.at[0], opposite(rim_sizes))
    add_rim()
    for c in range(comps):
        to_native(n_steps, c, rim=True)
    for c in range(comps):
        acc = gram_add(n_vec - 1, acc, pl.ds(c * 64, 8), None)
        acc = gram_add(n_vec - 1, acc, pl.ds(c * 64, 8, stride=8), jnp.logical_not(corner0))
    total = total + gram_close(n_vec - 1, acc)
    gram_send[...] = total

    def scatter(slot, device):
        pltpu.make_async_remote_copy(
            src_ref=gram_send,
            dst_ref=gram_recv.at[slot],
            send_sem=gram_sems.at[0],
            recv_sem=gram_sems.at[1],
            device_id=device,
            device_id_type=MESH,
        ).start()

    for j in range(1, len(reaches)):
        take_token(j)
        send_token(j + 1)
    each_other(scatter)
    write_out(n_steps - 1)
    write_out(n_steps)
    sent = [size for step in range(n_steps) for size in round_sizes(step)] * comps
    settle(send_sem.at[0], sent + rim_sizes + edge_sizes)
    for i in range(2):
        pltpu.make_async_copy(gram_recv, gram_recv, gram_sems.at[i]).wait()
    full = (total + jnp.sum(gram_recv[...], axis=0)) * (1.0 / (rows * 2 * half_y * n_dev))
    for i in range(n_vec):
        line = full if i == 0 else pltpu.roll(full, half_y - i * n_vec, 1)
        gram_ref[i : i + 1, :] = line[:, :n_vec]


def store(vec_ref, gram_ref, vec_out, gram_out, sems):
    copies = [pltpu.make_async_copy(gram_ref, gram_out, sems.at[0])]
    for i in range(vec_ref.shape[0]):
        copies.append(pltpu.make_async_copy(vec_ref.at[i], vec_out.at[i], sems.at[1 + i]))
    for copy in copies:
        copy.start()
    for copy in copies:
        copy.wait()


def on_device(residual, prev_basis, layer_ids, viscosity, shifts):
    n_lat = lax.axis_size("lat")
    n_rad = lax.axis_size("rad")
    comps, node_r, node_x, node_y = residual.shape
    n_prev = prev_basis.shape[0]
    n_steps = shifts.shape[0]
    n_vec = n_prev + n_steps + 1
    rows = comps * node_r * node_x
    half_y = node_y // 2
    assert node_r == 8 and node_x == 8 and half_y == 128
    rounds = n_steps
    tile = (8, half_y)
    vmem = pltpu.VMEM
    hbm_spec = pl.BlockSpec(memory_space=pltpu.HBM)
    vmem_spec = pl.BlockSpec(memory_space=pltpu.VMEM)
    out, gram = pl.pallas_call(
        functools.partial(kernel, n_lat, n_rad, n_steps, n_prev, comps),
        out_shape=(
            pltpu.VMEM((n_steps, rows, node_y), F32),
            pltpu.VMEM((n_vec, n_vec), F32),
        ),
        in_specs=[hbm_spec] * 5,
        out_specs=(vmem_spec, vmem_spec),
        scratch_shapes=[
            vmem((n_prev + 1, rows, node_y), F32),
            vmem(layer_ids.shape, jnp.int32),
            pltpu.SMEM(viscosity.shape, F32),
            pltpu.SMEM(shifts.shape, F32),
            vmem((n_vec, 2, rows, half_y), F32),
            vmem((2, comps, 4, 2, 2) + tile, F32),
            vmem((2, comps, 2, 2) + tile, F32),
            vmem((2, comps, 4, 2) + tile, F32),
            vmem((2, comps, 2) + tile, F32),
            vmem((2, 9) + tile, F32),
            vmem((rounds, comps, 2, 18, half_y), F32),
            vmem((rounds, comps, 2, 18, half_y), F32),
            vmem((rounds, comps, 4, 2, half_y), F32),
            vmem((rounds, comps, 2, 18, half_y), F32),
            vmem((rounds, comps, 2, 18, half_y), F32),
            vmem((rounds, comps, 4, 2, half_y), F32),
            vmem((1, half_y), F32),
            vmem((n_lat * n_rad - 1, 1, half_y), F32),
            vmem((rounds * comps * 80 + 128 * comps, half_y), F32),
            vmem((comps, 40) + tile, F32),
            vmem((comps, 20) + tile, F32),
            vmem((8,) + tile, F32),
            vmem((8,) + tile, F32),
            vmem((20,) + tile, F32),
            vmem((24,) + tile, F32),
            vmem((3,) + tile, F32),
            vmem((4,) + tile, F32),
            vmem((4, 9) + tile, F32),
            vmem((comps, 6) + tile, F32),
            pltpu.SemaphoreType.DMA((5,)),
            pltpu.SemaphoreType.DMA((1,)),
            pltpu.SemaphoreType.DMA((3, comps)),
            pltpu.SemaphoreType.DMA((2,)),
            pltpu.SemaphoreType.DMA((2,)),
            pltpu.SemaphoreType.REGULAR((max(n_lat, n_rad).bit_length(),)),
        ],
        compiler_params=pltpu.CompilerParams(
            collective_id=0, has_side_effects=True, vmem_limit_bytes=65000000
        ),
    )(
        residual.reshape(rows, node_y),
        prev_basis.reshape(n_prev, rows, node_y),
        layer_ids,
        viscosity,
        shifts,
    )
    out, gram = pl.pallas_call(
        store,
        out_shape=(
            jax.ShapeDtypeStruct(out.shape, F32),
            jax.ShapeDtypeStruct(gram.shape, F32),
        ),
        in_specs=[vmem_spec] * 2,
        out_specs=(hbm_spec, hbm_spec),
        scratch_shapes=[pltpu.SemaphoreType.DMA((1 + n_steps,))],
    )(*(pltpu.with_memory_space_constraint(a, pltpu.VMEM) for a in (out, gram)))
    return out.reshape((n_steps,) + residual.shape), gram


def solution(mesh):
    placed = (
        P(None, "rad", "lat", None),
        P(None, None, "rad", "lat", None),
        P("rad", "lat", None),
        P(),
        P(),
    )
    return jax.shard_map(
        on_device,
        mesh=mesh,
        in_specs=placed,
        out_specs=(P(None, None, "rad", "lat", None), P()),
        check_vma=False,
    )
```

```python
import functools

import jax
import jax.numpy as jnp
from jax import lax
from jax.experimental import pallas as pl
from jax.experimental.pallas import tpu as pltpu
from jax.sharding import PartitionSpec as P

MESH = pl.DeviceIdType.MESH
F32 = jnp.float32

mass = (1.0 / 36, 1.0 / 12, 1.0 / 45)
stiff = (0.0, 1.0, 4.0 / 3)

DIRS = ((-1, -1), (-1, 0), (-1, 1), (0, -1), (0, 1), (1, -1), (1, 0), (1, 1))
R_DIRS = {(-1, 0): 0, (1, 0): 1}
X_DIRS = {(0, -1): 0, (0, 1): 1}
C_DIRS = {(-1, -1): 0, (-1, 1): 1, (1, -1): 2, (1, 1): 3}
FIRST = ((-1, 0), (0, -1), (-1, -1))
LAST = ((1, 0), (0, 1), (1, 1))
ROWS_X, ROWS_G, ROWS_A, ROWS_C = 0, 8, 12, 16
RIM = (
    ((1, 0), (0, 8), (4, 4), ROWS_X, 0),
    ((0, 1), (8, 8), (4, 4), ROWS_X, 4),
    ((1, 0), (16, 4), (7, 1), ROWS_G, 3),
    ((0, 1), (20, 4), (7, 1), ROWS_G, 7),
    ((1, 1), (24, 4), (7, 1), ROWS_C, 0),
    ((1, 1), (28, 4), (7, 1), ROWS_C, 4),
    ((1, -1), (32, 4), (4, 1), ROWS_A, 3),
    ((-1, 1), (36, 4), (3, 1), ROWS_A, 7),
)
EDGE_T, EDGE_U, EDGE_H, EDGE_G = 0, 4, 8, 20
EDGES = (
    ((-1, -1), (8, 6), EDGE_H, 0),
    ((-1, -1), (14, 6), EDGE_H, 4),
    ((-1, 0), (8, 6), EDGE_H + 6, 0),
    ((0, -1), (14, 6), EDGE_H + 6, 4),
    ((1, 0), (0, 4), EDGE_T, 0),
    ((0, 1), (4, 4), EDGE_U, 0),
    ((1, -1), (0, 4), EDGE_G, 0),
    ((-1, 1), (4, 4), EDGE_G, 4),
)
ETAS = (
    ((-1, 0), 2, 0, 3, 2, 0),
    ((0, -1), 2, 4, 3, 2, 4),
    ((1, 0), 0, 4, 4, 0, 0),
    ((0, 1), 1, 4, 4, 0, 4),
    ((1, 1), 0, 7, 1, 1, 0),
    ((-1, 1), 2, 0, 3, 3, 0),
    ((1, -1), 2, 4, 3, 3, 4),
)


def weight(a, b, c):
    return (
        stiff[a] * mass[b] * mass[c] + mass[a] * stiff[b] * mass[c] + mass[a] * mass[b] * stiff[c]
    )


def forward(u0, u1, u2):
    total = u0 + u2
    twice = u1 + u1
    return total + (twice + twice), u0 - u2, total - twice


def backward(m0, m1, m2):
    both = m0 + m2
    half = m0 + m0 - m2
    return both + m1, half + half, both - m1


def kernel(
    n_lat,
    n_rad,
    n_steps,
    n_prev,
    comps,
    res_ref,
    prev_ref,
    ids_hbm,
    visc_hbm,
    shift_hbm,
    out_ref,
    gram_ref,
    stage,
    ids_ref,
    visc_ref,
    shift_ref,
    work,
    vec,
    ghost_r,
    ghost_x,
    ghost_c,
    scaled,
    send_r,
    send_x,
    send_c,
    recv_r,
    recv_x,
    recv_c,
    gram_send,
    gram_recv,
    bulk,
    rim_send,
    rim_recv,
    block_send,
    block_recv,
    edge_send,
    edge_recv,
    eta_send,
    eta_recv,
    rim_scaled,
    rim_own,
    in_sem,
    send_sem,
    recv_sem,
    rim_sems,
    gram_sems,
    token_sem,
):
    n_dev = n_lat * n_rad
    lat = lax.axis_index("lat")
    rad = lax.axis_index("rad")
    me = lat * n_rad + rad
    rows = res_ref.shape[0]
    half_y = res_ref.shape[1] // 2
    n_vec = n_prev + n_steps + 1

    res_copy = pltpu.make_async_copy(res_ref, stage.at[n_prev], in_sem.at[0])
    res_copy.start()
    prev_copy = pltpu.make_async_copy(prev_ref, stage.at[pl.ds(0, n_prev)], in_sem.at[1])
    small_copies = [
        pltpu.make_async_copy(a, b, in_sem.at[2 + i])
        for i, (a, b) in enumerate(
            ((ids_hbm, ids_ref), (visc_hbm, visc_ref), (shift_hbm, shift_ref))
        )
    ]
    for copy in small_copies:
        copy.start()
    prev_copy.start()

    barrier = pltpu.get_barrier_semaphore()

    def around(far, dirs):
        total = 0
        for dr, dx in dirs:
            if not ((dr and n_rad <= far) or (dx and n_lat <= far)):
                total += jnp.where(within(dr * far, dx * far), 1, 0)
        return total

    def within(dr, dx):
        ok = None
        for pos, step, count in ((rad, dr, n_rad), (lat, dx, n_lat)):
            if step:
                one = (pos >= -step) if step < 0 else (pos < count - step)
                ok = one if ok is None else jnp.logical_and(ok, one)
        return ok

    def signal_around(sem, far, dirs):
        for dr, dx in dirs:
            if (dr and n_rad <= far) or (dx and n_lat <= far):
                continue

            @pl.when(within(dr * far, dx * far))
            def _(dr=dr, dx=dx):
                pl.semaphore_signal(
                    sem,
                    inc=1,
                    device_id={"lat": lat + dx * far, "rad": rad + dr * far},
                    device_id_type=MESH,
                )

    for ref in (edge_recv, eta_recv):
        ref[...] = jnp.zeros_like(ref)
    signal_around(barrier, 1, DIRS)

    for d in DIRS:
        if d in R_DIRS:
            ref, slot = recv_r, R_DIRS[d]
        elif d in X_DIRS:
            ref, slot = recv_x, X_DIRS[d]
        else:
            ref, slot = recv_c, C_DIRS[d]

        @pl.when(jnp.logical_not(within(-d[0], -d[1])))
        def _(ref=ref, slot=slot):
            ref[:, :, slot] = jnp.zeros(ref.shape[:2] + ref.shape[3:], F32)

    for ref in (rim_recv, block_recv):
        ref[...] = jnp.zeros_like(ref)

    for ref in (ghost_r, ghost_x, ghost_c):
        ref[0] = jnp.zeros(ref.shape[1:], F32)

    reaches = []
    while (2 << len(reaches)) < max(n_lat, n_rad) - 1:
        reaches.append(2 << len(reaches))

    def send_token(j):
        if j < len(reaches):
            signal_around(token_sem.at[j], reaches[j], DIRS)

    def take_token(j):
        if j < len(reaches):
            pl.semaphore_wait(token_sem.at[j], around(reaches[j], DIRS))

    rad_targets = [lax.rem(rad + d, n_rad) for d in range(n_rad)]

    def each_other(visit):
        def row(i, carry):
            lat_target = lax.rem(lat + n_lat // 2 + i, n_lat)
            for d in range(n_rad):
                ahead = lax.rem(n_lat // 2 + i, n_lat)
                visit(ahead * n_rad + d - 1, {"lat": lat_target, "rad": rad_targets[d]})
            return carry

        lax.fori_loop(0, n_lat // 2, row, 0, unroll=n_lat <= 8)
        lax.fori_loop(n_lat // 2 + 1, n_lat, row, 0, unroll=n_lat <= 8)
        for d in range(1, n_rad):
            visit(d - 1, {"lat": lat, "rad": rad_targets[d]})

    sub = lax.broadcasted_iota(jnp.int32, (8, half_y), 0)
    lane = lax.broadcasted_iota(jnp.int32, (8, half_y), 1)
    upper = sub >= 4
    ex = lax.rem(sub, 4)
    first_x = ex == 0
    last_x = ex == 3
    corner0 = sub == 0
    corner3 = sub == 3
    corner4 = sub == 4
    corner7 = sub == 7
    has_up = rad < n_rad - 1
    has_right = lat < n_lat - 1
    up_f = jnp.where(has_up, 1.0, 0.0).astype(F32)
    right_f = jnp.where(has_right, 1.0, 0.0).astype(F32)
    both_f = up_f * right_f

    def roll_s(v, k):
        return pltpu.roll(v, k % 8, 0)

    def keep(mask, v):
        return jnp.where(mask, v, 0.0)

    src = lax.broadcasted_iota(jnp.int32, (2 * half_y, 2 * half_y), 0)
    dst = lax.broadcasted_iota(jnp.int32, (2 * half_y, 2 * half_y), 1)
    split_perm = jnp.where(
        src == jnp.where(dst < half_y, 2 * dst, 2 * (dst - half_y) + 1), 1.0, 0.0
    ).astype(jnp.bfloat16)
    join_perm = jnp.where(
        dst == jnp.where(src < half_y, 2 * src, 2 * (src - half_y) + 1), 1.0, 0.0
    ).astype(jnp.bfloat16)

    def exact_dot(a, b):
        high = a.astype(jnp.bfloat16)
        rest = a - high.astype(F32)
        mid = rest.astype(jnp.bfloat16)
        low = (rest - mid.astype(F32)).astype(jnp.bfloat16)
        out = [jnp.dot(part, b, preferred_element_type=F32) for part in (high, mid, low)]
        return out[0] + (out[1] + out[2])

    def split_columns(i):
        z = exact_dot(stage[i], split_perm)
        work[i, 0] = z[:, :half_y]
        work[i, 1] = z[:, half_y:]

    def native(c, ro, p, h):
        return pl.ds(c * 64 + (4 * h + ro) * 8 + p, 4, stride=2)

    kinds = {}
    for a in range(3):
        for b in range(3):
            for c in range(3):
                key = tuple(sorted((a, b, c)))
                if key != (0, 0, 0) and key not in kinds:
                    kinds[key] = len(kinds)
    def copy_of(step, c, d):
        if d in R_DIRS:
            a, b = send_r.at[step, c, R_DIRS[d]], recv_r.at[step, c, R_DIRS[d]]
        elif d in X_DIRS:
            a, b = send_x.at[step, c, X_DIRS[d]], recv_x.at[step, c, X_DIRS[d]]
        else:
            a, b = send_c.at[step, c, C_DIRS[d]], recv_c.at[step, c, C_DIRS[d]]
        return pltpu.make_async_remote_copy(
            src_ref=a,
            dst_ref=b,
            send_sem=send_sem.at[0],
            recv_sem=recv_sem.at[step % 3, c],
            device_id={"lat": lat + d[1], "rad": rad + d[0]},
            device_id_type=MESH,
        )

    order = ((-1, -1), (1, 1), (-1, 1), (1, -1), (1, 0), (-1, 0), (0, 1), (0, -1))

    def dirs_of(step):
        wanted = FIRST if step == 0 else DIRS
        return [d for d in order if d in wanted]

    def start_round(step, c, among=DIRS):
        for d in dirs_of(step):
            if d not in among:
                continue

            @pl.when(within(*d))
            def _(d=d):
                copy_of(step, c, d).start()

    def places(pos, count):
        out = [(pos == 0, False, True), (pos == count - 1, True, False)]
        if count > 2:
            middle = jnp.logical_and(pos > 0, pos < count - 1)
            out.append((middle, True, True))
        return out if count > 1 else [(pos == 0, False, False)]

    def rows_of(sizes, down, up, left, right):
        have = {-1: {0: True, -1: down, 1: up}, 1: {0: True, -1: left, 1: right}}
        return sum(n for (dr, dx), n in sizes if have[-1][dr] and have[1][dx])

    def settle(sem, sizes):
        groups = {}
        for at_r, down, up in places(rad, n_rad):
            for at_x, left, right in places(lat, n_lat):
                n = rows_of(sizes, down, up, left, right)
                here = jnp.logical_and(at_r, at_x)
                groups[n] = jnp.logical_or(groups[n], here) if n in groups else here
        for n, here in groups.items():
            if n:

                @pl.when(here)
                def _(n=n):
                    pltpu.make_async_copy(bulk.at[pl.ds(0, n)], bulk.at[pl.ds(0, n)], sem).wait()

    def opposite(sizes):
        return [((-dr, -dx), n) for (dr, dx), n in sizes]

    def round_sizes(step):
        return [(d, 2 if d[0] and d[1] else 18) for d in dirs_of(step)]

    rim_sizes = [(d, comps * count * high) for d, (_, count), (_, high), _, _ in RIM]
    rim_sizes.append(((1, 1), comps * 8))
    edge_sizes = [(d, comps * count) for d, (_, count), _, _ in EDGES]
    edge_sizes += [(d, high) for d, _, _, high, _, _ in ETAS]

    def finish_round(step, c):
        settle(recv_sem.at[step % 3, c], opposite(round_sizes(step)))

    def remote(a, b, recv, d):
        @pl.when(within(*d))
        def _():
            pltpu.make_async_remote_copy(
                src_ref=a,
                dst_ref=b,
                send_sem=send_sem.at[0],
                recv_sem=recv,
                device_id={"lat": lat + d[1], "rad": rad + d[0]},
                device_id_type=MESH,
            ).start()

    def start_layers(c):
        for d, (first, count), (row, high), to, to_row in RIM[:2]:
            remote(
                rim_send.at[c, pl.ds(first, count), pl.ds(row, high)],
                rim_recv.at[c, pl.ds(to, count), pl.ds(to_row, high)],
                rim_sems.at[0],
                d,
            )

    def start_rim():
        for d, (first, count), (row, high), to, to_row in RIM[2:]:
            remote(
                rim_send.at[:, pl.ds(first, count), pl.ds(row, high)],
                rim_recv.at[:, pl.ds(to, count), pl.ds(to_row, high)],
                rim_sems.at[0],
                d,
            )
        remote(
            block_send.at[:, pl.ds(0, comps)], block_recv.at[:, pl.ds(0, comps)], rim_sems.at[0], (1, 1)
        )

    def start_edges(among):
        for d, (first, count), to, to_row in EDGES:
            if d in among:
                remote(
                    edge_send.at[pl.ds(first, count), pl.ds(0, comps)],
                    edge_recv.at[pl.ds(to, count), pl.ds(to_row, comps)],
                    rim_sems.at[1],
                    d,
                )

    def start_etas(among):
        for d, slot, row, high, to, to_row in ETAS:
            if d in among:
                remote(
                    eta_send.at[slot, pl.ds(row, high)],
                    eta_recv.at[to, pl.ds(to_row, high)],
                    rim_sems.at[1],
                    d,
                )

    def pack_x(vals, at):
        out = None
        for ro in range(4):
            moved = roll_s(vals[ro], ro - at)
            out = moved if out is None else jnp.where(ex == ro, moved, out)
        return out

    def y_pass(x0, x1, a, b, scale):
        nxt = keep(lane != half_y - 1, pltpu.roll(x0, half_y - 1, 1))
        m = list(forward(x0, x1, nxt))
        for j in range(3):
            key = tuple(sorted((a, b, j)))
            m[j] = m[j] * scale(kinds[key]) if key in kinds else None
        if m[0] is None:
            r0 = m[1] + m[2]
            r1 = -(m[2] + m[2])
            r2 = m[2] - m[1]
        else:
            r0, r1, r2 = backward(*m)
        return r0 + keep(lane != 0, pltpu.roll(r2, 1, 1)), r1

    def to_column(low, high):
        moved = jnp.where(sub == 6, roll_s(low, -1), high)
        return jnp.where(sub == 4, roll_s(low, 1), jnp.where(sub == 5, roll_s(high, 2), moved))

    def apply(k, c, send=True, hold=True):
        s = shift_ref[k]
        cur = k % 2
        new = 1 - cur
        u = {}
        gx = {}
        for q in range(2):
            for ro in range(4):
                gx[ro, q] = ghost_x[cur, c, ro, q]
                for p in range(2):
                    u[ro, p, q] = vec[cur, c, ro, p, q]
            gx[4, q] = jnp.where(upper, ghost_c[cur, c, q], roll_s(gx[0, q], 4))
            for p in range(2):
                u[4, p, q] = jnp.where(upper, ghost_r[cur, c, p, q], roll_s(u[0, p, q], 4))
            for ro in range(5):
                u[ro, 2, q] = jnp.where(last_x, gx[ro, q], roll_s(u[ro, 0, q], -1))
        res = {}
        for e in range(2):
            t = {}
            for p in range(3):
                for q in range(2):
                    t[0, p, q], t[1, p, q], t[2, p, q] = forward(
                        u[2 * e, p, q], u[2 * e + 1, p, q], u[2 * e + 2, p, q]
                    )
            w = {}
            for a in range(3):
                x = {}
                for q in range(2):
                    x[0, q], x[1, q], x[2, q] = forward(t[a, 0, q], t[a, 1, q], t[a, 2, q])
                for b in range(3):
                    x[b, 0], x[b, 1] = y_pass(x[b, 0], x[b, 1], a, b, lambda i: scaled[e, i])
                for q in range(2):
                    w[a, 0, q], w[a, 1, q], w[a, 2, q] = backward(x[0, q], x[1, q], x[2, q])
            for p in range(3):
                for q in range(2):
                    r = backward(w[0, p, q], w[1, p, q], w[2, p, q])
                    for i in range(3):
                        key = (2 * e + i, p, q)
                        res[key] = res[key] + r[i] if key in res else r[i]
        px = {}
        for q in range(2):
            for ro in range(5):
                edge = res[ro, 2, q]
                px[ro, q] = edge
                res[ro, 0, q] = res[ro, 0, q] + keep(ex != 0, roll_s(edge, 1))
            for p in range(2):
                res[0, p, q] = res[0, p, q] + keep(upper, roll_s(res[4, p, q], 4))
            px[0, q] = px[0, q] + keep(upper, roll_s(px[4, q], 4))
        step = k + 1
        send = send and step < n_steps
        ghosts = hold and step < n_steps
        for q in range(2):
            face = slice(8 * q, 8 * q + 8)
            edge = slice(16 + q, 17 + q)
            row = slice(q, q + 1)
            if send:
                send_r[step, c, 1, face] = jnp.where(upper, res[4, 1, q], roll_s(res[4, 0, q], 4))
                send_r[step, c, 1, edge] = px[4, q][7:8]
                send_x[step, c, 1, face] = pack_x([px[ro, q] for ro in range(4)], 3)
                send_x[step, c, 1, edge] = px[4, q][7:8]
                send_c[step, c, 3, row] = px[4, q][7:8]
                send_r[step, c, 0, face] = jnp.where(upper, roll_s(res[0, 1, q], 4), res[0, 0, q])
                send_r[step, c, 0, edge] = px[0, q][3:4]
                send_x[step, c, 0, face] = pack_x([res[ro, 0, q] for ro in range(4)], 0)
                send_x[step, c, 0, edge] = res[4, 0, q][4:5]
                send_c[step, c, 0, row] = res[0, 0, q][0:1]
                send_c[step, c, 1, row] = px[0, q][3:4]
                send_c[step, c, 2, row] = res[4, 0, q][4:5]
            for ro in range(4 if hold else 0):
                for p in range(2):
                    vec[new, c, ro, p, q] = res[ro, p, q] - s * u[ro, p, q]
                if ghosts:
                    ghost_x[new, c, ro, q] = px[ro, q] - s * gx[ro, q]
            if ghosts:
                for p in range(2):
                    ghost_r[new, c, p, q] = res[4, p, q] - s * u[4, p, q]
                ghost_c[new, c, q] = px[4, q] - s * gx[4, q]
            if step == n_steps - 1:
                for n in range(2):
                    rim_send[c, 24 + 2 * n + q] = px[2 + n, q]
                    rim_send[c, 28 + 2 * n + q] = res[4, n, q]
                    rim_send[c, 32 + 2 * n + q] = res[2 + n, 0, q]
                    rim_send[c, 36 + 2 * n + q] = res[0, n, q]

    def pack_rim(c):
        new = (n_steps - 1) % 2
        for q in range(2):
            for n in range(2):
                for p in range(2):
                    v = vec[new, c, 2 + n, p, q]
                    rim_send[c, 4 * n + 2 * p + q] = v
                    block_send[4 * n + 2 * p + q, c : c + 1] = v[7:8]
                    rim_send[c, 8 + 4 * n + 2 * p + q] = to_column(
                        vec[new, c, p, n, q], vec[new, c, 2 + p, n, q]
                    )
                rim_send[c, 16 + 2 * n + q] = ghost_x[new, c, 2 + n, q]
                rim_send[c, 20 + 2 * n + q] = ghost_r[new, c, n, q]

    group_last = lax.rem(sub, 4) == 3
    group_first = lax.rem(sub, 4) == 0

    def own_planes(c, cur):
        for q in range(2):
            side = jnp.where(corner3, ghost_x[cur, c, 0, q], roll_s(ghost_r[cur, c, 0, q], 3))
            for p in range(2):
                column = to_column(
                    roll_s(vec[cur, c, p, 0, q], 3), roll_s(vec[cur, c, 2 + p, 0, q], 3)
                )
                plane = jnp.where(upper, column, vec[cur, c, 0, p, q])
                rim_own[c, 2 * p + q] = plane
                if p == 0:
                    rim_own[c, 4 + q] = jnp.where(group_last, side, roll_s(plane, -1))

    def across(u):
        t = {}
        for p in range(3):
            for q in range(2):
                t[0, p, q], t[1, p, q], t[2, p, q] = forward(u[0, p, q], u[1, p, q], u[2, p, q])
        return t

    def rim_elements(t, scale, upper_plane=True, only_end=False):
        w = {}
        for a in range(3):
            x = {}
            for q in range(2):
                if only_end:
                    end = t[a, 2, q]
                    x[0, q], x[1, q], x[2, q] = end, -end, end
                else:
                    x[0, q], x[1, q], x[2, q] = forward(t[a, 0, q], t[a, 1, q], t[a, 2, q])
            for b in range(3):
                x[b, 0], x[b, 1] = y_pass(x[b, 0], x[b, 1], a, b, scale)
            for q in range(2):
                w[a, 0, q], w[a, 1, q], w[a, 2, q] = backward(x[0, q], x[1, q], x[2, q])
        sign = -1.0 if upper_plane else 1.0
        return {
            (p, q): w[0, p, q] + w[2, p, q] + (w[1, p, q] if sign > 0 else -w[1, p, q])
            for p in range(3)
            for q in range(2)
        }

    def add_planes(new, c, side, tip):
        for q in range(2):
            out = [side[0, q] + keep(~group_first, roll_s(side[2, q], 1)), side[1, q]]
            for p in range(2):
                for e in range(2):
                    ro = 2 * e + p
                    add = keep(corner4, roll_s(out[p], -(2 + e)))
                    add = jnp.where(corner0, roll_s(out[p], -(4 + e)), add)
                    if ro == 0:
                        add = add + keep(~upper, out[0]) + keep(corner0, roll_s(tip[2, q], -c))
                    vec[new, c, ro, 0, q] += add
            vec[new, c, 0, 1, q] += keep(~upper, out[1])

    def add_first():
        sides = {}
        corner = {}
        zero = jnp.zeros((8, half_y), F32)
        for c in range(comps):
            own_planes(c, 0)
            t = {}
            for q in range(2):
                u = [keep(group_last, roll_s(edge_recv[EDGE_G + 2 * n + q], 3 - c)) for n in range(2)]
                for p in range(2):
                    plane = rim_own[c, 2 * p + q]
                    t[0, p, q], t[1, p, q], t[2, p, q] = plane, -plane, plane
                    if p == 0:
                        part = keep(sub == c, roll_s(plane, c))
                        corner[2, 2, q] = corner[2, 2, q] + part if c else part
                t[0, 2, q], t[1, 2, q], t[2, 2, q] = forward(u[0], u[1], rim_own[c, 4 + q])
            sides[c] = rim_elements(t, lambda i: rim_scaled[0, i])
        for q in range(2):
            for n in range(2):
                corner[n, 2, q] = edge_recv[EDGE_T + 2 * n + q]
                corner[2, n, q] = edge_recv[EDGE_U + 2 * n + q]
                for p in range(2):
                    corner[n, p, q] = zero
        tip = rim_elements(across(corner), lambda i: rim_scaled[1, i])
        high = []
        for g in range(2):
            t = {}
            for q in range(2):
                t[0, 2, q], t[1, 2, q], t[2, 2, q] = forward(
                    *(edge_recv[EDGE_H + 6 * g + 2 * n + q] for n in range(3))
                )
            high.append(rim_elements(t, lambda i, g=g: rim_scaled[2 + g, i], False, True))
        for c in range(comps):
            add_planes(1, c, sides[c], tip)
            for q in range(2):
                far = sides[c][2, q]
                ghost_x[1, c, 0, q] += keep(corner3, far + roll_s(high[1][2, q], -1 - c))
                ghost_r[1, c, 0, q] += (
                    keep(corner4, roll_s(far, -3) + roll_s(high[1][2, q], 4 - c))
                    + keep(corner7, roll_s(high[0][0, q], 7 - c))
                )
                ghost_r[1, c, 1, q] += keep(corner7, roll_s(high[0][1, q], 7 - c))
                for t in range(2):
                    ghost_x[1, c, 2 + t, q] += keep(corner7, roll_s(high[0][t, q], 3 - c))
                ghost_c[1, c, q] += keep(
                    corner7, roll_s(high[0][2, q], 7 - c) + roll_s(high[0][2, q], 3 - c)
                )

    def add_rim():
        cur = (n_steps - 1) % 2
        new = 1 - cur
        inner = jnp.where(upper, up_f, right_f)
        corner = {}
        sides = {}
        for c in range(comps):
            u = {}
            for q in range(2):
                for n in range(2):
                    for p in range(2):
                        u[n, p, q] = rim_recv[c, ROWS_X + 4 * n + 2 * p + q]
                    u[n, 0, q] = u[n, 0, q] + rim_recv[c, ROWS_C + 2 * n + q]
                    ghost = rim_recv[c, ROWS_G + 2 * n + q] + rim_recv[c, ROWS_A + 2 * n + q]
                    u[n, 2, q] = jnp.where(group_last, ghost * inner, roll_s(u[n, 0, q], -1))
                for p in range(3):
                    u[2, p, q] = rim_own[c, 2 * p + q]
            for q in range(2):
                parts = {(2, 2): roll_s(u[2, 0, q], c)}
                for n in range(2):
                    parts[n, 2] = roll_s(u[n, 0, q], c)
                    parts[2, n] = roll_s(u[n, 0, q], c - 4)
                for key, part in parts.items():
                    part = keep(sub == c, part)
                    key = key + (q,)
                    corner[key] = corner[key] + part if c else part
            sides[c] = rim_elements(across(u), lambda i: rim_scaled[0, i])
        for q in range(2):
            for n in range(2):
                for p in range(2):
                    corner[n, p, q] = block_recv[4 * n + 2 * p + q]
        tip = rim_elements(across(corner), lambda i: rim_scaled[1, i])
        for c in range(comps):
            add_planes(new, c, sides[c], tip)

    def absorb(step, c):
        new = step % 2
        first, last = step == 0, False
        for q in range(2):
            face = slice(8 * q, 8 * q + 8)
            line = slice(16 + q, 17 + q)
            row = slice(q, q + 1)

            def spot(ref_row, mask):
                return keep(mask, jnp.broadcast_to(ref_row, (8, half_y)))

            if not first:
                from_low = recv_r[step, c, 1, face]
                from_left = recv_x[step, c, 1, face]
                corner = spot(recv_c[step, c, 3, row], corner0)
                vec[new, c, 0, 0, q] += (
                    keep(~upper, from_low) + keep(first_x, from_left) + corner
                )
                vec[new, c, 0, 1, q] += keep(~upper, roll_s(from_low, 4))
                for ro in range(1, 4):
                    vec[new, c, ro, 0, q] += keep(first_x, roll_s(from_left, -ro))
            if not last:
                from_up = recv_r[step, c, 0, face]
                from_right = recv_x[step, c, 0, face]
                add0 = keep(upper, roll_s(from_up, 4))
                add1 = keep(upper, from_up)
                edge = keep(last_x, roll_s(from_right, 3))
                far = (
                    spot(recv_r[step, c, 0, line], corner7)
                    + spot(recv_x[step, c, 0, line], corner7)
                    + spot(recv_c[step, c, 0, row], corner7)
                )
                if not first:
                    add0 = (
                        add0
                        + spot(recv_x[step, c, 1, line], corner4)
                        + spot(recv_c[step, c, 1, row], corner4)
                    )
                    edge = (
                        edge
                        + spot(recv_r[step, c, 1, line], corner3)
                        + spot(recv_c[step, c, 2, row], corner3)
                    )
                    add0 = add0 + ghost_r[new, c, 0, q]
                    add1 = add1 + ghost_r[new, c, 1, q]
                    edge = edge + ghost_x[new, c, 0, q]
                    far = far + ghost_c[new, c, q]
                ghost_r[new, c, 0, q] = add0 * up_f
                ghost_r[new, c, 1, q] = add1 * up_f
                ghost_x[new, c, 0, q] = edge * right_f
                ghost_c[new, c, q] = far * both_f
                for ro in range(1, 4):
                    edge = keep(last_x, roll_s(from_right, 3 - ro))
                    if not first:
                        edge = edge + ghost_x[new, c, ro, q]
                    ghost_x[new, c, ro, q] = edge * right_f

    def to_native(k, c, rim=False):
        cur = k % 2
        for ro in range(4):
            for p in range(2):
                if rim and ro and p:
                    continue
                for q in range(2):
                    v = vec[cur, c, ro, p, q]
                    for h in range(2):
                        work[n_prev + k, q, native(c, ro, p, h), :] = v[4 * h : 4 * h + 4]

    def write_out(k):
        z = jnp.concatenate([work[n_prev + k, 0], work[n_prev + k, 1]], 1)
        out_ref[k - 1] = exact_dot(z, join_perm)

    lane16 = lax.broadcasted_iota(jnp.int32, (16, half_y), 1)
    row16 = lax.broadcasted_iota(jnp.int32, (16, half_y), 0)

    def gram_part(i, acc, first, count):
        def chunk(t, acc):
            at = pl.ds(pl.multiple_of(8 * t, 8), 8)
            for q in range(2):
                mine = work[i, q, at, :]
                acc = tuple(
                    acc[j] + mine * (mine if j == i else work[j, q, at, :]) for j in range(i + 1)
                )
            return acc

        return lax.fori_loop(first, first + count, chunk, acc, unroll=4)

    def gram_add(i, acc, at, mask):
        for q in range(2):
            mine = work[i, q, at, :]
            mine = mine if mask is None else keep(mask, mine)
            acc = tuple(
                acc[j] + mine * (mine if j == i else work[j, q, at, :]) for j in range(i + 1)
            )
        return acc

    def gram_zero(i):
        return (jnp.zeros((8, half_y), F32),) * (i + 1)

    def gram_close(i, acc):
        sums = [jnp.sum(a, axis=0, keepdims=True) for a in acc]
        sums.append(jnp.zeros((16 - len(sums), half_y), F32))
        total = jnp.sum(jnp.concatenate(sums, 0), axis=1, keepdims=True)
        hit = jnp.logical_or(lane16 == i * n_vec + row16, lane16 == row16 * n_vec + i)
        hit = jnp.logical_and(hit, row16 <= i)
        return jnp.sum(jnp.where(hit, jnp.broadcast_to(total, hit.shape), 0.0), 0, keepdims=True)

    def gram_row(i):
        return gram_close(i, gram_part(i, gram_zero(i), 0, rows // 8))

    res_copy.wait()
    edge_rows = []
    for c in range(comps):
        picked = [2 * x + p for p in range(2) for x in range(4)] + [8 * r for r in range(8)]
        edge_rows += [stage[n_prev, pl.ds(c * 64 + at, 1), :] for at in picked]
    edge = exact_dot(jnp.concatenate(edge_rows, 0), split_perm)
    zero_rows = jnp.zeros((2, half_y), F32)
    for c in range(comps):
        send_r[0, c, 0, 16:18] = zero_rows
        send_x[0, c, 0, 16:18] = zero_rows
        for q in range(2):
            face = slice(8 * q, 8 * q + 8)
            lanes = slice(half_y * q, half_y * (q + 1))
            send_r[0, c, 0, face] = edge[16 * c : 16 * c + 8, lanes]
            send_x[0, c, 0, face] = edge[16 * c + 8 : 16 * c + 16, lanes]
            send_c[0, c, 0, q : q + 1] = edge[16 * c : 16 * c + 1, lanes]
            along = [8 + 6, 8 + 7, 3, 7, 8, 9, 10, 0, 4, 1]
            for slot, row in enumerate(along):
                at = 16 * c + row
                edge_send[2 * slot + q, c : c + 1] = edge[at : at + 1, lanes]

    pl.semaphore_wait(barrier, around(1, DIRS))
    for c in range(comps):
        start_round(0, c)
    start_edges(DIRS)
    split_columns(n_prev)
    for c in range(comps):
        for ro in range(4):
            for p in range(2):
                for q in range(2):
                    vec[0, c, ro, p, q] = jnp.concatenate(
                        [work[n_prev, q, native(c, ro, p, h), :] for h in range(2)], 0
                    )
    for copy in small_copies:
        copy.wait()
    etas = []
    for e in range(2):
        ids = jnp.concatenate([ids_ref[e], ids_ref[2 + e]], 0)
        eta = jnp.zeros((8, half_y), F32)
        for layer in range(visc_ref.shape[0]):
            eta = eta + jnp.where(ids == layer, visc_ref[layer], 0.0)
        etas.append(eta)
        for key, i in kinds.items():
            scaled[e, i] = eta * weight(*key)
    eta_send[0] = etas[1]
    eta_send[1] = to_column(*etas)
    eta_send[2] = jnp.where(
        upper,
        jnp.broadcast_to(etas[1][4:5], (8, half_y)),
        jnp.broadcast_to(etas[0][3:4], (8, half_y)),
    )
    start_etas(DIRS)
    for c in range(comps):
        apply(0, c, hold=False)
        start_round(1, c)

    total = jnp.zeros((1, half_y), F32)
    prev_copy.wait()
    for i in range(n_prev):
        split_columns(i)

    for i in range(n_prev + 1):
        total = total + gram_row(i)

    for c in range(comps):
        finish_round(0, c)
        absorb(0, c)
        apply(0, c, send=False)
    settle(rim_sems.at[1], opposite(edge_sizes))
    tip_eta = jnp.broadcast_to(eta_recv[1, 0:1], (8, half_y))
    for key, i in kinds.items():
        for slot in range(4):
            rim_scaled[slot, i] = (tip_eta if slot == 1 else eta_recv[slot]) * weight(*key)
    add_first()
    for k in range(1, n_steps - 1):
        for c in range(comps):
            finish_round(k, c)
            absorb(k, c)
            apply(k, c)
            start_round(k + 1, c)
            if k == n_steps - 2:
                if c:
                    start_layers(c - 1)
                pack_rim(c)
        if k == n_steps - 2:
            start_layers(comps - 1)
            start_rim()
        if k == n_steps - 2:
            send_token(0)
        for c in range(comps):
            to_native(k, c)
        write_out(k)
        total = total + gram_row(n_prev + k)
    assert n_steps >= 3
    k = n_steps - 1
    per = rows // 8 // comps
    whole = gram_zero(n_vec - 2)
    acc = gram_zero(n_vec - 1)
    for c in range(comps):
        finish_round(k, c)
        absorb(k, c)
        apply(k, c)
        if c == 0:
            take_token(0)
            send_token(1)
        own_planes(c, k % 2)
        to_native(k, c)
        to_native(n_steps, c)
        whole = gram_part(n_vec - 2, whole, c * per, per)
        acc = lax.fori_loop(
            8 * c + 1,
            8 * c + 8,
            lambda t, acc: gram_add(
                n_vec - 1, acc, pl.ds(pl.multiple_of(8 * t, 8), 8), jnp.logical_not(corner0)
            ),
            acc,
            unroll=7,
        )
    total = total + gram_close(n_vec - 2, whole)
    settle(rim_sems.at[0], opposite(rim_sizes))
    add_rim()
    for c in range(comps):
        to_native(n_steps, c, rim=True)
    for c in range(comps):
        acc = gram_add(n_vec - 1, acc, pl.ds(c * 64, 8), None)
        acc = gram_add(n_vec - 1, acc, pl.ds(c * 64, 8, stride=8), jnp.logical_not(corner0))
    total = total + gram_close(n_vec - 1, acc)
    gram_send[...] = total

    def scatter(slot, device):
        pltpu.make_async_remote_copy(
            src_ref=gram_send,
            dst_ref=gram_recv.at[slot],
            send_sem=gram_sems.at[0],
            recv_sem=gram_sems.at[1],
            device_id=device,
            device_id_type=MESH,
        ).start()

    for j in range(1, len(reaches)):
        take_token(j)
        send_token(j + 1)
    each_other(scatter)
    write_out(n_steps - 1)
    write_out(n_steps)
    sent = [size for step in range(n_steps) for size in round_sizes(step)] * comps
    settle(send_sem.at[0], sent + rim_sizes + edge_sizes)
    for i in range(2):
        pltpu.make_async_copy(gram_recv, gram_recv, gram_sems.at[i]).wait()
    full = (total + jnp.sum(gram_recv[...], axis=0)) * (1.0 / (rows * 2 * half_y * n_dev))
    for i in range(n_vec):
        line = full if i == 0 else pltpu.roll(full, half_y - i * n_vec, 1)
        gram_ref[i : i + 1, :] = line[:, :n_vec]


def store(vec_ref, gram_ref, vec_out, gram_out, sems):
    copies = [pltpu.make_async_copy(gram_ref, gram_out, sems.at[0])]
    for i in range(vec_ref.shape[0]):
        copies.append(pltpu.make_async_copy(vec_ref.at[i], vec_out.at[i], sems.at[1 + i]))
    for copy in copies:
        copy.start()
    for copy in copies:
        copy.wait()


def on_device(residual, prev_basis, layer_ids, viscosity, shifts):
    n_lat = lax.axis_size("lat")
    n_rad = lax.axis_size("rad")
    comps, node_r, node_x, node_y = residual.shape
    n_prev = prev_basis.shape[0]
    n_steps = shifts.shape[0]
    n_vec = n_prev + n_steps + 1
    rows = comps * node_r * node_x
    half_y = node_y // 2
    assert node_r == 8 and node_x == 8 and half_y == 128
    rounds = n_steps
    tile = (8, half_y)
    vmem = pltpu.VMEM
    hbm_spec = pl.BlockSpec(memory_space=pltpu.HBM)
    vmem_spec = pl.BlockSpec(memory_space=pltpu.VMEM)
    out, gram = pl.pallas_call(
        functools.partial(kernel, n_lat, n_rad, n_steps, n_prev, comps),
        out_shape=(
            pltpu.VMEM((n_steps, rows, node_y), F32),
            pltpu.VMEM((n_vec, n_vec), F32),
        ),
        in_specs=[hbm_spec] * 5,
        out_specs=(vmem_spec, vmem_spec),
        scratch_shapes=[
            vmem((n_prev + 1, rows, node_y), F32),
            vmem(layer_ids.shape, jnp.int32),
            pltpu.SMEM(viscosity.shape, F32),
            pltpu.SMEM(shifts.shape, F32),
            vmem((n_vec, 2, rows, half_y), F32),
            vmem((2, comps, 4, 2, 2) + tile, F32),
            vmem((2, comps, 2, 2) + tile, F32),
            vmem((2, comps, 4, 2) + tile, F32),
            vmem((2, comps, 2) + tile, F32),
            vmem((2, 9) + tile, F32),
            vmem((rounds, comps, 2, 18, half_y), F32),
            vmem((rounds, comps, 2, 18, half_y), F32),
            vmem((rounds, comps, 4, 2, half_y), F32),
            vmem((rounds, comps, 2, 18, half_y), F32),
            vmem((rounds, comps, 2, 18, half_y), F32),
            vmem((rounds, comps, 4, 2, half_y), F32),
            vmem((1, half_y), F32),
            vmem((n_lat * n_rad - 1, 1, half_y), F32),
            vmem((rounds * comps * 80 + 128 * comps, half_y), F32),
            vmem((comps, 40) + tile, F32),
            vmem((comps, 20) + tile, F32),
            vmem((8,) + tile, F32),
            vmem((8,) + tile, F32),
            vmem((20,) + tile, F32),
            vmem((24,) + tile, F32),
            vmem((3,) + tile, F32),
            vmem((4,) + tile, F32),
            vmem((4, 9) + tile, F32),
            vmem((comps, 6) + tile, F32),
            pltpu.SemaphoreType.DMA((5,)),
            pltpu.SemaphoreType.DMA((1,)),
            pltpu.SemaphoreType.DMA((3, comps)),
            pltpu.SemaphoreType.DMA((2,)),
            pltpu.SemaphoreType.DMA((2,)),
            pltpu.SemaphoreType.REGULAR((max(n_lat, n_rad).bit_length(),)),
        ],
        compiler_params=pltpu.CompilerParams(
            collective_id=0, has_side_effects=True, vmem_limit_bytes=65000000
        ),
    )(
        residual.reshape(rows, node_y),
        prev_basis.reshape(n_prev, rows, node_y),
        layer_ids,
        viscosity,
        shifts,
    )
    out, gram = pl.pallas_call(
        store,
        out_shape=(
            jax.ShapeDtypeStruct(out.shape, F32),
            jax.ShapeDtypeStruct(gram.shape, F32),
        ),
        in_specs=[vmem_spec] * 2,
        out_specs=(hbm_spec, hbm_spec),
        scratch_shapes=[pltpu.SemaphoreType.DMA((1 + n_steps,))],
    )(*(pltpu.with_memory_space_constraint(a, pltpu.VMEM) for a in (out, gram)))
    return out.reshape((n_steps,) + residual.shape), gram


def solution(mesh):
    placed = (
        P(None, "rad", "lat", None),
        P(None, None, "rad", "lat", None),
        P("rad", "lat", None),
        P(),
        P(),
    )
    return jax.shard_map(
        on_device,
        mesh=mesh,
        in_specs=placed,
        out_specs=(P(None, None, "rad", "lat", None), P()),
        check_vma=False,
    )
```

```python
import functools

import jax
import jax.numpy as jnp
from jax import lax
from jax.experimental import pallas as pl
from jax.experimental.pallas import tpu as pltpu
from jax.sharding import PartitionSpec as P

MESH = pl.DeviceIdType.MESH
F32 = jnp.float32

mass = (1.0 / 36, 1.0 / 12, 1.0 / 45)
stiff = (0.0, 1.0, 4.0 / 3)

DIRS = ((-1, -1), (-1, 0), (-1, 1), (0, -1), (0, 1), (1, -1), (1, 0), (1, 1))
R_DIRS = {(-1, 0): 0, (1, 0): 1}
X_DIRS = {(0, -1): 0, (0, 1): 1}
C_DIRS = {(-1, -1): 0, (-1, 1): 1, (1, -1): 2, (1, 1): 3}
FIRST = ((-1, 0), (0, -1), (-1, -1))
LAST = ((1, 0), (0, 1), (1, 1))
ROWS_X, ROWS_G, ROWS_A, ROWS_C = 0, 8, 12, 16
RIM = (
    ((1, 0), (0, 8), (4, 4), ROWS_X, 0),
    ((0, 1), (8, 8), (4, 4), ROWS_X, 4),
    ((1, 0), (16, 4), (7, 1), ROWS_G, 3),
    ((0, 1), (20, 4), (7, 1), ROWS_G, 7),
    ((1, 1), (24, 4), (7, 1), ROWS_C, 0),
    ((1, 1), (28, 4), (7, 1), ROWS_C, 4),
    ((1, -1), (32, 4), (4, 1), ROWS_A, 3),
    ((-1, 1), (36, 4), (3, 1), ROWS_A, 7),
)
EDGE_T, EDGE_U, EDGE_H, EDGE_G = 0, 4, 8, 16
EDGES = (
    ((-1, -1), (8, 4), EDGE_H, 0),
    ((-1, -1), (12, 4), EDGE_H, 4),
    ((-1, 0), (8, 4), EDGE_H + 4, 0),
    ((0, -1), (12, 4), EDGE_H + 4, 4),
    ((1, 0), (0, 4), EDGE_T, 0),
    ((0, 1), (4, 4), EDGE_U, 0),
    ((1, -1), (0, 4), EDGE_G, 0),
    ((-1, 1), (4, 4), EDGE_G, 4),
)
ETAS = (
    ((-1, 0), 2, 0, 3, 2, 0),
    ((0, -1), 2, 4, 3, 2, 4),
    ((1, 0), 0, 4, 4, 0, 0),
    ((0, 1), 1, 4, 4, 0, 4),
    ((1, 1), 0, 7, 1, 1, 0),
    ((-1, 1), 2, 0, 3, 3, 0),
    ((1, -1), 2, 4, 3, 3, 4),
)


def weight(a, b, c):
    return (
        stiff[a] * mass[b] * mass[c] + mass[a] * stiff[b] * mass[c] + mass[a] * mass[b] * stiff[c]
    )


def forward(u0, u1, u2):
    total = u0 + u2
    twice = u1 + u1
    return total + (twice + twice), u0 - u2, total - twice


def backward(m0, m1, m2):
    both = m0 + m2
    half = m0 + m0 - m2
    return both + m1, half + half, both - m1


def kernel(
    n_lat,
    n_rad,
    n_steps,
    n_prev,
    comps,
    res_ref,
    prev_ref,
    ids_hbm,
    visc_hbm,
    shift_hbm,
    out_ref,
    gram_ref,
    stage,
    ids_ref,
    visc_ref,
    shift_ref,
    work,
    vec,
    ghost_r,
    ghost_x,
    ghost_c,
    scaled,
    send_r,
    send_x,
    send_c,
    recv_r,
    recv_x,
    recv_c,
    gram_send,
    gram_recv,
    bulk,
    rim_send,
    rim_recv,
    block_send,
    block_recv,
    edge_send,
    edge_recv,
    eta_send,
    eta_recv,
    rim_scaled,
    rim_own,
    in_sem,
    send_sem,
    recv_sem,
    rim_sems,
    gram_sems,
    token_sem,
):
    n_dev = n_lat * n_rad
    lat = lax.axis_index("lat")
    rad = lax.axis_index("rad")
    me = lat * n_rad + rad
    rows = res_ref.shape[0]
    half_y = res_ref.shape[1] // 2
    n_vec = n_prev + n_steps + 1

    res_copy = pltpu.make_async_copy(res_ref, stage.at[n_prev], in_sem.at[0])
    res_copy.start()
    prev_copy = pltpu.make_async_copy(prev_ref, stage.at[pl.ds(0, n_prev)], in_sem.at[1])
    small_copies = [
        pltpu.make_async_copy(a, b, in_sem.at[2 + i])
        for i, (a, b) in enumerate(
            ((ids_hbm, ids_ref), (visc_hbm, visc_ref), (shift_hbm, shift_ref))
        )
    ]
    for copy in small_copies:
        copy.start()
    prev_copy.start()

    barrier = pltpu.get_barrier_semaphore()

    def around(far, dirs):
        total = 0
        for dr, dx in dirs:
            if not ((dr and n_rad <= far) or (dx and n_lat <= far)):
                total += jnp.where(within(dr * far, dx * far), 1, 0)
        return total

    def within(dr, dx):
        ok = None
        for pos, step, count in ((rad, dr, n_rad), (lat, dx, n_lat)):
            if step:
                one = (pos >= -step) if step < 0 else (pos < count - step)
                ok = one if ok is None else jnp.logical_and(ok, one)
        return ok

    def signal_around(sem, far, dirs):
        for dr, dx in dirs:
            if (dr and n_rad <= far) or (dx and n_lat <= far):
                continue

            @pl.when(within(dr * far, dx * far))
            def _(dr=dr, dx=dx):
                pl.semaphore_signal(
                    sem,
                    inc=1,
                    device_id={"lat": lat + dx * far, "rad": rad + dr * far},
                    device_id_type=MESH,
                )

    for ref in (edge_recv, eta_recv):
        ref[...] = jnp.zeros_like(ref)
    signal_around(barrier, 1, DIRS)

    for d in DIRS:
        if d in R_DIRS:
            ref, slot = recv_r, R_DIRS[d]
        elif d in X_DIRS:
            ref, slot = recv_x, X_DIRS[d]
        else:
            ref, slot = recv_c, C_DIRS[d]

        @pl.when(jnp.logical_not(within(-d[0], -d[1])))
        def _(ref=ref, slot=slot):
            ref[:, :, slot] = jnp.zeros(ref.shape[:2] + ref.shape[3:], F32)

    for ref in (rim_recv, block_recv):
        ref[...] = jnp.zeros_like(ref)

    for ref in (ghost_r, ghost_x, ghost_c):
        ref[0] = jnp.zeros(ref.shape[1:], F32)

    reaches = []
    while (2 << len(reaches)) < max(n_lat, n_rad) - 1:
        reaches.append(2 << len(reaches))

    def send_token(j):
        if j < len(reaches):
            signal_around(token_sem.at[j], reaches[j], DIRS)

    def take_token(j):
        if j < len(reaches):
            pl.semaphore_wait(token_sem.at[j], around(reaches[j], DIRS))

    rad_targets = [lax.rem(rad + d, n_rad) for d in range(n_rad)]

    def each_other(visit):
        def row(i, carry):
            lat_target = lax.rem(lat + n_lat // 2 + i, n_lat)
            for d in range(n_rad):
                ahead = lax.rem(n_lat // 2 + i, n_lat)
                visit(ahead * n_rad + d - 1, {"lat": lat_target, "rad": rad_targets[d]})
            return carry

        lax.fori_loop(0, n_lat // 2, row, 0, unroll=n_lat <= 8)
        lax.fori_loop(n_lat // 2 + 1, n_lat, row, 0, unroll=n_lat <= 8)
        for d in range(1, n_rad):
            visit(d - 1, {"lat": lat, "rad": rad_targets[d]})

    sub = lax.broadcasted_iota(jnp.int32, (8, half_y), 0)
    lane = lax.broadcasted_iota(jnp.int32, (8, half_y), 1)
    upper = sub >= 4
    ex = lax.rem(sub, 4)
    first_x = ex == 0
    last_x = ex == 3
    corner0 = sub == 0
    corner3 = sub == 3
    corner4 = sub == 4
    corner7 = sub == 7
    has_up = rad < n_rad - 1
    has_right = lat < n_lat - 1
    up_f = jnp.where(has_up, 1.0, 0.0).astype(F32)
    right_f = jnp.where(has_right, 1.0, 0.0).astype(F32)
    both_f = up_f * right_f

    def roll_s(v, k):
        return pltpu.roll(v, k % 8, 0)

    def keep(mask, v):
        return jnp.where(mask, v, 0.0)

    src = lax.broadcasted_iota(jnp.int32, (2 * half_y, 2 * half_y), 0)
    dst = lax.broadcasted_iota(jnp.int32, (2 * half_y, 2 * half_y), 1)
    split_perm = jnp.where(
        src == jnp.where(dst < half_y, 2 * dst, 2 * (dst - half_y) + 1), 1.0, 0.0
    ).astype(jnp.bfloat16)
    join_perm = jnp.where(
        dst == jnp.where(src < half_y, 2 * src, 2 * (src - half_y) + 1), 1.0, 0.0
    ).astype(jnp.bfloat16)

    def exact_dot(a, b):
        high = a.astype(jnp.bfloat16)
        rest = a - high.astype(F32)
        mid = rest.astype(jnp.bfloat16)
        low = (rest - mid.astype(F32)).astype(jnp.bfloat16)
        out = [jnp.dot(part, b, preferred_element_type=F32) for part in (high, mid, low)]
        return out[0] + (out[1] + out[2])

    def split_columns(i):
        z = exact_dot(stage[i], split_perm)
        work[i, 0] = z[:, :half_y]
        work[i, 1] = z[:, half_y:]

    def native(c, ro, p, h):
        return pl.ds(c * 64 + (4 * h + ro) * 8 + p, 4, stride=2)

    kinds = {}
    for a in range(3):
        for b in range(3):
            for c in range(3):
                key = tuple(sorted((a, b, c)))
                if key != (0, 0, 0) and key not in kinds:
                    kinds[key] = len(kinds)
    def copy_of(step, c, d):
        if d in R_DIRS:
            a, b = send_r.at[step, c, R_DIRS[d]], recv_r.at[step, c, R_DIRS[d]]
        elif d in X_DIRS:
            a, b = send_x.at[step, c, X_DIRS[d]], recv_x.at[step, c, X_DIRS[d]]
        else:
            a, b = send_c.at[step, c, C_DIRS[d]], recv_c.at[step, c, C_DIRS[d]]
        return pltpu.make_async_remote_copy(
            src_ref=a,
            dst_ref=b,
            send_sem=send_sem.at[0],
            recv_sem=recv_sem.at[step % 3, c],
            device_id={"lat": lat + d[1], "rad": rad + d[0]},
            device_id_type=MESH,
        )

    order = ((-1, -1), (1, 1), (-1, 1), (1, -1), (1, 0), (-1, 0), (0, 1), (0, -1))

    def dirs_of(step):
        wanted = FIRST if step == 0 else DIRS
        return [d for d in order if d in wanted]

    def start_round(step, c, among=DIRS):
        for d in dirs_of(step):
            if d not in among:
                continue

            @pl.when(within(*d))
            def _(d=d):
                copy_of(step, c, d).start()

    def places(pos, count):
        out = [(pos == 0, False, True), (pos == count - 1, True, False)]
        if count > 2:
            middle = jnp.logical_and(pos > 0, pos < count - 1)
            out.append((middle, True, True))
        return out if count > 1 else [(pos == 0, False, False)]

    def rows_of(sizes, down, up, left, right):
        have = {-1: {0: True, -1: down, 1: up}, 1: {0: True, -1: left, 1: right}}
        return sum(n for (dr, dx), n in sizes if have[-1][dr] and have[1][dx])

    def settle(sem, sizes):
        groups = {}
        for at_r, down, up in places(rad, n_rad):
            for at_x, left, right in places(lat, n_lat):
                n = rows_of(sizes, down, up, left, right)
                here = jnp.logical_and(at_r, at_x)
                groups[n] = jnp.logical_or(groups[n], here) if n in groups else here
        for n, here in groups.items():
            if n:

                @pl.when(here)
                def _(n=n):
                    pltpu.make_async_copy(bulk.at[pl.ds(0, n)], bulk.at[pl.ds(0, n)], sem).wait()

    def opposite(sizes):
        return [((-dr, -dx), n) for (dr, dx), n in sizes]

    def round_sizes(step):
        return [(d, 2 if d[0] and d[1] else 18) for d in dirs_of(step)]

    rim_sizes = [(d, comps * count * high) for d, (_, count), (_, high), _, _ in RIM]
    rim_sizes.append(((1, 1), comps * 8))
    edge_sizes = [(d, comps * count) for d, (_, count), _, _ in EDGES]
    edge_sizes += [(d, high) for d, _, _, high, _, _ in ETAS]

    def finish_round(step, c):
        settle(recv_sem.at[step % 3, c], opposite(round_sizes(step)))

    def remote(a, b, recv, d):
        @pl.when(within(*d))
        def _():
            pltpu.make_async_remote_copy(
                src_ref=a,
                dst_ref=b,
                send_sem=send_sem.at[0],
                recv_sem=recv,
                device_id={"lat": lat + d[1], "rad": rad + d[0]},
                device_id_type=MESH,
            ).start()

    def start_layers(c):
        for d, (first, count), (row, high), to, to_row in RIM[:2]:
            remote(
                rim_send.at[c, pl.ds(first, count), pl.ds(row, high)],
                rim_recv.at[c, pl.ds(to, count), pl.ds(to_row, high)],
                rim_sems.at[0],
                d,
            )

    def start_rim():
        for d, (first, count), (row, high), to, to_row in RIM[2:]:
            remote(
                rim_send.at[:, pl.ds(first, count), pl.ds(row, high)],
                rim_recv.at[:, pl.ds(to, count), pl.ds(to_row, high)],
                rim_sems.at[0],
                d,
            )
        remote(
            block_send.at[:, pl.ds(0, comps)], block_recv.at[:, pl.ds(0, comps)], rim_sems.at[0], (1, 1)
        )

    def start_edges(among):
        for d, (first, count), to, to_row in EDGES:
            if d in among:
                remote(
                    edge_send.at[pl.ds(first, count), pl.ds(0, comps)],
                    edge_recv.at[pl.ds(to, count), pl.ds(to_row, comps)],
                    rim_sems.at[1],
                    d,
                )

    def start_etas(among):
        for d, slot, row, high, to, to_row in ETAS:
            if d in among:
                remote(
                    eta_send.at[slot, pl.ds(row, high)],
                    eta_recv.at[to, pl.ds(to_row, high)],
                    rim_sems.at[1],
                    d,
                )

    def pack_x(vals, at):
        out = None
        for ro in range(4):
            moved = roll_s(vals[ro], ro - at)
            out = moved if out is None else jnp.where(ex == ro, moved, out)
        return out

    def y_pass(x0, x1, a, b, scale):
        nxt = keep(lane != half_y - 1, pltpu.roll(x0, half_y - 1, 1))
        m = list(forward(x0, x1, nxt))
        for j in range(3):
            key = tuple(sorted((a, b, j)))
            m[j] = m[j] * scale(kinds[key]) if key in kinds else None
        if m[0] is None:
            r0 = m[1] + m[2]
            r1 = -(m[2] + m[2])
            r2 = m[2] - m[1]
        else:
            r0, r1, r2 = backward(*m)
        return r0 + keep(lane != 0, pltpu.roll(r2, 1, 1)), r1

    def to_column(low, high):
        moved = jnp.where(sub == 6, roll_s(low, -1), high)
        return jnp.where(sub == 4, roll_s(low, 1), jnp.where(sub == 5, roll_s(high, 2), moved))

    def apply(k, c, send=True, hold=True):
        s = shift_ref[k]
        cur = k % 2
        new = 1 - cur
        u = {}
        gx = {}
        for q in range(2):
            for ro in range(4):
                gx[ro, q] = ghost_x[cur, c, ro, q]
                for p in range(2):
                    u[ro, p, q] = vec[cur, c, ro, p, q]
            gx[4, q] = jnp.where(upper, ghost_c[cur, c, q], roll_s(gx[0, q], 4))
            for p in range(2):
                u[4, p, q] = jnp.where(upper, ghost_r[cur, c, p, q], roll_s(u[0, p, q], 4))
            for ro in range(5):
                u[ro, 2, q] = jnp.where(last_x, gx[ro, q], roll_s(u[ro, 0, q], -1))
        res = {}
        for e in range(2):
            t = {}
            for p in range(3):
                for q in range(2):
                    t[0, p, q], t[1, p, q], t[2, p, q] = forward(
                        u[2 * e, p, q], u[2 * e + 1, p, q], u[2 * e + 2, p, q]
                    )
            w = {}
            for a in range(3):
                x = {}
                for q in range(2):
                    x[0, q], x[1, q], x[2, q] = forward(t[a, 0, q], t[a, 1, q], t[a, 2, q])
                for b in range(3):
                    x[b, 0], x[b, 1] = y_pass(x[b, 0], x[b, 1], a, b, lambda i: scaled[e, i])
                for q in range(2):
                    w[a, 0, q], w[a, 1, q], w[a, 2, q] = backward(x[0, q], x[1, q], x[2, q])
            for p in range(3):
                for q in range(2):
                    r = backward(w[0, p, q], w[1, p, q], w[2, p, q])
                    for i in range(3):
                        key = (2 * e + i, p, q)
                        res[key] = res[key] + r[i] if key in res else r[i]
        px = {}
        for q in range(2):
            for ro in range(5):
                edge = res[ro, 2, q]
                px[ro, q] = edge
                res[ro, 0, q] = res[ro, 0, q] + keep(ex != 0, roll_s(edge, 1))
            for p in range(2):
                res[0, p, q] = res[0, p, q] + keep(upper, roll_s(res[4, p, q], 4))
            px[0, q] = px[0, q] + keep(upper, roll_s(px[4, q], 4))
        step = k + 1
        send = send and step < n_steps
        ghosts = hold and step < n_steps
        for q in range(2):
            face = slice(8 * q, 8 * q + 8)
            edge = slice(16 + q, 17 + q)
            row = slice(q, q + 1)
            if send:
                send_r[step, c, 1, face] = jnp.where(upper, res[4, 1, q], roll_s(res[4, 0, q], 4))
                send_r[step, c, 1, edge] = px[4, q][7:8]
                send_x[step, c, 1, face] = pack_x([px[ro, q] for ro in range(4)], 3)
                send_x[step, c, 1, edge] = px[4, q][7:8]
                send_c[step, c, 3, row] = px[4, q][7:8]
                send_r[step, c, 0, face] = jnp.where(upper, roll_s(res[0, 1, q], 4), res[0, 0, q])
                send_r[step, c, 0, edge] = px[0, q][3:4]
                send_x[step, c, 0, face] = pack_x([res[ro, 0, q] for ro in range(4)], 0)
                send_x[step, c, 0, edge] = res[4, 0, q][4:5]
                send_c[step, c, 0, row] = res[0, 0, q][0:1]
                send_c[step, c, 1, row] = px[0, q][3:4]
                send_c[step, c, 2, row] = res[4, 0, q][4:5]
            for ro in range(4 if hold else 0):
                for p in range(2):
                    vec[new, c, ro, p, q] = res[ro, p, q] - s * u[ro, p, q]
                if ghosts:
                    ghost_x[new, c, ro, q] = px[ro, q] - s * gx[ro, q]
            if ghosts:
                for p in range(2):
                    ghost_r[new, c, p, q] = res[4, p, q] - s * u[4, p, q]
                ghost_c[new, c, q] = px[4, q] - s * gx[4, q]
            if step == n_steps - 1:
                for n in range(2):
                    rim_send[c, 24 + 2 * n + q] = px[2 + n, q]
                    rim_send[c, 28 + 2 * n + q] = res[4, n, q]
                    rim_send[c, 32 + 2 * n + q] = res[2 + n, 0, q]
                    rim_send[c, 36 + 2 * n + q] = res[0, n, q]

    def pack_rim(c):
        new = (n_steps - 1) % 2
        for q in range(2):
            for n in range(2):
                for p in range(2):
                    v = vec[new, c, 2 + n, p, q]
                    rim_send[c, 4 * n + 2 * p + q] = v
                    block_send[4 * n + 2 * p + q, c : c + 1] = v[7:8]
                    rim_send[c, 8 + 4 * n + 2 * p + q] = to_column(
                        vec[new, c, p, n, q], vec[new, c, 2 + p, n, q]
                    )
                rim_send[c, 16 + 2 * n + q] = ghost_x[new, c, 2 + n, q]
                rim_send[c, 20 + 2 * n + q] = ghost_r[new, c, n, q]

    group_last = lax.rem(sub, 4) == 3
    group_first = lax.rem(sub, 4) == 0

    def own_planes(c, cur):
        for q in range(2):
            side = jnp.where(corner3, ghost_x[cur, c, 0, q], roll_s(ghost_r[cur, c, 0, q], 3))
            for p in range(2):
                column = to_column(
                    roll_s(vec[cur, c, p, 0, q], 3), roll_s(vec[cur, c, 2 + p, 0, q], 3)
                )
                plane = jnp.where(upper, column, vec[cur, c, 0, p, q])
                rim_own[c, 2 * p + q] = plane
                if p == 0:
                    rim_own[c, 4 + q] = jnp.where(group_last, side, roll_s(plane, -1))

    def across(u):
        t = {}
        for p in range(3):
            for q in range(2):
                t[0, p, q], t[1, p, q], t[2, p, q] = forward(u[0, p, q], u[1, p, q], u[2, p, q])
        return t

    def rim_elements(t, scale, upper_plane=True, only_end=False):
        w = {}
        for a in range(3):
            x = {}
            for q in range(2):
                if only_end:
                    end = t[a, 2, q]
                    x[0, q], x[1, q], x[2, q] = end, -end, end
                else:
                    x[0, q], x[1, q], x[2, q] = forward(t[a, 0, q], t[a, 1, q], t[a, 2, q])
            for b in range(3):
                x[b, 0], x[b, 1] = y_pass(x[b, 0], x[b, 1], a, b, scale)
            for q in range(2):
                w[a, 0, q], w[a, 1, q], w[a, 2, q] = backward(x[0, q], x[1, q], x[2, q])
        sign = -1.0 if upper_plane else 1.0
        return {
            (p, q): w[0, p, q] + w[2, p, q] + (w[1, p, q] if sign > 0 else -w[1, p, q])
            for p in range(3)
            for q in range(2)
        }

    def add_planes(new, c, side, tip):
        for q in range(2):
            out = [side[0, q] + keep(~group_first, roll_s(side[2, q], 1)), side[1, q]]
            for p in range(2):
                for e in range(2):
                    ro = 2 * e + p
                    add = keep(corner4, roll_s(out[p], -(2 + e)))
                    add = jnp.where(corner0, roll_s(out[p], -(4 + e)), add)
                    if ro == 0:
                        add = add + keep(~upper, out[0]) + keep(corner0, roll_s(tip[2, q], -c))
                    vec[new, c, ro, 0, q] += add
            vec[new, c, 0, 1, q] += keep(~upper, out[1])

    def add_first():
        sides = {}
        corner = {}
        zero = jnp.zeros((8, half_y), F32)
        for c in range(comps):
            own_planes(c, 0)
            t = {}
            for q in range(2):
                u = [keep(group_last, roll_s(edge_recv[EDGE_G + 2 * n + q], 3 - c)) for n in range(2)]
                for p in range(2):
                    plane = rim_own[c, 2 * p + q]
                    t[0, p, q], t[1, p, q], t[2, p, q] = plane, -plane, plane
                    if p == 0:
                        part = keep(sub == c, roll_s(plane, c))
                        corner[2, 2, q] = corner[2, 2, q] + part if c else part
                t[0, 2, q], t[1, 2, q], t[2, 2, q] = forward(u[0], u[1], rim_own[c, 4 + q])
            sides[c] = rim_elements(t, lambda i: rim_scaled[0, i])
        for q in range(2):
            for n in range(2):
                corner[n, 2, q] = edge_recv[EDGE_T + 2 * n + q]
                corner[2, n, q] = edge_recv[EDGE_U + 2 * n + q]
                for p in range(2):
                    corner[n, p, q] = zero
        tip = rim_elements(across(corner), lambda i: rim_scaled[1, i])
        high = []
        for g in range(2):
            t = {}
            for q in range(2):
                near = zero
                for c in range(comps):
                    if g == 0:
                        low = roll_s(ghost_c[0, c, q], c - 7)
                        high_part = roll_s(ghost_c[0, c, q], c - 3)
                    else:
                        low = roll_s(ghost_r[0, c, 0, q], c - 4)
                        high_part = roll_s(ghost_x[0, c, 0, q], c + 1)
                    near = jnp.where(sub == c, low, jnp.where(sub == 4 + c, high_part, near))
                t[0, 2, q], t[1, 2, q], t[2, 2, q] = forward(
                    near, *(edge_recv[EDGE_H + 4 * g + 2 * n + q] for n in range(2))
                )
            high.append(rim_elements(t, lambda i, g=g: rim_scaled[2 + g, i], False, True))
        for c in range(comps):
            add_planes(1, c, sides[c], tip)
            for q in range(2):
                far = sides[c][2, q]
                ghost_x[1, c, 0, q] += keep(corner3, far + roll_s(high[1][2, q], -1 - c))
                ghost_r[1, c, 0, q] += (
                    keep(corner4, roll_s(far, -3) + roll_s(high[1][2, q], 4 - c))
                    + keep(corner7, roll_s(high[0][0, q], 7 - c))
                )
                ghost_r[1, c, 1, q] += keep(corner7, roll_s(high[0][1, q], 7 - c))
                for t in range(2):
                    ghost_x[1, c, 2 + t, q] += keep(corner7, roll_s(high[0][t, q], 3 - c))
                ghost_c[1, c, q] += keep(
                    corner7, roll_s(high[0][2, q], 7 - c) + roll_s(high[0][2, q], 3 - c)
                )

    def add_rim():
        cur = (n_steps - 1) % 2
        new = 1 - cur
        inner = jnp.where(upper, up_f, right_f)
        corner = {}
        sides = {}
        for c in range(comps):
            u = {}
            for q in range(2):
                for n in range(2):
                    for p in range(2):
                        u[n, p, q] = rim_recv[c, ROWS_X + 4 * n + 2 * p + q]
                    u[n, 0, q] = u[n, 0, q] + rim_recv[c, ROWS_C + 2 * n + q]
                    ghost = rim_recv[c, ROWS_G + 2 * n + q] + rim_recv[c, ROWS_A + 2 * n + q]
                    u[n, 2, q] = jnp.where(group_last, ghost * inner, roll_s(u[n, 0, q], -1))
                for p in range(3):
                    u[2, p, q] = rim_own[c, 2 * p + q]
            for q in range(2):
                parts = {(2, 2): roll_s(u[2, 0, q], c)}
                for n in range(2):
                    parts[n, 2] = roll_s(u[n, 0, q], c)
                    parts[2, n] = roll_s(u[n, 0, q], c - 4)
                for key, part in parts.items():
                    part = keep(sub == c, part)
                    key = key + (q,)
                    corner[key] = corner[key] + part if c else part
            sides[c] = rim_elements(across(u), lambda i: rim_scaled[0, i])
        for q in range(2):
            for n in range(2):
                for p in range(2):
                    corner[n, p, q] = block_recv[4 * n + 2 * p + q]
        tip = rim_elements(across(corner), lambda i: rim_scaled[1, i])
        for c in range(comps):
            add_planes(new, c, sides[c], tip)

    def absorb(step, c):
        new = step % 2
        first, last = step == 0, False
        for q in range(2):
            face = slice(8 * q, 8 * q + 8)
            line = slice(16 + q, 17 + q)
            row = slice(q, q + 1)

            def spot(ref_row, mask):
                return keep(mask, jnp.broadcast_to(ref_row, (8, half_y)))

            if not first:
                from_low = recv_r[step, c, 1, face]
                from_left = recv_x[step, c, 1, face]
                corner = spot(recv_c[step, c, 3, row], corner0)
                vec[new, c, 0, 0, q] += (
                    keep(~upper, from_low) + keep(first_x, from_left) + corner
                )
                vec[new, c, 0, 1, q] += keep(~upper, roll_s(from_low, 4))
                for ro in range(1, 4):
                    vec[new, c, ro, 0, q] += keep(first_x, roll_s(from_left, -ro))
            if not last:
                from_up = recv_r[step, c, 0, face]
                from_right = recv_x[step, c, 0, face]
                add0 = keep(upper, roll_s(from_up, 4))
                add1 = keep(upper, from_up)
                edge = keep(last_x, roll_s(from_right, 3))
                far = (
                    spot(recv_r[step, c, 0, line], corner7)
                    + spot(recv_x[step, c, 0, line], corner7)
                    + spot(recv_c[step, c, 0, row], corner7)
                )
                if not first:
                    add0 = (
                        add0
                        + spot(recv_x[step, c, 1, line], corner4)
                        + spot(recv_c[step, c, 1, row], corner4)
                    )
                    edge = (
                        edge
                        + spot(recv_r[step, c, 1, line], corner3)
                        + spot(recv_c[step, c, 2, row], corner3)
                    )
                    add0 = add0 + ghost_r[new, c, 0, q]
                    add1 = add1 + ghost_r[new, c, 1, q]
                    edge = edge + ghost_x[new, c, 0, q]
                    far = far + ghost_c[new, c, q]
                ghost_r[new, c, 0, q] = add0 * up_f
                ghost_r[new, c, 1, q] = add1 * up_f
                ghost_x[new, c, 0, q] = edge * right_f
                ghost_c[new, c, q] = far * both_f
                for ro in range(1, 4):
                    edge = keep(last_x, roll_s(from_right, 3 - ro))
                    if not first:
                        edge = edge + ghost_x[new, c, ro, q]
                    ghost_x[new, c, ro, q] = edge * right_f

    def to_native(k, c, rim=False):
        cur = k % 2
        for ro in range(4):
            for p in range(2):
                if rim and ro and p:
                    continue
                for q in range(2):
                    v = vec[cur, c, ro, p, q]
                    for h in range(2):
                        work[n_prev + k, q, native(c, ro, p, h), :] = v[4 * h : 4 * h + 4]

    def write_out(k):
        z = jnp.concatenate([work[n_prev + k, 0], work[n_prev + k, 1]], 1)
        out_ref[k - 1] = exact_dot(z, join_perm)

    lane16 = lax.broadcasted_iota(jnp.int32, (16, half_y), 1)
    row16 = lax.broadcasted_iota(jnp.int32, (16, half_y), 0)

    def gram_part(i, acc, first, count):
        def chunk(t, acc):
            at = pl.ds(pl.multiple_of(8 * t, 8), 8)
            for q in range(2):
                mine = work[i, q, at, :]
                acc = tuple(
                    acc[j] + mine * (mine if j == i else work[j, q, at, :]) for j in range(i + 1)
                )
            return acc

        return lax.fori_loop(first, first + count, chunk, acc, unroll=4)

    def gram_add(i, acc, at, mask):
        for q in range(2):
            mine = work[i, q, at, :]
            mine = mine if mask is None else keep(mask, mine)
            acc = tuple(
                acc[j] + mine * (mine if j == i else work[j, q, at, :]) for j in range(i + 1)
            )
        return acc

    def gram_zero(i):
        return (jnp.zeros((8, half_y), F32),) * (i + 1)

    def gram_close(i, acc):
        sums = [jnp.sum(a, axis=0, keepdims=True) for a in acc]
        sums.append(jnp.zeros((16 - len(sums), half_y), F32))
        total = jnp.sum(jnp.concatenate(sums, 0), axis=1, keepdims=True)
        hit = jnp.logical_or(lane16 == i * n_vec + row16, lane16 == row16 * n_vec + i)
        hit = jnp.logical_and(hit, row16 <= i)
        return jnp.sum(jnp.where(hit, jnp.broadcast_to(total, hit.shape), 0.0), 0, keepdims=True)

    def gram_row(i):
        return gram_close(i, gram_part(i, gram_zero(i), 0, rows // 8))

    res_copy.wait()
    edge_rows = []
    for c in range(comps):
        picked = [2 * x + p for p in range(2) for x in range(4)] + [8 * r for r in range(8)]
        edge_rows += [stage[n_prev, pl.ds(c * 64 + at, 1), :] for at in picked]
    edge = exact_dot(jnp.concatenate(edge_rows, 0), split_perm)
    zero_rows = jnp.zeros((2, half_y), F32)
    for c in range(comps):
        send_r[0, c, 0, 16:18] = zero_rows
        send_x[0, c, 0, 16:18] = zero_rows
        for q in range(2):
            face = slice(8 * q, 8 * q + 8)
            lanes = slice(half_y * q, half_y * (q + 1))
            send_r[0, c, 0, face] = edge[16 * c : 16 * c + 8, lanes]
            send_x[0, c, 0, face] = edge[16 * c + 8 : 16 * c + 16, lanes]
            send_c[0, c, 0, q : q + 1] = edge[16 * c : 16 * c + 1, lanes]
            along = [8 + 6, 8 + 7, 3, 7, 8 + 1, 8 + 2, 4, 1]
            for slot, row in enumerate(along):
                at = 16 * c + row
                edge_send[2 * slot + q, c : c + 1] = edge[at : at + 1, lanes]

    pl.semaphore_wait(barrier, around(1, DIRS))
    for c in range(comps):
        start_round(0, c)
    start_edges(DIRS)
    split_columns(n_prev)
    for c in range(comps):
        for ro in range(4):
            for p in range(2):
                for q in range(2):
                    vec[0, c, ro, p, q] = jnp.concatenate(
                        [work[n_prev, q, native(c, ro, p, h), :] for h in range(2)], 0
                    )
    for copy in small_copies:
        copy.wait()
    etas = []
    for e in range(2):
        ids = jnp.concatenate([ids_ref[e], ids_ref[2 + e]], 0)
        eta = jnp.zeros((8, half_y), F32)
        for layer in range(visc_ref.shape[0]):
            eta = eta + jnp.where(ids == layer, visc_ref[layer], 0.0)
        etas.append(eta)
        for key, i in kinds.items():
            scaled[e, i] = eta * weight(*key)
    eta_send[0] = etas[1]
    eta_send[1] = to_column(*etas)
    eta_send[2] = jnp.where(
        upper,
        jnp.broadcast_to(etas[1][4:5], (8, half_y)),
        jnp.broadcast_to(etas[0][3:4], (8, half_y)),
    )
    start_etas(DIRS)
    for c in range(comps):
        apply(0, c, hold=False)
        start_round(1, c)

    total = jnp.zeros((1, half_y), F32)
    prev_copy.wait()
    for i in range(n_prev):
        split_columns(i)

    for i in range(n_prev + 1):
        total = total + gram_row(i)

    for c in range(comps):
        finish_round(0, c)
        absorb(0, c)
        apply(0, c, send=False)
    settle(rim_sems.at[1], opposite(edge_sizes))
    tip_eta = jnp.broadcast_to(eta_recv[1, 0:1], (8, half_y))
    for key, i in kinds.items():
        for slot in range(4):
            rim_scaled[slot, i] = (tip_eta if slot == 1 else eta_recv[slot]) * weight(*key)
    add_first()
    for k in range(1, n_steps - 1):
        for c in range(comps):
            finish_round(k, c)
            absorb(k, c)
            apply(k, c)
            start_round(k + 1, c)
            if k == n_steps - 2:
                if c:
                    start_layers(c - 1)
                pack_rim(c)
        if k == n_steps - 2:
            start_layers(comps - 1)
            start_rim()
        if k == n_steps - 2:
            send_token(0)
        for c in range(comps):
            to_native(k, c)
        write_out(k)
        total = total + gram_row(n_prev + k)
    assert n_steps >= 3
    k = n_steps - 1
    per = rows // 8 // comps
    whole = gram_zero(n_vec - 2)
    acc = gram_zero(n_vec - 1)
    for c in range(comps):
        finish_round(k, c)
        absorb(k, c)
        apply(k, c)
        if c == 0:
            take_token(0)
            send_token(1)
        own_planes(c, k % 2)
        to_native(k, c)
        to_native(n_steps, c)
        whole = gram_part(n_vec - 2, whole, c * per, per)
        acc = lax.fori_loop(
            8 * c + 1,
            8 * c + 8,
            lambda t, acc: gram_add(
                n_vec - 1, acc, pl.ds(pl.multiple_of(8 * t, 8), 8), jnp.logical_not(corner0)
            ),
            acc,
            unroll=7,
        )
    total = total + gram_close(n_vec - 2, whole)
    settle(rim_sems.at[0], opposite(rim_sizes))
    add_rim()
    for c in range(comps):
        to_native(n_steps, c, rim=True)
    for c in range(comps):
        acc = gram_add(n_vec - 1, acc, pl.ds(c * 64, 8), None)
        acc = gram_add(n_vec - 1, acc, pl.ds(c * 64, 8, stride=8), jnp.logical_not(corner0))
    total = total + gram_close(n_vec - 1, acc)
    gram_send[...] = total

    def scatter(slot, device):
        pltpu.make_async_remote_copy(
            src_ref=gram_send,
            dst_ref=gram_recv.at[slot],
            send_sem=gram_sems.at[0],
            recv_sem=gram_sems.at[1],
            device_id=device,
            device_id_type=MESH,
        ).start()

    for j in range(1, len(reaches)):
        take_token(j)
        send_token(j + 1)
    each_other(scatter)
    write_out(n_steps - 1)
    write_out(n_steps)
    sent = [size for step in range(n_steps) for size in round_sizes(step)] * comps
    settle(send_sem.at[0], sent + rim_sizes + edge_sizes)
    for i in range(2):
        pltpu.make_async_copy(gram_recv, gram_recv, gram_sems.at[i]).wait()
    full = (total + jnp.sum(gram_recv[...], axis=0)) * (1.0 / (rows * 2 * half_y * n_dev))
    for i in range(n_vec):
        line = full if i == 0 else pltpu.roll(full, half_y - i * n_vec, 1)
        gram_ref[i : i + 1, :] = line[:, :n_vec]


def store(vec_ref, gram_ref, vec_out, gram_out, sems):
    copies = [pltpu.make_async_copy(gram_ref, gram_out, sems.at[0])]
    for i in range(vec_ref.shape[0]):
        copies.append(pltpu.make_async_copy(vec_ref.at[i], vec_out.at[i], sems.at[1 + i]))
    for copy in copies:
        copy.start()
    for copy in copies:
        copy.wait()


def on_device(residual, prev_basis, layer_ids, viscosity, shifts):
    n_lat = lax.axis_size("lat")
    n_rad = lax.axis_size("rad")
    comps, node_r, node_x, node_y = residual.shape
    n_prev = prev_basis.shape[0]
    n_steps = shifts.shape[0]
    n_vec = n_prev + n_steps + 1
    rows = comps * node_r * node_x
    half_y = node_y // 2
    assert node_r == 8 and node_x == 8 and half_y == 128
    rounds = n_steps
    tile = (8, half_y)
    vmem = pltpu.VMEM
    hbm_spec = pl.BlockSpec(memory_space=pltpu.HBM)
    vmem_spec = pl.BlockSpec(memory_space=pltpu.VMEM)
    out, gram = pl.pallas_call(
        functools.partial(kernel, n_lat, n_rad, n_steps, n_prev, comps),
        out_shape=(
            pltpu.VMEM((n_steps, rows, node_y), F32),
            pltpu.VMEM((n_vec, n_vec), F32),
        ),
        in_specs=[hbm_spec] * 5,
        out_specs=(vmem_spec, vmem_spec),
        scratch_shapes=[
            vmem((n_prev + 1, rows, node_y), F32),
            vmem(layer_ids.shape, jnp.int32),
            pltpu.SMEM(viscosity.shape, F32),
            pltpu.SMEM(shifts.shape, F32),
            vmem((n_vec, 2, rows, half_y), F32),
            vmem((2, comps, 4, 2, 2) + tile, F32),
            vmem((2, comps, 2, 2) + tile, F32),
            vmem((2, comps, 4, 2) + tile, F32),
            vmem((2, comps, 2) + tile, F32),
            vmem((2, 9) + tile, F32),
            vmem((rounds, comps, 2, 18, half_y), F32),
            vmem((rounds, comps, 2, 18, half_y), F32),
            vmem((rounds, comps, 4, 2, half_y), F32),
            vmem((rounds, comps, 2, 18, half_y), F32),
            vmem((rounds, comps, 2, 18, half_y), F32),
            vmem((rounds, comps, 4, 2, half_y), F32),
            vmem((1, half_y), F32),
            vmem((n_lat * n_rad - 1, 1, half_y), F32),
            vmem((rounds * comps * 80 + 128 * comps, half_y), F32),
            vmem((comps, 40) + tile, F32),
            vmem((comps, 20) + tile, F32),
            vmem((8,) + tile, F32),
            vmem((8,) + tile, F32),
            vmem((16,) + tile, F32),
            vmem((20,) + tile, F32),
            vmem((3,) + tile, F32),
            vmem((4,) + tile, F32),
            vmem((4, 9) + tile, F32),
            vmem((comps, 6) + tile, F32),
            pltpu.SemaphoreType.DMA((5,)),
            pltpu.SemaphoreType.DMA((1,)),
            pltpu.SemaphoreType.DMA((3, comps)),
            pltpu.SemaphoreType.DMA((2,)),
            pltpu.SemaphoreType.DMA((2,)),
            pltpu.SemaphoreType.REGULAR((max(n_lat, n_rad).bit_length(),)),
        ],
        compiler_params=pltpu.CompilerParams(
            collective_id=0, has_side_effects=True, vmem_limit_bytes=65000000
        ),
    )(
        residual.reshape(rows, node_y),
        prev_basis.reshape(n_prev, rows, node_y),
        layer_ids,
        viscosity,
        shifts,
    )
    out, gram = pl.pallas_call(
        store,
        out_shape=(
            jax.ShapeDtypeStruct(out.shape, F32),
            jax.ShapeDtypeStruct(gram.shape, F32),
        ),
        in_specs=[vmem_spec] * 2,
        out_specs=(hbm_spec, hbm_spec),
        scratch_shapes=[pltpu.SemaphoreType.DMA((1 + n_steps,))],
    )(*(pltpu.with_memory_space_constraint(a, pltpu.VMEM) for a in (out, gram)))
    return out.reshape((n_steps,) + residual.shape), gram


def solution(mesh):
    placed = (
        P(None, "rad", "lat", None),
        P(None, None, "rad", "lat", None),
        P("rad", "lat", None),
        P(),
        P(),
    )
    return jax.shard_map(
        on_device,
        mesh=mesh,
        in_specs=placed,
        out_specs=(P(None, None, "rad", "lat", None), P()),
        check_vma=False,
    )
```

```python
import functools

import jax
import jax.numpy as jnp
from jax import lax
from jax.experimental import pallas as pl
from jax.experimental.pallas import tpu as pltpu
from jax.sharding import PartitionSpec as P

MESH = pl.DeviceIdType.MESH
F32 = jnp.float32

mass = (1.0 / 36, 1.0 / 12, 1.0 / 45)
stiff = (0.0, 1.0, 4.0 / 3)

DIRS = ((-1, -1), (-1, 0), (-1, 1), (0, -1), (0, 1), (1, -1), (1, 0), (1, 1))
R_DIRS = {(-1, 0): 0, (1, 0): 1}
X_DIRS = {(0, -1): 0, (0, 1): 1}
C_DIRS = {(-1, -1): 0, (-1, 1): 1, (1, -1): 2, (1, 1): 3}
FIRST = ((-1, 0), (0, -1), (-1, -1))
LAST = ((1, 0), (0, 1), (1, 1))
ROWS_X, ROWS_G, ROWS_A, ROWS_C = 0, 8, 12, 16
RIM = (
    ((1, 0), (0, 8), (4, 4), ROWS_X, 0),
    ((0, 1), (8, 8), (4, 4), ROWS_X, 4),
    ((1, 0), (16, 4), (7, 1), ROWS_G, 3),
    ((0, 1), (20, 4), (7, 1), ROWS_G, 7),
    ((1, 1), (24, 4), (7, 1), ROWS_C, 0),
    ((1, 1), (28, 4), (7, 1), ROWS_C, 4),
    ((1, -1), (32, 4), (4, 1), ROWS_A, 3),
    ((-1, 1), (36, 4), (3, 1), ROWS_A, 7),
)
EDGE_T, EDGE_U, EDGE_H, EDGE_G = 0, 4, 8, 16
EDGES = (
    ((-1, -1), (8, 4), EDGE_H, 0),
    ((-1, -1), (12, 4), EDGE_H, 4),
    ((-1, 0), (8, 4), EDGE_H + 4, 0),
    ((0, -1), (12, 4), EDGE_H + 4, 4),
    ((1, 0), (0, 4), EDGE_T, 0),
    ((0, 1), (4, 4), EDGE_U, 0),
    ((1, -1), (0, 4), EDGE_G, 0),
    ((-1, 1), (4, 4), EDGE_G, 4),
)
ETAS = (
    ((-1, 0), 2, 0, 3, 2, 0),
    ((0, -1), 2, 4, 3, 2, 4),
    ((1, 0), 0, 4, 4, 0, 0),
    ((0, 1), 1, 4, 4, 0, 4),
    ((1, 1), 0, 7, 1, 1, 0),
    ((-1, 1), 2, 0, 3, 3, 0),
    ((1, -1), 2, 4, 3, 3, 4),
)


def weight(a, b, c):
    return (
        stiff[a] * mass[b] * mass[c] + mass[a] * stiff[b] * mass[c] + mass[a] * mass[b] * stiff[c]
    )


def forward(u0, u1, u2):
    total = u0 + u2
    twice = u1 + u1
    return total + (twice + twice), u0 - u2, total - twice


def backward(m0, m1, m2):
    both = m0 + m2
    half = m0 + m0 - m2
    return both + m1, half + half, both - m1


def kernel(
    n_lat,
    n_rad,
    n_steps,
    n_prev,
    comps,
    res_ref,
    prev_ref,
    ids_hbm,
    visc_hbm,
    shift_hbm,
    out_ref,
    gram_ref,
    stage,
    ids_ref,
    visc_ref,
    shift_ref,
    work,
    vec,
    ghost_r,
    ghost_x,
    ghost_c,
    scaled,
    send_r,
    send_x,
    send_c,
    recv_r,
    recv_x,
    recv_c,
    gram_send,
    gram_recv,
    bulk,
    rim_send,
    rim_recv,
    block_send,
    block_recv,
    edge_send,
    edge_recv,
    eta_send,
    eta_recv,
    rim_scaled,
    rim_own,
    in_sem,
    send_sem,
    recv_sem,
    rim_sems,
    gram_sems,
    token_sem,
):
    n_dev = n_lat * n_rad
    lat = lax.axis_index("lat")
    rad = lax.axis_index("rad")
    me = lat * n_rad + rad
    rows = res_ref.shape[0]
    half_y = res_ref.shape[1] // 2
    n_vec = n_prev + n_steps + 1

    res_copy = pltpu.make_async_copy(res_ref, stage.at[n_prev], in_sem.at[0])
    res_copy.start()
    prev_copy = pltpu.make_async_copy(prev_ref, stage.at[pl.ds(0, n_prev)], in_sem.at[1])
    small_copies = [
        pltpu.make_async_copy(a, b, in_sem.at[2 + i])
        for i, (a, b) in enumerate(
            ((ids_hbm, ids_ref), (visc_hbm, visc_ref), (shift_hbm, shift_ref))
        )
    ]
    for copy in small_copies:
        copy.start()
    prev_copy.start()

    barrier = pltpu.get_barrier_semaphore()

    def around(far, dirs):
        total = 0
        for dr, dx in dirs:
            if not ((dr and n_rad <= far) or (dx and n_lat <= far)):
                total += jnp.where(within(dr * far, dx * far), 1, 0)
        return total

    def within(dr, dx):
        ok = None
        for pos, step, count in ((rad, dr, n_rad), (lat, dx, n_lat)):
            if step:
                one = (pos >= -step) if step < 0 else (pos < count - step)
                ok = one if ok is None else jnp.logical_and(ok, one)
        return ok

    def signal_around(sem, far, dirs):
        for dr, dx in dirs:
            if (dr and n_rad <= far) or (dx and n_lat <= far):
                continue

            @pl.when(within(dr * far, dx * far))
            def _(dr=dr, dx=dx):
                pl.semaphore_signal(
                    sem,
                    inc=1,
                    device_id={"lat": lat + dx * far, "rad": rad + dr * far},
                    device_id_type=MESH,
                )

    for ref in (edge_recv, eta_recv):
        ref[...] = jnp.zeros_like(ref)
    signal_around(barrier, 1, DIRS)

    for d in DIRS:
        if d in R_DIRS:
            ref, slot = recv_r, R_DIRS[d]
        elif d in X_DIRS:
            ref, slot = recv_x, X_DIRS[d]
        else:
            ref, slot = recv_c, C_DIRS[d]

        @pl.when(jnp.logical_not(within(-d[0], -d[1])))
        def _(ref=ref, slot=slot):
            ref[:, :, slot] = jnp.zeros(ref.shape[:2] + ref.shape[3:], F32)

    for ref in (rim_recv, block_recv):
        ref[...] = jnp.zeros_like(ref)

    for ref in (ghost_r, ghost_x, ghost_c):
        ref[0] = jnp.zeros(ref.shape[1:], F32)

    reaches = []
    while (2 << len(reaches)) < max(n_lat, n_rad) - 1:
        reaches.append(2 << len(reaches))

    def send_token(j):
        if j < len(reaches):
            signal_around(token_sem.at[j], reaches[j], DIRS)

    def take_token(j):
        if j < len(reaches):
            pl.semaphore_wait(token_sem.at[j], around(reaches[j], DIRS))

    rad_targets = [lax.rem(rad + d, n_rad) for d in range(n_rad)]

    def each_other(visit):
        def row(i, carry):
            lat_target = lax.rem(lat + n_lat // 2 + i, n_lat)
            for d in range(n_rad):
                ahead = lax.rem(n_lat // 2 + i, n_lat)
                visit(ahead * n_rad + d - 1, {"lat": lat_target, "rad": rad_targets[d]})
            return carry

        lax.fori_loop(0, n_lat // 2, row, 0, unroll=n_lat <= 8)
        lax.fori_loop(n_lat // 2 + 1, n_lat, row, 0, unroll=n_lat <= 8)
        for d in range(1, n_rad):
            visit(d - 1, {"lat": lat, "rad": rad_targets[d]})

    sub = lax.broadcasted_iota(jnp.int32, (8, half_y), 0)
    lane = lax.broadcasted_iota(jnp.int32, (8, half_y), 1)
    upper = sub >= 4
    ex = lax.rem(sub, 4)
    first_x = ex == 0
    last_x = ex == 3
    corner0 = sub == 0
    corner3 = sub == 3
    corner4 = sub == 4
    corner7 = sub == 7
    has_up = rad < n_rad - 1
    has_right = lat < n_lat - 1
    up_f = jnp.where(has_up, 1.0, 0.0).astype(F32)
    right_f = jnp.where(has_right, 1.0, 0.0).astype(F32)
    both_f = up_f * right_f

    def roll_s(v, k):
        return pltpu.roll(v, k % 8, 0)

    def keep(mask, v):
        return jnp.where(mask, v, 0.0)

    src = lax.broadcasted_iota(jnp.int32, (2 * half_y, 2 * half_y), 0)
    dst = lax.broadcasted_iota(jnp.int32, (2 * half_y, 2 * half_y), 1)
    split_perm = jnp.where(
        src == jnp.where(dst < half_y, 2 * dst, 2 * (dst - half_y) + 1), 1.0, 0.0
    ).astype(jnp.bfloat16)
    join_perm = jnp.where(
        dst == jnp.where(src < half_y, 2 * src, 2 * (src - half_y) + 1), 1.0, 0.0
    ).astype(jnp.bfloat16)

    def exact_dot(a, b):
        high = a.astype(jnp.bfloat16)
        rest = a - high.astype(F32)
        mid = rest.astype(jnp.bfloat16)
        low = (rest - mid.astype(F32)).astype(jnp.bfloat16)
        out = [jnp.dot(part, b, preferred_element_type=F32) for part in (high, mid, low)]
        return out[0] + (out[1] + out[2])

    def split_columns(i):
        z = exact_dot(stage[i], split_perm)
        work[i, 0] = z[:, :half_y]
        work[i, 1] = z[:, half_y:]

    def native(c, ro, p, h):
        return pl.ds(c * 64 + (4 * h + ro) * 8 + p, 4, stride=2)

    kinds = {}
    for a in range(3):
        for b in range(3):
            for c in range(3):
                key = tuple(sorted((a, b, c)))
                if key != (0, 0, 0) and key not in kinds:
                    kinds[key] = len(kinds)
    def copy_of(step, c, d):
        if d in R_DIRS:
            a, b = send_r.at[step, c, R_DIRS[d]], recv_r.at[step, c, R_DIRS[d]]
        elif d in X_DIRS:
            a, b = send_x.at[step, c, X_DIRS[d]], recv_x.at[step, c, X_DIRS[d]]
        else:
            a, b = send_c.at[step, c, C_DIRS[d]], recv_c.at[step, c, C_DIRS[d]]
        return pltpu.make_async_remote_copy(
            src_ref=a,
            dst_ref=b,
            send_sem=send_sem.at[0],
            recv_sem=recv_sem.at[step % 3, c],
            device_id={"lat": lat + d[1], "rad": rad + d[0]},
            device_id_type=MESH,
        )

    order = ((-1, -1), (1, 1), (-1, 1), (1, -1), (1, 0), (-1, 0), (0, 1), (0, -1))

    def dirs_of(step):
        wanted = FIRST if step == 0 else DIRS
        return [d for d in order if d in wanted]

    def start_round(step, c, among=DIRS):
        for d in dirs_of(step):
            if d not in among:
                continue

            @pl.when(within(*d))
            def _(d=d):
                copy_of(step, c, d).start()

    def places(pos, count):
        out = [(pos == 0, False, True), (pos == count - 1, True, False)]
        if count > 2:
            middle = jnp.logical_and(pos > 0, pos < count - 1)
            out.append((middle, True, True))
        return out if count > 1 else [(pos == 0, False, False)]

    def rows_of(sizes, down, up, left, right):
        have = {-1: {0: True, -1: down, 1: up}, 1: {0: True, -1: left, 1: right}}
        return sum(n for (dr, dx), n in sizes if have[-1][dr] and have[1][dx])

    def settle(sem, sizes):
        groups = {}
        for at_r, down, up in places(rad, n_rad):
            for at_x, left, right in places(lat, n_lat):
                n = rows_of(sizes, down, up, left, right)
                here = jnp.logical_and(at_r, at_x)
                groups[n] = jnp.logical_or(groups[n], here) if n in groups else here
        for n, here in groups.items():
            if n:

                @pl.when(here)
                def _(n=n):
                    pltpu.make_async_copy(bulk.at[pl.ds(0, n)], bulk.at[pl.ds(0, n)], sem).wait()

    def opposite(sizes):
        return [((-dr, -dx), n) for (dr, dx), n in sizes]

    def round_sizes(step):
        return [(d, 2 if d[0] and d[1] else 18) for d in dirs_of(step)]

    rim_sizes = [(d, comps * count * high) for d, (_, count), (_, high), _, _ in RIM]
    rim_sizes.append(((1, 1), comps * 8))
    edge_sizes = [(d, comps * count) for d, (_, count), _, _ in EDGES]
    edge_sizes += [(d, high) for d, _, _, high, _, _ in ETAS]

    def finish_round(step, c):
        settle(recv_sem.at[step % 3, c], opposite(round_sizes(step)))

    def remote(a, b, recv, d):
        @pl.when(within(*d))
        def _():
            pltpu.make_async_remote_copy(
                src_ref=a,
                dst_ref=b,
                send_sem=send_sem.at[0],
                recv_sem=recv,
                device_id={"lat": lat + d[1], "rad": rad + d[0]},
                device_id_type=MESH,
            ).start()

    def start_layers(c):
        for d, (first, count), (row, high), to, to_row in RIM[:2]:
            remote(
                rim_send.at[c, pl.ds(first, count), pl.ds(row, high)],
                rim_recv.at[c, pl.ds(to, count), pl.ds(to_row, high)],
                rim_sems.at[0],
                d,
            )

    def start_rim():
        for d, (first, count), (row, high), to, to_row in RIM[2:]:
            remote(
                rim_send.at[:, pl.ds(first, count), pl.ds(row, high)],
                rim_recv.at[:, pl.ds(to, count), pl.ds(to_row, high)],
                rim_sems.at[0],
                d,
            )
        remote(
            block_send.at[:, pl.ds(0, comps)], block_recv.at[:, pl.ds(0, comps)], rim_sems.at[0], (1, 1)
        )

    def start_edges(among):
        for d, (first, count), to, to_row in EDGES:
            if d in among:
                remote(
                    edge_send.at[pl.ds(first, count), pl.ds(0, comps)],
                    edge_recv.at[pl.ds(to, count), pl.ds(to_row, comps)],
                    rim_sems.at[1],
                    d,
                )

    def start_etas(among):
        for d, slot, row, high, to, to_row in ETAS:
            if d in among:
                remote(
                    eta_send.at[slot, pl.ds(row, high)],
                    eta_recv.at[to, pl.ds(to_row, high)],
                    rim_sems.at[1],
                    d,
                )

    def pack_x(vals, at):
        out = None
        for ro in range(4):
            moved = roll_s(vals[ro], ro - at)
            out = moved if out is None else jnp.where(ex == ro, moved, out)
        return out

    def y_pass(x0, x1, a, b, scale):
        nxt = keep(lane != half_y - 1, pltpu.roll(x0, half_y - 1, 1))
        m = list(forward(x0, x1, nxt))
        for j in range(3):
            key = tuple(sorted((a, b, j)))
            m[j] = m[j] * scale(kinds[key]) if key in kinds else None
        if m[0] is None:
            r0 = m[1] + m[2]
            r1 = -(m[2] + m[2])
            r2 = m[2] - m[1]
        else:
            r0, r1, r2 = backward(*m)
        return r0 + keep(lane != 0, pltpu.roll(r2, 1, 1)), r1

    def to_column(low, high):
        moved = jnp.where(sub == 6, roll_s(low, -1), high)
        return jnp.where(sub == 4, roll_s(low, 1), jnp.where(sub == 5, roll_s(high, 2), moved))

    def apply(k, c, send=True, hold=True):
        s = shift_ref[k]
        cur = k % 2
        new = 1 - cur
        u = {}
        gx = {}
        for q in range(2):
            for ro in range(4):
                gx[ro, q] = ghost_x[cur, c, ro, q]
                for p in range(2):
                    u[ro, p, q] = vec[cur, c, ro, p, q]
            gx[4, q] = jnp.where(upper, ghost_c[cur, c, q], roll_s(gx[0, q], 4))
            for p in range(2):
                u[4, p, q] = jnp.where(upper, ghost_r[cur, c, p, q], roll_s(u[0, p, q], 4))
            for ro in range(5):
                u[ro, 2, q] = jnp.where(last_x, gx[ro, q], roll_s(u[ro, 0, q], -1))
        res = {}
        for e in range(2):
            t = {}
            for p in range(3):
                for q in range(2):
                    t[0, p, q], t[1, p, q], t[2, p, q] = forward(
                        u[2 * e, p, q], u[2 * e + 1, p, q], u[2 * e + 2, p, q]
                    )
            w = {}
            for a in range(3):
                x = {}
                for q in range(2):
                    x[0, q], x[1, q], x[2, q] = forward(t[a, 0, q], t[a, 1, q], t[a, 2, q])
                for b in range(3):
                    x[b, 0], x[b, 1] = y_pass(x[b, 0], x[b, 1], a, b, lambda i: scaled[e, i])
                for q in range(2):
                    w[a, 0, q], w[a, 1, q], w[a, 2, q] = backward(x[0, q], x[1, q], x[2, q])
            for p in range(3):
                for q in range(2):
                    r = backward(w[0, p, q], w[1, p, q], w[2, p, q])
                    for i in range(3):
                        key = (2 * e + i, p, q)
                        res[key] = res[key] + r[i] if key in res else r[i]
        px = {}
        for q in range(2):
            for ro in range(5):
                edge = res[ro, 2, q]
                px[ro, q] = edge
                res[ro, 0, q] = res[ro, 0, q] + keep(ex != 0, roll_s(edge, 1))
            for p in range(2):
                res[0, p, q] = res[0, p, q] + keep(upper, roll_s(res[4, p, q], 4))
            px[0, q] = px[0, q] + keep(upper, roll_s(px[4, q], 4))
        step = k + 1
        send = send and step < n_steps
        ghosts = hold and step < n_steps
        for q in range(2):
            face = slice(8 * q, 8 * q + 8)
            edge = slice(16 + q, 17 + q)
            row = slice(q, q + 1)
            if send:
                send_r[step, c, 1, face] = jnp.where(upper, res[4, 1, q], roll_s(res[4, 0, q], 4))
                send_r[step, c, 1, edge] = px[4, q][7:8]
                send_x[step, c, 1, face] = pack_x([px[ro, q] for ro in range(4)], 3)
                send_x[step, c, 1, edge] = px[4, q][7:8]
                send_c[step, c, 3, row] = px[4, q][7:8]
                send_r[step, c, 0, face] = jnp.where(upper, roll_s(res[0, 1, q], 4), res[0, 0, q])
                send_r[step, c, 0, edge] = px[0, q][3:4]
                send_x[step, c, 0, face] = pack_x([res[ro, 0, q] for ro in range(4)], 0)
                send_x[step, c, 0, edge] = res[4, 0, q][4:5]
                send_c[step, c, 0, row] = res[0, 0, q][0:1]
                send_c[step, c, 1, row] = px[0, q][3:4]
                send_c[step, c, 2, row] = res[4, 0, q][4:5]
            for ro in range(4 if hold else 0):
                for p in range(2):
                    vec[new, c, ro, p, q] = res[ro, p, q] - s * u[ro, p, q]
                if ghosts:
                    ghost_x[new, c, ro, q] = px[ro, q] - s * gx[ro, q]
            if ghosts:
                for p in range(2):
                    ghost_r[new, c, p, q] = res[4, p, q] - s * u[4, p, q]
                ghost_c[new, c, q] = px[4, q] - s * gx[4, q]
            if step == n_steps - 1:
                for n in range(2):
                    rim_send[c, 24 + 2 * n + q] = px[2 + n, q]
                    rim_send[c, 28 + 2 * n + q] = res[4, n, q]
                    rim_send[c, 32 + 2 * n + q] = res[2 + n, 0, q]
                    rim_send[c, 36 + 2 * n + q] = res[0, n, q]

    def pack_rim(c):
        new = (n_steps - 1) % 2
        for q in range(2):
            for n in range(2):
                for p in range(2):
                    v = vec[new, c, 2 + n, p, q]
                    rim_send[c, 4 * n + 2 * p + q] = v
                    block_send[4 * n + 2 * p + q, c : c + 1] = v[7:8]
                    rim_send[c, 8 + 4 * n + 2 * p + q] = to_column(
                        vec[new, c, p, n, q], vec[new, c, 2 + p, n, q]
                    )
                rim_send[c, 16 + 2 * n + q] = ghost_x[new, c, 2 + n, q]
                rim_send[c, 20 + 2 * n + q] = ghost_r[new, c, n, q]

    group_last = lax.rem(sub, 4) == 3
    group_first = lax.rem(sub, 4) == 0

    def own_planes(c, cur):
        for q in range(2):
            side = jnp.where(corner3, ghost_x[cur, c, 0, q], roll_s(ghost_r[cur, c, 0, q], 3))
            for p in range(2):
                column = to_column(
                    roll_s(vec[cur, c, p, 0, q], 3), roll_s(vec[cur, c, 2 + p, 0, q], 3)
                )
                plane = jnp.where(upper, column, vec[cur, c, 0, p, q])
                rim_own[c, 2 * p + q] = plane
                if p == 0:
                    rim_own[c, 4 + q] = jnp.where(group_last, side, roll_s(plane, -1))

    def across(u):
        t = {}
        for p in range(3):
            for q in range(2):
                t[0, p, q], t[1, p, q], t[2, p, q] = forward(u[0, p, q], u[1, p, q], u[2, p, q])
        return t

    def rim_elements(t, scale, upper_plane=True, only_end=False):
        w = {}
        for a in range(3):
            x = {}
            for q in range(2):
                if only_end:
                    end = t[a, 2, q]
                    x[0, q], x[1, q], x[2, q] = end, -end, end
                else:
                    x[0, q], x[1, q], x[2, q] = forward(t[a, 0, q], t[a, 1, q], t[a, 2, q])
            for b in range(3):
                x[b, 0], x[b, 1] = y_pass(x[b, 0], x[b, 1], a, b, scale)
            for q in range(2):
                w[a, 0, q], w[a, 1, q], w[a, 2, q] = backward(x[0, q], x[1, q], x[2, q])
        sign = -1.0 if upper_plane else 1.0
        return {
            (p, q): w[0, p, q] + w[2, p, q] + (w[1, p, q] if sign > 0 else -w[1, p, q])
            for p in range(3)
            for q in range(2)
        }

    def add_planes(new, c, side, tip):
        for q in range(2):
            out = [side[0, q] + keep(~group_first, roll_s(side[2, q], 1)), side[1, q]]
            for p in range(2):
                for e in range(2):
                    ro = 2 * e + p
                    add = keep(corner4, roll_s(out[p], -(2 + e)))
                    add = jnp.where(corner0, roll_s(out[p], -(4 + e)), add)
                    if ro == 0:
                        add = add + keep(~upper, out[0]) + keep(corner0, roll_s(tip[2, q], -c))
                    vec[new, c, ro, 0, q] += add
            vec[new, c, 0, 1, q] += keep(~upper, out[1])

    def add_first():
        sides = {}
        corner = {}
        zero = jnp.zeros((8, half_y), F32)
        for c in range(comps):
            own_planes(c, 0)
            t = {}
            for q in range(2):
                u = [keep(group_last, roll_s(edge_recv[EDGE_G + 2 * n + q], 3 - c)) for n in range(2)]
                for p in range(2):
                    plane = rim_own[c, 2 * p + q]
                    t[0, p, q], t[1, p, q], t[2, p, q] = plane, -plane, plane
                    if p == 0:
                        part = keep(sub == c, roll_s(plane, c))
                        corner[2, 2, q] = corner[2, 2, q] + part if c else part
                t[0, 2, q], t[1, 2, q], t[2, 2, q] = forward(u[0], u[1], rim_own[c, 4 + q])
            sides[c] = rim_elements(t, lambda i: rim_scaled[0, i])
        for q in range(2):
            for n in range(2):
                corner[n, 2, q] = edge_recv[EDGE_T + 2 * n + q]
                corner[2, n, q] = edge_recv[EDGE_U + 2 * n + q]
                for p in range(2):
                    corner[n, p, q] = zero
        tip = rim_elements(across(corner), lambda i: rim_scaled[1, i])
        high = []
        for g in range(2):
            t = {}
            for q in range(2):
                near = zero
                for c in range(comps):
                    if g == 0:
                        low = roll_s(ghost_c[0, c, q], c - 7)
                        high_part = roll_s(ghost_c[0, c, q], c - 3)
                    else:
                        low = roll_s(ghost_r[0, c, 0, q], c - 4)
                        high_part = roll_s(ghost_x[0, c, 0, q], c + 1)
                    near = jnp.where(sub == c, low, jnp.where(sub == 4 + c, high_part, near))
                t[0, 2, q], t[1, 2, q], t[2, 2, q] = forward(
                    near, *(edge_recv[EDGE_H + 4 * g + 2 * n + q] for n in range(2))
                )
            high.append(rim_elements(t, lambda i, g=g: rim_scaled[2 + g, i], False, True))
        for c in range(comps):
            add_planes(1, c, sides[c], tip)
            for q in range(2):
                far = sides[c][2, q]
                ghost_x[1, c, 0, q] += keep(corner3, far + roll_s(high[1][2, q], -1 - c))
                ghost_r[1, c, 0, q] += (
                    keep(corner4, roll_s(far, -3) + roll_s(high[1][2, q], 4 - c))
                    + keep(corner7, roll_s(high[0][0, q], 7 - c))
                )
                ghost_r[1, c, 1, q] += keep(corner7, roll_s(high[0][1, q], 7 - c))
                for t in range(2):
                    ghost_x[1, c, 2 + t, q] += keep(corner7, roll_s(high[0][t, q], 3 - c))
                ghost_c[1, c, q] += keep(
                    corner7, roll_s(high[0][2, q], 7 - c) + roll_s(high[0][2, q], 3 - c)
                )

    def add_rim():
        cur = (n_steps - 1) % 2
        new = 1 - cur
        inner = jnp.where(upper, up_f, right_f)
        corner = {}
        sides = {}
        for c in range(comps):
            u = {}
            for q in range(2):
                for n in range(2):
                    for p in range(2):
                        u[n, p, q] = rim_recv[c, ROWS_X + 4 * n + 2 * p + q]
                    u[n, 0, q] = u[n, 0, q] + rim_recv[c, ROWS_C + 2 * n + q]
                    ghost = rim_recv[c, ROWS_G + 2 * n + q] + rim_recv[c, ROWS_A + 2 * n + q]
                    u[n, 2, q] = jnp.where(group_last, ghost * inner, roll_s(u[n, 0, q], -1))
                for p in range(3):
                    u[2, p, q] = rim_own[c, 2 * p + q]
            for q in range(2):
                parts = {(2, 2): roll_s(u[2, 0, q], c)}
                for n in range(2):
                    parts[n, 2] = roll_s(u[n, 0, q], c)
                    parts[2, n] = roll_s(u[n, 0, q], c - 4)
                for key, part in parts.items():
                    part = keep(sub == c, part)
                    key = key + (q,)
                    corner[key] = corner[key] + part if c else part
            sides[c] = rim_elements(across(u), lambda i: rim_scaled[0, i])
        for q in range(2):
            for n in range(2):
                for p in range(2):
                    corner[n, p, q] = block_recv[4 * n + 2 * p + q]
        tip = rim_elements(across(corner), lambda i: rim_scaled[1, i])
        for c in range(comps):
            add_planes(new, c, sides[c], tip)

    def absorb(step, c):
        new = step % 2
        first, last = step == 0, False
        for q in range(2):
            face = slice(8 * q, 8 * q + 8)
            line = slice(16 + q, 17 + q)
            row = slice(q, q + 1)

            def spot(ref_row, mask):
                return keep(mask, jnp.broadcast_to(ref_row, (8, half_y)))

            if not first:
                from_low = recv_r[step, c, 1, face]
                from_left = recv_x[step, c, 1, face]
                corner = spot(recv_c[step, c, 3, row], corner0)
                vec[new, c, 0, 0, q] += (
                    keep(~upper, from_low) + keep(first_x, from_left) + corner
                )
                vec[new, c, 0, 1, q] += keep(~upper, roll_s(from_low, 4))
                for ro in range(1, 4):
                    vec[new, c, ro, 0, q] += keep(first_x, roll_s(from_left, -ro))
            if not last:
                from_up = recv_r[step, c, 0, face]
                from_right = recv_x[step, c, 0, face]
                add0 = keep(upper, roll_s(from_up, 4))
                add1 = keep(upper, from_up)
                edge = keep(last_x, roll_s(from_right, 3))
                far = (
                    spot(recv_r[step, c, 0, line], corner7)
                    + spot(recv_x[step, c, 0, line], corner7)
                    + spot(recv_c[step, c, 0, row], corner7)
                )
                if not first:
                    add0 = (
                        add0
                        + spot(recv_x[step, c, 1, line], corner4)
                        + spot(recv_c[step, c, 1, row], corner4)
                    )
                    edge = (
                        edge
                        + spot(recv_r[step, c, 1, line], corner3)
                        + spot(recv_c[step, c, 2, row], corner3)
                    )
                    add0 = add0 + ghost_r[new, c, 0, q]
                    add1 = add1 + ghost_r[new, c, 1, q]
                    edge = edge + ghost_x[new, c, 0, q]
                    far = far + ghost_c[new, c, q]
                ghost_r[new, c, 0, q] = add0 * up_f
                ghost_r[new, c, 1, q] = add1 * up_f
                ghost_x[new, c, 0, q] = edge * right_f
                ghost_c[new, c, q] = far * both_f
                for ro in range(1, 4):
                    edge = keep(last_x, roll_s(from_right, 3 - ro))
                    if not first:
                        edge = edge + ghost_x[new, c, ro, q]
                    ghost_x[new, c, ro, q] = edge * right_f

    def to_native(k, c, rim=False):
        cur = k % 2
        for ro in range(4):
            for p in range(2):
                if rim and ro and p:
                    continue
                for q in range(2):
                    v = vec[cur, c, ro, p, q]
                    for h in range(2):
                        work[n_prev + k, q, native(c, ro, p, h), :] = v[4 * h : 4 * h + 4]

    def write_out(k):
        z = jnp.concatenate([work[n_prev + k, 0], work[n_prev + k, 1]], 1)
        out_ref[k - 1] = exact_dot(z, join_perm)

    lane16 = lax.broadcasted_iota(jnp.int32, (16, half_y), 1)
    row16 = lax.broadcasted_iota(jnp.int32, (16, half_y), 0)

    def gram_part(i, acc, first, count):
        def chunk(t, acc):
            at = pl.ds(pl.multiple_of(8 * t, 8), 8)
            for q in range(2):
                mine = work[i, q, at, :]
                acc = tuple(
                    acc[j] + mine * (mine if j == i else work[j, q, at, :]) for j in range(i + 1)
                )
            return acc

        return lax.fori_loop(first, first + count, chunk, acc, unroll=4)

    def gram_add(i, acc, at, mask):
        for q in range(2):
            mine = work[i, q, at, :]
            mine = mine if mask is None else keep(mask, mine)
            acc = tuple(
                acc[j] + mine * (mine if j == i else work[j, q, at, :]) for j in range(i + 1)
            )
        return acc

    def gram_zero(i):
        return (jnp.zeros((8, half_y), F32),) * (i + 1)

    def gram_close(i, acc):
        sums = [jnp.sum(a, axis=0, keepdims=True) for a in acc]
        sums.append(jnp.zeros((16 - len(sums), half_y), F32))
        total = jnp.sum(jnp.concatenate(sums, 0), axis=1, keepdims=True)
        hit = jnp.logical_or(lane16 == i * n_vec + row16, lane16 == row16 * n_vec + i)
        hit = jnp.logical_and(hit, row16 <= i)
        return jnp.sum(jnp.where(hit, jnp.broadcast_to(total, hit.shape), 0.0), 0, keepdims=True)

    def gram_row(i):
        return gram_close(i, gram_part(i, gram_zero(i), 0, rows // 8))

    res_copy.wait()
    edge_rows = []
    for c in range(comps):
        picked = [2 * x + p for p in range(2) for x in range(4)] + [8 * r for r in range(8)]
        edge_rows += [stage[n_prev, pl.ds(c * 64 + at, 1), :] for at in picked]
    edge = exact_dot(jnp.concatenate(edge_rows, 0), split_perm)
    zero_rows = jnp.zeros((2, half_y), F32)
    for c in range(comps):
        send_r[0, c, 0, 16:18] = zero_rows
        send_x[0, c, 0, 16:18] = zero_rows
        for q in range(2):
            face = slice(8 * q, 8 * q + 8)
            lanes = slice(half_y * q, half_y * (q + 1))
            send_r[0, c, 0, face] = edge[16 * c : 16 * c + 8, lanes]
            send_x[0, c, 0, face] = edge[16 * c + 8 : 16 * c + 16, lanes]
            send_c[0, c, 0, q : q + 1] = edge[16 * c : 16 * c + 1, lanes]
            along = [8 + 6, 8 + 7, 3, 7, 8 + 1, 8 + 2, 4, 1]
            for slot, row in enumerate(along):
                at = 16 * c + row
                edge_send[2 * slot + q, c : c + 1] = edge[at : at + 1, lanes]

    pl.semaphore_wait(barrier, around(1, DIRS))
    for c in range(comps):
        start_round(0, c)
    start_edges(DIRS)
    split_columns(n_prev)
    for c in range(comps):
        for ro in range(4):
            for p in range(2):
                for q in range(2):
                    vec[0, c, ro, p, q] = jnp.concatenate(
                        [work[n_prev, q, native(c, ro, p, h), :] for h in range(2)], 0
                    )
    for copy in small_copies:
        copy.wait()
    etas = []
    for e in range(2):
        ids = jnp.concatenate([ids_ref[e], ids_ref[2 + e]], 0)
        eta = jnp.zeros((8, half_y), F32)
        for layer in range(visc_ref.shape[0]):
            eta = eta + jnp.where(ids == layer, visc_ref[layer], 0.0)
        etas.append(eta)
        for key, i in kinds.items():
            scaled[e, i] = eta * weight(*key)
    eta_send[0] = etas[1]
    eta_send[1] = to_column(*etas)
    eta_send[2] = jnp.where(
        upper,
        jnp.broadcast_to(etas[1][4:5], (8, half_y)),
        jnp.broadcast_to(etas[0][3:4], (8, half_y)),
    )
    start_etas(DIRS)
    for c in range(comps):
        apply(0, c, hold=False)
        start_round(1, c)

    total = jnp.zeros((1, half_y), F32)
    prev_copy.wait()
    for i in range(n_prev):
        split_columns(i)

    for i in range(n_prev + 1):
        total = total + gram_row(i)

    for c in range(comps):
        finish_round(0, c)
        absorb(0, c)
        apply(0, c, send=False)
    settle(rim_sems.at[1], opposite(edge_sizes))
    tip_eta = jnp.broadcast_to(eta_recv[1, 0:1], (8, half_y))
    for key, i in kinds.items():
        for slot in range(4):
            rim_scaled[slot, i] = (tip_eta if slot == 1 else eta_recv[slot]) * weight(*key)
    add_first()
    for k in range(1, n_steps - 1):
        for c in range(comps):
            finish_round(k, c)
            absorb(k, c)
            apply(k, c)
            start_round(k + 1, c)
            if k == n_steps - 2:
                if c:
                    start_layers(c - 1)
                pack_rim(c)
        if k == n_steps - 2:
            start_layers(comps - 1)
            start_rim()
        if k == n_steps - 2:
            send_token(0)
        for c in range(comps):
            to_native(k, c)
        write_out(k)
        total = total + gram_row(n_prev + k)
    assert n_steps >= 3
    k = n_steps - 1
    per = rows // 8 // comps
    whole = gram_zero(n_vec - 2)
    acc = gram_zero(n_vec - 1)
    for c in range(comps):
        finish_round(k, c)
        absorb(k, c)
        apply(k, c)
        if c == 0:
            take_token(0)
            send_token(1)
        own_planes(c, k % 2)
        to_native(k, c)
        to_native(n_steps, c)
        whole = gram_part(n_vec - 2, whole, c * per, per)
        acc = lax.fori_loop(
            8 * c + 1,
            8 * c + 8,
            lambda t, acc: gram_add(
                n_vec - 1, acc, pl.ds(pl.multiple_of(8 * t, 8), 8), jnp.logical_not(corner0)
            ),
            acc,
            unroll=7,
        )
    total = total + gram_close(n_vec - 2, whole)
    settle(rim_sems.at[0], opposite(rim_sizes))
    add_rim()
    for c in range(comps):
        to_native(n_steps, c, rim=True)
    for c in range(comps):
        acc = gram_add(n_vec - 1, acc, pl.ds(c * 64, 8), None)
        acc = gram_add(n_vec - 1, acc, pl.ds(c * 64, 8, stride=8), jnp.logical_not(corner0))
    total = total + gram_close(n_vec - 1, acc)
    gram_send[...] = total

    def scatter(slot, device):
        pltpu.make_async_remote_copy(
            src_ref=gram_send,
            dst_ref=gram_recv.at[slot],
            send_sem=gram_sems.at[0],
            recv_sem=gram_sems.at[1],
            device_id=device,
            device_id_type=MESH,
        ).start()

    for j in range(1, len(reaches)):
        take_token(j)
        send_token(j + 1)
    each_other(scatter)
    write_out(n_steps - 1)
    write_out(n_steps)
    sent = [size for step in range(n_steps) for size in round_sizes(step)] * comps
    settle(send_sem.at[0], sent + rim_sizes + edge_sizes)
    for i in range(2):
        pltpu.make_async_copy(gram_recv, gram_recv, gram_sems.at[i]).wait()
    full = (total + jnp.sum(gram_recv[...], axis=0)) * (1.0 / (rows * 2 * half_y * n_dev))
    for i in range(n_vec):
        line = full if i == 0 else pltpu.roll(full, half_y - i * n_vec, 1)
        gram_ref[i : i + 1, :] = line[:, :n_vec]


def store(vec_ref, gram_ref, vec_out, gram_out, sems):
    copies = [pltpu.make_async_copy(gram_ref, gram_out, sems.at[0])]
    copies.insert(0, pltpu.make_async_copy(vec_ref, vec_out, sems.at[1]))
    for copy in copies:
        copy.start()
    for copy in copies:
        copy.wait()


def on_device(residual, prev_basis, layer_ids, viscosity, shifts):
    n_lat = lax.axis_size("lat")
    n_rad = lax.axis_size("rad")
    comps, node_r, node_x, node_y = residual.shape
    n_prev = prev_basis.shape[0]
    n_steps = shifts.shape[0]
    n_vec = n_prev + n_steps + 1
    rows = comps * node_r * node_x
    half_y = node_y // 2
    assert node_r == 8 and node_x == 8 and half_y == 128
    rounds = n_steps
    tile = (8, half_y)
    vmem = pltpu.VMEM
    hbm_spec = pl.BlockSpec(memory_space=pltpu.HBM)
    vmem_spec = pl.BlockSpec(memory_space=pltpu.VMEM)
    out, gram = pl.pallas_call(
        functools.partial(kernel, n_lat, n_rad, n_steps, n_prev, comps),
        out_shape=(
            pltpu.VMEM((n_steps, rows, node_y), F32),
            pltpu.VMEM((n_vec, n_vec), F32),
        ),
        in_specs=[hbm_spec] * 5,
        out_specs=(vmem_spec, vmem_spec),
        scratch_shapes=[
            vmem((n_prev + 1, rows, node_y), F32),
            vmem(layer_ids.shape, jnp.int32),
            pltpu.SMEM(viscosity.shape, F32),
            pltpu.SMEM(shifts.shape, F32),
            vmem((n_vec, 2, rows, half_y), F32),
            vmem((2, comps, 4, 2, 2) + tile, F32),
            vmem((2, comps, 2, 2) + tile, F32),
            vmem((2, comps, 4, 2) + tile, F32),
            vmem((2, comps, 2) + tile, F32),
            vmem((2, 9) + tile, F32),
            vmem((rounds, comps, 2, 18, half_y), F32),
            vmem((rounds, comps, 2, 18, half_y), F32),
            vmem((rounds, comps, 4, 2, half_y), F32),
            vmem((rounds, comps, 2, 18, half_y), F32),
            vmem((rounds, comps, 2, 18, half_y), F32),
            vmem((rounds, comps, 4, 2, half_y), F32),
            vmem((1, half_y), F32),
            vmem((n_lat * n_rad - 1, 1, half_y), F32),
            vmem((rounds * comps * 80 + 128 * comps, half_y), F32),
            vmem((comps, 40) + tile, F32),
            vmem((comps, 20) + tile, F32),
            vmem((8,) + tile, F32),
            vmem((8,) + tile, F32),
            vmem((16,) + tile, F32),
            vmem((20,) + tile, F32),
            vmem((3,) + tile, F32),
            vmem((4,) + tile, F32),
            vmem((4, 9) + tile, F32),
            vmem((comps, 6) + tile, F32),
            pltpu.SemaphoreType.DMA((5,)),
            pltpu.SemaphoreType.DMA((1,)),
            pltpu.SemaphoreType.DMA((3, comps)),
            pltpu.SemaphoreType.DMA((2,)),
            pltpu.SemaphoreType.DMA((2,)),
            pltpu.SemaphoreType.REGULAR((max(n_lat, n_rad).bit_length(),)),
        ],
        compiler_params=pltpu.CompilerParams(
            collective_id=0, has_side_effects=True, vmem_limit_bytes=65000000
        ),
    )(
        residual.reshape(rows, node_y),
        prev_basis.reshape(n_prev, rows, node_y),
        layer_ids,
        viscosity,
        shifts,
    )
    out, gram = pl.pallas_call(
        store,
        out_shape=(
            jax.ShapeDtypeStruct(out.shape, F32),
            jax.ShapeDtypeStruct(gram.shape, F32),
        ),
        in_specs=[vmem_spec] * 2,
        out_specs=(hbm_spec, hbm_spec),
        scratch_shapes=[pltpu.SemaphoreType.DMA((2,))],
    )(*(pltpu.with_memory_space_constraint(a, pltpu.VMEM) for a in (out, gram)))
    return out.reshape((n_steps,) + residual.shape), gram


def solution(mesh):
    placed = (
        P(None, "rad", "lat", None),
        P(None, None, "rad", "lat", None),
        P("rad", "lat", None),
        P(),
        P(),
    )
    return jax.shard_map(
        on_device,
        mesh=mesh,
        in_specs=placed,
        out_specs=(P(None, None, "rad", "lat", None), P()),
        check_vma=False,
    )
```
